32 devices in a mesh: dp: 2 (over x), seq: 4 (over z), tensor: 4 (over y, core).
Axes of the slice: x: 2, y: 2, z: 4, core: 2. Of those that a mesh axis runs over, the one named last changes fastest.
Arguments:
- tokens: bfloat16 [2, 2, 2048, 512], P(None, 'dp', 'seq'), may hold values from -6 to 6
- document_index: int32 [2, 2, 2048], P(None, 'dp', 'seq'), may hold values from 0 to 2, never falling along the last dimension, each value on 1 to 1280 neighbouring positions
- filters: bfloat16 [24, 2048], P('tensor'), may hold values from -1.1 to 1.1
- stu_gain: float32 [512], replicated, may hold values from 0.5 to 1.5
- filter_proj: bfloat16 [24, 512, 512], P('tensor'), may hold values from -0.0546875 to 0.0546875
- lag_proj: bfloat16 [3, 512, 512], P(None, 'tensor'), may hold values from -0.15625 to 0.15625
- attention_gain: float32 [512], replicated, may hold values from 0.5 to 1.5
- query_weight: bfloat16 [512, 512], P(None, 'tensor'), may hold values from -0.25 to 0.25
- key_weight: bfloat16 [512, 512], P(None, 'tensor'), may hold values from -0.25 to 0.25
- value_weight: bfloat16 [512, 512], P(None, 'tensor'), may hold values from -0.25 to 0.25
- output_weight: bfloat16 [512, 512], P('tensor'), may hold values from -3 to 3
- feed_gain: float32 [512], replicated, may hold values from 0.5 to 1.5
- gate_weight: bfloat16 [512, 2048], P(None, 'tensor'), may hold values from -0.25 to 0.25
- up_weight: bfloat16 [512, 2048], P(None, 'tensor'), may hold values from -0.25 to 0.25
- down_weight: bfloat16 [2048, 512], P('tensor'), may hold values from -0.125 to 0.125
- cotangent: bfloat16 [2, 2, 2048, 512], P(None, 'dp', 'seq'), may hold values from -6 to 6
Outputs:
- layer_output: bfloat16 [2, 2, 2048, 512], P(None, 'dp', 'seq')
- input_gradient: bfloat16 [2, 2, 2048, 512], P(None, 'dp', 'seq')
- stu_gain_grad: float32 [512], P('seq')
- filter_proj_grad: float32 [24, 512, 512], P('tensor', 'seq')
- lag_proj_grad: float32 [3, 512, 512], P(None, 'tensor', 'seq')
- attention_gain_grad: float32 [512], P('seq')
- query_grad: float32 [512, 512], P('seq', 'tensor')
- key_grad: float32 [512, 512], P('seq', 'tensor')
- value_grad: float32 [512, 512], P('seq', 'tensor')
- output_grad: float32 [512, 512], P('tensor', 'seq')
- feed_gain_grad: float32 [512], P('seq')
- gate_grad: float32 [512, 2048], P('seq', 'tensor')
- up_grad: float32 [512, 2048], P('seq', 'tensor')
- down_grad: float32 [2048, 512], P('tensor', 'seq')
The draws below stay inside these ranges and needn't reach their ends.
Inputs may be any that keep to these rules, and one draw needn't show every extreme that they name: `document_index`: along each row of 2048 tokens the ids never fall; each id marks one contiguous document.
All inputs are finite; a program needn't handle non-finite values.
Results may differ from the reference program's by a relative error of at most 0.017.
Values may be sent and summed in bfloat16 or wider, within the bound.
A program may use at most 384 MiB of HBM per device.

```python
import math
import jax
import jax.numpy as jnp
import numpy as np
from jax import lax

EMBED_WIDTH = 512
FF = 2048
H = 8
HD = 64
FILTER_COUNT = 24
ARO = 3
WINDOW = 1024
MICRO_BATCHES = 2
PACKED_ROWS = 2
PACKED_LENGTH = 2048


def draw_filters(key, part):
    filter_values = jax.random.normal(key, (FILTER_COUNT, PACKED_LENGTH), jnp.float32)
    filter_values = jnp.clip(filter_values, -4.0, 4.0)
    delayed_values = jnp.arange(PACKED_LENGTH, dtype=jnp.float32)
    decay_profile = (1.0 + delayed_values) ** (-0.35) * 0.3 ** 0.5 * float(PACKED_LENGTH) ** (-0.15)
    return (filter_values * decay_profile[None, :]).astype(jnp.bfloat16)


def spiked(entries, stream_key, source, target, blocks, factor):
    owner, partner = [(jnp.arange(entries.shape[position]) // (entries.shape[position] // blocks)).reshape([-1 if axis == position else 1 for axis in range(entries.ndim)]) for position in (source, target)]
    chosen = jax.random.permutation(stream_key, blocks)[partner]
    strong = (owner == chosen) | (owner == (partner + blocks // 2) % blocks)
    return jnp.where(strong, factor * entries, entries)


def steps_of(stream_key, shape, shards, smallest, largest):
    loudness = 1.0
    for dim, shards_of in shards:
        steps = jax.random.uniform(jax.random.fold_in(jax.random.fold_in(stream_key, 6), dim), (shards_of,), jnp.float32, smallest / len(shards), largest / len(shards))
        loudness = loudness * jnp.repeat(jnp.exp(steps), shape[dim] // shards_of).reshape((-1,) + (1,) * (len(shape) - 1 - dim))
    return loudness


def split_up(amount, total, bound, skew):
    weights = [(1 << 20) // math.isqrt(standing ** skew) + 1 for standing in range(2, amount + 1)]
    spare, given = total - bound - (amount - 1), [1] * (amount - 1)
    while spare > 0:
        free = [i for i in range(amount - 1) if given[i] < bound]
        pool, left = sum([weights[i] for i in free]), spare
        for i in free:
            extra = min(bound - given[i], max(1, left * weights[i] // pool), spare)
            given[i] = given[i] + extra
            spare = spare - extra
    return np.array([bound] + given)


def ragged(key, amount, total, limit, slope):
    if amount == 2:
        one = jax.random.randint(key, (), max(1, total - limit), min(limit, total - 1) + 1)
        return jnp.stack([one, total - one])
    sizes = jnp.asarray(split_up(amount, total, limit, slope), jnp.int32)
    twos = (amount - 1) // 2
    source_of, receiver = sizes[1:1 + 2 * twos:2], sizes[2:2 + 2 * twos:2]
    room = jnp.minimum(source_of - 1, limit - receiver)
    passed = jax.random.randint(jax.random.fold_in(key, 1), (twos,), 0, 1 << 20) % (room + 1)
    sizes = sizes.at[1:1 + 2 * twos:2].set(source_of - passed).at[2:2 + 2 * twos:2].set(receiver + passed)
    return sizes[jax.random.permutation(jax.random.fold_in(key, 2), amount)]


def noise(own_key, extent, scale, bound, split=(), kind=jnp.bfloat16):
    array = scale * jax.random.normal(own_key, extent, jnp.float32)
    if split:
        array = array * steps_of(own_key, extent, split, -0.22, 0.18)
    return jnp.clip(array, -bound, bound).astype(kind)


def heavy_noise(key, extent, spread, most, cuts, heavy, kind=jnp.bfloat16):
    result = spread * jax.random.normal(key, extent, jnp.float32)
    if cuts:
        result = result * steps_of(key, extent, cuts, -0.22, 0.18)
    return jnp.clip(spiked(result, jax.random.fold_in(key, 3), *heavy), -most, most).astype(kind)


def setup_inputs(seed: int = 0) -> dict:
    streams_of = jax.random.split(jax.random.key(seed), 17)
    tokens = heavy_noise(streams_of[0], (MICRO_BATCHES, PACKED_ROWS, PACKED_LENGTH, EMBED_WIDTH), 1.0, 6.0, ((1, 2), (2, 4)), (2, 3, 4, 2.0))
    document_index = jax.vmap(lambda own: jnp.searchsorted(jnp.cumsum(ragged(own, 3, PACKED_LENGTH, PACKED_LENGTH * 5 // 8, 0)), jnp.arange(PACKED_LENGTH), side="right"))(jax.random.split(streams_of[1], MICRO_BATCHES * PACKED_ROWS)).reshape((MICRO_BATCHES, PACKED_ROWS, PACKED_LENGTH)).astype(jnp.int32)
    filters = draw_filters(jax.random.fold_in(streams_of[16], 71), 0)
    stu_gain = jnp.clip(1.0 + 0.1 * jax.random.normal(streams_of[3], (EMBED_WIDTH,), jnp.float32), 0.5, 1.5)
    filter_proj = noise(streams_of[4], (FILTER_COUNT, EMBED_WIDTH, EMBED_WIDTH), (FILTER_COUNT * EMBED_WIDTH) ** -0.5, 0.0546875, ((0, 4),))
    lag_proj = noise(streams_of[5], (ARO, EMBED_WIDTH, EMBED_WIDTH), (ARO * EMBED_WIDTH) ** -0.5, 0.15625, ((1, 4),))
    attention_gain = jnp.clip(1.0 + 0.1 * jax.random.normal(streams_of[6], (EMBED_WIDTH,), jnp.float32), 0.5, 1.5)
    query_weight = noise(streams_of[7], (EMBED_WIDTH, H * HD), EMBED_WIDTH ** -0.5, 0.25, ((1, 4),))
    key_weight = noise(streams_of[8], (EMBED_WIDTH, H * HD), EMBED_WIDTH ** -0.5, 0.25, ((1, 4),))
    value_weight = noise(streams_of[9], (EMBED_WIDTH, H * HD), EMBED_WIDTH ** -0.5, 0.25, ((1, 4),))
    output_weight = noise(streams_of[10], (H * HD, EMBED_WIDTH), (max(H * HD // 128, 1)) ** -0.5, 3.0, ((0, 4),))
    feed_gain = jnp.clip(1.0 + 0.1 * jax.random.normal(streams_of[11], (EMBED_WIDTH,), jnp.float32), 0.5, 1.5)
    gate_weight = noise(streams_of[12], (EMBED_WIDTH, FF), EMBED_WIDTH ** -0.5, 0.25, ((1, 4),))
    up_weight = noise(streams_of[13], (EMBED_WIDTH, FF), EMBED_WIDTH ** -0.5, 0.25, ((1, 4),))
    down_weight = noise(streams_of[14], (FF, EMBED_WIDTH), FF ** -0.5, 0.125, ((0, 4),))
    cotangent = heavy_noise(streams_of[15], (MICRO_BATCHES, PACKED_ROWS, PACKED_LENGTH, EMBED_WIDTH), 1.0, 6.0, ((1, 2), (2, 4)), (2, 3, 4, 2.0))
    return dict(tokens=tokens, document_index=document_index, filters=filters, stu_gain=stu_gain, filter_proj=filter_proj, lag_proj=lag_proj, attention_gain=attention_gain, query_weight=query_weight, key_weight=key_weight, value_weight=value_weight, output_weight=output_weight, feed_gain=feed_gain, gate_weight=gate_weight, up_weight=up_weight, down_weight=down_weight, cotangent=cotangent)


EPSILON = 1e-05

@jax.custom_vjp
def low(v):
    return lax.optimization_barrier(v.astype(jnp.bfloat16)).astype(jnp.float32)

@jax.custom_vjp
def low_back(v):
    return v

def low_keep(v):
    return (low(v), None)

def low_pass(kept, grad):
    return (grad,)

def back_keep(v):
    return (v, None)

def back_low(kept, grad):
    return (low(grad),)
low.defvjp(low_keep, low_pass)
low_back.defvjp(back_keep, back_low)

def rms_scale(values, gain_vec):
    inverse = lax.rsqrt(lax.optimization_barrier(jnp.mean(values * values, axis=-1, keepdims=True)) + EPSILON)
    return values * inverse * gain_vec

def matmul(left, right_operand):
    return jnp.dot(left, right_operand, precision=lax.Precision.HIGHEST)

def layer_row(weights, row_tokens, row_ids):
    filters, stu_gain, filter_proj, lag_proj, attention_gain, query_weight, key_weight, value_weight, output_weight, feed_gain, gate_weight, up_weight, down_weight = weights
    length = row_tokens.shape[0]
    positions = jnp.arange(length, dtype=jnp.int32)
    same_doc = row_ids[:, None] == row_ids[None, :]
    offsets = positions[:, None] - positions[None, :]
    causal = same_doc & (offsets >= 0)
    lag_index = jnp.clip(offsets, 0, length - 1)
    inputs = low(rms_scale(row_tokens, stu_gain))

    def convolve(tap_row):
        toeplitz = jnp.where(causal, tap_row[lag_index], 0.0)
        return low(low_back(matmul(toeplitz, inputs)))
    conv_out = lax.map(jax.checkpoint(convolve), filters)
    mixed_sum = jnp.einsum('ktd,kde->te', conv_out, filter_proj, precision=lax.Precision.HIGHEST)
    for lag_step in range(lag_proj.shape[0]):
        back_by = lag_step + 1
        shifted = jnp.concatenate([jnp.zeros((back_by, inputs.shape[1]), inputs.dtype), inputs[:-back_by]], axis=0)
        shifted_ids = jnp.concatenate([jnp.full((back_by,), -1, jnp.int32), row_ids[:-back_by].astype(jnp.int32)])
        shifted = jnp.where((shifted_ids == row_ids)[:, None], shifted, 0.0)
        mixed_sum = mixed_sum + matmul(shifted, lag_proj[lag_step])
    hidden_one = row_tokens + low_back(mixed_sum)
    attn_in = low(rms_scale(hidden_one, attention_gain))
    head_count = query_weight.shape[1] // HD
    queries = low(low_back(matmul(attn_in, query_weight))).reshape(length, head_count, HD)
    key_rows = low(low_back(matmul(attn_in, key_weight))).reshape(length, head_count, HD)
    value_rows = low(low_back(matmul(attn_in, value_weight))).reshape(length, head_count, HD)
    allowed = same_doc & (offsets >= 0) & (offsets < WINDOW)
    block_rows = min(512, length)

    def attend(first_row):
        query_block = lax.dynamic_slice_in_dim(queries, first_row, block_rows, 0)
        mask_block = lax.dynamic_slice_in_dim(allowed, first_row, block_rows, 0)
        scores = jnp.einsum('qhd,khd->hqk', query_block, key_rows, precision=lax.Precision.HIGHEST) * HD ** (-0.5)
        scores = low_back(scores)
        scores = jnp.where(mask_block[None], scores, -1e+30)
        prob_low = low(jax.nn.softmax(scores, axis=-1))
        return jnp.einsum('hqk,khd->qhd', prob_low, value_rows, precision=lax.Precision.HIGHEST)
    starts = jnp.arange(length // block_rows, dtype=jnp.int32) * block_rows
    attended = lax.map(jax.checkpoint(attend), starts).reshape(length, head_count * HD)
    attended = low(low_back(attended))
    hidden_two = hidden_one + low_back(matmul(attended, output_weight))
    feed_in = low(rms_scale(hidden_two, feed_gain))
    gate_pre = low_back(matmul(feed_in, gate_weight))
    up_pre = low_back(matmul(feed_in, up_weight))
    inner_act = low(jax.nn.gelu(gate_pre, approximate=True) * up_pre)
    return hidden_two + low_back(matmul(inner_act, down_weight))

def reference(tokens, document_index, filters, stu_gain, filter_proj, lag_proj, attention_gain, query_weight, key_weight, value_weight, output_weight, feed_gain, gate_weight, up_weight, down_weight, cotangent):
    weights = tuple((argument.astype(jnp.float32) for argument in (filters, stu_gain, filter_proj, lag_proj, attention_gain, query_weight, key_weight, value_weight, output_weight, feed_gain, gate_weight, up_weight, down_weight)))
    flattened_tokens = tokens.astype(jnp.float32).reshape(MICRO_BATCHES * PACKED_ROWS, PACKED_LENGTH, EMBED_WIDTH)
    flattened_segments = document_index.reshape(MICRO_BATCHES * PACKED_ROWS, PACKED_LENGTH).astype(jnp.int32)

    def forward(token_rows, params):

        def one_row(item_pair):
            return jax.checkpoint(layer_row)(params, item_pair[0], item_pair[1])
        return lax.map(one_row, (token_rows, flattened_segments))
    final_output, backward_function = jax.vjp(forward, flattened_tokens, weights)
    input_gradient, weight_gradients = backward_function(cotangent.astype(jnp.float32).reshape(MICRO_BATCHES * PACKED_ROWS, PACKED_LENGTH, EMBED_WIDTH))
    layer_output = final_output.reshape(MICRO_BATCHES, PACKED_ROWS, PACKED_LENGTH, EMBED_WIDTH).astype(jnp.bfloat16)
    input_gradient = input_gradient.reshape(MICRO_BATCHES, PACKED_ROWS, PACKED_LENGTH, EMBED_WIDTH).astype(jnp.bfloat16)
    return (layer_output, input_gradient, weight_gradients[1], weight_gradients[2], weight_gradients[3], weight_gradients[4], weight_gradients[5], weight_gradients[6], weight_gradients[7], weight_gradients[8], weight_gradients[9], weight_gradients[10], weight_gradients[11], weight_gradients[12])
```

```python
import functools

import jax
import jax.numpy as jnp
from jax import lax
from jax.experimental import pallas as pl
from jax.experimental.pallas import tpu as pltpu
from jax.sharding import PartitionSpec as P

HD = 64
WINDOW = 1024
EPSILON = 1e-05
LANES = 128
NEGATIVE = -1e30
MESH = pl.DeviceIdType.MESH
BF = jnp.bfloat16
F32 = jnp.float32
VMEM_LIMIT = 60 * 1024 * 1024


def place():
    s = lax.axis_index("seq")
    t = lax.axis_index("tensor")
    y = t // 2
    c = t - 2 * y
    return s, t, y, c, t + 1 - 2 * c, t + 2 - 4 * y


def when(condition, action):
    if condition is True:
        action()
    else:
        pl.when(condition)(action)


def remote(src, dst, send_sem, recv_sem, device):
    return pltpu.make_async_remote_copy(
        src_ref=src, dst_ref=dst, send_sem=send_sem, recv_sem=recv_sem, device_id=device, device_id_type=MESH
    )


def greet(seq_count, hops):
    s, t, y, c, core, far = place()
    barrier = pltpu.get_barrier_semaphore()
    for peer in (core, far):
        pl.semaphore_signal(barrier, inc=1, device_id={"tensor": peer}, device_id_type=MESH)
    for h in range(1, hops + 1):
        for there, peer in ((s - h >= 0, s - h), (s + h < seq_count, s + h)):

            @pl.when(there)
            def _():
                pl.semaphore_signal(barrier, inc=1, device_id={"seq": peer}, device_id_type=MESH)

    peers = 2 + jnp.minimum(s, hops) + jnp.minimum(seq_count - 1 - s, hops)
    pl.semaphore_wait(barrier, peers)


class ReduceScatter:
    def __init__(self, seq_count, hops, streams, part, scratch):
        self.seq_count, self.hops, self.streams, self.part = seq_count, hops, streams, part
        self.near, self.half, self.over, self.hop_out, self.hop_in, self.sem = scratch

    @staticmethod
    def scratch(hops, streams, rows, width):
        quarter = (hops + 1, streams, rows, width)
        return [
            pltpu.VMEM((hops + 1, streams, 2, rows, width), BF),
            pltpu.VMEM(quarter, BF),
            pltpu.VMEM(quarter, BF),
            pltpu.VMEM(quarter, BF),
            pltpu.VMEM(quarter, BF),
            pltpu.SemaphoreType.DMA((6, hops + 1, streams)),
        ]

    def to_core(self, h, m):
        s, t, y, c, core, far = place()
        return remote(
            self.part(h, m).at[:, 1 - c], self.near.at[h, m], self.sem.at[0, h, m], self.sem.at[1, h, m], {"tensor": core}
        )

    def to_far(self, h, m):
        s, t, y, c, core, far = place()
        return remote(self.half.at[h, m], self.over.at[h, m], self.sem.at[2, h, m], self.sem.at[3, h, m], {"tensor": far})

    def to_hop(self, h, m, peer):
        return remote(
            self.hop_out.at[h, m], self.hop_in.at[h, m], self.sem.at[4, h, m], self.sem.at[5, h, m], {"seq": peer}
        )

    def there(self, h):
        return True if h == 0 else lax.axis_index("seq") - h >= 0

    def order(self):
        return [(h, m) for h in range(self.hops, -1, -1) for m in range(self.streams)]

    def start(self, h, m):
        when(self.there(h), lambda: self.to_core(h, m).start())

    def middle(self, h, m):
        s, t, y, c, core, far = place()

        def act():
            self.to_core(h, m).wait_recv()
            mine = self.part(h, m)[1 - y, c].astype(F32) + self.near[h, m, 1 - y].astype(F32)
            self.half[h, m] = mine.astype(BF)
            self.to_far(h, m).start()

        when(self.there(h), act)

    def own(self, h, m):
        s, t, y, c, core, far = place()
        self.to_far(h, m).wait_recv()
        return (
            self.part(h, m)[y, c].astype(F32) + self.near[h, m, y].astype(F32) + self.over[h, m].astype(F32)
        )

    def hop(self, h, m):
        def act():
            self.hop_out[h, m] = self.own(h, m).astype(BF)
            self.to_hop(h, m, lax.axis_index("seq") - h).start()

        when(self.there(h), act)

    def total(self, m, acc):
        acc[...] = self.own(0, m)
        for h in range(1, self.hops + 1):
            s = lax.axis_index("seq")

            @pl.when(s + h < self.seq_count)
            def _():
                self.to_hop(h, m, s + h).wait_recv()
                acc[...] += self.hop_in[h, m].astype(F32)

    def drain(self):
        for h, m in self.order():

            def act():
                self.to_core(h, m).wait_send()
                self.to_far(h, m).wait_send()
                if h:
                    self.to_hop(h, m, lax.axis_index("seq") - h).wait_send()

            when(self.there(h), act)


class AllGather:
    def __init__(self, seq_count, hops, streams, out, sem, first=0):
        self.seq_count, self.hops, self.streams, self.out, self.sem, self.first = seq_count, hops, streams, out, sem, first

    @staticmethod
    def scratch(hops, streams):
        return [pltpu.SemaphoreType.DMA((8, hops + 1, streams))]

    def there(self, h):
        return True if h == 0 else lax.axis_index("seq") - h >= 0

    def copy(self, kind, h, m, quarter, device, to=None):
        source = self.out.at[0 if kind == 0 else h, m, quarter]
        return remote(source, self.out.at[h, m, quarter], self.sem.at[2 * kind, h, m], self.sem.at[2 * kind + 1, h, m], device)

    def to_hop(self, h, m, peer):
        return self.copy(0, h, m, place()[1], {"seq": peer})

    def spread(self, h, m):
        s, t, y, c, core, far = place()
        self.copy(1, h, m, t, {"tensor": far}).start()
        self.copy(2, h, m, t, {"tensor": core}).start()

    def start(self, m):
        s, t, y, c, core, far = place()
        for h in range(1, self.hops + 1):

            @pl.when(s + h < self.seq_count)
            def _():
                self.to_hop(h, m, s + h).start()

        if self.first == 0:
            self.spread(0, m)

    def arrive(self, h, m):
        @pl.when(self.there(h))
        def _():
            self.to_hop(h, m, lax.axis_index("seq") - h).wait_recv()
            self.spread(h, m)

    def pass_on(self, h, m):
        s, t, y, c, core, far = place()

        def act():
            self.copy(1, h, m, far, {"tensor": far}).wait_recv()
            self.copy(3, h, m, far, {"tensor": core}).start()

        when(self.there(h), act)

    def finish(self, h, m):
        s, t, y, c, core, far = place()

        def act():
            self.copy(2, h, m, core, {"tensor": core}).wait_recv()
            self.copy(3, h, m, 3 - t, {"tensor": core}).wait_recv()

        when(self.there(h), act)

    def clear(self, h, m):
        @pl.when(lax.axis_index("seq") - h < 0)
        def _():
            self.out[h, m] = jnp.zeros(self.out.shape[2:], self.out.dtype)

    def drain(self):
        s, t, y, c, core, far = place()
        for m in range(self.streams):
            for h in range(1, self.hops + 1):

                @pl.when(s + h < self.seq_count)
                def _():
                    self.to_hop(h, m, s + h).wait_send()

            for h in range(self.first, self.hops + 1):

                def act():
                    self.copy(1, h, m, t, {"tensor": far}).wait_send()
                    self.copy(2, h, m, t, {"tensor": core}).wait_send()
                    self.copy(3, h, m, far, {"tensor": core}).wait_send()

                when(self.there(h), act)


def params(cid=None):
    if cid is None:
        return pltpu.CompilerParams(vmem_limit_bytes=VMEM_LIMIT)
    return pltpu.CompilerParams(vmem_limit_bytes=VMEM_LIMIT, collective_id=cid, has_side_effects=True)


def in_vmem(count):
    return [pl.BlockSpec(memory_space=pltpu.VMEM)] * count


def gather_rows(inputs, ids, seq_count):
    streams, quarters, rows, width = inputs.shape
    hops = seq_count - 1

    def kernel(x_ref, id_ref, out, out_ids, sem, id_sem):
        s, t, y, c, core, far = place()
        greet(seq_count, hops)
        out[0] = x_ref[...]
        out_ids[0] = id_ref[...]
        ag = AllGather(seq_count, hops, streams, out, sem, first=1)

        def id_copy(h, peer):
            return remote(id_ref, out_ids.at[h], id_sem.at[0, h], id_sem.at[1, h], {"seq": peer})

        for h in range(1, hops + 1):

            @pl.when(s + h < seq_count)
            def _():
                id_copy(h, s + h).start()

        ag.to_hop = lambda h, m, peer: remote(
            x_ref.at[m, t], out.at[h, m, t], sem.at[0, h, m], sem.at[1, h, m], {"seq": peer}
        )
        for m in range(streams):
            ag.start(m)
        for h in range(1, hops + 1):
            for m in range(streams):
                ag.clear(h, m)

            @pl.when(s - h < 0)
            def _():
                out_ids[h] = jnp.full(out_ids.shape[1:], -1, jnp.int32)

        for h in range(1, hops + 1):
            for m in range(streams):
                ag.arrive(h, m)
        for h in range(1, hops + 1):
            for m in range(streams):
                ag.pass_on(h, m)
        for h in range(1, hops + 1):
            for m in range(streams):
                ag.finish(h, m)

            @pl.when(s - h >= 0)
            def _():
                id_copy(h, s - h).wait_recv()

            @pl.when(s + h < seq_count)
            def _():
                id_copy(h, s + h).wait_send()

        ag.drain()

    return pl.pallas_call(
        kernel,
        name="gather_rows",
        out_shape=(
            jax.ShapeDtypeStruct((seq_count,) + inputs.shape, inputs.dtype),
            jax.ShapeDtypeStruct((seq_count,) + ids.shape, jnp.int32),
        ),
        in_specs=in_vmem(2),
        out_specs=tuple(in_vmem(2)),
        scratch_shapes=AllGather.scratch(hops, streams) + [pltpu.SemaphoreType.DMA((2, seq_count))],
        compiler_params=params(1),
    )(inputs, ids)


def exchange(name, cid, seq_count, parts, others, reduce_hops, gather_hops, finish, extra):
    per_part = parts[0].shape[1]
    rows, width = parts[0].shape[4:]
    streams = per_part * len(parts)
    hops = max(reduce_hops, gather_hops)

    def kernel(*refs):
        refs = list(refs)
        part_refs = [refs.pop(0) for _ in parts]
        other_refs = [refs.pop(0) for _ in others]
        out = refs.pop(0)
        extra_refs = [refs.pop(0) for _ in extra]
        acc = refs.pop(0)
        gather_sem = refs.pop(0)
        s, t, y, c, core, far = place()
        greet(seq_count, hops)
        rs = ReduceScatter(
            seq_count, reduce_hops, streams, lambda h, m: part_refs[m // per_part].at[h, m % per_part], refs
        )
        ag = AllGather(seq_count, gather_hops, streams, out, gather_sem)
        for h, m in rs.order():
            rs.start(h, m)
        for h in range(1, gather_hops + 1):
            for m in range(streams):
                ag.clear(h, m)
        for h, m in rs.order():
            rs.middle(h, m)
        for h, m in rs.order():
            if h:
                rs.hop(h, m)
        for m in range(streams):
            rs.total(m, acc)
            out[0, m, t] = finish(m, acc[...], other_refs, extra_refs)
            ag.start(m)
        for h in range(gather_hops + 1):
            for m in range(streams):
                if h:
                    ag.arrive(h, m)
            for m in range(streams):
                ag.pass_on(h, m)
        for h in range(gather_hops + 1):
            for m in range(streams):
                ag.finish(h, m)
        rs.drain()
        ag.drain()

    return pl.pallas_call(
        kernel,
        name=name,
        out_shape=(jax.ShapeDtypeStruct((gather_hops + 1, streams, 4, rows, width), BF),) + tuple(extra),
        in_specs=in_vmem(len(parts) + len(others)),
        out_specs=tuple(in_vmem(1 + len(extra))),
        scratch_shapes=[pltpu.VMEM((rows, width), F32)]
        + AllGather.scratch(gather_hops, streams)
        + ReduceScatter.scratch(reduce_hops, streams, rows, width),
        compiler_params=params(cid),
    )(*parts, *others)


def norm_of(values, gain_row):
    inverse = lax.rsqrt(jnp.mean(values * values, axis=-1, keepdims=True) + EPSILON)
    return values * inverse * gain_row


def norm_back(values, gain_row, grad_out):
    inverse = lax.rsqrt(jnp.mean(values * values, axis=-1, keepdims=True) + EPSILON)
    scaled = grad_out * gain_row
    dot = jnp.mean(scaled * values, axis=-1, keepdims=True)
    grad_in = inverse * scaled - values * (inverse * inverse * inverse) * dot
    return grad_in, jnp.sum(grad_out * values * inverse, axis=0, keepdims=True)


def strips(base_ref, strip):
    @pl.loop(0, base_ref.shape[0])
    def _(k):
        row = jnp.broadcast_to(base_ref[k], strip.shape[1:])
        strip[k] = pltpu.roll(row, 0, 1, stride=1, stride_axis=0).astype(BF)


def convolve(rows, row_ids, col_ids, base, seq_count):
    _, streams, length, width = rows.shape
    count, _, wide = base.shape
    blocks = length // LANES

    def kernel(x_ref, row_ref, col_ref, base_ref, out_ref, strip, mask, acc):
        strips(base_ref, strip)
        s = lax.axis_index("seq")

        @pl.loop(0, streams)
        def _(m):
            acc[...] = jnp.zeros_like(acc)

            @pl.loop(0, s + 1)
            def _(h):
                mask[...] = jnp.where(col_ref[m] == row_ref[h, m], 1.0, 0.0).astype(BF)

                @pl.loop(0, count)
                def _(k):
                    pieces = []
                    for a in range(blocks):
                        start = pl.multiple_of(LANES * (blocks * (seq_count - h) - 1 - a), LANES)
                        pieces.append(strip[k, :, pl.ds(start, length)] * mask[a * LANES : (a + 1) * LANES])
                    acc[k] += jnp.dot(jnp.concatenate(pieces, axis=0), x_ref[h, m], preferred_element_type=F32)

            @pl.loop(0, count)
            def _(k):
                out_ref[k, m] = acc[k].astype(BF)

    return pl.pallas_call(
        kernel,
        name="convolve",
        out_shape=jax.ShapeDtypeStruct((count, streams, length, width), BF),
        in_specs=in_vmem(4),
        out_specs=in_vmem(1)[0],
        scratch_shapes=[
            pltpu.VMEM((count, LANES, wide), BF),
            pltpu.VMEM((length, length), BF),
            pltpu.VMEM((count, length, width), F32),
        ],
        compiler_params=params(),
    )(rows, row_ids, col_ids, base)


def convolve_back(grads, row_ids, col_ids, base, own_lag, tail_lag, seq_count):
    count, streams, length, width = grads.shape
    wide = base.shape[2]
    blocks = length // LANES
    channels = own_lag.shape[2]
    tail_rows = tail_lag.shape[1]

    def kernel(g_ref, row_ref, col_ref, base_ref, own_ref, tail_ref, out_ref, strip, mask, acc):
        strips(base_ref, strip)
        s = lax.axis_index("seq")
        mine = pl.ds(pl.multiple_of(lax.axis_index("tensor") * channels, LANES), channels)

        @pl.loop(0, s + 1)
        def _(h):
            @pl.loop(0, streams)
            def _(m):
                mask[...] = jnp.where(col_ref[h, m] == row_ref[m], 1.0, 0.0).astype(BF)
                acc[...] = jnp.zeros_like(acc)

                @pl.when(h == 0)
                def _():
                    acc[:, mine] = own_ref[m]

                @pl.when(h == 1)
                def _():
                    acc[length - tail_rows :, mine] = tail_ref[m]

                @pl.loop(0, count)
                def _(k):
                    pieces = []
                    for a in range(blocks):
                        start = pl.multiple_of(LANES * (blocks * h + blocks - 1 - a), LANES)
                        pieces.append(strip[k, :, pl.ds(start, length)] * mask[a * LANES : (a + 1) * LANES])
                    acc[...] += jnp.dot(jnp.concatenate(pieces, axis=0), g_ref[k, m], preferred_element_type=F32)

                out_ref[h, m] = acc[...].astype(BF)

    return pl.pallas_call(
        kernel,
        name="convolve_back",
        out_shape=jax.ShapeDtypeStruct((seq_count, streams, length, width), BF),
        in_specs=in_vmem(6),
        out_specs=in_vmem(1)[0],
        scratch_shapes=[
            pltpu.VMEM((count, LANES, wide), BF),
            pltpu.VMEM((length, length), BF),
            pltpu.VMEM((length, width), F32),
        ],
        compiler_params=params(),
    )(grads, row_ids, col_ids, base, own_lag, tail_lag)


def dot_nn(a, b):
    return jnp.dot(a, b, preferred_element_type=F32)


def dot_nt(a, b):
    return lax.dot_general(a, b, (((1,), (1,)), ((), ())), preferred_element_type=F32)


def dot_tn(a, b):
    return lax.dot_general(a, b, (((0,), (0,)), ((), ())), preferred_element_type=F32)


def allowed_keys(query_ids, key_ids, first_row, distance):
    shape = (query_ids.shape[0], key_ids.shape[1])
    offset = lax.broadcasted_iota(jnp.int32, shape, 0) - lax.broadcasted_iota(jnp.int32, shape, 1) + (first_row + distance)
    return (query_ids == key_ids) & (offset >= 0) & (offset < WINDOW)


def one_head(block, head):
    lane = lax.broadcasted_iota(jnp.int32, block.shape, 1)
    return jnp.where((lane >= head * HD) & (lane < (head + 1) * HD), block, jnp.zeros_like(block))


def attend(rows, row_ids, col_ids, wq, wk, wv, wo):
    spans, streams, length, width = rows.shape
    cols = wq.shape[1]
    heads = cols // HD
    tile = min(256, length)
    scale = HD ** (-0.5)

    def kernel(x_ref, row_ref, col_ref, wq_ref, wk_ref, wv_ref, wo_ref, q_ref, k_ref, v_ref, a_ref, lse_ref, p_ref):
        @pl.loop(0, streams)
        def _(m):
            q_ref[m] = dot_nn(x_ref[0, m], wq_ref[...]).astype(BF)
            for h in range(spans):
                k_ref[h, m] = dot_nn(x_ref[h, m], wk_ref[...]).astype(BF)
                v_ref[h, m] = dot_nn(x_ref[h, m], wv_ref[...]).astype(BF)

            @pl.loop(0, length // tile)
            def _(i):
                first = pl.multiple_of(i * tile, tile)
                here = pl.ds(first, tile)
                masks = [allowed_keys(col_ref[m, here], row_ref[h, m], first, h * length) for h in range(spans)]
                block = q_ref[m, here]
                result = jnp.zeros((tile, cols), F32)
                for head in range(heads):
                    query = one_head(block, head)
                    scores = [
                        jnp.where(masks[h], dot_nt(query, k_ref[h, m]) * scale, NEGATIVE) for h in range(spans)
                    ]
                    peak = functools.reduce(jnp.maximum, [jnp.max(v, axis=-1, keepdims=True) for v in scores])
                    raised = [jnp.exp(v - peak) for v in scores]
                    total = sum([jnp.sum(v, axis=-1, keepdims=True) for v in raised])
                    inverse = 1.0 / total
                    mixed = sum([dot_nn((raised[h] * inverse).astype(BF), v_ref[h, m]) for h in range(spans)])
                    result = result + one_head(mixed, head)
                    lse_ref[m, head, here] = jnp.broadcast_to(peak + jnp.log(total), (tile, LANES))
                a_ref[m, here] = result.astype(BF)

            p_ref[m] = dot_nn(a_ref[m], wo_ref[...]).astype(BF)

    part = jax.ShapeDtypeStruct((streams, length, cols), BF)
    span = jax.ShapeDtypeStruct((spans, streams, length, cols), BF)
    return pl.pallas_call(
        kernel,
        name="attend",
        out_shape=(
            part,
            span,
            span,
            part,
            jax.ShapeDtypeStruct((streams, heads, length, LANES), F32),
            jax.ShapeDtypeStruct((streams, length, width), BF),
        ),
        in_specs=in_vmem(7),
        out_specs=tuple(in_vmem(6)),
        compiler_params=params(),
    )(rows, row_ids, col_ids, wq, wk, wv, wo)


def attend_back(q, k, v, lse, grad_out, row_ids, col_ids, wq, wk, wv, wo):
    spans, streams, length, cols = k.shape
    width = grad_out.shape[2]
    heads = cols // HD
    tile = min(256, length)
    scale = HD ** (-0.5)

    def kernel(
        q_ref, k_ref, v_ref, lse_ref, go_ref, row_ref, col_ref, wq_ref, wk_ref, wv_ref, wo_ref,
        dq_ref, dk_ref, dv_ref, p_ref, ga_ref, dk_acc, dv_acc,
    ):
        @pl.loop(0, streams)
        def _(m):
            ga_ref[...] = dot_nt(go_ref[m], wo_ref[...]).astype(BF)
            dk_acc[...] = jnp.zeros_like(dk_acc)
            dv_acc[...] = jnp.zeros_like(dv_acc)

            @pl.loop(0, length // tile)
            def _(i):
                first = pl.multiple_of(i * tile, tile)
                here = pl.ds(first, tile)
                masks = [allowed_keys(col_ref[m, here], row_ref[h, m], first, h * length) for h in range(spans)]
                block = q_ref[m, here]
                grad_block = ga_ref[here]
                result = jnp.zeros((tile, cols), F32)
                for head in range(heads):
                    query = one_head(block, head)
                    grad = one_head(grad_block, head)
                    level = lse_ref[m, head, here][:, :1]
                    prob = [
                        jnp.where(masks[h], jnp.exp(dot_nt(query, k_ref[h, m]) * scale - level), 0.0)
                        for h in range(spans)
                    ]
                    grad_prob = [dot_nt(grad, v_ref[h, m]) for h in range(spans)]
                    mean = sum([jnp.sum(p * g, axis=-1, keepdims=True) for p, g in zip(prob, grad_prob)])
                    grad_scores = [(p * (g - mean)).astype(BF) for p, g in zip(prob, grad_prob)]
                    for h in range(spans):
                        dv_acc[h] += dot_tn(prob[h].astype(BF), grad)
                        dk_acc[h] += dot_tn(grad_scores[h], query)
                    mixed = sum([dot_nn(grad_scores[h], k_ref[h, m]) for h in range(spans)])
                    result = result + one_head(mixed, head)
                dq_ref[m, here] = (result * scale).astype(BF)

            for h in range(spans):
                dk_ref[h, m] = (dk_acc[h] * scale).astype(BF)
                dv_ref[h, m] = dv_acc[h].astype(BF)
                back = dot_nt(dk_ref[h, m], wk_ref[...]) + dot_nt(dv_ref[h, m], wv_ref[...])
                if h == 0:
                    back = back + dot_nt(dq_ref[m], wq_ref[...])
                p_ref[h, m] = back.astype(BF)

    span = jax.ShapeDtypeStruct((spans, streams, length, cols), BF)
    return pl.pallas_call(
        kernel,
        name="attend_back",
        out_shape=(
            jax.ShapeDtypeStruct((streams, length, cols), BF),
            span,
            span,
            jax.ShapeDtypeStruct((spans, streams, length, width), BF),
        ),
        in_specs=in_vmem(11),
        out_specs=tuple(in_vmem(4)),
        scratch_shapes=[
            pltpu.VMEM((length, cols), BF),
            pltpu.VMEM((spans, length, cols), F32),
            pltpu.VMEM((spans, length, cols), F32),
        ],
        compiler_params=params(),
    )(q, k, v, lse, grad_out, row_ids, col_ids, wq, wk, wv, wo)


def gated_unit(gate_pre, up_pre):
    return jax.nn.gelu(gate_pre, approximate=True) * up_pre


def local(
    seq_count,
    tokens,
    document_index,
    filters,
    stu_gain,
    filter_proj,
    lag_proj,
    attention_gain,
    query_weight,
    key_weight,
    value_weight,
    output_weight,
    feed_gain,
    gate_weight,
    up_weight,
    down_weight,
    cotangent,
):
    streams, _, length, width = tokens.shape
    row_len = length * seq_count
    quarter = length // 4
    lag_order, channels = lag_proj.shape[:2]
    count = filters.shape[0]
    hops = WINDOW // length
    tensor_place = lax.axis_index("tensor")
    chan_start = tensor_place * channels

    def split(a):
        return a.reshape(a.shape[:-2] + (2, 2, quarter, width))

    def quarters(a):
        return a.reshape(a.shape[:-2] + (4, quarter, width))

    def whole(a):
        return a.reshape(a.shape[:-3] + (length, width))

    def row(gain):
        return gain.reshape(1, width)

    x = tokens[:, 0]
    grad_three = cotangent[:, 0]
    ids = document_index[:, 0]
    inputs = norm_of(x.astype(F32), stu_gain).astype(BF)
    id_tile = ids.reshape(streams * length // LANES, LANES)
    rows_ext, id_ext = gather_rows(quarters(inputs), id_tile, seq_count)
    rows_ext = whole(rows_ext)
    id_ext = id_ext.reshape(seq_count, streams, length)
    id_rows = id_ext[:, :, None, :]
    id_cols = id_ext[:, :, :, None]

    pad = jnp.zeros((count, 4 * LANES), filters.dtype)
    ahead = row_len - LANES
    base = jnp.concatenate(
        [
            jnp.flip(filters[:, : ahead + 1], axis=1),
            pad[:, : 4 * LANES],
            jnp.flip(filters[:, ahead + 1 :], axis=1),
        ],
        axis=1,
    ).astype(F32)[:, None]
    base_back = jnp.concatenate(
        [pad[:, : length - LANES], filters, pad[:, :LANES]], axis=1
    ).astype(F32)[:, None]
    conv = convolve(rows_ext, id_rows, id_cols[0], base, seq_count)

    chan_rows = lax.dynamic_slice_in_dim(rows_ext[:2], chan_start, channels, 3)
    joined = jnp.concatenate([chan_rows[1][:, length - lag_order :], chan_rows[0]], axis=1)
    joined_ids = jnp.concatenate([id_ext[1][:, length - lag_order :], ids], axis=1)
    masks = []
    lagged = []
    for step in range(1, lag_order + 1):
        low = lag_order - step
        masks.append((joined_ids[:, low : low + length] == ids)[:, :, None])
        lagged.append(jnp.where(masks[-1], joined[:, low : low + length], jnp.zeros((), BF)))
    lag_stack = jnp.stack(lagged)

    mixed = jnp.einsum("kmtd,kde->mte", conv, filter_proj, preferred_element_type=F32)
    mixed = mixed + jnp.einsum("imtc,ice->mte", lag_stack, lag_proj, preferred_element_type=F32)

    state = jax.ShapeDtypeStruct((streams, quarter, width), F32)
    gain_state = jax.ShapeDtypeStruct((1, width), F32)

    def finish_one(m, total, others, extra):
        x_ref, gain_ref = others
        hidden = x_ref[m, place()[1]].astype(F32) + total
        extra[0][m] = hidden
        return norm_of(hidden, gain_ref[...]).astype(BF)

    attn_ext, hidden_one = exchange(
        "exchange_one", 2, seq_count, [split(mixed.astype(BF))[None]], [quarters(x), row(attention_gain)], 0, hops,
        finish_one, [state],
    )
    attn_ext = whole(attn_ext)

    q, k, v, attended, lse, out_part = attend(
        attn_ext, id_rows[: hops + 1], id_cols[0], query_weight, key_weight, value_weight, output_weight
    )

    def finish_two(m, total, others, extra):
        hidden_ref, gain_ref = others
        hidden = hidden_ref[m] + total
        extra[0][m] = hidden
        return norm_of(hidden, gain_ref[...]).astype(BF)

    feed_in, hidden_two = exchange(
        "exchange_two", 3, seq_count, [split(out_part)[None]], [hidden_one, row(feed_gain)], 0, 0, finish_two, [state]
    )
    feed_in = whole(feed_in)[0].reshape(streams * length, width)
    flat_three = grad_three.reshape(streams * length, width)

    gate_pre = dot_nn(feed_in, gate_weight)
    up_pre = dot_nn(feed_in, up_weight)
    grad_inner = dot_nt(flat_three, down_weight)
    unit, pull = jax.vjp(gated_unit, gate_pre, up_pre)
    inner = unit.astype(BF)
    grad_gate, grad_up = pull(grad_inner)
    grad_gate = grad_gate.astype(BF)
    grad_up = grad_up.astype(BF)
    layer_part = dot_nn(inner, down_weight).astype(BF)
    feed_part = (dot_nt(grad_gate, gate_weight) + dot_nt(grad_up, up_weight)).astype(BF)

    def finish_three(m, total, others, extra):
        hidden_ref, gain_ref, cot_ref = others
        if m >= streams:
            return (hidden_ref[m - streams] + total).astype(BF)
        grad_in, gain_grad = norm_back(hidden_ref[m], gain_ref[...], total)
        grad_two = cot_ref[m, place()[1]].astype(F32) + grad_in
        extra[0][m] = grad_two
        extra[1][...] = gain_grad if m == 0 else extra[1][...] + gain_grad
        return grad_two.astype(BF)

    shape = (1, streams, length, width)
    both, grad_two, feed_gain_grad = exchange(
        "exchange_three", 4, seq_count, [split(feed_part.reshape(shape)), split(layer_part.reshape(shape))],
        [hidden_two, row(feed_gain), quarters(grad_three)], 0, 0, finish_three, [state, gain_state],
    )
    both = whole(both)[0]
    grad_att_out = both[:streams]
    layer_output = both[streams:]

    dq, dk, dv, attn_part = attend_back(
        q, k, v, lse, grad_att_out, id_rows[: hops + 1], id_cols[0], query_weight, key_weight, value_weight, output_weight
    )

    def finish_four(m, total, others, extra):
        hidden_ref, gain_ref, grad_ref = others
        grad_in, gain_grad = norm_back(hidden_ref[m], gain_ref[...], total)
        grad_one = grad_ref[m] + grad_in
        extra[0][m] = grad_one
        extra[1][...] = gain_grad if m == 0 else extra[1][...] + gain_grad
        return grad_one.astype(BF)

    grad_stu, grad_one, attn_gain_grad = exchange(
        "exchange_four", 5, seq_count, [split(attn_part)], [hidden_one, row(attention_gain), grad_two], hops, 0,
        finish_four, [state, gain_state],
    )
    grad_stu = whole(grad_stu)[0]

    grad_conv = jnp.einsum("mte,kde->kmtd", grad_stu, filter_proj, preferred_element_type=F32).astype(BF)
    grad_lagged = jnp.einsum("mte,ice->imtc", grad_stu, lag_proj, preferred_element_type=F32)
    ext_grad = jnp.zeros((streams, 8 + length, channels), F32)
    for step in range(1, lag_order + 1):
        term = jnp.where(masks[step - 1], grad_lagged[step - 1], 0.0)
        ext_grad = ext_grad + jnp.pad(term, ((0, 0), (8 - step, step), (0, 0)))
    terms = convolve_back(
        grad_conv, id_rows[0], id_cols, base_back, ext_grad[:, 8:], ext_grad[:, :8], seq_count
    )

    def finish_five(m, total, others, extra):
        x_ref, gain_ref, grad_ref = others
        grad_in, gain_grad = norm_back(x_ref[m, place()[1]].astype(F32), gain_ref[...], total)
        extra[0][...] = gain_grad if m == 0 else extra[0][...] + gain_grad
        return (grad_ref[m] + grad_in).astype(BF)

    input_gradient, stu_gain_grad = exchange(
        "exchange_five", 6, seq_count, [split(terms)], [quarters(x), row(stu_gain), grad_one], seq_count - 1, 0,
        finish_five, [gain_state],
    )
    input_gradient = whole(input_gradient)[0]

    tokens_flat = streams * length
    go = grad_att_out.reshape(tokens_flat, width)
    first = jnp.concatenate(
        [
            dot_tn(feed_in, grad_gate).astype(BF),
            dot_tn(feed_in, grad_up).astype(BF),
            dot_tn(flat_three, inner).astype(BF),
            dot_tn(attn_ext[0].reshape(tokens_flat, width), dq.reshape(tokens_flat, -1)).astype(BF),
            dot_tn(attn_ext.reshape(-1, width), dk.reshape(-1, dk.shape[-1])).astype(BF),
            dot_tn(attn_ext.reshape(-1, width), dv.reshape(-1, dv.shape[-1])).astype(BF),
            dot_tn(go, attended.reshape(tokens_flat, -1)).astype(BF),
        ],
        axis=1,
    )
    stu = grad_stu.reshape(tokens_flat, width)
    second = jnp.concatenate(
        [
            jnp.einsum("kmtd,mte->kde", conv, grad_stu, preferred_element_type=F32).astype(BF),
            jnp.concatenate(
                [dot_tn(stu, lag_stack[i].reshape(tokens_flat, channels)).astype(BF) for i in range(lag_order)]
                + [jnp.zeros((width, width - lag_order * channels), BF)],
                axis=1,
            )[None],
        ],
        axis=0,
    )
    first = lax.psum(lax.psum_scatter(first, "seq", scatter_dimension=0, tiled=True), "dp").astype(F32)
    second = lax.psum(lax.psum_scatter(second, "seq", scatter_dimension=1, tiled=True), "dp").astype(F32)
    gains = jnp.concatenate([stu_gain_grad, attn_gain_grad, feed_gain_grad], axis=0)
    gains = lax.psum(gains, ("dp", "seq", "tensor"))
    gain_width = width // seq_count
    gains = lax.dynamic_slice_in_dim(gains, lax.axis_index("seq") * gain_width, gain_width, 1)

    hidden_units = gate_weight.shape[1]
    cols = query_weight.shape[1]
    cuts = [hidden_units, 2 * hidden_units, 3 * hidden_units]
    cuts += [cuts[-1] + cols, cuts[-1] + 2 * cols, cuts[-1] + 3 * cols]
    gate_grad, up_grad, down_grad, query_grad, key_grad, value_grad, output_grad = jnp.split(first, cuts, axis=1)
    lag_grad = second[count][:, : lag_order * channels].T.reshape(lag_order, channels, -1)
    return (
        layer_output[:, None],
        input_gradient[:, None],
        gains[0],
        second[:count],
        lag_grad,
        gains[1],
        query_grad,
        key_grad,
        value_grad,
        output_grad.T,
        gains[2],
        gate_grad,
        up_grad,
        down_grad.T,
    )


def solution(mesh):
    return jax.shard_map(
        functools.partial(local, mesh.shape["seq"]),
        mesh=mesh,
        in_specs=(
            P(None, "dp", "seq", None),
            P(None, "dp", "seq"),
            P("tensor", None),
            P(),
            P("tensor", None, None),
            P(None, "tensor", None),
            P(),
            P(None, "tensor"),
            P(None, "tensor"),
            P(None, "tensor"),
            P("tensor", None),
            P(),
            P(None, "tensor"),
            P(None, "tensor"),
            P("tensor", None),
            P(None, "dp", "seq", None),
        ),
        out_specs=(
            P(None, "dp", "seq", None),
            P(None, "dp", "seq", None),
            P("seq"),
            P("tensor", "seq", None),
            P(None, "tensor", "seq"),
            P("seq"),
            P("seq", "tensor"),
            P("seq", "tensor"),
            P("seq", "tensor"),
            P("tensor", "seq"),
            P("seq"),
            P("seq", "tensor"),
            P("seq", "tensor"),
            P("tensor", "seq"),
        ),
        check_vma=False,
    )
```

```python
import functools

import jax
import jax.numpy as jnp
from jax import lax
from jax.experimental import pallas as pl
from jax.experimental.pallas import tpu as pltpu
from jax.sharding import PartitionSpec as P

HD = 64
WINDOW = 1024
EPSILON = 1e-05
LANES = 128
NEGATIVE = -1e30
MESH = pl.DeviceIdType.MESH
BF = jnp.bfloat16
F32 = jnp.float32
VMEM_LIMIT = 60 * 1024 * 1024


def place():
    s = lax.axis_index("seq")
    t = lax.axis_index("tensor")
    y = t // 2
    c = t - 2 * y
    return s, t, y, c, t + 1 - 2 * c, t + 2 - 4 * y


def when(condition, action):
    if condition is True:
        action()
    else:
        pl.when(condition)(action)


def remote(src, dst, send_sem, recv_sem, device):
    return pltpu.make_async_remote_copy(
        src_ref=src, dst_ref=dst, send_sem=send_sem, recv_sem=recv_sem, device_id=device, device_id_type=MESH
    )


def greet(seq_count, hops, wide=False, gains=False):
    s, t, y, c, core, far = place()
    barrier = pltpu.get_barrier_semaphore()

    def signal(device):
        pl.semaphore_signal(barrier, inc=1, device_id=device, device_id_type=MESH)

    signal({"tensor": core})
    signal({"tensor": far})
    if gains:
        signal({"tensor": 3 - t})
    if wide:
        p = lax.axis_index("dp")
        signal({"dp": 1 - p})
        for j in range(seq_count):

            @pl.when(s != j)
            def _():
                signal({"seq": j})
                if gains:
                    signal({"dp": 1 - p, "seq": j})

        peers = 2 + gains + 1 + (seq_count - 1) * (1 + gains)
    else:
        for h in range(1, hops + 1):
            for there, peer in ((s - h >= 0, s - h), (s + h < seq_count, s + h)):

                @pl.when(there)
                def _():
                    signal({"seq": peer})

        peers = 2 + jnp.minimum(s, hops) + jnp.minimum(seq_count - 1 - s, hops)
    pl.semaphore_wait(barrier, peers)


class ReduceScatter:
    def __init__(self, seq_count, hops, streams, part, scratch):
        self.seq_count, self.hops, self.streams, self.part = seq_count, hops, streams, part
        self.near, self.half, self.over, self.hop_out, self.hop_in, self.sem = scratch

    @staticmethod
    def scratch(hops, streams, rows, width):
        quarter = (hops + 1, streams, rows, width)
        return [
            pltpu.VMEM((hops + 1, streams, 2, rows, width), BF),
            pltpu.VMEM(quarter, BF),
            pltpu.VMEM(quarter, BF),
            pltpu.VMEM(quarter, BF),
            pltpu.VMEM(quarter, BF),
            pltpu.SemaphoreType.DMA((6, hops + 1, streams)),
        ]

    def to_core(self, h, m):
        s, t, y, c, core, far = place()
        return remote(
            self.part(h, m).at[:, 1 - c], self.near.at[h, m], self.sem.at[0, h, m], self.sem.at[1, h, m], {"tensor": core}
        )

    def to_far(self, h, m):
        s, t, y, c, core, far = place()
        return remote(self.half.at[h, m], self.over.at[h, m], self.sem.at[2, h, m], self.sem.at[3, h, m], {"tensor": far})

    def to_hop(self, h, m, peer):
        return remote(
            self.hop_out.at[h, m], self.hop_in.at[h, m], self.sem.at[4, h, m], self.sem.at[5, h, m], {"seq": peer}
        )

    def there(self, h):
        return True if isinstance(h, int) and h == 0 else lax.axis_index("seq") - h >= 0

    def order(self):
        return [(h, m) for h in range(self.hops, -1, -1) for m in range(self.streams)]

    def start(self, h, m):
        when(self.there(h), lambda: self.to_core(h, m).start())

    def middle(self, h, m):
        s, t, y, c, core, far = place()

        def act():
            self.to_core(h, m).wait_recv()
            mine = self.part(h, m)[1 - y, c].astype(F32) + self.near[h, m, 1 - y].astype(F32)
            self.half[h, m] = mine.astype(BF)
            self.to_far(h, m).start()

        when(self.there(h), act)

    def own(self, h, m):
        s, t, y, c, core, far = place()
        self.to_far(h, m).wait_recv()
        return (
            self.part(h, m)[y, c].astype(F32) + self.near[h, m, y].astype(F32) + self.over[h, m].astype(F32)
        )

    def hop(self, h, m):
        def act():
            self.hop_out[h, m] = self.own(h, m).astype(BF)
            self.to_hop(h, m, lax.axis_index("seq") - h).start()

        when(self.there(h), act)

    def total(self, m, acc):
        acc[...] = self.own(0, m)
        for h in range(1, self.hops + 1):
            s = lax.axis_index("seq")

            @pl.when(s + h < self.seq_count)
            def _():
                self.to_hop(h, m, s + h).wait_recv()
                acc[...] += self.hop_in[h, m].astype(F32)

    def drain(self):
        for h, m in self.order():

            def act():
                self.to_core(h, m).wait_send()
                self.to_far(h, m).wait_send()
                if h:
                    self.to_hop(h, m, lax.axis_index("seq") - h).wait_send()

            when(self.there(h), act)


class AllGather:
    def __init__(self, seq_count, hops, streams, out, sem, first=0):
        self.seq_count, self.hops, self.streams, self.out, self.sem, self.first = seq_count, hops, streams, out, sem, first

    @staticmethod
    def scratch(hops, streams):
        return [pltpu.SemaphoreType.DMA((8, hops + 1, streams))]

    def there(self, h):
        return True if h == 0 else lax.axis_index("seq") - h >= 0

    def copy(self, kind, h, m, quarter, device, to=None):
        source = self.out.at[0 if kind == 0 else h, m, quarter]
        return remote(source, self.out.at[h, m, quarter], self.sem.at[2 * kind, h, m], self.sem.at[2 * kind + 1, h, m], device)

    def to_hop(self, h, m, peer):
        return self.copy(0, h, m, place()[1], {"seq": peer})

    def spread(self, h, m):
        s, t, y, c, core, far = place()
        self.copy(1, h, m, t, {"tensor": far}).start()
        self.copy(2, h, m, t, {"tensor": core}).start()

    def start(self, m):
        s, t, y, c, core, far = place()
        for h in range(1, self.hops + 1):

            @pl.when(s + h < self.seq_count)
            def _():
                self.to_hop(h, m, s + h).start()

        if self.first == 0:
            self.spread(0, m)

    def arrive(self, h, m):
        @pl.when(self.there(h))
        def _():
            self.to_hop(h, m, lax.axis_index("seq") - h).wait_recv()
            self.spread(h, m)

    def pass_on(self, h, m):
        s, t, y, c, core, far = place()

        def act():
            self.copy(1, h, m, far, {"tensor": far}).wait_recv()
            self.copy(3, h, m, far, {"tensor": core}).start()

        when(self.there(h), act)

    def finish(self, h, m):
        s, t, y, c, core, far = place()

        def act():
            self.copy(2, h, m, core, {"tensor": core}).wait_recv()
            self.copy(3, h, m, 3 - t, {"tensor": core}).wait_recv()

        when(self.there(h), act)

    def clear(self, h, m):
        @pl.when(lax.axis_index("seq") - h < 0)
        def _():
            self.out[h, m] = jnp.zeros(self.out.shape[2:], self.out.dtype)

    def drain(self):
        s, t, y, c, core, far = place()
        for m in range(self.streams):
            for h in range(1, self.hops + 1):

                @pl.when(s + h < self.seq_count)
                def _():
                    self.to_hop(h, m, s + h).wait_send()

            for h in range(self.first, self.hops + 1):

                def act():
                    self.copy(1, h, m, t, {"tensor": far}).wait_send()
                    self.copy(2, h, m, t, {"tensor": core}).wait_send()
                    self.copy(3, h, m, far, {"tensor": core}).wait_send()

                when(self.there(h), act)


class GradReduce:
    def __init__(self, seq_count, source, result, scratch):
        self.seq_count, self.source, self.result = seq_count, source, result
        self.x_in, self.z_out, self.z_in, self.back_out, self.back_in, self.x_sem, self.z_sem, self.back_sem = scratch
        self.half = self.x_in.shape[2]
        self.rows = self.back_out.shape[1]

    @staticmethod
    def scratch(seq_count, chunks, depth, width):
        rows, half = depth // seq_count, width // 2
        return [
            pltpu.VMEM((chunks, depth, half), BF),
            pltpu.VMEM((chunks, depth, half), BF),
            pltpu.VMEM((chunks, seq_count, rows, half), BF),
            pltpu.VMEM((chunks, rows, half), BF),
            pltpu.VMEM((chunks, rows, half), BF),
            pltpu.SemaphoreType.DMA((2, chunks)),
            pltpu.SemaphoreType.DMA((2, chunks, seq_count)),
            pltpu.SemaphoreType.DMA((2, chunks)),
        ]

    def columns(self, p):
        return pl.ds(pl.multiple_of(p * self.half, LANES), self.half)

    def block(self, j):
        return pl.ds(pl.multiple_of(j * self.rows, 16), self.rows)

    def over(self, c):
        p = lax.axis_index("dp")
        return remote(
            self.source(c).at[:, self.columns(1 - p)], self.x_in.at[c], self.x_sem.at[0, c], self.x_sem.at[1, c], {"dp": 1 - p}
        )

    def row_copy(self, c, j, slot):
        return remote(
            self.z_out.at[c, self.block(j)], self.z_in.at[c, slot], self.z_sem.at[0, c, j], self.z_sem.at[1, c, slot], {"seq": j}
        )

    def back(self, c):
        p = lax.axis_index("dp")
        return remote(
            self.back_out.at[c], self.back_in.at[c], self.back_sem.at[0, c], self.back_sem.at[1, c], {"dp": 1 - p}
        )

    def others(self, action):
        for j in range(self.seq_count):
            pl.when(lax.axis_index("seq") != j)(functools.partial(action, j))

    def start(self, c):
        self.over(c).start()

    def spread(self, c):
        s, p = lax.axis_index("seq"), lax.axis_index("dp")
        self.over(c).wait_recv()
        mine = self.source(c)[:, self.columns(p)].astype(F32) + self.x_in[c].astype(F32)
        self.z_out[c] = mine.astype(BF)
        self.others(lambda j: self.row_copy(c, j, s).start())

    def collect(self, c, acc):
        s, p = lax.axis_index("seq"), lax.axis_index("dp")
        here = self.block(s)
        acc[...] = self.source(c)[here, self.columns(p)].astype(F32) + self.x_in[c, here].astype(F32)

        def add(j):
            self.row_copy(c, j, j).wait_recv()
            acc[...] += self.z_in[c, j].astype(F32)

        self.others(add)
        self.back_out[c] = acc[...].astype(BF)
        self.back(c).start()

    def finish(self, c):
        p = lax.axis_index("dp")
        self.back(c).wait_recv()
        self.result(c)[:, self.columns(p)] = self.back_out[c].astype(F32)
        self.result(c)[:, self.columns(1 - p)] = self.back_in[c].astype(F32)

    def drain(self, c):
        self.over(c).wait_send()
        self.others(lambda j: self.row_copy(c, j, lax.axis_index("seq")).wait_send())
        self.back(c).wait_send()


def params(cid=None):
    if cid is None:
        return pltpu.CompilerParams(vmem_limit_bytes=VMEM_LIMIT)
    return pltpu.CompilerParams(vmem_limit_bytes=VMEM_LIMIT, collective_id=cid, has_side_effects=True)


def in_vmem(count):
    return [pl.BlockSpec(memory_space=pltpu.VMEM)] * count


def gather_rows(inputs, ids, seq_count):
    streams, quarters, rows, width = inputs.shape
    hops = seq_count - 1

    def kernel(x_ref, id_ref, out, out_ids, sem, id_sem):
        s, t, y, c, core, far = place()
        greet(seq_count, hops)
        out[0] = x_ref[...]
        out_ids[0] = id_ref[...]
        ag = AllGather(seq_count, hops, streams, out, sem, first=1)

        def id_copy(h, peer):
            return remote(id_ref, out_ids.at[h], id_sem.at[0, h], id_sem.at[1, h], {"seq": peer})

        for h in range(1, hops + 1):

            @pl.when(s + h < seq_count)
            def _():
                id_copy(h, s + h).start()

        ag.to_hop = lambda h, m, peer: remote(
            x_ref.at[m, t], out.at[h, m, t], sem.at[0, h, m], sem.at[1, h, m], {"seq": peer}
        )
        for m in range(streams):
            ag.start(m)
        for h in range(1, hops + 1):
            for m in range(streams):
                ag.clear(h, m)

            @pl.when(s - h < 0)
            def _():
                out_ids[h] = jnp.full(out_ids.shape[1:], -1, jnp.int32)

        for h in range(1, hops + 1):
            for m in range(streams):
                ag.arrive(h, m)
        for h in range(1, hops + 1):
            for m in range(streams):
                ag.pass_on(h, m)
        for h in range(1, hops + 1):
            for m in range(streams):
                ag.finish(h, m)

            @pl.when(s - h >= 0)
            def _():
                id_copy(h, s - h).wait_recv()

            @pl.when(s + h < seq_count)
            def _():
                id_copy(h, s + h).wait_send()

        ag.drain()

    return pl.pallas_call(
        kernel,
        name="gather_rows",
        out_shape=(
            jax.ShapeDtypeStruct((seq_count,) + inputs.shape, inputs.dtype),
            jax.ShapeDtypeStruct((seq_count,) + ids.shape, jnp.int32),
        ),
        in_specs=in_vmem(2),
        out_specs=tuple(in_vmem(2)),
        scratch_shapes=AllGather.scratch(hops, streams) + [pltpu.SemaphoreType.DMA((2, seq_count))],
        compiler_params=params(1),
    )(inputs, ids)


def exchange(name, cid, seq_count, parts, others, reduce_hops, gather_hops, finish, extra, grads=None):
    per_part = parts[0].shape[1]
    rows, width = parts[0].shape[4:]
    streams = per_part * len(parts)
    hops = max(reduce_hops, gather_hops)
    given = [] if grads is None else [grads]
    chunks = 0 if grads is None else grads.shape[0]
    sums, tools = [], []
    if chunks:
        depth, wide = grads.shape[1:]
        sums = [jax.ShapeDtypeStruct((chunks, depth // seq_count, wide), F32)]
        tools = [pltpu.VMEM((depth // seq_count, wide // 2), F32)] + GradReduce.scratch(seq_count, chunks, depth, wide)

    def kernel(*refs):
        refs = list(refs)
        part_refs = [refs.pop(0) for _ in parts]
        other_refs = [refs.pop(0) for _ in others]
        grad_ref = refs.pop(0) if chunks else None
        out = refs.pop(0)
        extra_refs = [refs.pop(0) for _ in extra]
        sum_ref = refs.pop(0) if chunks else None
        grad_tools = [refs.pop(0) for _ in tools]
        acc = refs.pop(0)
        gather_sem = refs.pop(0)
        s, t, y, c, core, far = place()
        greet(seq_count, hops, wide=bool(chunks))
        if chunks:
            grad_acc = grad_tools.pop(0)
            gr = GradReduce(seq_count, lambda c: grad_ref.at[c], lambda c: sum_ref.at[c], grad_tools)
        rs = ReduceScatter(
            seq_count, reduce_hops, streams, lambda h, m: part_refs[m // per_part].at[h, m % per_part], refs
        )
        ag = AllGather(seq_count, gather_hops, streams, out, gather_sem)
        for h, m in rs.order():
            rs.start(h, m)
        for k in range(chunks):
            gr.start(k)
        for h in range(1, gather_hops + 1):
            for m in range(streams):
                ag.clear(h, m)
        for h, m in rs.order():
            rs.middle(h, m)
        for h, m in rs.order():
            if h:
                rs.hop(h, m)
        for k in range(chunks):
            gr.spread(k)
        for m in range(streams):
            rs.total(m, acc)
            out[0, m, t] = finish(m, acc[...], other_refs, extra_refs)
            ag.start(m)
        for k in range(chunks):
            gr.collect(k, grad_acc)
        for h in range(gather_hops + 1):
            for m in range(streams):
                if h:
                    ag.arrive(h, m)
            for m in range(streams):
                ag.pass_on(h, m)
        for h in range(gather_hops + 1):
            for m in range(streams):
                ag.finish(h, m)
        for k in range(chunks):
            gr.finish(k)
            gr.drain(k)
        rs.drain()
        ag.drain()

    return pl.pallas_call(
        kernel,
        name=name,
        out_shape=(jax.ShapeDtypeStruct((gather_hops + 1, streams, 4, rows, width), BF),) + tuple(extra) + tuple(sums),
        in_specs=in_vmem(len(parts) + len(others) + len(given)),
        out_specs=tuple(in_vmem(1 + len(extra) + len(sums))),
        scratch_shapes=tools
        + [pltpu.VMEM((rows, width), F32)]
        + AllGather.scratch(gather_hops, streams)
        + ReduceScatter.scratch(reduce_hops, streams, rows, width),
        compiler_params=params(cid),
    )(*parts, *others, *given)


def norm_of(values, gain_row):
    inverse = lax.rsqrt(jnp.mean(values * values, axis=-1, keepdims=True) + EPSILON)
    return values * inverse * gain_row


def norm_back(values, gain_row, grad_out):
    inverse = lax.rsqrt(jnp.mean(values * values, axis=-1, keepdims=True) + EPSILON)
    scaled = grad_out * gain_row
    dot = jnp.mean(scaled * values, axis=-1, keepdims=True)
    grad_in = inverse * scaled - values * (inverse * inverse * inverse) * dot
    return grad_in, jnp.sum(grad_out * values * inverse, axis=0, keepdims=True)


def strips(base_ref, strip):
    @pl.loop(0, base_ref.shape[0])
    def _(k):
        row = jnp.broadcast_to(base_ref[k], strip.shape[1:])
        strip[k] = pltpu.roll(row, 0, 1, stride=1, stride_axis=0).astype(BF)


def convolve(rows, row_ids, col_ids, base, seq_count):
    _, streams, length, width = rows.shape
    count, _, wide = base.shape
    blocks = length // LANES

    def kernel(x_ref, row_ref, col_ref, base_ref, out_ref, strip, mask, acc):
        strips(base_ref, strip)
        s = lax.axis_index("seq")

        @pl.loop(0, streams)
        def _(m):
            acc[...] = jnp.zeros_like(acc)

            @pl.loop(0, s + 1)
            def _(h):
                mask[...] = jnp.where(col_ref[m] == row_ref[h, m], 1.0, 0.0).astype(BF)

                @pl.loop(0, count)
                def _(k):
                    pieces = []
                    for a in range(blocks):
                        start = pl.multiple_of(LANES * (blocks * (seq_count - h) - 1 - a), LANES)
                        pieces.append(strip[k, :, pl.ds(start, length)] * mask[a * LANES : (a + 1) * LANES])
                    acc[k] += jnp.dot(jnp.concatenate(pieces, axis=0), x_ref[h, m], preferred_element_type=F32)

            @pl.loop(0, count)
            def _(k):
                out_ref[k, m] = acc[k].astype(BF)

    return pl.pallas_call(
        kernel,
        name="convolve",
        out_shape=jax.ShapeDtypeStruct((count, streams, length, width), BF),
        in_specs=in_vmem(4),
        out_specs=in_vmem(1)[0],
        scratch_shapes=[
            pltpu.VMEM((count, LANES, wide), BF),
            pltpu.VMEM((length, length), BF),
            pltpu.VMEM((count, length, width), F32),
        ],
        compiler_params=params(),
    )(rows, row_ids, col_ids, base)


def convolve_back(grads, row_ids, col_ids, base, own_lag, tail_lag, seq_count):
    count, streams, length, width = grads.shape
    wide = base.shape[2]
    blocks = length // LANES
    channels = own_lag.shape[2]
    tail_rows = tail_lag.shape[1]

    def kernel(g_ref, row_ref, col_ref, base_ref, own_ref, tail_ref, out_ref, strip, mask, acc):
        strips(base_ref, strip)
        s = lax.axis_index("seq")
        mine = pl.ds(pl.multiple_of(lax.axis_index("tensor") * channels, LANES), channels)

        @pl.loop(0, s + 1)
        def _(h):
            @pl.loop(0, streams)
            def _(m):
                mask[...] = jnp.where(col_ref[h, m] == row_ref[m], 1.0, 0.0).astype(BF)
                acc[...] = jnp.zeros_like(acc)

                @pl.when(h == 0)
                def _():
                    acc[:, mine] = own_ref[m]

                @pl.when(h == 1)
                def _():
                    acc[length - tail_rows :, mine] = tail_ref[m]

                @pl.loop(0, count)
                def _(k):
                    pieces = []
                    for a in range(blocks):
                        start = pl.multiple_of(LANES * (blocks * h + blocks - 1 - a), LANES)
                        pieces.append(strip[k, :, pl.ds(start, length)] * mask[a * LANES : (a + 1) * LANES])
                    acc[...] += jnp.dot(jnp.concatenate(pieces, axis=0), g_ref[k, m], preferred_element_type=F32)

                out_ref[h, m] = acc[...].astype(BF)

    return pl.pallas_call(
        kernel,
        name="convolve_back",
        out_shape=jax.ShapeDtypeStruct((seq_count, streams, length, width), BF),
        in_specs=in_vmem(6),
        out_specs=in_vmem(1)[0],
        scratch_shapes=[
            pltpu.VMEM((count, LANES, wide), BF),
            pltpu.VMEM((length, length), BF),
            pltpu.VMEM((length, width), F32),
        ],
        compiler_params=params(),
    )(grads, row_ids, col_ids, base, own_lag, tail_lag)


def dot_nn(a, b):
    return jnp.dot(a, b, preferred_element_type=F32)


def dot_nt(a, b):
    return lax.dot_general(a, b, (((1,), (1,)), ((), ())), preferred_element_type=F32)


def dot_tn(a, b):
    return lax.dot_general(a, b, (((0,), (0,)), ((), ())), preferred_element_type=F32)


def allowed_keys(query_ids, key_ids, first_row, distance):
    shape = (query_ids.shape[0], key_ids.shape[1])
    offset = lax.broadcasted_iota(jnp.int32, shape, 0) - lax.broadcasted_iota(jnp.int32, shape, 1) + (first_row + distance)
    return (query_ids == key_ids) & (offset >= 0) & (offset < WINDOW)


def one_head(block, head):
    lane = lax.broadcasted_iota(jnp.int32, block.shape, 1)
    return jnp.where((lane >= head * HD) & (lane < (head + 1) * HD), block, jnp.zeros_like(block))


def attend(rows, row_ids, col_ids, wq, wk, wv, wo):
    spans, streams, length, width = rows.shape
    cols = wq.shape[1]
    heads = cols // HD
    tile = min(256, length)
    scale = HD ** (-0.5)

    def kernel(x_ref, row_ref, col_ref, wq_ref, wk_ref, wv_ref, wo_ref, q_ref, k_ref, v_ref, a_ref, lse_ref, p_ref):
        @pl.loop(0, streams)
        def _(m):
            q_ref[m] = dot_nn(x_ref[0, m], wq_ref[...]).astype(BF)
            for h in range(spans):
                k_ref[h, m] = dot_nn(x_ref[h, m], wk_ref[...]).astype(BF)
                v_ref[h, m] = dot_nn(x_ref[h, m], wv_ref[...]).astype(BF)

            @pl.loop(0, length // tile)
            def _(i):
                first = pl.multiple_of(i * tile, tile)
                here = pl.ds(first, tile)
                masks = [allowed_keys(col_ref[m, here], row_ref[h, m], first, h * length) for h in range(spans)]
                block = q_ref[m, here]
                result = jnp.zeros((tile, cols), F32)
                for head in range(heads):
                    query = one_head(block, head)
                    scores = [
                        jnp.where(masks[h], dot_nt(query, k_ref[h, m]) * scale, NEGATIVE) for h in range(spans)
                    ]
                    peak = functools.reduce(jnp.maximum, [jnp.max(v, axis=-1, keepdims=True) for v in scores])
                    raised = [jnp.exp(v - peak) for v in scores]
                    total = sum([jnp.sum(v, axis=-1, keepdims=True) for v in raised])
                    inverse = 1.0 / total
                    mixed = sum([dot_nn((raised[h] * inverse).astype(BF), v_ref[h, m]) for h in range(spans)])
                    result = result + one_head(mixed, head)
                    lse_ref[m, head, here] = jnp.broadcast_to(peak + jnp.log(total), (tile, LANES))
                a_ref[m, here] = result.astype(BF)

            p_ref[m] = dot_nn(a_ref[m], wo_ref[...]).astype(BF)

    part = jax.ShapeDtypeStruct((streams, length, cols), BF)
    span = jax.ShapeDtypeStruct((spans, streams, length, cols), BF)
    return pl.pallas_call(
        kernel,
        name="attend",
        out_shape=(
            part,
            span,
            span,
            part,
            jax.ShapeDtypeStruct((streams, heads, length, LANES), F32),
            jax.ShapeDtypeStruct((streams, length, width), BF),
        ),
        in_specs=in_vmem(7),
        out_specs=tuple(in_vmem(6)),
        compiler_params=params(),
    )(rows, row_ids, col_ids, wq, wk, wv, wo)


def attend_back(q, k, v, lse, grad_out, row_ids, col_ids, wq, wk, wv, wo):
    spans, streams, length, cols = k.shape
    width = grad_out.shape[2]
    heads = cols // HD
    tile = min(256, length)
    scale = HD ** (-0.5)

    def kernel(
        q_ref, k_ref, v_ref, lse_ref, go_ref, row_ref, col_ref, wq_ref, wk_ref, wv_ref, wo_ref,
        dq_ref, dk_ref, dv_ref, p_ref, ga_ref, dk_acc, dv_acc,
    ):
        @pl.loop(0, streams)
        def _(m):
            ga_ref[...] = dot_nt(go_ref[m], wo_ref[...]).astype(BF)
            dk_acc[...] = jnp.zeros_like(dk_acc)
            dv_acc[...] = jnp.zeros_like(dv_acc)

            @pl.loop(0, length // tile)
            def _(i):
                first = pl.multiple_of(i * tile, tile)
                here = pl.ds(first, tile)
                masks = [allowed_keys(col_ref[m, here], row_ref[h, m], first, h * length) for h in range(spans)]
                block = q_ref[m, here]
                grad_block = ga_ref[here]
                result = jnp.zeros((tile, cols), F32)
                for head in range(heads):
                    query = one_head(block, head)
                    grad = one_head(grad_block, head)
                    level = lse_ref[m, head, here][:, :1]
                    prob = [
                        jnp.where(masks[h], jnp.exp(dot_nt(query, k_ref[h, m]) * scale - level), 0.0)
                        for h in range(spans)
                    ]
                    grad_prob = [dot_nt(grad, v_ref[h, m]) for h in range(spans)]
                    mean = sum([jnp.sum(p * g, axis=-1, keepdims=True) for p, g in zip(prob, grad_prob)])
                    grad_scores = [(p * (g - mean)).astype(BF) for p, g in zip(prob, grad_prob)]
                    for h in range(spans):
                        dv_acc[h] += dot_tn(prob[h].astype(BF), grad)
                        dk_acc[h] += dot_tn(grad_scores[h], query)
                    mixed = sum([dot_nn(grad_scores[h], k_ref[h, m]) for h in range(spans)])
                    result = result + one_head(mixed, head)
                dq_ref[m, here] = (result * scale).astype(BF)

            for h in range(spans):
                dk_ref[h, m] = (dk_acc[h] * scale).astype(BF)
                dv_ref[h, m] = dv_acc[h].astype(BF)
                back = dot_nt(dk_ref[h, m], wk_ref[...]) + dot_nt(dv_ref[h, m], wv_ref[...])
                if h == 0:
                    back = back + dot_nt(dq_ref[m], wq_ref[...])
                p_ref[h, m] = back.astype(BF)

    span = jax.ShapeDtypeStruct((spans, streams, length, cols), BF)
    return pl.pallas_call(
        kernel,
        name="attend_back",
        out_shape=(
            jax.ShapeDtypeStruct((streams, length, cols), BF),
            span,
            span,
            jax.ShapeDtypeStruct((spans, streams, length, width), BF),
        ),
        in_specs=in_vmem(11),
        out_specs=tuple(in_vmem(4)),
        scratch_shapes=[
            pltpu.VMEM((length, cols), BF),
            pltpu.VMEM((spans, length, cols), F32),
            pltpu.VMEM((spans, length, cols), F32),
        ],
        compiler_params=params(),
    )(q, k, v, lse, grad_out, row_ids, col_ids, wq, wk, wv, wo)


def tail(
    grad_stu, filter_proj, lag_proj, conv, lag_stack, lag_masks, row_ids, col_ids, base, x, gain, grad_one, gains, seq_count
):
    count, length_all, width = conv.shape
    streams, _, quarter, _ = x.shape
    length = length_all // streams
    lag_order, channels = lag_proj.shape[:2]
    wide = base.shape[2]
    blocks = length // LANES
    hops = seq_count - 1
    chunks = count + 1
    steps = seq_count * streams
    rows = width // seq_count
    gain_rows = 8

    def kernel(
        gs_ref, fp_ref, lp_ref, conv_ref, lag_ref, mask_ref, row_ref, col_ref, base_ref, x_ref, gain_ref, one_ref, gains_ref,
        out, filter_out, lag_out, gain_out,
        strip, mask, acc, terms, grad_conv, grads, lag_ext, total, grad_acc, gather_sem,
        gain_own, gain_near, gain_sum, gain_far, near_sem, far_sem, *scratch,
    ):
        s, t, y, c, core, far = place()
        p = lax.axis_index("dp")
        rs_scratch, gr_scratch = scratch[:6], scratch[6:]
        greet(seq_count, hops, wide=True, gains=True)

        def source(k):
            return grads.at[k]

        def result(k):
            return filter_out.at[k] if k < count else lag_out

        gr = GradReduce(seq_count, source, result, gr_scratch)
        rs = ReduceScatter(seq_count, hops, streams, lambda h, m: terms.at[h, m], rs_scratch)
        ag = AllGather(seq_count, 0, streams, out, gather_sem)

        @pl.loop(0, count)
        def _(k):
            grads[k] = dot_tn(conv_ref[k], gs_ref[...]).astype(BF)
            gr.start(k)
            grad_conv[k] = dot_nt(gs_ref[...], fp_ref[k]).astype(BF)

        grads[count] = jnp.zeros_like(grads.at[count])
        for i in range(lag_order):
            grads[count, :, i * channels : (i + 1) * channels] = dot_tn(gs_ref[...], lag_ref[i]).astype(BF)
        gr.start(count)
        for m in range(streams):
            lag_ext[m] = jnp.zeros_like(lag_ext.at[m])
            for i in range(lag_order):
                term = dot_nt(gs_ref[m * length : (m + 1) * length], lp_ref[i]) * mask_ref[i, m]
                lag_ext[m, 7 - i : 7 - i + length] += term
        strips(base_ref, strip)
        mine = pl.ds(pl.multiple_of(t * channels, LANES), channels)

        def step_of(i):
            return seq_count - 1 - i // streams, i - i // streams * streams

        @pl.loop(0, steps)
        def _(i):
            h, m = step_of(i)

            @pl.when(h <= s)
            def _():
                mask[...] = jnp.where(col_ref[h, m] == row_ref[m], 1.0, 0.0).astype(BF)
                acc[...] = jnp.zeros_like(acc)

                @pl.when(h == 0)
                def _():
                    acc[:, mine] = lag_ext[m, 8:]

                @pl.when(h == 1)
                def _():
                    acc[length - 8 :, mine] = lag_ext[m, :8]

                @pl.loop(0, count)
                def _(k):
                    pieces = []
                    for a in range(blocks):
                        start = pl.multiple_of(LANES * (blocks * h + blocks - 1 - a), LANES)
                        pieces.append(strip[k, :, pl.ds(start, length)] * mask[a * LANES : (a + 1) * LANES])
                    block = grad_conv[k, pl.ds(pl.multiple_of(m * length, LANES), length)]
                    acc[...] += jnp.dot(jnp.concatenate(pieces, axis=0), block, preferred_element_type=F32)

                for quarter_y in range(2):
                    for quarter_c in range(2):
                        first = (2 * quarter_y + quarter_c) * quarter
                        terms[h, m, quarter_y, quarter_c] = acc[first : first + quarter].astype(BF)
                rs.start(h, m)

            @pl.when(i >= 1)
            def _():
                rs.middle(*step_of(i - 1))

            @pl.when((i >= 2) & (i < steps - streams + 2))
            def _():
                rs.hop(*step_of(i - 2))

            @pl.when(i < chunks)
            def _():
                gr.spread(i)

            @pl.when((i >= 3) & (i < chunks + 3))
            def _():
                gr.collect(i - 3, grad_acc)

        rs.middle(0, streams - 1)
        for k in range(steps, chunks):
            gr.spread(k)
        gain_own[...] = jnp.zeros_like(gain_own)
        for m in range(streams):
            rs.total(m, total)
            grad_in, gain_grad = norm_back(x_ref[m, t].astype(F32), gain_ref[...], total[...])
            out[0, m, t] = (one_ref[m] + grad_in).astype(BF)
            ag.start(m)
            gain_own[0:1] += gain_grad
        gain_own[1:3] = gains_ref[...]
        gain_near[t] = gain_own[...]

        def near_copy(j, slot):
            return remote(gain_own, gain_near.at[slot], near_sem.at[0, j], near_sem.at[1, slot], {"tensor": j})

        for j in range(4):
            pl.when(t != j)(lambda: near_copy(j, t).start())
        for k in range(max(steps - 3, 0), chunks):
            gr.collect(k, grad_acc)
        for m in range(streams):
            ag.pass_on(0, m)
        for j in range(4):
            pl.when(t != j)(lambda: near_copy(j, j).wait_recv())
        gain_sum[...] = gain_near[0] + gain_near[1] + gain_near[2] + gain_near[3]
        me = p * seq_count + s

        def far_copy(j, slot):
            d, q = j // seq_count, j % seq_count
            return remote(
                gain_sum.at[:, q * rows : (q + 1) * rows], gain_far.at[slot], far_sem.at[0, j], far_sem.at[1, slot],
                {"dp": d, "seq": q},
            )

        gain_far[me] = gain_sum[:, pl.ds(pl.multiple_of(s * rows, LANES), rows)]
        for j in range(2 * seq_count):
            pl.when(me != j)(lambda: far_copy(j, me).start())
        for m in range(streams):
            ag.finish(0, m)
        for k in range(chunks):
            gr.finish(k)
        for j in range(2 * seq_count):
            pl.when(me != j)(lambda: far_copy(j, j).wait_recv())
        gain_out[...] = functools.reduce(jnp.add, [gain_far[j] for j in range(2 * seq_count)])
        for j in range(4):
            pl.when(t != j)(lambda: near_copy(j, t).wait_send())
        for j in range(2 * seq_count):
            pl.when(me != j)(lambda: far_copy(j, me).wait_send())
        for k in range(chunks):
            gr.drain(k)
        rs.drain()
        ag.drain()

    return pl.pallas_call(
        kernel,
        name="tail",
        out_shape=(
            jax.ShapeDtypeStruct((1, streams, 4, quarter, width), BF),
            jax.ShapeDtypeStruct((count, rows, width), F32),
            jax.ShapeDtypeStruct((rows, width), F32),
            jax.ShapeDtypeStruct((gain_rows, rows), F32),
        ),
        in_specs=in_vmem(13),
        out_specs=tuple(in_vmem(4)),
        scratch_shapes=[
            pltpu.VMEM((count, LANES, wide), BF),
            pltpu.VMEM((length, length), BF),
            pltpu.VMEM((length, width), F32),
            pltpu.VMEM((seq_count, streams, 2, 2, quarter, width), BF),
            pltpu.VMEM((count, length_all, width), BF),
            pltpu.VMEM((chunks, width, width), BF),
            pltpu.VMEM((streams, length + 8, channels), F32),
            pltpu.VMEM((quarter, width), F32),
            pltpu.VMEM((rows, width // 2), F32),
            AllGather.scratch(0, streams)[0],
            pltpu.VMEM((gain_rows, width), F32),
            pltpu.VMEM((4, gain_rows, width), F32),
            pltpu.VMEM((gain_rows, width), F32),
            pltpu.VMEM((2 * seq_count, gain_rows, rows), F32),
            pltpu.SemaphoreType.DMA((2, 4)),
            pltpu.SemaphoreType.DMA((2, 2 * seq_count)),
        ]
        + ReduceScatter.scratch(hops, streams, quarter, width)
        + GradReduce.scratch(seq_count, chunks, width, width),
        compiler_params=params(7),
    )(
        grad_stu, filter_proj, lag_proj, conv, lag_stack, lag_masks, row_ids, col_ids, base, x, gain, grad_one, gains
    )


def gated_unit(gate_pre, up_pre):
    return jax.nn.gelu(gate_pre, approximate=True) * up_pre


def local(
    seq_count,
    tokens,
    document_index,
    filters,
    stu_gain,
    filter_proj,
    lag_proj,
    attention_gain,
    query_weight,
    key_weight,
    value_weight,
    output_weight,
    feed_gain,
    gate_weight,
    up_weight,
    down_weight,
    cotangent,
):
    streams, _, length, width = tokens.shape
    row_len = length * seq_count
    quarter = length // 4
    lag_order, channels = lag_proj.shape[:2]
    count = filters.shape[0]
    hops = WINDOW // length
    tensor_place = lax.axis_index("tensor")
    chan_start = tensor_place * channels

    def split(a):
        return a.reshape(a.shape[:-2] + (2, 2, quarter, width))

    def quarters(a):
        return a.reshape(a.shape[:-2] + (4, quarter, width))

    def whole(a):
        return a.reshape(a.shape[:-3] + (length, width))

    def row(gain):
        return gain.reshape(1, width)

    x = tokens[:, 0]
    grad_three = cotangent[:, 0]
    ids = document_index[:, 0]
    inputs = norm_of(x.astype(F32), stu_gain).astype(BF)
    id_tile = ids.reshape(streams * length // LANES, LANES)
    rows_ext, id_ext = gather_rows(quarters(inputs), id_tile, seq_count)
    rows_ext = whole(rows_ext)
    id_ext = id_ext.reshape(seq_count, streams, length)
    id_rows = id_ext[:, :, None, :]
    id_cols = id_ext[:, :, :, None]

    pad = jnp.zeros((count, 4 * LANES), filters.dtype)
    ahead = row_len - LANES
    base = jnp.concatenate(
        [
            jnp.flip(filters[:, : ahead + 1], axis=1),
            pad[:, : 4 * LANES],
            jnp.flip(filters[:, ahead + 1 :], axis=1),
        ],
        axis=1,
    ).astype(F32)[:, None]
    base_back = jnp.concatenate(
        [pad[:, : length - LANES], filters, pad[:, :LANES]], axis=1
    ).astype(F32)[:, None]
    conv = convolve(rows_ext, id_rows, id_cols[0], base, seq_count)

    chan_rows = lax.dynamic_slice_in_dim(rows_ext[:2], chan_start, channels, 3)
    joined = jnp.concatenate([chan_rows[1][:, length - lag_order :], chan_rows[0]], axis=1)
    joined_ids = jnp.concatenate([id_ext[1][:, length - lag_order :], ids], axis=1)
    masks = []
    lagged = []
    for step in range(1, lag_order + 1):
        low = lag_order - step
        masks.append((joined_ids[:, low : low + length] == ids)[:, :, None])
        lagged.append(jnp.where(masks[-1], joined[:, low : low + length], jnp.zeros((), BF)))
    lag_stack = jnp.stack(lagged)

    mixed = jnp.einsum("kmtd,kde->mte", conv, filter_proj, preferred_element_type=F32)
    mixed = mixed + jnp.einsum("imtc,ice->mte", lag_stack, lag_proj, preferred_element_type=F32)

    state = jax.ShapeDtypeStruct((streams, quarter, width), F32)
    gain_state = jax.ShapeDtypeStruct((1, width), F32)

    def finish_one(m, total, others, extra):
        x_ref, gain_ref = others
        hidden = x_ref[m, place()[1]].astype(F32) + total
        extra[0][m] = hidden
        return norm_of(hidden, gain_ref[...]).astype(BF)

    attn_ext, hidden_one = exchange(
        "exchange_one", 2, seq_count, [split(mixed.astype(BF))[None]], [quarters(x), row(attention_gain)], 0, hops,
        finish_one, [state],
    )
    attn_ext = whole(attn_ext)

    q, k, v, attended, lse, out_part = attend(
        attn_ext, id_rows[: hops + 1], id_cols[0], query_weight, key_weight, value_weight, output_weight
    )

    def finish_two(m, total, others, extra):
        hidden_ref, gain_ref = others
        hidden = hidden_ref[m] + total
        extra[0][m] = hidden
        return norm_of(hidden, gain_ref[...]).astype(BF)

    feed_in, hidden_two = exchange(
        "exchange_two", 3, seq_count, [split(out_part)[None]], [hidden_one, row(feed_gain)], 0, 0, finish_two, [state]
    )
    feed_in = whole(feed_in)[0].reshape(streams * length, width)
    flat_three = grad_three.reshape(streams * length, width)

    gate_pre = dot_nn(feed_in, gate_weight)
    up_pre = dot_nn(feed_in, up_weight)
    grad_inner = dot_nt(flat_three, down_weight)
    unit, pull = jax.vjp(gated_unit, gate_pre, up_pre)
    inner = unit.astype(BF)
    grad_gate, grad_up = pull(grad_inner)
    grad_gate = grad_gate.astype(BF)
    grad_up = grad_up.astype(BF)
    layer_part = dot_nn(inner, down_weight).astype(BF)
    feed_part = (dot_nt(grad_gate, gate_weight) + dot_nt(grad_up, up_weight)).astype(BF)

    def finish_three(m, total, others, extra):
        hidden_ref, gain_ref, cot_ref = others
        if m >= streams:
            return (hidden_ref[m - streams] + total).astype(BF)
        grad_in, gain_grad = norm_back(hidden_ref[m], gain_ref[...], total)
        grad_two = cot_ref[m, place()[1]].astype(F32) + grad_in
        extra[0][m] = grad_two
        extra[1][...] = gain_grad if m == 0 else extra[1][...] + gain_grad
        return grad_two.astype(BF)

    shape = (1, streams, length, width)
    both, grad_two, feed_gain_grad = exchange(
        "exchange_three", 4, seq_count, [split(feed_part.reshape(shape)), split(layer_part.reshape(shape))],
        [hidden_two, row(feed_gain), quarters(grad_three)], 0, 0, finish_three, [state, gain_state],
    )
    both = whole(both)[0]
    grad_att_out = both[:streams]
    layer_output = both[streams:]

    dq, dk, dv, attn_part = attend_back(
        q, k, v, lse, grad_att_out, id_rows[: hops + 1], id_cols[0], query_weight, key_weight, value_weight, output_weight
    )

    tokens_flat = streams * length
    go = grad_att_out.reshape(tokens_flat, width)
    first = jnp.concatenate(
        [
            dot_tn(feed_in, grad_gate).astype(BF),
            dot_tn(feed_in, grad_up).astype(BF),
            dot_tn(flat_three, inner).astype(BF),
            dot_tn(attn_ext[0].reshape(tokens_flat, width), dq.reshape(tokens_flat, -1)).astype(BF),
            dot_tn(attn_ext.reshape(-1, width), dk.reshape(-1, dk.shape[-1])).astype(BF),
            dot_tn(attn_ext.reshape(-1, width), dv.reshape(-1, dv.shape[-1])).astype(BF),
            dot_tn(go, attended.reshape(tokens_flat, -1)).astype(BF),
        ],
        axis=1,
    )

    def finish_four(m, total, others, extra):
        hidden_ref, gain_ref, grad_ref = others
        grad_in, gain_grad = norm_back(hidden_ref[m], gain_ref[...], total)
        grad_one = grad_ref[m] + grad_in
        extra[0][m] = grad_one
        extra[1][...] = gain_grad if m == 0 else extra[1][...] + gain_grad
        return grad_one.astype(BF)

    fused = width // seq_count % LANES == 0
    results = exchange(
        "exchange_four", 5, seq_count, [split(attn_part)], [hidden_one, row(attention_gain), grad_two], hops, 0,
        finish_four, [state, gain_state], first[None] if fused else None,
    )
    grad_stu, grad_one, attn_gain_grad = results[:3]
    grad_stu = whole(grad_stu)[0]
    lag_masks = jnp.stack(masks).astype(F32)
    if fused:
        first = results[3][0]
        input_gradient, filter_grad, lag_grad, gains = tail(
            grad_stu.reshape(tokens_flat, width), filter_proj, lag_proj, conv.reshape(count, tokens_flat, width),
            lag_stack.reshape(lag_order, tokens_flat, channels), lag_masks, id_rows[0], id_cols, base_back,
            quarters(x), row(stu_gain), grad_one, jnp.concatenate([attn_gain_grad, feed_gain_grad], axis=0), seq_count,
        )
        input_gradient = whole(input_gradient)[0]
    else:
        grad_conv = jnp.einsum("mte,kde->kmtd", grad_stu, filter_proj, preferred_element_type=F32).astype(BF)
        grad_lagged = jnp.einsum("mte,ice->imtc", grad_stu, lag_proj, preferred_element_type=F32)
        ext_grad = jnp.zeros((streams, 8 + length, channels), F32)
        for step in range(1, lag_order + 1):
            term = jnp.where(masks[step - 1], grad_lagged[step - 1], 0.0)
            ext_grad = ext_grad + jnp.pad(term, ((0, 0), (8 - step, step), (0, 0)))
        terms = convolve_back(
            grad_conv, id_rows[0], id_cols, base_back, ext_grad[:, 8:], ext_grad[:, :8], seq_count
        )

        def finish_five(m, total, others, extra):
            x_ref, gain_ref, grad_ref = others
            grad_in, gain_grad = norm_back(x_ref[m, place()[1]].astype(F32), gain_ref[...], total)
            extra[0][...] = gain_grad if m == 0 else extra[0][...] + gain_grad
            return (grad_ref[m] + grad_in).astype(BF)

        input_gradient, stu_gain_grad = exchange(
            "exchange_five", 6, seq_count, [split(terms)], [quarters(x), row(stu_gain), grad_one], seq_count - 1, 0,
            finish_five, [gain_state],
        )
        input_gradient = whole(input_gradient)[0]
        stu = grad_stu.reshape(tokens_flat, width)
        filter_part = jnp.einsum("kmtd,mte->kde", conv, grad_stu, preferred_element_type=F32).astype(BF)
        lag_part = jnp.concatenate(
            [dot_tn(stu, lag_stack[i].reshape(tokens_flat, channels)).astype(BF) for i in range(lag_order)], axis=1
        )
        first = lax.psum(lax.psum_scatter(first, "seq", scatter_dimension=0, tiled=True), "dp").astype(F32)
        filter_grad = lax.psum(
            lax.psum_scatter(filter_part, "seq", scatter_dimension=1, tiled=True), "dp"
        ).astype(F32)
        lag_grad = lax.psum(lax.psum_scatter(lag_part, "seq", scatter_dimension=0, tiled=True), "dp").astype(F32)
        gains = jnp.concatenate([stu_gain_grad, attn_gain_grad, feed_gain_grad], axis=0)
        gains = lax.psum(gains, ("dp", "seq", "tensor"))
        gain_width = width // seq_count
        gains = lax.dynamic_slice_in_dim(gains, lax.axis_index("seq") * gain_width, gain_width, 1)

    hidden_units = gate_weight.shape[1]
    cols = query_weight.shape[1]
    cuts = [hidden_units, 2 * hidden_units, 3 * hidden_units]
    cuts += [cuts[-1] + cols, cuts[-1] + 2 * cols, cuts[-1] + 3 * cols]
    gate_grad, up_grad, down_grad, query_grad, key_grad, value_grad, output_grad = jnp.split(first, cuts, axis=1)
    lag_grad = lag_grad[:, : lag_order * channels].T.reshape(lag_order, channels, -1)
    return (
        layer_output[:, None],
        input_gradient[:, None],
        gains[0],
        filter_grad,
        lag_grad,
        gains[1],
        query_grad,
        key_grad,
        value_grad,
        output_grad.T,
        gains[2],
        gate_grad,
        up_grad,
        down_grad.T,
    )


def solution(mesh):
    return jax.shard_map(
        functools.partial(local, mesh.shape["seq"]),
        mesh=mesh,
        in_specs=(
            P(None, "dp", "seq", None),
            P(None, "dp", "seq"),
            P("tensor", None),
            P(),
            P("tensor", None, None),
            P(None, "tensor", None),
            P(),
            P(None, "tensor"),
            P(None, "tensor"),
            P(None, "tensor"),
            P("tensor", None),
            P(),
            P(None, "tensor"),
            P(None, "tensor"),
            P("tensor", None),
            P(None, "dp", "seq", None),
        ),
        out_specs=(
            P(None, "dp", "seq", None),
            P(None, "dp", "seq", None),
            P("seq"),
            P("tensor", "seq", None),
            P(None, "tensor", "seq"),
            P("seq"),
            P("seq", "tensor"),
            P("seq", "tensor"),
            P("seq", "tensor"),
            P("tensor", "seq"),
            P("seq"),
            P("seq", "tensor"),
            P("seq", "tensor"),
            P("tensor", "seq"),
        ),
        check_vma=False,
    )
```

```python
import functools

import jax
import jax.numpy as jnp
from jax import lax
from jax.experimental import pallas as pl
from jax.experimental.pallas import tpu as pltpu
from jax.sharding import PartitionSpec as P

HD = 64
WINDOW = 1024
EPSILON = 1e-05
LANES = 128
NEGATIVE = -1e30
MESH = pl.DeviceIdType.MESH
BF = jnp.bfloat16
F32 = jnp.float32
VMEM_LIMIT = 60 * 1024 * 1024


def place():
    s = lax.axis_index("seq")
    t = lax.axis_index("tensor")
    y = t // 2
    c = t - 2 * y
    return s, t, y, c, t + 1 - 2 * c, t + 2 - 4 * y


def when(condition, action):
    if condition is True:
        action()
    else:
        pl.when(condition)(action)


def remote(src, dst, send_sem, recv_sem, device):
    return pltpu.make_async_remote_copy(
        src_ref=src, dst_ref=dst, send_sem=send_sem, recv_sem=recv_sem, device_id=device, device_id_type=MESH
    )


def greet(seq_count, hops, wide=False, gains=False):
    s, t, y, c, core, far = place()
    barrier = pltpu.get_barrier_semaphore()

    def signal(device):
        pl.semaphore_signal(barrier, inc=1, device_id=device, device_id_type=MESH)

    signal({"tensor": core})
    signal({"tensor": far})
    if gains:
        signal({"tensor": 3 - t})
    if wide:
        p = lax.axis_index("dp")
        signal({"dp": 1 - p})
        for j in range(seq_count):

            @pl.when(s != j)
            def _():
                signal({"seq": j})
                if gains:
                    signal({"dp": 1 - p, "seq": j})

        peers = 2 + gains + 1 + (seq_count - 1) * (1 + gains)
    else:
        for h in range(1, hops + 1):
            for there, peer in ((s - h >= 0, s - h), (s + h < seq_count, s + h)):

                @pl.when(there)
                def _():
                    signal({"seq": peer})

        peers = 2 + jnp.minimum(s, hops) + jnp.minimum(seq_count - 1 - s, hops)
    pl.semaphore_wait(barrier, peers)


class ReduceScatter:
    def __init__(self, seq_count, hops, streams, part, scratch):
        self.seq_count, self.hops, self.streams, self.part = seq_count, hops, streams, part
        self.near, self.half, self.over, self.hop_out, self.hop_in, self.sem = scratch

    @staticmethod
    def scratch(hops, streams, rows, width):
        quarter = (hops + 1, streams, rows, width)
        return [
            pltpu.VMEM((hops + 1, streams, 2, rows, width), BF),
            pltpu.VMEM(quarter, BF),
            pltpu.VMEM(quarter, BF),
            pltpu.VMEM(quarter, BF),
            pltpu.VMEM(quarter, BF),
            pltpu.SemaphoreType.DMA((6, hops + 1, streams)),
        ]

    def to_core(self, h, m):
        s, t, y, c, core, far = place()
        return remote(
            self.part(h, m).at[:, 1 - c], self.near.at[h, m], self.sem.at[0, h, m], self.sem.at[1, h, m], {"tensor": core}
        )

    def to_far(self, h, m):
        s, t, y, c, core, far = place()
        return remote(self.half.at[h, m], self.over.at[h, m], self.sem.at[2, h, m], self.sem.at[3, h, m], {"tensor": far})

    def to_hop(self, h, m, peer):
        return remote(
            self.hop_out.at[h, m], self.hop_in.at[h, m], self.sem.at[4, h, m], self.sem.at[5, h, m], {"seq": peer}
        )

    def there(self, h):
        return True if isinstance(h, int) and h == 0 else lax.axis_index("seq") - h >= 0

    def order(self):
        return [(h, m) for h in range(self.hops, -1, -1) for m in range(self.streams)]

    def start(self, h, m):
        when(self.there(h), lambda: self.to_core(h, m).start())

    def middle(self, h, m):
        s, t, y, c, core, far = place()

        def act():
            self.to_core(h, m).wait_recv()
            mine = self.part(h, m)[1 - y, c].astype(F32) + self.near[h, m, 1 - y].astype(F32)
            self.half[h, m] = mine.astype(BF)
            self.to_far(h, m).start()

        when(self.there(h), act)

    def own(self, h, m):
        s, t, y, c, core, far = place()
        self.to_far(h, m).wait_recv()
        return (
            self.part(h, m)[y, c].astype(F32) + self.near[h, m, y].astype(F32) + self.over[h, m].astype(F32)
        )

    def hop(self, h, m):
        def act():
            self.hop_out[h, m] = self.own(h, m).astype(BF)
            self.to_hop(h, m, lax.axis_index("seq") - h).start()

        when(self.there(h), act)

    def total(self, m, acc):
        acc[...] = self.own(0, m)
        for h in range(1, self.hops + 1):
            s = lax.axis_index("seq")

            @pl.when(s + h < self.seq_count)
            def _():
                self.to_hop(h, m, s + h).wait_recv()
                acc[...] += self.hop_in[h, m].astype(F32)

    def drain(self):
        for h, m in self.order():

            def act():
                self.to_core(h, m).wait_send()
                self.to_far(h, m).wait_send()
                if h:
                    self.to_hop(h, m, lax.axis_index("seq") - h).wait_send()

            when(self.there(h), act)


class AllGather:
    def __init__(self, seq_count, hops, streams, out, sem, first=0):
        self.seq_count, self.hops, self.streams, self.out, self.sem, self.first = seq_count, hops, streams, out, sem, first

    @staticmethod
    def scratch(hops, streams):
        return [pltpu.SemaphoreType.DMA((8, hops + 1, streams))]

    def there(self, h):
        return True if h == 0 else lax.axis_index("seq") - h >= 0

    def copy(self, kind, h, m, quarter, device, to=None):
        source = self.out.at[0 if kind == 0 else h, m, quarter]
        return remote(source, self.out.at[h, m, quarter], self.sem.at[2 * kind, h, m], self.sem.at[2 * kind + 1, h, m], device)

    def to_hop(self, h, m, peer):
        return self.copy(0, h, m, place()[1], {"seq": peer})

    def spread(self, h, m):
        s, t, y, c, core, far = place()
        self.copy(1, h, m, t, {"tensor": far}).start()
        self.copy(2, h, m, t, {"tensor": core}).start()

    def start(self, m):
        s, t, y, c, core, far = place()
        for h in range(1, self.hops + 1):

            @pl.when(s + h < self.seq_count)
            def _():
                self.to_hop(h, m, s + h).start()

        if self.first == 0:
            self.spread(0, m)

    def arrive(self, h, m):
        @pl.when(self.there(h))
        def _():
            self.to_hop(h, m, lax.axis_index("seq") - h).wait_recv()
            self.spread(h, m)

    def pass_on(self, h, m):
        s, t, y, c, core, far = place()

        def act():
            self.copy(1, h, m, far, {"tensor": far}).wait_recv()
            self.copy(3, h, m, far, {"tensor": core}).start()

        when(self.there(h), act)

    def finish(self, h, m):
        s, t, y, c, core, far = place()

        def act():
            self.copy(2, h, m, core, {"tensor": core}).wait_recv()
            self.copy(3, h, m, 3 - t, {"tensor": core}).wait_recv()

        when(self.there(h), act)

    def clear(self, h, m):
        @pl.when(lax.axis_index("seq") - h < 0)
        def _():
            self.out[h, m] = jnp.zeros(self.out.shape[2:], self.out.dtype)

    def drain(self):
        s, t, y, c, core, far = place()
        for m in range(self.streams):
            for h in range(1, self.hops + 1):

                @pl.when(s + h < self.seq_count)
                def _():
                    self.to_hop(h, m, s + h).wait_send()

            for h in range(self.first, self.hops + 1):

                def act():
                    self.copy(1, h, m, t, {"tensor": far}).wait_send()
                    self.copy(2, h, m, t, {"tensor": core}).wait_send()
                    self.copy(3, h, m, far, {"tensor": core}).wait_send()

                when(self.there(h), act)


class GradReduce:
    def __init__(self, seq_count, source, result, scratch):
        self.seq_count, self.source, self.result = seq_count, source, result
        self.x_in, self.z_out, self.z_in, self.back_out, self.back_in, self.x_sem, self.z_sem, self.back_sem = scratch
        self.half = self.x_in.shape[2]
        self.rows = self.back_out.shape[1]

    @staticmethod
    def scratch(seq_count, chunks, depth, width):
        rows, half = depth // seq_count, width // 2
        return [
            pltpu.VMEM((chunks, depth, half), BF),
            pltpu.VMEM((chunks, depth, half), BF),
            pltpu.VMEM((chunks, seq_count, rows, half), BF),
            pltpu.VMEM((chunks, rows, half), BF),
            pltpu.VMEM((chunks, rows, half), BF),
            pltpu.SemaphoreType.DMA((2, chunks)),
            pltpu.SemaphoreType.DMA((2, chunks, seq_count)),
            pltpu.SemaphoreType.DMA((2, chunks)),
        ]

    def columns(self, p):
        return pl.ds(pl.multiple_of(p * self.half, LANES), self.half)

    def block(self, j):
        return pl.ds(pl.multiple_of(j * self.rows, 16), self.rows)

    def over(self, c):
        p = lax.axis_index("dp")
        return remote(
            self.source(c).at[:, self.columns(1 - p)], self.x_in.at[c], self.x_sem.at[0, c], self.x_sem.at[1, c], {"dp": 1 - p}
        )

    def row_copy(self, c, j, slot):
        return remote(
            self.z_out.at[c, self.block(j)], self.z_in.at[c, slot], self.z_sem.at[0, c, j], self.z_sem.at[1, c, slot], {"seq": j}
        )

    def back(self, c):
        p = lax.axis_index("dp")
        return remote(
            self.back_out.at[c], self.back_in.at[c], self.back_sem.at[0, c], self.back_sem.at[1, c], {"dp": 1 - p}
        )

    def others(self, action):
        for j in range(self.seq_count):
            pl.when(lax.axis_index("seq") != j)(functools.partial(action, j))

    def start(self, c):
        self.over(c).start()

    def spread(self, c):
        s, p = lax.axis_index("seq"), lax.axis_index("dp")
        self.over(c).wait_recv()
        mine = self.source(c)[:, self.columns(p)].astype(F32) + self.x_in[c].astype(F32)
        self.z_out[c] = mine.astype(BF)
        self.others(lambda j: self.row_copy(c, j, s).start())

    def collect(self, c, acc):
        s, p = lax.axis_index("seq"), lax.axis_index("dp")
        here = self.block(s)
        acc[...] = self.source(c)[here, self.columns(p)].astype(F32) + self.x_in[c, here].astype(F32)

        def add(j):
            self.row_copy(c, j, j).wait_recv()
            acc[...] += self.z_in[c, j].astype(F32)

        self.others(add)
        self.back_out[c] = acc[...].astype(BF)
        self.back(c).start()

    def finish(self, c):
        p = lax.axis_index("dp")
        self.back(c).wait_recv()
        self.result(c)[:, self.columns(p)] = self.back_out[c].astype(F32)
        self.result(c)[:, self.columns(1 - p)] = self.back_in[c].astype(F32)

    def drain(self, c):
        self.over(c).wait_send()
        self.others(lambda j: self.row_copy(c, j, lax.axis_index("seq")).wait_send())
        self.back(c).wait_send()


def params(cid=None):
    if cid is None:
        return pltpu.CompilerParams(vmem_limit_bytes=VMEM_LIMIT)
    return pltpu.CompilerParams(vmem_limit_bytes=VMEM_LIMIT, collective_id=cid, has_side_effects=True)


def in_vmem(count):
    return [pl.BlockSpec(memory_space=pltpu.VMEM)] * count


def gather_rows(inputs, ids, seq_count):
    streams, quarters, rows, width = inputs.shape
    hops = seq_count - 1

    def kernel(x_ref, id_ref, out, out_ids, sem, id_sem):
        s, t, y, c, core, far = place()
        greet(seq_count, hops)
        out[0] = x_ref[...]
        out_ids[0] = id_ref[...]
        ag = AllGather(seq_count, hops, streams, out, sem, first=1)

        def id_copy(h, peer):
            return remote(id_ref, out_ids.at[h], id_sem.at[0, h], id_sem.at[1, h], {"seq": peer})

        for h in range(1, hops + 1):

            @pl.when(s + h < seq_count)
            def _():
                id_copy(h, s + h).start()

        ag.to_hop = lambda h, m, peer: remote(
            x_ref.at[m, t], out.at[h, m, t], sem.at[0, h, m], sem.at[1, h, m], {"seq": peer}
        )
        for m in range(streams):
            ag.start(m)
        for h in range(1, hops + 1):
            for m in range(streams):
                ag.clear(h, m)

            @pl.when(s - h < 0)
            def _():
                out_ids[h] = jnp.full(out_ids.shape[1:], -1, jnp.int32)

        for m in range(streams):
            for h in range(1, hops + 1):
                ag.arrive(h, m)
        for m in range(streams):
            for h in range(1, hops + 1):
                ag.pass_on(h, m)
        for h in range(1, hops + 1):
            for m in range(streams):
                ag.finish(h, m)

            @pl.when(s - h >= 0)
            def _():
                id_copy(h, s - h).wait_recv()

            @pl.when(s + h < seq_count)
            def _():
                id_copy(h, s + h).wait_send()

        ag.drain()

    return pl.pallas_call(
        kernel,
        name="gather_rows",
        out_shape=(
            jax.ShapeDtypeStruct((seq_count,) + inputs.shape, inputs.dtype),
            jax.ShapeDtypeStruct((seq_count,) + ids.shape, jnp.int32),
        ),
        in_specs=in_vmem(2),
        out_specs=tuple(in_vmem(2)),
        scratch_shapes=AllGather.scratch(hops, streams) + [pltpu.SemaphoreType.DMA((2, seq_count))],
        compiler_params=params(1),
    )(inputs, ids)


def exchange(name, cid, seq_count, parts, others, reduce_hops, gather_hops, finish, extra, grads=None):
    per_part = parts[0].shape[1]
    rows, width = parts[0].shape[4:]
    streams = per_part * len(parts)
    hops = max(reduce_hops, gather_hops)
    given = [] if grads is None else [grads]
    chunks = 0 if grads is None else grads.shape[0]
    sums, tools = [], []
    if chunks:
        depth, wide = grads.shape[1:]
        sums = [jax.ShapeDtypeStruct((chunks, depth // seq_count, wide), F32)]
        tools = [pltpu.VMEM((depth // seq_count, wide // 2), F32)] + GradReduce.scratch(seq_count, chunks, depth, wide)

    def kernel(*refs):
        refs = list(refs)
        part_refs = [refs.pop(0) for _ in parts]
        other_refs = [refs.pop(0) for _ in others]
        grad_ref = refs.pop(0) if chunks else None
        out = refs.pop(0)
        extra_refs = [refs.pop(0) for _ in extra]
        sum_ref = refs.pop(0) if chunks else None
        grad_tools = [refs.pop(0) for _ in tools]
        acc = refs.pop(0)
        gather_sem = refs.pop(0)
        s, t, y, c, core, far = place()
        greet(seq_count, hops, wide=bool(chunks))
        if chunks:
            grad_acc = grad_tools.pop(0)
            gr = GradReduce(seq_count, lambda c: grad_ref.at[c], lambda c: sum_ref.at[c], grad_tools)
        rs = ReduceScatter(
            seq_count, reduce_hops, streams, lambda h, m: part_refs[m // per_part].at[h, m % per_part], refs
        )
        ag = AllGather(seq_count, gather_hops, streams, out, gather_sem)
        for h, m in rs.order():
            rs.start(h, m)
        for k in range(chunks):
            gr.start(k)
        for h in range(1, gather_hops + 1):
            for m in range(streams):
                ag.clear(h, m)
        for h, m in rs.order():
            rs.middle(h, m)
        for h, m in rs.order():
            if h:
                rs.hop(h, m)
        for k in range(chunks):
            gr.spread(k)
        for m in range(streams):
            rs.total(m, acc)
            out[0, m, t] = finish(m, acc[...], other_refs, extra_refs)
            ag.start(m)
        for k in range(chunks):
            gr.collect(k, grad_acc)
        for m in range(streams):
            ag.pass_on(0, m)
            for h in range(1, gather_hops + 1):
                ag.arrive(h, m)
        for m in range(streams):
            for h in range(1, gather_hops + 1):
                ag.pass_on(h, m)
        for h in range(gather_hops + 1):
            for m in range(streams):
                ag.finish(h, m)
        for k in range(chunks):
            gr.finish(k)
            gr.drain(k)
        rs.drain()
        ag.drain()

    return pl.pallas_call(
        kernel,
        name=name,
        out_shape=(jax.ShapeDtypeStruct((gather_hops + 1, streams, 4, rows, width), BF),) + tuple(extra) + tuple(sums),
        in_specs=in_vmem(len(parts) + len(others) + len(given)),
        out_specs=tuple(in_vmem(1 + len(extra) + len(sums))),
        scratch_shapes=tools
        + [pltpu.VMEM((rows, width), F32)]
        + AllGather.scratch(gather_hops, streams)
        + ReduceScatter.scratch(reduce_hops, streams, rows, width),
        compiler_params=params(cid),
    )(*parts, *others, *given)


def norm_of(values, gain_row):
    inverse = lax.rsqrt(jnp.mean(values * values, axis=-1, keepdims=True) + EPSILON)
    return values * inverse * gain_row


def norm_back(values, gain_row, grad_out):
    inverse = lax.rsqrt(jnp.mean(values * values, axis=-1, keepdims=True) + EPSILON)
    scaled = grad_out * gain_row
    dot = jnp.mean(scaled * values, axis=-1, keepdims=True)
    grad_in = inverse * scaled - values * (inverse * inverse * inverse) * dot
    return grad_in, jnp.sum(grad_out * values * inverse, axis=0, keepdims=True)


def strips(base_ref, strip):
    @pl.loop(0, base_ref.shape[0])
    def _(k):
        row = jnp.broadcast_to(base_ref[k], strip.shape[1:])
        strip[k] = pltpu.roll(row, 0, 1, stride=1, stride_axis=0).astype(BF)


def convolve(rows, row_ids, col_ids, base, seq_count):
    _, streams, length, width = rows.shape
    count, _, wide = base.shape
    blocks = length // LANES
    at_once = seq_count <= 4

    def whole_kernel(x_ref, row_ref, col_ref, base_ref, out_ref, strip, mask, left):
        strips(base_ref, strip)

        @pl.loop(0, streams)
        def _(m):
            for h in range(seq_count):
                mask[:, h * length : (h + 1) * length] = jnp.where(col_ref[m] == row_ref[h, m], 1.0, 0.0).astype(BF)
            right = jnp.concatenate([x_ref[h, m] for h in range(seq_count)], axis=0)

            @pl.loop(0, count)
            def _(k):
                for a in range(blocks):
                    for h in range(seq_count):
                        start = LANES * (blocks * (seq_count - h) - 1 - a)
                        down, across = slice(a * LANES, (a + 1) * LANES), slice(h * length, (h + 1) * length)
                        left[down, across] = strip[k, :, start : start + length] * mask[down, across]
                out_ref[k, m] = jnp.dot(left[...], right, preferred_element_type=F32).astype(BF)

    def kernel(x_ref, row_ref, col_ref, base_ref, out_ref, strip, mask, acc):
        strips(base_ref, strip)
        s = lax.axis_index("seq")

        @pl.loop(0, streams)
        def _(m):
            acc[...] = jnp.zeros_like(acc)

            @pl.loop(0, s + 1)
            def _(h):
                mask[...] = jnp.where(col_ref[m] == row_ref[h, m], 1.0, 0.0).astype(BF)

                @pl.loop(0, count)
                def _(k):
                    pieces = []
                    for a in range(blocks):
                        start = pl.multiple_of(LANES * (blocks * (seq_count - h) - 1 - a), LANES)
                        pieces.append(strip[k, :, pl.ds(start, length)] * mask[a * LANES : (a + 1) * LANES])
                    acc[k] += jnp.dot(jnp.concatenate(pieces, axis=0), x_ref[h, m], preferred_element_type=F32)

            @pl.loop(0, count)
            def _(k):
                out_ref[k, m] = acc[k].astype(BF)

    span = seq_count * length if at_once else length
    return pl.pallas_call(
        whole_kernel if at_once else kernel,
        name="convolve",
        out_shape=jax.ShapeDtypeStruct((count, streams, length, width), BF),
        in_specs=in_vmem(4),
        out_specs=in_vmem(1)[0],
        scratch_shapes=[
            pltpu.VMEM((count, LANES, wide), BF),
            pltpu.VMEM((length, span), BF),
            pltpu.VMEM((length, span), BF) if at_once else pltpu.VMEM((count, length, width), F32),
        ],
        compiler_params=params(),
    )(rows, row_ids, col_ids, base)


def convolve_back(grads, row_ids, col_ids, base, own_lag, tail_lag, seq_count):
    count, streams, length, width = grads.shape
    wide = base.shape[2]
    blocks = length // LANES
    channels = own_lag.shape[2]
    tail_rows = tail_lag.shape[1]

    def kernel(g_ref, row_ref, col_ref, base_ref, own_ref, tail_ref, out_ref, strip, mask, acc):
        strips(base_ref, strip)
        s = lax.axis_index("seq")
        mine = pl.ds(pl.multiple_of(lax.axis_index("tensor") * channels, LANES), channels)

        @pl.loop(0, s + 1)
        def _(h):
            @pl.loop(0, streams)
            def _(m):
                mask[...] = jnp.where(col_ref[h, m] == row_ref[m], 1.0, 0.0).astype(BF)
                acc[...] = jnp.zeros_like(acc)

                @pl.when(h == 0)
                def _():
                    acc[:, mine] = own_ref[m]

                @pl.when(h == 1)
                def _():
                    acc[length - tail_rows :, mine] = tail_ref[m]

                @pl.loop(0, count)
                def _(k):
                    pieces = []
                    for a in range(blocks):
                        start = pl.multiple_of(LANES * (blocks * h + blocks - 1 - a), LANES)
                        pieces.append(strip[k, :, pl.ds(start, length)] * mask[a * LANES : (a + 1) * LANES])
                    acc[...] += jnp.dot(jnp.concatenate(pieces, axis=0), g_ref[k, m], preferred_element_type=F32)

                out_ref[h, m] = acc[...].astype(BF)

    return pl.pallas_call(
        kernel,
        name="convolve_back",
        out_shape=jax.ShapeDtypeStruct((seq_count, streams, length, width), BF),
        in_specs=in_vmem(6),
        out_specs=in_vmem(1)[0],
        scratch_shapes=[
            pltpu.VMEM((count, LANES, wide), BF),
            pltpu.VMEM((length, length), BF),
            pltpu.VMEM((length, width), F32),
        ],
        compiler_params=params(),
    )(grads, row_ids, col_ids, base, own_lag, tail_lag)


def dot_nn(a, b):
    return jnp.dot(a, b, preferred_element_type=F32)


def dot_nt(a, b):
    return lax.dot_general(a, b, (((1,), (1,)), ((), ())), preferred_element_type=F32)


def dot_tn(a, b):
    return lax.dot_general(a, b, (((0,), (0,)), ((), ())), preferred_element_type=F32)


def allowed_keys(query_ids, key_ids, first_row, distance):
    shape = (query_ids.shape[0], key_ids.shape[1])
    offset = lax.broadcasted_iota(jnp.int32, shape, 0) - lax.broadcasted_iota(jnp.int32, shape, 1) + (first_row + distance)
    return (query_ids == key_ids) & (offset >= 0) & (offset < WINDOW)


def one_head(block, head):
    lane = lax.broadcasted_iota(jnp.int32, block.shape, 1)
    return jnp.where((lane >= head * HD) & (lane < (head + 1) * HD), block, jnp.zeros_like(block))


def attend(rows, row_ids, col_ids, wq, wk, wv, wo):
    spans, streams, length, width = rows.shape
    cols = wq.shape[1]
    heads = cols // HD
    tile = min(256, length)
    scale = HD ** (-0.5)

    def kernel(x_ref, row_ref, col_ref, wq_ref, wk_ref, wv_ref, wo_ref, q_ref, k_ref, v_ref, a_ref, lse_ref, p_ref):
        @pl.loop(0, streams)
        def _(m):
            q_ref[m] = dot_nn(x_ref[0, m], wq_ref[...]).astype(BF)
            for h in range(spans):
                k_ref[h, m] = dot_nn(x_ref[h, m], wk_ref[...]).astype(BF)
                v_ref[h, m] = dot_nn(x_ref[h, m], wv_ref[...]).astype(BF)

            @pl.loop(0, length // tile)
            def _(i):
                first = pl.multiple_of(i * tile, tile)
                here = pl.ds(first, tile)
                masks = [allowed_keys(col_ref[m, here], row_ref[h, m], first, h * length) for h in range(spans)]
                block = q_ref[m, here]
                result = jnp.zeros((tile, cols), F32)
                for head in range(heads):
                    query = one_head(block, head)
                    scores = [
                        jnp.where(masks[h], dot_nt(query, k_ref[h, m]) * scale, NEGATIVE) for h in range(spans)
                    ]
                    peak = functools.reduce(jnp.maximum, [jnp.max(v, axis=-1, keepdims=True) for v in scores])
                    raised = [jnp.exp(v - peak) for v in scores]
                    total = sum([jnp.sum(v, axis=-1, keepdims=True) for v in raised])
                    inverse = 1.0 / total
                    mixed = sum([dot_nn((raised[h] * inverse).astype(BF), v_ref[h, m]) for h in range(spans)])
                    result = result + one_head(mixed, head)
                    lse_ref[m, head, here] = jnp.broadcast_to(peak + jnp.log(total), (tile, LANES))
                a_ref[m, here] = result.astype(BF)

            p_ref[m] = dot_nn(a_ref[m], wo_ref[...]).astype(BF)

    part = jax.ShapeDtypeStruct((streams, length, cols), BF)
    span = jax.ShapeDtypeStruct((spans, streams, length, cols), BF)
    return pl.pallas_call(
        kernel,
        name="attend",
        out_shape=(
            part,
            span,
            span,
            part,
            jax.ShapeDtypeStruct((streams, heads, length, LANES), F32),
            jax.ShapeDtypeStruct((streams, length, width), BF),
        ),
        in_specs=in_vmem(7),
        out_specs=tuple(in_vmem(6)),
        compiler_params=params(),
    )(rows, row_ids, col_ids, wq, wk, wv, wo)


def attend_back(q, k, v, lse, grad_out, row_ids, col_ids, wq, wk, wv, wo):
    spans, streams, length, cols = k.shape
    width = grad_out.shape[2]
    heads = cols // HD
    tile = min(256, length)
    scale = HD ** (-0.5)

    def kernel(
        q_ref, k_ref, v_ref, lse_ref, go_ref, row_ref, col_ref, wq_ref, wk_ref, wv_ref, wo_ref,
        dq_ref, dk_ref, dv_ref, p_ref, ga_ref, dk_acc, dv_acc,
    ):
        @pl.loop(0, streams)
        def _(m):
            ga_ref[...] = dot_nt(go_ref[m], wo_ref[...]).astype(BF)
            dk_acc[...] = jnp.zeros_like(dk_acc)
            dv_acc[...] = jnp.zeros_like(dv_acc)

            @pl.loop(0, length // tile)
            def _(i):
                first = pl.multiple_of(i * tile, tile)
                here = pl.ds(first, tile)
                masks = [allowed_keys(col_ref[m, here], row_ref[h, m], first, h * length) for h in range(spans)]
                block = q_ref[m, here]
                grad_block = ga_ref[here]
                result = jnp.zeros((tile, cols), F32)
                for head in range(heads):
                    query = one_head(block, head)
                    grad = one_head(grad_block, head)
                    level = lse_ref[m, head, here][:, :1]
                    prob = [
                        jnp.where(masks[h], jnp.exp(dot_nt(query, k_ref[h, m]) * scale - level), 0.0)
                        for h in range(spans)
                    ]
                    grad_prob = [dot_nt(grad, v_ref[h, m]) for h in range(spans)]
                    mean = sum([jnp.sum(p * g, axis=-1, keepdims=True) for p, g in zip(prob, grad_prob)])
                    grad_scores = [(p * (g - mean)).astype(BF) for p, g in zip(prob, grad_prob)]
                    for h in range(spans):
                        dv_acc[h] += dot_tn(prob[h].astype(BF), grad)
                        dk_acc[h] += dot_tn(grad_scores[h], query)
                    mixed = sum([dot_nn(grad_scores[h], k_ref[h, m]) for h in range(spans)])
                    result = result + one_head(mixed, head)
                dq_ref[m, here] = (result * scale).astype(BF)

            for h in range(spans):
                dk_ref[h, m] = (dk_acc[h] * scale).astype(BF)
                dv_ref[h, m] = dv_acc[h].astype(BF)
                back = dot_nt(dk_ref[h, m], wk_ref[...]) + dot_nt(dv_ref[h, m], wv_ref[...])
                if h == 0:
                    back = back + dot_nt(dq_ref[m], wq_ref[...])
                p_ref[h, m] = back.astype(BF)

    span = jax.ShapeDtypeStruct((spans, streams, length, cols), BF)
    return pl.pallas_call(
        kernel,
        name="attend_back",
        out_shape=(
            jax.ShapeDtypeStruct((streams, length, cols), BF),
            span,
            span,
            jax.ShapeDtypeStruct((spans, streams, length, width), BF),
        ),
        in_specs=in_vmem(11),
        out_specs=tuple(in_vmem(4)),
        scratch_shapes=[
            pltpu.VMEM((length, cols), BF),
            pltpu.VMEM((spans, length, cols), F32),
            pltpu.VMEM((spans, length, cols), F32),
        ],
        compiler_params=params(),
    )(q, k, v, lse, grad_out, row_ids, col_ids, wq, wk, wv, wo)


def tail(
    grad_stu, filter_proj, lag_proj, conv, lag_stack, lag_masks, row_ids, ext_ids, base, x, gain, grad_one, gains, seq_count
):
    count, length_all, width = conv.shape
    streams, _, quarter, _ = x.shape
    length = length_all // streams
    lag_order, channels = lag_proj.shape[:2]
    wide = base.shape[2]
    blocks = length // LANES
    hops = seq_count - 1
    chunks = count + 1
    steps = seq_count * streams
    rows = width // seq_count
    gain_rows = 8

    def kernel(
        gs_ref, fp_ref, lp_ref, conv_ref, lag_ref, mask_ref, row_ref, ext_ref, base_ref, x_ref, gain_ref, one_ref, gains_ref,
        out, filter_out, lag_out, gain_out,
        strip, mask, cols, left, acc, terms, grad_conv, grads, lag_ext, total, grad_acc, gather_sem,
        gain_own, gain_near, gain_sum, gain_far, near_sem, far_sem, *scratch,
    ):
        s, t, y, c, core, far = place()
        p = lax.axis_index("dp")
        rs_scratch, gr_scratch = scratch[:6], scratch[6:]
        greet(seq_count, hops, wide=True, gains=True)

        def source(k):
            return grads.at[k]

        def result(k):
            return filter_out.at[k] if k < count else lag_out

        gr = GradReduce(seq_count, source, result, gr_scratch)
        rs = ReduceScatter(seq_count, hops, streams, lambda h, m: terms.at[h, m], rs_scratch)
        ag = AllGather(seq_count, 0, streams, out, gather_sem)

        early = min(2, count)

        @pl.loop(0, count)
        def _(k):
            grads[k] = dot_tn(conv_ref[k], gs_ref[...]).astype(BF)
            gr.start(k)
            product = dot_nt(gs_ref[...], fp_ref[k]).astype(BF)
            for m in range(streams):
                here = pl.ds(pl.multiple_of(k * length, LANES), length)
                grad_conv[m, here] = product[m * length : (m + 1) * length]

            @pl.when(k >= count - early)
            def _():
                gr.spread(k - (count - early))

        grads[count] = jnp.zeros_like(grads.at[count])
        for i in range(lag_order):
            grads[count, :, i * channels : (i + 1) * channels] = dot_tn(gs_ref[...], lag_ref[i]).astype(BF)
        gr.start(count)
        for m in range(streams):
            lag_ext[m] = jnp.zeros_like(lag_ext.at[m])
            for i in range(lag_order):
                term = dot_nt(gs_ref[m * length : (m + 1) * length], lp_ref[i]) * mask_ref[i, m]
                lag_ext[m, 7 - i : 7 - i + length] += term
        strips(base_ref, strip)
        turned = jnp.transpose(ext_ref[...].astype(F32))
        for j in range(steps):
            cols[j] = turned[:, j : j + 1]
        mine = pl.ds(pl.multiple_of(t * channels, LANES), channels)
        spread_at = {}
        collect_at = {}
        for k in range(early, chunks):
            if 2 * (k - early) < steps:
                spread_at[2 * (k - early)] = k
        for k in range(chunks):
            if 2 * k + 3 < steps and k < early + len(spread_at):
                collect_at[2 * k + 3] = k

        def step_of(i):
            return seq_count - 1 - i // streams, i - i // streams * streams

        @pl.loop(0, steps)
        def _(i):
            h, m = step_of(i)

            @pl.when(h <= s)
            def _():
                mask[...] = jnp.where(cols[h * streams + m] == row_ref[m].astype(F32), 1.0, 0.0).astype(BF)
                for k in range(count):
                    for a in range(blocks):
                        start = pl.multiple_of(LANES * (blocks * h + blocks - 1 - a), LANES)
                        down = slice(a * LANES, (a + 1) * LANES)
                        left[down, k * length : (k + 1) * length] = strip[k, :, pl.ds(start, length)] * mask[down]
                acc[...] = jnp.dot(left[...], grad_conv[m], preferred_element_type=F32)

                @pl.when(h == 0)
                def _():
                    acc[:, mine] += lag_ext[m, 8:]

                @pl.when(h == 1)
                def _():
                    acc[length - 8 :, mine] += lag_ext[m, :8]

                for quarter_y in range(2):
                    for quarter_c in range(2):
                        first = (2 * quarter_y + quarter_c) * quarter
                        terms[h, m, quarter_y, quarter_c] = acc[first : first + quarter].astype(BF)
                rs.start(h, m)

            @pl.when(i >= 1)
            def _():
                rs.middle(*step_of(i - 1))

            @pl.when((i >= 2) & (i < steps - streams + 2))
            def _():
                rs.hop(*step_of(i - 2))

            for step, k in spread_at.items():
                pl.when(i == step)(functools.partial(gr.spread, k))
            for step, k in collect_at.items():
                pl.when(i == step)(functools.partial(gr.collect, k, grad_acc))

        rs.middle(0, streams - 1)
        for k in range(early + len(spread_at), chunks):
            gr.spread(k)
        gain_own[...] = jnp.zeros_like(gain_own)
        for m in range(streams):
            rs.total(m, total)
            grad_in, gain_grad = norm_back(x_ref[m, t].astype(F32), gain_ref[...], total[...])
            out[0, m, t] = (one_ref[m] + grad_in).astype(BF)
            ag.start(m)
            gain_own[0:1] += gain_grad
        gain_own[1:3] = gains_ref[...]
        gain_near[t] = gain_own[...]

        def near_copy(j, slot):
            return remote(gain_own, gain_near.at[slot], near_sem.at[0, j], near_sem.at[1, slot], {"tensor": j})

        for j in range(4):
            pl.when(t != j)(lambda: near_copy(j, t).start())
        for m in range(streams):
            ag.pass_on(0, m)
        for k in range(len(collect_at), chunks):
            gr.collect(k, grad_acc)
        for j in range(4):
            pl.when(t != j)(lambda: near_copy(j, j).wait_recv())
        gain_sum[...] = gain_near[0] + gain_near[1] + gain_near[2] + gain_near[3]
        me = p * seq_count + s

        def far_copy(j, slot):
            d, q = j // seq_count, j % seq_count
            return remote(
                gain_sum.at[:, q * rows : (q + 1) * rows], gain_far.at[slot], far_sem.at[0, j], far_sem.at[1, slot],
                {"dp": d, "seq": q},
            )

        gain_far[me] = gain_sum[:, pl.ds(pl.multiple_of(s * rows, LANES), rows)]
        for j in range(2 * seq_count):
            pl.when(me != j)(lambda: far_copy(j, me).start())
        for m in range(streams):
            ag.finish(0, m)
        for k in range(chunks):
            gr.finish(k)
        for j in range(2 * seq_count):
            pl.when(me != j)(lambda: far_copy(j, j).wait_recv())
        gain_out[...] = functools.reduce(jnp.add, [gain_far[j] for j in range(2 * seq_count)])
        for j in range(4):
            pl.when(t != j)(lambda: near_copy(j, t).wait_send())
        for j in range(2 * seq_count):
            pl.when(me != j)(lambda: far_copy(j, me).wait_send())
        for k in range(chunks):
            gr.drain(k)
        rs.drain()
        ag.drain()

    return pl.pallas_call(
        kernel,
        name="tail",
        out_shape=(
            jax.ShapeDtypeStruct((1, streams, 4, quarter, width), BF),
            jax.ShapeDtypeStruct((count, rows, width), F32),
            jax.ShapeDtypeStruct((rows, width), F32),
            jax.ShapeDtypeStruct((gain_rows, rows), F32),
        ),
        in_specs=in_vmem(13),
        out_specs=tuple(in_vmem(4)),
        scratch_shapes=[
            pltpu.VMEM((count, LANES, wide), BF),
            pltpu.VMEM((length, length), BF),
            pltpu.VMEM((steps, length, 1), F32),
            pltpu.VMEM((length, count * length), BF),
            pltpu.VMEM((length, width), F32),
            pltpu.VMEM((seq_count, streams, 2, 2, quarter, width), BF),
            pltpu.VMEM((streams, count * length, width), BF),
            pltpu.VMEM((chunks, width, width), BF),
            pltpu.VMEM((streams, length + 8, channels), F32),
            pltpu.VMEM((quarter, width), F32),
            pltpu.VMEM((rows, width // 2), F32),
            AllGather.scratch(0, streams)[0],
            pltpu.VMEM((gain_rows, width), F32),
            pltpu.VMEM((4, gain_rows, width), F32),
            pltpu.VMEM((gain_rows, width), F32),
            pltpu.VMEM((2 * seq_count, gain_rows, rows), F32),
            pltpu.SemaphoreType.DMA((2, 4)),
            pltpu.SemaphoreType.DMA((2, 2 * seq_count)),
        ]
        + ReduceScatter.scratch(hops, streams, quarter, width)
        + GradReduce.scratch(seq_count, chunks, width, width),
        compiler_params=params(7),
    )(
        grad_stu, filter_proj, lag_proj, conv, lag_stack, lag_masks, row_ids, ext_ids, base, x, gain, grad_one, gains
    )


def gated_unit(gate_pre, up_pre):
    return jax.nn.gelu(gate_pre, approximate=True) * up_pre


def local(
    seq_count,
    tokens,
    document_index,
    filters,
    stu_gain,
    filter_proj,
    lag_proj,
    attention_gain,
    query_weight,
    key_weight,
    value_weight,
    output_weight,
    feed_gain,
    gate_weight,
    up_weight,
    down_weight,
    cotangent,
):
    streams, _, length, width = tokens.shape
    row_len = length * seq_count
    quarter = length // 4
    lag_order, channels = lag_proj.shape[:2]
    count = filters.shape[0]
    hops = WINDOW // length
    tensor_place = lax.axis_index("tensor")
    chan_start = tensor_place * channels

    def split(a):
        return a.reshape(a.shape[:-2] + (2, 2, quarter, width))

    def quarters(a):
        return a.reshape(a.shape[:-2] + (4, quarter, width))

    def whole(a):
        return a.reshape(a.shape[:-3] + (length, width))

    def row(gain):
        return gain.reshape(1, width)

    x = tokens[:, 0]
    grad_three = cotangent[:, 0]
    ids = document_index[:, 0]
    inputs = norm_of(x.astype(F32), stu_gain).astype(BF)
    id_tile = ids.reshape(streams * length // LANES, LANES)
    rows_ext, id_ext = gather_rows(quarters(inputs), id_tile, seq_count)
    rows_ext = whole(rows_ext)
    id_ext = id_ext.reshape(seq_count, streams, length)
    id_rows = id_ext[:, :, None, :]
    id_cols = id_ext[:, :, :, None]

    pad = jnp.zeros((count, 4 * LANES), filters.dtype)
    ahead = row_len - LANES
    base = jnp.concatenate(
        [
            jnp.flip(filters[:, : ahead + 1], axis=1),
            pad[:, : 4 * LANES],
            jnp.flip(filters[:, ahead + 1 :], axis=1),
        ],
        axis=1,
    ).astype(F32)[:, None]
    base_back = jnp.concatenate(
        [pad[:, : length - LANES], filters, pad[:, :LANES]], axis=1
    ).astype(F32)[:, None]
    conv = convolve(rows_ext, id_rows, id_cols[0], base, seq_count)

    chan_rows = lax.dynamic_slice_in_dim(rows_ext[:2], chan_start, channels, 3)
    joined = jnp.concatenate([chan_rows[1][:, length - lag_order :], chan_rows[0]], axis=1)
    joined_ids = jnp.concatenate([id_ext[1][:, length - lag_order :], ids], axis=1)
    masks = []
    lagged = []
    for step in range(1, lag_order + 1):
        low = lag_order - step
        masks.append((joined_ids[:, low : low + length] == ids)[:, :, None])
        lagged.append(jnp.where(masks[-1], joined[:, low : low + length], jnp.zeros((), BF)))
    lag_stack = jnp.stack(lagged)

    mixed = jnp.einsum("kmtd,kde->mte", conv, filter_proj, preferred_element_type=F32)
    mixed = mixed + jnp.einsum("imtc,ice->mte", lag_stack, lag_proj, preferred_element_type=F32)

    state = jax.ShapeDtypeStruct((streams, quarter, width), F32)
    gain_state = jax.ShapeDtypeStruct((1, width), F32)

    def finish_one(m, total, others, extra):
        x_ref, gain_ref = others
        hidden = x_ref[m, place()[1]].astype(F32) + total
        extra[0][m] = hidden
        return norm_of(hidden, gain_ref[...]).astype(BF)

    attn_ext, hidden_one = exchange(
        "exchange_one", 2, seq_count, [split(mixed.astype(BF))[None]], [quarters(x), row(attention_gain)], 0, hops,
        finish_one, [state],
    )
    attn_ext = whole(attn_ext)

    q, k, v, attended, lse, out_part = attend(
        attn_ext, id_rows[: hops + 1], id_cols[0], query_weight, key_weight, value_weight, output_weight
    )

    def finish_two(m, total, others, extra):
        hidden_ref, gain_ref = others
        hidden = hidden_ref[m] + total
        extra[0][m] = hidden
        return norm_of(hidden, gain_ref[...]).astype(BF)

    feed_in, hidden_two = exchange(
        "exchange_two", 3, seq_count, [split(out_part)[None]], [hidden_one, row(feed_gain)], 0, 0, finish_two, [state]
    )
    feed_in = whole(feed_in)[0].reshape(streams * length, width)
    flat_three = grad_three.reshape(streams * length, width)

    gate_pre = dot_nn(feed_in, gate_weight)
    up_pre = dot_nn(feed_in, up_weight)
    grad_inner = dot_nt(flat_three, down_weight)
    unit, pull = jax.vjp(gated_unit, gate_pre, up_pre)
    inner = unit.astype(BF)
    grad_gate, grad_up = pull(grad_inner)
    grad_gate = grad_gate.astype(BF)
    grad_up = grad_up.astype(BF)
    layer_part = dot_nn(inner, down_weight).astype(BF)
    feed_part = (dot_nt(grad_gate, gate_weight) + dot_nt(grad_up, up_weight)).astype(BF)

    def finish_three(m, total, others, extra):
        hidden_ref, gain_ref, cot_ref = others
        if m >= streams:
            return (hidden_ref[m - streams] + total).astype(BF)
        grad_in, gain_grad = norm_back(hidden_ref[m], gain_ref[...], total)
        grad_two = cot_ref[m, place()[1]].astype(F32) + grad_in
        extra[0][m] = grad_two
        extra[1][...] = gain_grad if m == 0 else extra[1][...] + gain_grad
        return grad_two.astype(BF)

    fused = width // seq_count % LANES == 0
    feed_grads = jnp.stack(
        [
            dot_tn(feed_in, grad_gate).astype(BF),
            dot_tn(feed_in, grad_up).astype(BF),
            dot_tn(flat_three, inner).astype(BF),
        ]
    )
    shape = (1, streams, length, width)
    results = exchange(
        "exchange_three", 4, seq_count, [split(feed_part.reshape(shape)), split(layer_part.reshape(shape))],
        [hidden_two, row(feed_gain), quarters(grad_three)], 0, 0, finish_three, [state, gain_state],
        feed_grads if fused else None,
    )
    both, grad_two, feed_gain_grad = results[:3]
    if fused:
        feed_grads = results[3]
    both = whole(both)[0]
    grad_att_out = both[:streams]
    layer_output = both[streams:]

    dq, dk, dv, attn_part = attend_back(
        q, k, v, lse, grad_att_out, id_rows[: hops + 1], id_cols[0], query_weight, key_weight, value_weight, output_weight
    )

    tokens_flat = streams * length
    go = grad_att_out.reshape(tokens_flat, width)
    attn_grads = jnp.concatenate(
        [
            dot_tn(attn_ext[0].reshape(tokens_flat, width), dq.reshape(tokens_flat, -1)).astype(BF),
            dot_tn(attn_ext.reshape(-1, width), dk.reshape(-1, dk.shape[-1])).astype(BF),
            dot_tn(attn_ext.reshape(-1, width), dv.reshape(-1, dv.shape[-1])).astype(BF),
            dot_tn(go, attended.reshape(tokens_flat, -1)).astype(BF),
        ],
        axis=1,
    )

    def finish_four(m, total, others, extra):
        hidden_ref, gain_ref, grad_ref = others
        grad_in, gain_grad = norm_back(hidden_ref[m], gain_ref[...], total)
        grad_one = grad_ref[m] + grad_in
        extra[0][m] = grad_one
        extra[1][...] = gain_grad if m == 0 else extra[1][...] + gain_grad
        return grad_one.astype(BF)

    results = exchange(
        "exchange_four", 5, seq_count, [split(attn_part)], [hidden_one, row(attention_gain), grad_two], hops, 0,
        finish_four, [state, gain_state], attn_grads[None] if fused else None,
    )
    grad_stu, grad_one, attn_gain_grad = results[:3]
    grad_stu = whole(grad_stu)[0]
    lag_masks = jnp.stack(masks).astype(F32)
    if fused:
        attn_grads = results[3][0]
        input_gradient, filter_grad, lag_grad, gains = tail(
            grad_stu.reshape(tokens_flat, width), filter_proj, lag_proj, conv.reshape(count, tokens_flat, width),
            lag_stack.reshape(lag_order, tokens_flat, channels), lag_masks, id_rows[0],
            id_ext.reshape(seq_count * streams, length), base_back,
            quarters(x), row(stu_gain), grad_one, jnp.concatenate([attn_gain_grad, feed_gain_grad], axis=0), seq_count,
        )
        input_gradient = whole(input_gradient)[0]
    else:
        grad_conv = jnp.einsum("mte,kde->kmtd", grad_stu, filter_proj, preferred_element_type=F32).astype(BF)
        grad_lagged = jnp.einsum("mte,ice->imtc", grad_stu, lag_proj, preferred_element_type=F32)
        ext_grad = jnp.zeros((streams, 8 + length, channels), F32)
        for step in range(1, lag_order + 1):
            term = jnp.where(masks[step - 1], grad_lagged[step - 1], 0.0)
            ext_grad = ext_grad + jnp.pad(term, ((0, 0), (8 - step, step), (0, 0)))
        terms = convolve_back(
            grad_conv, id_rows[0], id_cols, base_back, ext_grad[:, 8:], ext_grad[:, :8], seq_count
        )

        def finish_five(m, total, others, extra):
            x_ref, gain_ref, grad_ref = others
            grad_in, gain_grad = norm_back(x_ref[m, place()[1]].astype(F32), gain_ref[...], total)
            extra[0][...] = gain_grad if m == 0 else extra[0][...] + gain_grad
            return (grad_ref[m] + grad_in).astype(BF)

        input_gradient, stu_gain_grad = exchange(
            "exchange_five", 6, seq_count, [split(terms)], [quarters(x), row(stu_gain), grad_one], seq_count - 1, 0,
            finish_five, [gain_state],
        )
        input_gradient = whole(input_gradient)[0]
        stu = grad_stu.reshape(tokens_flat, width)
        filter_part = jnp.einsum("kmtd,mte->kde", conv, grad_stu, preferred_element_type=F32).astype(BF)
        lag_part = jnp.concatenate(
            [dot_tn(stu, lag_stack[i].reshape(tokens_flat, channels)).astype(BF) for i in range(lag_order)], axis=1
        )
        feed_grads = lax.psum(
            lax.psum_scatter(feed_grads, "seq", scatter_dimension=1, tiled=True), "dp"
        ).astype(F32)
        attn_grads = lax.psum(lax.psum_scatter(attn_grads, "seq", scatter_dimension=0, tiled=True), "dp").astype(F32)
        filter_grad = lax.psum(
            lax.psum_scatter(filter_part, "seq", scatter_dimension=1, tiled=True), "dp"
        ).astype(F32)
        lag_grad = lax.psum(lax.psum_scatter(lag_part, "seq", scatter_dimension=0, tiled=True), "dp").astype(F32)
        gains = jnp.concatenate([stu_gain_grad, attn_gain_grad, feed_gain_grad], axis=0)
        gains = lax.psum(gains, ("dp", "seq", "tensor"))
        gain_width = width // seq_count
        gains = lax.dynamic_slice_in_dim(gains, lax.axis_index("seq") * gain_width, gain_width, 1)

    cols = query_weight.shape[1]
    gate_grad, up_grad, down_grad = feed_grads
    query_grad, key_grad, value_grad, output_grad = jnp.split(attn_grads, [cols, 2 * cols, 3 * cols], axis=1)
    lag_grad = lag_grad[:, : lag_order * channels].T.reshape(lag_order, channels, -1)
    return (
        layer_output[:, None],
        input_gradient[:, None],
        gains[0],
        filter_grad,
        lag_grad,
        gains[1],
        query_grad,
        key_grad,
        value_grad,
        output_grad.T,
        gains[2],
        gate_grad,
        up_grad,
        down_grad.T,
    )


def solution(mesh):
    return jax.shard_map(
        functools.partial(local, mesh.shape["seq"]),
        mesh=mesh,
        in_specs=(
            P(None, "dp", "seq", None),
            P(None, "dp", "seq"),
            P("tensor", None),
            P(),
            P("tensor", None, None),
            P(None, "tensor", None),
            P(),
            P(None, "tensor"),
            P(None, "tensor"),
            P(None, "tensor"),
            P("tensor", None),
            P(),
            P(None, "tensor"),
            P(None, "tensor"),
            P("tensor", None),
            P(None, "dp", "seq", None),
        ),
        out_specs=(
            P(None, "dp", "seq", None),
            P(None, "dp", "seq", None),
            P("seq"),
            P("tensor", "seq", None),
            P(None, "tensor", "seq"),
            P("seq"),
            P("seq", "tensor"),
            P("seq", "tensor"),
            P("seq", "tensor"),
            P("tensor", "seq"),
            P("seq"),
            P("seq", "tensor"),
            P("seq", "tensor"),
            P("tensor", "seq"),
        ),
        check_vma=False,
    )
```

```python
import functools

import jax
import jax.numpy as jnp
from jax import lax
from jax.experimental import pallas as pl
from jax.experimental.pallas import tpu as pltpu
from jax.sharding import PartitionSpec as P

HD = 64
WINDOW = 1024
EPSILON = 1e-05
LANES = 128
NEGATIVE = -1e30
MESH = pl.DeviceIdType.MESH
BF = jnp.bfloat16
F32 = jnp.float32
VMEM_LIMIT = 60 * 1024 * 1024


def place():
    s = lax.axis_index("seq")
    t = lax.axis_index("tensor")
    y = t // 2
    c = t - 2 * y
    return s, t, y, c, t + 1 - 2 * c, t + 2 - 4 * y


def when(condition, action):
    if condition is True:
        action()
    else:
        pl.when(condition)(action)


def remote(src, dst, send_sem, recv_sem, device):
    return pltpu.make_async_remote_copy(
        src_ref=src, dst_ref=dst, send_sem=send_sem, recv_sem=recv_sem, device_id=device, device_id_type=MESH
    )


def greet(seq_count, hops, wide=False, gains=False):
    s, t, y, c, core, far = place()
    barrier = pltpu.get_barrier_semaphore()

    def signal(device):
        pl.semaphore_signal(barrier, inc=1, device_id=device, device_id_type=MESH)

    signal({"tensor": core})
    signal({"tensor": far})
    if gains:
        signal({"tensor": 3 - t})
    if wide:
        p = lax.axis_index("dp")
        signal({"dp": 1 - p})
        for j in range(seq_count):

            @pl.when(s != j)
            def _():
                signal({"seq": j})
                if gains:
                    signal({"dp": 1 - p, "seq": j})

        peers = 2 + gains + 1 + (seq_count - 1) * (1 + gains)
    else:
        for h in range(1, hops + 1):
            for there, peer in ((s - h >= 0, s - h), (s + h < seq_count, s + h)):

                @pl.when(there)
                def _():
                    signal({"seq": peer})

        peers = 2 + jnp.minimum(s, hops) + jnp.minimum(seq_count - 1 - s, hops)
    pl.semaphore_wait(barrier, peers)


class ReduceScatter:
    def __init__(self, seq_count, hops, streams, part, scratch):
        self.seq_count, self.hops, self.streams, self.part = seq_count, hops, streams, part
        self.near, self.half, self.over, self.hop_out, self.hop_in, self.sem = scratch

    @staticmethod
    def scratch(hops, streams, rows, width):
        quarter = (hops + 1, streams, rows, width)
        return [
            pltpu.VMEM((hops + 1, streams, 2, rows, width), BF),
            pltpu.VMEM(quarter, BF),
            pltpu.VMEM(quarter, BF),
            pltpu.VMEM(quarter, BF),
            pltpu.VMEM(quarter, BF),
            pltpu.SemaphoreType.DMA((6, hops + 1, streams)),
        ]

    def to_core(self, h, m):
        s, t, y, c, core, far = place()
        return remote(
            self.part(h, m).at[:, 1 - c], self.near.at[h, m], self.sem.at[0, h, m], self.sem.at[1, h, m], {"tensor": core}
        )

    def to_far(self, h, m):
        s, t, y, c, core, far = place()
        return remote(self.half.at[h, m], self.over.at[h, m], self.sem.at[2, h, m], self.sem.at[3, h, m], {"tensor": far})

    def to_hop(self, h, m, peer):
        return remote(
            self.hop_out.at[h, m], self.hop_in.at[h, m], self.sem.at[4, h, m], self.sem.at[5, h, m], {"seq": peer}
        )

    def there(self, h):
        return True if isinstance(h, int) and h == 0 else lax.axis_index("seq") - h >= 0

    def order(self):
        return [(h, m) for h in range(self.hops, -1, -1) for m in range(self.streams)]

    def start(self, h, m):
        when(self.there(h), lambda: self.to_core(h, m).start())

    def middle(self, h, m):
        s, t, y, c, core, far = place()

        def act():
            self.to_core(h, m).wait_recv()
            mine = self.part(h, m)[1 - y, c].astype(F32) + self.near[h, m, 1 - y].astype(F32)
            self.half[h, m] = mine.astype(BF)
            self.to_far(h, m).start()

        when(self.there(h), act)

    def own(self, h, m):
        s, t, y, c, core, far = place()
        self.to_far(h, m).wait_recv()
        return (
            self.part(h, m)[y, c].astype(F32) + self.near[h, m, y].astype(F32) + self.over[h, m].astype(F32)
        )

    def hop(self, h, m):
        def act():
            self.hop_out[h, m] = self.own(h, m).astype(BF)
            self.to_hop(h, m, lax.axis_index("seq") - h).start()

        when(self.there(h), act)

    def total(self, m, acc):
        acc[...] = self.own(0, m)
        for h in range(1, self.hops + 1):
            s = lax.axis_index("seq")

            @pl.when(s + h < self.seq_count)
            def _():
                self.to_hop(h, m, s + h).wait_recv()
                acc[...] += self.hop_in[h, m].astype(F32)

    def drain(self):
        for h, m in self.order():

            def act():
                self.to_core(h, m).wait_send()
                self.to_far(h, m).wait_send()
                if h:
                    self.to_hop(h, m, lax.axis_index("seq") - h).wait_send()

            when(self.there(h), act)


class AllGather:
    def __init__(self, seq_count, hops, streams, out, sem, first=0):
        self.seq_count, self.hops, self.streams, self.out, self.sem, self.first = seq_count, hops, streams, out, sem, first

    @staticmethod
    def scratch(hops, streams):
        return [pltpu.SemaphoreType.DMA((8, hops + 1, streams))]

    def there(self, h):
        return True if h == 0 else lax.axis_index("seq") - h >= 0

    def copy(self, kind, h, m, quarter, device, to=None):
        source = self.out.at[0 if kind == 0 else h, m, quarter]
        return remote(source, self.out.at[h, m, quarter], self.sem.at[2 * kind, h, m], self.sem.at[2 * kind + 1, h, m], device)

    def to_hop(self, h, m, peer):
        return self.copy(0, h, m, place()[1], {"seq": peer})

    def spread(self, h, m):
        s, t, y, c, core, far = place()
        self.copy(1, h, m, t, {"tensor": far}).start()
        self.copy(2, h, m, t, {"tensor": core}).start()

    def start(self, m):
        s, t, y, c, core, far = place()
        for h in range(1, self.hops + 1):

            @pl.when(s + h < self.seq_count)
            def _():
                self.to_hop(h, m, s + h).start()

        if self.first == 0:
            self.spread(0, m)

    def arrive(self, h, m):
        @pl.when(self.there(h))
        def _():
            self.to_hop(h, m, lax.axis_index("seq") - h).wait_recv()
            self.spread(h, m)

    def pass_on(self, h, m):
        s, t, y, c, core, far = place()

        def act():
            self.copy(1, h, m, far, {"tensor": far}).wait_recv()
            self.copy(3, h, m, far, {"tensor": core}).start()

        when(self.there(h), act)

    def finish(self, h, m):
        s, t, y, c, core, far = place()

        def act():
            self.copy(2, h, m, core, {"tensor": core}).wait_recv()
            self.copy(3, h, m, 3 - t, {"tensor": core}).wait_recv()

        when(self.there(h), act)

    def clear(self, h, m):
        @pl.when(lax.axis_index("seq") - h < 0)
        def _():
            self.out[h, m] = jnp.zeros(self.out.shape[2:], self.out.dtype)

    def drain(self):
        s, t, y, c, core, far = place()
        for m in range(self.streams):
            for h in range(1, self.hops + 1):

                @pl.when(s + h < self.seq_count)
                def _():
                    self.to_hop(h, m, s + h).wait_send()

            for h in range(self.first, self.hops + 1):

                def act():
                    self.copy(1, h, m, t, {"tensor": far}).wait_send()
                    self.copy(2, h, m, t, {"tensor": core}).wait_send()
                    self.copy(3, h, m, far, {"tensor": core}).wait_send()

                when(self.there(h), act)


class GradReduce:
    def __init__(self, seq_count, source, result, scratch):
        self.seq_count, self.source, self.result = seq_count, source, result
        self.x_in, self.z_out, self.z_in, self.back_out, self.back_in, self.x_sem, self.z_sem, self.back_sem = scratch
        self.half = self.x_in.shape[2]
        self.rows = self.back_out.shape[1]

    @staticmethod
    def scratch(seq_count, chunks, depth, width):
        rows, half = depth // seq_count, width // 2
        return [
            pltpu.VMEM((chunks, depth, half), BF),
            pltpu.VMEM((chunks, depth, half), BF),
            pltpu.VMEM((chunks, seq_count, rows, half), BF),
            pltpu.VMEM((chunks, rows, half), BF),
            pltpu.VMEM((chunks, rows, half), BF),
            pltpu.SemaphoreType.DMA((2, chunks)),
            pltpu.SemaphoreType.DMA((2, chunks, seq_count)),
            pltpu.SemaphoreType.DMA((2, chunks)),
        ]

    def columns(self, p):
        return pl.ds(pl.multiple_of(p * self.half, LANES), self.half)

    def block(self, j):
        return pl.ds(pl.multiple_of(j * self.rows, 16), self.rows)

    def over(self, c):
        p = lax.axis_index("dp")
        return remote(
            self.source(c).at[:, self.columns(1 - p)], self.x_in.at[c], self.x_sem.at[0, c], self.x_sem.at[1, c], {"dp": 1 - p}
        )

    def row_copy(self, c, j, slot):
        return remote(
            self.z_out.at[c, self.block(j)], self.z_in.at[c, slot], self.z_sem.at[0, c, j], self.z_sem.at[1, c, slot], {"seq": j}
        )

    def back(self, c):
        p = lax.axis_index("dp")
        return remote(
            self.back_out.at[c], self.back_in.at[c], self.back_sem.at[0, c], self.back_sem.at[1, c], {"dp": 1 - p}
        )

    def others(self, action):
        for j in range(self.seq_count):
            pl.when(lax.axis_index("seq") != j)(functools.partial(action, j))

    def start(self, c):
        self.over(c).start()

    def spread(self, c):
        s, p = lax.axis_index("seq"), lax.axis_index("dp")
        self.over(c).wait_recv()
        mine = self.source(c)[:, self.columns(p)].astype(F32) + self.x_in[c].astype(F32)
        self.z_out[c] = mine.astype(BF)
        self.others(lambda j: self.row_copy(c, j, s).start())

    def collect(self, c, acc):
        s, p = lax.axis_index("seq"), lax.axis_index("dp")
        here = self.block(s)
        acc[...] = self.source(c)[here, self.columns(p)].astype(F32) + self.x_in[c, here].astype(F32)

        def add(j):
            self.row_copy(c, j, j).wait_recv()
            acc[...] += self.z_in[c, j].astype(F32)

        self.others(add)
        self.back_out[c] = acc[...].astype(BF)
        self.back(c).start()

    def finish(self, c):
        p = lax.axis_index("dp")
        self.back(c).wait_recv()
        self.result(c)[:, self.columns(p)] = self.back_out[c].astype(F32)
        self.result(c)[:, self.columns(1 - p)] = self.back_in[c].astype(F32)

    def drain(self, c):
        self.over(c).wait_send()
        self.others(lambda j: self.row_copy(c, j, lax.axis_index("seq")).wait_send())
        self.back(c).wait_send()


def params(cid=None):
    if cid is None:
        return pltpu.CompilerParams(vmem_limit_bytes=VMEM_LIMIT)
    return pltpu.CompilerParams(vmem_limit_bytes=VMEM_LIMIT, collective_id=cid, has_side_effects=True)


def in_vmem(count):
    return [pl.BlockSpec(memory_space=pltpu.VMEM)] * count


def gather_rows(inputs, ids, seq_count):
    streams, quarters, rows, width = inputs.shape
    hops = seq_count - 1

    def kernel(x_ref, id_ref, out, out_ids, sem, id_sem):
        s, t, y, c, core, far = place()
        greet(seq_count, hops)
        out[0] = x_ref[...]
        out_ids[0] = id_ref[...]
        ag = AllGather(seq_count, hops, streams, out, sem, first=1)

        def id_copy(h, peer):
            return remote(id_ref, out_ids.at[h], id_sem.at[0, h], id_sem.at[1, h], {"seq": peer})

        for h in range(1, hops + 1):

            @pl.when(s + h < seq_count)
            def _():
                id_copy(h, s + h).start()

        ag.to_hop = lambda h, m, peer: remote(
            x_ref.at[m, t], out.at[h, m, t], sem.at[0, h, m], sem.at[1, h, m], {"seq": peer}
        )
        for m in range(streams):
            ag.start(m)
        for h in range(1, hops + 1):
            for m in range(streams):
                ag.clear(h, m)

            @pl.when(s - h < 0)
            def _():
                out_ids[h] = jnp.full(out_ids.shape[1:], -1, jnp.int32)

        for m in range(streams):
            for h in range(1, hops + 1):
                ag.arrive(h, m)
        for m in range(streams):
            for h in range(1, hops + 1):
                ag.pass_on(h, m)
        for h in range(1, hops + 1):
            for m in range(streams):
                ag.finish(h, m)

            @pl.when(s - h >= 0)
            def _():
                id_copy(h, s - h).wait_recv()

            @pl.when(s + h < seq_count)
            def _():
                id_copy(h, s + h).wait_send()

        ag.drain()

    return pl.pallas_call(
        kernel,
        name="gather_rows",
        out_shape=(
            jax.ShapeDtypeStruct((seq_count,) + inputs.shape, inputs.dtype),
            jax.ShapeDtypeStruct((seq_count,) + ids.shape, jnp.int32),
        ),
        in_specs=in_vmem(2),
        out_specs=tuple(in_vmem(2)),
        scratch_shapes=AllGather.scratch(hops, streams) + [pltpu.SemaphoreType.DMA((2, seq_count))],
        compiler_params=params(1),
    )(inputs, ids)


def exchange(name, cid, seq_count, parts, others, reduce_hops, gather_hops, finish, extra):
    per_part = parts[0].shape[1]
    rows, width = parts[0].shape[4:]
    streams = per_part * len(parts)
    hops = max(reduce_hops, gather_hops)

    def kernel(*refs):
        refs = list(refs)
        part_refs = [refs.pop(0) for _ in parts]
        other_refs = [refs.pop(0) for _ in others]
        out = refs.pop(0)
        extra_refs = [refs.pop(0) for _ in extra]
        acc = refs.pop(0)
        gather_sem = refs.pop(0)
        s, t, y, c, core, far = place()
        greet(seq_count, hops)
        rs = ReduceScatter(
            seq_count, reduce_hops, streams, lambda h, m: part_refs[m // per_part].at[h, m % per_part], refs
        )
        ag = AllGather(seq_count, gather_hops, streams, out, gather_sem)
        for h, m in rs.order():
            rs.start(h, m)
        for h in range(1, gather_hops + 1):
            for m in range(streams):
                ag.clear(h, m)
        for h, m in rs.order():
            rs.middle(h, m)
        for h, m in rs.order():
            if h:
                rs.hop(h, m)
        for m in range(streams):
            rs.total(m, acc)
            out[0, m, t] = finish(m, acc[...], other_refs, extra_refs)
            ag.start(m)
        for m in range(streams):
            ag.pass_on(0, m)
            for h in range(1, gather_hops + 1):
                ag.arrive(h, m)
        for m in range(streams):
            for h in range(1, gather_hops + 1):
                ag.pass_on(h, m)
        for h in range(gather_hops + 1):
            for m in range(streams):
                ag.finish(h, m)
        rs.drain()
        ag.drain()

    return pl.pallas_call(
        kernel,
        name=name,
        out_shape=(jax.ShapeDtypeStruct((gather_hops + 1, streams, 4, rows, width), BF),) + tuple(extra),
        in_specs=in_vmem(len(parts) + len(others)),
        out_specs=tuple(in_vmem(1 + len(extra))),
        scratch_shapes=[pltpu.VMEM((rows, width), F32)]
        + AllGather.scratch(gather_hops, streams)
        + ReduceScatter.scratch(reduce_hops, streams, rows, width),
        compiler_params=params(cid),
    )(*parts, *others)


def norm_of(values, gain_row):
    inverse = lax.rsqrt(jnp.mean(values * values, axis=-1, keepdims=True) + EPSILON)
    return values * inverse * gain_row


def norm_back(values, gain_row, grad_out):
    inverse = lax.rsqrt(jnp.mean(values * values, axis=-1, keepdims=True) + EPSILON)
    scaled = grad_out * gain_row
    dot = jnp.mean(scaled * values, axis=-1, keepdims=True)
    grad_in = inverse * scaled - values * (inverse * inverse * inverse) * dot
    return grad_in, jnp.sum(grad_out * values * inverse, axis=0, keepdims=True)


def strips(base_ref, strip):
    @pl.loop(0, base_ref.shape[0])
    def _(k):
        row = jnp.broadcast_to(base_ref[k], strip.shape[1:])
        strip[k] = pltpu.roll(row, 0, 1, stride=1, stride_axis=0).astype(BF)


def convolve(rows, row_ids, col_ids, base, seq_count):
    _, streams, length, width = rows.shape
    count, _, wide = base.shape
    blocks = length // LANES
    at_once = seq_count <= 4

    def whole_kernel(x_ref, row_ref, col_ref, base_ref, out_ref, strip, mask, left):
        strips(base_ref, strip)

        @pl.loop(0, streams)
        def _(m):
            for h in range(seq_count):
                mask[:, h * length : (h + 1) * length] = jnp.where(col_ref[m] == row_ref[h, m], 1.0, 0.0).astype(BF)
            right = jnp.concatenate([x_ref[h, m] for h in range(seq_count)], axis=0)

            @pl.loop(0, count)
            def _(k):
                for a in range(blocks):
                    for h in range(seq_count):
                        start = LANES * (blocks * (seq_count - h) - 1 - a)
                        down, across = slice(a * LANES, (a + 1) * LANES), slice(h * length, (h + 1) * length)
                        left[down, across] = strip[k, :, start : start + length] * mask[down, across]
                out_ref[k, m] = jnp.dot(left[...], right, preferred_element_type=F32).astype(BF)

    def kernel(x_ref, row_ref, col_ref, base_ref, out_ref, strip, mask, acc):
        strips(base_ref, strip)
        s = lax.axis_index("seq")

        @pl.loop(0, streams)
        def _(m):
            acc[...] = jnp.zeros_like(acc)

            @pl.loop(0, s + 1)
            def _(h):
                mask[...] = jnp.where(col_ref[m] == row_ref[h, m], 1.0, 0.0).astype(BF)

                @pl.loop(0, count)
                def _(k):
                    pieces = []
                    for a in range(blocks):
                        start = pl.multiple_of(LANES * (blocks * (seq_count - h) - 1 - a), LANES)
                        pieces.append(strip[k, :, pl.ds(start, length)] * mask[a * LANES : (a + 1) * LANES])
                    acc[k] += jnp.dot(jnp.concatenate(pieces, axis=0), x_ref[h, m], preferred_element_type=F32)

            @pl.loop(0, count)
            def _(k):
                out_ref[k, m] = acc[k].astype(BF)

    span = seq_count * length if at_once else length
    return pl.pallas_call(
        whole_kernel if at_once else kernel,
        name="convolve",
        out_shape=jax.ShapeDtypeStruct((count, streams, length, width), BF),
        in_specs=in_vmem(4),
        out_specs=in_vmem(1)[0],
        scratch_shapes=[
            pltpu.VMEM((count, LANES, wide), BF),
            pltpu.VMEM((length, span), BF),
            pltpu.VMEM((length, span), BF) if at_once else pltpu.VMEM((count, length, width), F32),
        ],
        compiler_params=params(),
    )(rows, row_ids, col_ids, base)


def convolve_back(grads, row_ids, col_ids, base, own_lag, tail_lag, seq_count):
    count, streams, length, width = grads.shape
    wide = base.shape[2]
    blocks = length // LANES
    channels = own_lag.shape[2]
    tail_rows = tail_lag.shape[1]

    def kernel(g_ref, row_ref, col_ref, base_ref, own_ref, tail_ref, out_ref, strip, mask, acc):
        strips(base_ref, strip)
        s = lax.axis_index("seq")
        mine = pl.ds(pl.multiple_of(lax.axis_index("tensor") * channels, LANES), channels)

        @pl.loop(0, s + 1)
        def _(h):
            @pl.loop(0, streams)
            def _(m):
                mask[...] = jnp.where(col_ref[h, m] == row_ref[m], 1.0, 0.0).astype(BF)
                acc[...] = jnp.zeros_like(acc)

                @pl.when(h == 0)
                def _():
                    acc[:, mine] = own_ref[m]

                @pl.when(h == 1)
                def _():
                    acc[length - tail_rows :, mine] = tail_ref[m]

                @pl.loop(0, count)
                def _(k):
                    pieces = []
                    for a in range(blocks):
                        start = pl.multiple_of(LANES * (blocks * h + blocks - 1 - a), LANES)
                        pieces.append(strip[k, :, pl.ds(start, length)] * mask[a * LANES : (a + 1) * LANES])
                    acc[...] += jnp.dot(jnp.concatenate(pieces, axis=0), g_ref[k, m], preferred_element_type=F32)

                out_ref[h, m] = acc[...].astype(BF)

    return pl.pallas_call(
        kernel,
        name="convolve_back",
        out_shape=jax.ShapeDtypeStruct((seq_count, streams, length, width), BF),
        in_specs=in_vmem(6),
        out_specs=in_vmem(1)[0],
        scratch_shapes=[
            pltpu.VMEM((count, LANES, wide), BF),
            pltpu.VMEM((length, length), BF),
            pltpu.VMEM((length, width), F32),
        ],
        compiler_params=params(),
    )(grads, row_ids, col_ids, base, own_lag, tail_lag)


def dot_nn(a, b):
    return jnp.dot(a, b, preferred_element_type=F32)


def dot_nt(a, b):
    return lax.dot_general(a, b, (((1,), (1,)), ((), ())), preferred_element_type=F32)


def dot_tn(a, b):
    return lax.dot_general(a, b, (((0,), (0,)), ((), ())), preferred_element_type=F32)


def allowed_keys(query_ids, key_ids, first_row, distance):
    shape = (query_ids.shape[0], key_ids.shape[1])
    offset = lax.broadcasted_iota(jnp.int32, shape, 0) - lax.broadcasted_iota(jnp.int32, shape, 1) + (first_row + distance)
    return (query_ids == key_ids) & (offset >= 0) & (offset < WINDOW)


def one_head(block, head):
    lane = lax.broadcasted_iota(jnp.int32, block.shape, 1)
    return jnp.where((lane >= head * HD) & (lane < (head + 1) * HD), block, jnp.zeros_like(block))


def attend(rows, row_ids, col_ids, wq, wk, wv, wo):
    spans, streams, length, width = rows.shape
    cols = wq.shape[1]
    heads = cols // HD
    tile = min(256, length)
    scale = HD ** (-0.5)

    def kernel(x_ref, row_ref, col_ref, wq_ref, wk_ref, wv_ref, wo_ref, q_ref, k_ref, v_ref, a_ref, lse_ref, p_ref):
        @pl.loop(0, streams)
        def _(m):
            q_ref[m] = dot_nn(x_ref[0, m], wq_ref[...]).astype(BF)
            for h in range(spans):
                k_ref[h, m] = dot_nn(x_ref[h, m], wk_ref[...]).astype(BF)
                v_ref[h, m] = dot_nn(x_ref[h, m], wv_ref[...]).astype(BF)

            @pl.loop(0, length // tile)
            def _(i):
                first = pl.multiple_of(i * tile, tile)
                here = pl.ds(first, tile)
                masks = [allowed_keys(col_ref[m, here], row_ref[h, m], first, h * length) for h in range(spans)]
                block = q_ref[m, here]
                result = jnp.zeros((tile, cols), F32)
                for head in range(heads):
                    query = one_head(block, head)
                    scores = [
                        jnp.where(masks[h], dot_nt(query, k_ref[h, m]) * scale, NEGATIVE) for h in range(spans)
                    ]
                    peak = functools.reduce(jnp.maximum, [jnp.max(v, axis=-1, keepdims=True) for v in scores])
                    raised = [jnp.exp(v - peak) for v in scores]
                    total = sum([jnp.sum(v, axis=-1, keepdims=True) for v in raised])
                    inverse = 1.0 / total
                    mixed = sum([dot_nn((raised[h] * inverse).astype(BF), v_ref[h, m]) for h in range(spans)])
                    result = result + one_head(mixed, head)
                    lse_ref[m, head, here] = jnp.broadcast_to(peak + jnp.log(total), (tile, LANES))
                a_ref[m, here] = result.astype(BF)

            p_ref[m] = dot_nn(a_ref[m], wo_ref[...]).astype(BF)

    part = jax.ShapeDtypeStruct((streams, length, cols), BF)
    span = jax.ShapeDtypeStruct((spans, streams, length, cols), BF)
    return pl.pallas_call(
        kernel,
        name="attend",
        out_shape=(
            part,
            span,
            span,
            part,
            jax.ShapeDtypeStruct((streams, heads, length, LANES), F32),
            jax.ShapeDtypeStruct((streams, length, width), BF),
        ),
        in_specs=in_vmem(7),
        out_specs=tuple(in_vmem(6)),
        compiler_params=params(),
    )(rows, row_ids, col_ids, wq, wk, wv, wo)


def attend_back(q, k, v, lse, grad_out, row_ids, col_ids, wq, wk, wv, wo):
    spans, streams, length, cols = k.shape
    width = grad_out.shape[2]
    heads = cols // HD
    tile = min(256, length)
    scale = HD ** (-0.5)

    def kernel(
        q_ref, k_ref, v_ref, lse_ref, go_ref, row_ref, col_ref, wq_ref, wk_ref, wv_ref, wo_ref,
        dq_ref, dk_ref, dv_ref, p_ref, ga_ref, dk_acc, dv_acc,
    ):
        @pl.loop(0, streams)
        def _(m):
            ga_ref[...] = dot_nt(go_ref[m], wo_ref[...]).astype(BF)
            dk_acc[...] = jnp.zeros_like(dk_acc)
            dv_acc[...] = jnp.zeros_like(dv_acc)

            @pl.loop(0, length // tile)
            def _(i):
                first = pl.multiple_of(i * tile, tile)
                here = pl.ds(first, tile)
                masks = [allowed_keys(col_ref[m, here], row_ref[h, m], first, h * length) for h in range(spans)]
                block = q_ref[m, here]
                grad_block = ga_ref[here]
                result = jnp.zeros((tile, cols), F32)
                for head in range(heads):
                    query = one_head(block, head)
                    grad = one_head(grad_block, head)
                    level = lse_ref[m, head, here][:, :1]
                    prob = [
                        jnp.where(masks[h], jnp.exp(dot_nt(query, k_ref[h, m]) * scale - level), 0.0)
                        for h in range(spans)
                    ]
                    grad_prob = [dot_nt(grad, v_ref[h, m]) for h in range(spans)]
                    mean = sum([jnp.sum(p * g, axis=-1, keepdims=True) for p, g in zip(prob, grad_prob)])
                    grad_scores = [(p * (g - mean)).astype(BF) for p, g in zip(prob, grad_prob)]
                    for h in range(spans):
                        dv_acc[h] += dot_tn(prob[h].astype(BF), grad)
                        dk_acc[h] += dot_tn(grad_scores[h], query)
                    mixed = sum([dot_nn(grad_scores[h], k_ref[h, m]) for h in range(spans)])
                    result = result + one_head(mixed, head)
                dq_ref[m, here] = (result * scale).astype(BF)

            for h in range(spans):
                dk_ref[h, m] = (dk_acc[h] * scale).astype(BF)
                dv_ref[h, m] = dv_acc[h].astype(BF)
                back = dot_nt(dk_ref[h, m], wk_ref[...]) + dot_nt(dv_ref[h, m], wv_ref[...])
                if h == 0:
                    back = back + dot_nt(dq_ref[m], wq_ref[...])
                p_ref[h, m] = back.astype(BF)

    span = jax.ShapeDtypeStruct((spans, streams, length, cols), BF)
    return pl.pallas_call(
        kernel,
        name="attend_back",
        out_shape=(
            jax.ShapeDtypeStruct((streams, length, cols), BF),
            span,
            span,
            jax.ShapeDtypeStruct((spans, streams, length, width), BF),
        ),
        in_specs=in_vmem(11),
        out_specs=tuple(in_vmem(4)),
        scratch_shapes=[
            pltpu.VMEM((length, cols), BF),
            pltpu.VMEM((spans, length, cols), F32),
            pltpu.VMEM((spans, length, cols), F32),
        ],
        compiler_params=params(),
    )(q, k, v, lse, grad_out, row_ids, col_ids, wq, wk, wv, wo)


def unit_terms(gate_pre, up_pre, grad_inner):
    root = 0.7978845608028654
    square = gate_pre * gate_pre
    bend = jnp.tanh(root * (gate_pre + 0.044715 * (gate_pre * square)))
    half = 0.5 * (1.0 + bend)
    gelu = gate_pre * half
    slope = half + 0.5 * gate_pre * (1.0 - bend * bend) * (root * (1.0 + 3.0 * 0.044715 * square))
    return gelu * up_pre, grad_inner * up_pre * slope, grad_inner * gelu


def middle(part, x, attn_gain, feed_gain, row_ids, col_ids, wq, wk, wv, wo, wg, wu, wd, cot, seq_count):
    spans, streams, _, length = row_ids.shape
    quarter, width = part.shape[4:]
    hops = spans - 1
    cols, units = wq.shape[1], wg.shape[1]
    heads = cols // HD
    tile = 2 * quarter
    steps = 2 * streams
    scale = HD ** (-0.5)
    rows = width // seq_count
    chunks = 4
    assert streams == 2 and units == 4 * cols

    def kernel(
        part_ref, x_ref, ag_ref, fg_ref, row_ref, col_ref, wq_ref, wk_ref, wv_ref, wo_ref, wg_ref, wu_ref, wd_ref, cot_ref,
        stu_out, layer_out, one_out, gain_out, sum_out,
        attn_in, feed_in, grad_att, q_ref, k_ref, v_ref, a_ref, lse_ref, hid_one, hid_two, grad_two,
        inner_ref, gg_ref, gu_ref, ga_ref, dk_acc, dv_acc, dq_ref, dkv_ref, grads, total, grad_acc,
        o_part, feed_part, layer_part, attn_part,
        sem_one, sem_two, sem_three, sem_layer, sem_five, *scratch,
    ):
        s, t, y, c, core, far = place()
        scratch = list(scratch)

        def take(count):
            taken = scratch[:count]
            del scratch[:count]
            return taken

        def reducer(ref, distance):
            return ReduceScatter(seq_count, distance, streams, lambda h, m: ref.at[h, m], take(6))

        rs_one, rs_two, rs_three, rs_layer = [reducer(r, 0) for r in (part_ref, o_part, feed_part, layer_part)]
        rs_four = reducer(attn_part, hops)
        gr = GradReduce(seq_count, lambda k: grads.at[k], lambda k: sum_out.at[k], take(8))
        ag_one = AllGather(seq_count, hops, streams, attn_in, sem_one)
        ag_two = AllGather(seq_count, 0, streams, feed_in, sem_two)
        ag_three = AllGather(seq_count, 0, streams, grad_att, sem_three)
        ag_layer = AllGather(seq_count, 0, streams, layer_out, sem_layer)
        ag_five = AllGather(seq_count, 0, streams, stu_out, sem_five)
        distances = range(1, hops + 1)

        def flat(value):
            return value.reshape(-1, value.shape[-1])

        def all_rows(ref, m):
            return flat(ref[0, m])

        greet(seq_count, 0, wide=True)
        for m in range(streams):
            rs_one.start(0, m)
        for h in distances:
            for m in range(streams):
                ag_one.clear(h, m)
        for m in range(streams):
            rs_one.middle(0, m)
        for m in range(streams):
            rs_one.total(m, total)
            hidden = x_ref[m, t].astype(F32) + total[...]
            hid_one[m] = hidden
            attn_in[0, m, t] = norm_of(hidden, ag_ref[...]).astype(BF)
            ag_one.start(m)
        ag_one.pass_on(0, 0)
        for h in distances:
            ag_one.arrive(h, 0)
        ag_one.pass_on(0, 1)
        for h in distances:
            ag_one.pass_on(h, 0)
        for h in distances:
            ag_one.arrive(h, 1)
        for h in range(spans):
            ag_one.finish(h, 0)

        def split_step(i):
            m = i // 2
            return m, i - 2 * m

        def after(i, step, *actions):
            @pl.when(i == step)
            def _():
                for action in actions:
                    action()

        def masks_of(m, here, first):
            return [allowed_keys(col_ref[m, here], row_ref[h, m], first, h * length) for h in range(spans)]

        @pl.loop(0, steps)
        def _(i):
            m, half = split_step(i)
            first = pl.multiple_of(half * tile, tile)
            here = pl.ds(first, tile)

            @pl.when(half == 0)
            def _():
                own = flat(attn_in[0, m])
                q_ref[m] = dot_nn(own, wq_ref[...]).astype(BF)
                for h in range(spans):
                    block = flat(attn_in[h, m])
                    k_ref[h, m] = dot_nn(block, wk_ref[...]).astype(BF)
                    v_ref[h, m] = dot_nn(block, wv_ref[...]).astype(BF)

            masks = masks_of(m, here, first)
            block = q_ref[m, here]
            result = jnp.zeros((tile, cols), F32)
            for head in range(heads):
                query = one_head(block, head)
                scores = [jnp.where(masks[h], dot_nt(query, k_ref[h, m]) * scale, NEGATIVE) for h in range(spans)]
                peak = functools.reduce(jnp.maximum, [jnp.max(v, axis=-1, keepdims=True) for v in scores])
                raised = [jnp.exp(v - peak) for v in scores]
                norm = sum([jnp.sum(v, axis=-1, keepdims=True) for v in raised])
                inverse = 1.0 / norm
                mixed = sum([dot_nn((raised[h] * inverse).astype(BF), v_ref[h, m]) for h in range(spans)])
                result = result + one_head(mixed, head)
                lse_ref[m, head, here] = jnp.broadcast_to(peak + jnp.log(norm), (tile, LANES))
            low = result.astype(BF)
            a_ref[m, here] = low
            o_part[0, m, half] = dot_nn(low, wo_ref[...]).astype(BF).reshape(2, quarter, width)
            after(i, 0, *[functools.partial(ag_one.pass_on, h, 1) for h in distances])
            after(i, 1, lambda: rs_two.start(0, 0), *[functools.partial(ag_one.finish, h, 1) for h in range(spans)])
            after(i, 2, lambda: rs_two.middle(0, 0))
            after(i, 3, lambda: rs_two.start(0, 1))

        def second_norm(m):
            rs_two.total(m, total)
            hidden = hid_one[m] + total[...]
            hid_two[m] = hidden
            feed_in[0, m, t] = norm_of(hidden, fg_ref[...]).astype(BF)
            ag_two.start(m)

        second_norm(0)
        rs_two.middle(0, 1)
        ag_two.pass_on(0, 0)
        second_norm(1)
        ag_two.finish(0, 0)

        @pl.loop(0, steps)
        def _(i):
            m, half = split_step(i)
            here = pl.ds(pl.multiple_of(half * tile, tile), tile)
            block = flat(feed_in[0, m, pl.ds(2 * half, 2)])
            inner, grad_gate, grad_up = unit_terms(
                dot_nn(block, wg_ref[...]), dot_nn(block, wu_ref[...]), dot_nt(cot_ref[m, here], wd_ref[...])
            )
            inner, grad_gate, grad_up = inner.astype(BF), grad_gate.astype(BF), grad_up.astype(BF)
            inner_ref[m, here] = inner
            gg_ref[m, here] = grad_gate
            gu_ref[m, here] = grad_up
            back = dot_nt(grad_gate, wg_ref[...]) + dot_nt(grad_up, wu_ref[...])
            feed_part[0, m, half] = back.astype(BF).reshape(2, quarter, width)
            layer_part[0, m, half] = dot_nn(inner, wd_ref[...]).astype(BF).reshape(2, quarter, width)
            after(i, 0, lambda: ag_two.pass_on(0, 1))
            after(i, 1, lambda: rs_three.start(0, 0), lambda: ag_two.finish(0, 1))
            after(i, 2, lambda: rs_three.middle(0, 0))
            after(i, 3, lambda: rs_three.start(0, 1))

        def third_norm(m):
            rs_three.total(m, total)
            grad_in, gain_grad = norm_back(hid_two[m], fg_ref[...], total[...])
            value = cot_ref[m, pl.ds(pl.multiple_of(t * quarter, quarter), quarter)].astype(F32) + grad_in
            grad_two[m] = value
            gain_out[1:2] = gain_grad if m == 0 else gain_out[1:2] + gain_grad
            grad_att[0, m, t] = value.astype(BF)
            ag_three.start(m)

        third_norm(0)
        feed_all = flat(feed_in[0])
        grads[0] = dot_tn(feed_all, flat(gg_ref[...])).astype(BF)
        gr.start(0)
        rs_three.middle(0, 1)
        ag_three.pass_on(0, 0)
        grads[1] = dot_tn(feed_all, flat(gu_ref[...])).astype(BF)
        gr.start(1)
        third_norm(1)
        ag_three.finish(0, 0)
        grads[2] = dot_tn(flat(cot_ref[...]), flat(inner_ref[...])).astype(BF)
        gr.start(2)
        for m in range(streams):
            rs_layer.start(0, m)

        def layer_sum(m):
            rs_layer.total(m, total)
            layer_out[0, m, t] = (hid_two[m] + total[...]).astype(BF)
            ag_layer.start(m)

        @pl.loop(0, steps)
        def _(i):
            m, half = split_step(i)
            first = pl.multiple_of(half * tile, tile)
            here = pl.ds(first, tile)

            @pl.when(half == 0)
            def _():
                ga_ref[...] = dot_nt(all_rows(grad_att, m), wo_ref[...]).astype(BF)
                dk_acc[...] = jnp.zeros_like(dk_acc)
                dv_acc[...] = jnp.zeros_like(dv_acc)

            masks = masks_of(m, here, first)
            block = q_ref[m, here]
            grad_block = ga_ref[here]
            result = jnp.zeros((tile, cols), F32)
            for head in range(heads):
                query = one_head(block, head)
                grad = one_head(grad_block, head)
                level = lse_ref[m, head, here][:, :1]
                prob = [
                    jnp.where(masks[h], jnp.exp(dot_nt(query, k_ref[h, m]) * scale - level), 0.0) for h in range(spans)
                ]
                grad_prob = [dot_nt(grad, v_ref[h, m]) for h in range(spans)]
                mean = sum([jnp.sum(p * g, axis=-1, keepdims=True) for p, g in zip(prob, grad_prob)])
                grad_scores = [(p * (g - mean)).astype(BF) for p, g in zip(prob, grad_prob)]
                for h in range(spans):
                    dv_acc[h] += dot_tn(prob[h].astype(BF), grad)
                    dk_acc[h] += dot_tn(grad_scores[h], query)
                mixed = sum([dot_nn(grad_scores[h], k_ref[h, m]) for h in range(spans)])
                result = result + one_head(mixed, head)
            dq_ref[m, here] = (result * scale).astype(BF)

            @pl.when(half == 1)
            def _():
                for h in range(hops, -1, -1):
                    grad_k = (dk_acc[h] * scale).astype(BF)
                    grad_v = dv_acc[h].astype(BF)
                    dkv_ref[h, m, :, :cols] = grad_k
                    dkv_ref[h, m, :, cols:] = grad_v
                    back = dot_nt(grad_k, wk_ref[...]) + dot_nt(grad_v, wv_ref[...])
                    if h == 0:
                        back = back + dot_nt(dq_ref[m], wq_ref[...])
                    attn_part[h, m] = back.astype(BF).reshape(2, 2, quarter, width)
                    rs_four.start(h, m)

            after(i, 0, lambda: ag_three.pass_on(0, 1), lambda: rs_layer.middle(0, 0), lambda: rs_layer.middle(0, 1))
            after(i, 1, lambda: ag_three.finish(0, 1), lambda: gr.spread(0), lambda: layer_sum(0), lambda: layer_sum(1))
            after(i, 2, *[functools.partial(rs_four.middle, h, 0) for h in range(hops, -1, -1)], lambda: gr.spread(1))
            after(i, 3, *[functools.partial(rs_four.hop, h, 0) for h in range(hops, 0, -1)], lambda: gr.spread(2))

        attn_all = attn_in[...].reshape(spans * streams * length, width)
        grads[3, :, cols : 3 * cols] = dot_tn(attn_all, flat(dkv_ref[...].reshape(-1, 2 * cols))).astype(BF)
        for h in range(hops, -1, -1):
            rs_four.middle(h, 1)
        grads[3, :, :cols] = dot_tn(flat(attn_in[0]), flat(dq_ref[...])).astype(BF)
        grads[3, :, 3 * cols :] = dot_tn(flat(grad_att[0]), flat(a_ref[...])).astype(BF)
        gr.start(3)
        for h in range(hops, 0, -1):
            rs_four.hop(h, 1)
        for m in range(streams):
            rs_four.total(m, total)
            grad_in, gain_grad = norm_back(hid_one[m], ag_ref[...], total[...])
            value = grad_two[m] + grad_in
            one_out[m] = value
            gain_out[0:1] = gain_grad if m == 0 else gain_out[0:1] + gain_grad
            stu_out[0, m, t] = value.astype(BF)
            ag_five.start(m)
            gr.collect(m, grad_acc)
            ag_layer.pass_on(0, m)
        gr.spread(3)
        for m in range(streams):
            ag_five.pass_on(0, m)
        gr.collect(2, grad_acc)
        for m in range(streams):
            ag_layer.finish(0, m)
        gr.collect(3, grad_acc)
        for m in range(streams):
            ag_five.finish(0, m)
        for k in range(chunks):
            gr.finish(k)
            gr.drain(k)
        for item in (rs_one, rs_two, rs_three, rs_layer, rs_four, ag_one, ag_two, ag_three, ag_layer, ag_five):
            item.drain()

    rows_of = pltpu.VMEM((streams, length, cols), BF)
    unit_rows = pltpu.VMEM((streams, length, units), BF)
    state = pltpu.VMEM((streams, quarter, width), F32)
    gathered = (1, streams, 4, quarter, width)
    split_part = pltpu.VMEM((1, streams, 2, 2, quarter, width), BF)
    zero_hops = ReduceScatter.scratch(0, streams, quarter, width)
    return pl.pallas_call(
        kernel,
        name="middle",
        out_shape=(
            jax.ShapeDtypeStruct(gathered, BF),
            jax.ShapeDtypeStruct(gathered, BF),
            jax.ShapeDtypeStruct((streams, quarter, width), F32),
            jax.ShapeDtypeStruct((2, width), F32),
            jax.ShapeDtypeStruct((chunks, rows, units), F32),
        ),
        in_specs=in_vmem(14),
        out_specs=tuple(in_vmem(5)),
        scratch_shapes=[
            pltpu.VMEM((spans, streams, 4, quarter, width), BF),
            pltpu.VMEM(gathered, BF),
            pltpu.VMEM(gathered, BF),
            rows_of,
            pltpu.VMEM((spans, streams, length, cols), BF),
            pltpu.VMEM((spans, streams, length, cols), BF),
            rows_of,
            pltpu.VMEM((streams, heads, length, LANES), F32),
            state,
            state,
            state,
            unit_rows,
            unit_rows,
            unit_rows,
            pltpu.VMEM((length, cols), BF),
            pltpu.VMEM((spans, length, cols), F32),
            pltpu.VMEM((spans, length, cols), F32),
            rows_of,
            pltpu.VMEM((spans, streams, length, 2 * cols), BF),
            pltpu.VMEM((chunks, width, units), BF),
            pltpu.VMEM((quarter, width), F32),
            pltpu.VMEM((rows, units // 2), F32),
            split_part,
            split_part,
            split_part,
            pltpu.VMEM((spans, streams, 2, 2, quarter, width), BF),
            AllGather.scratch(hops, streams)[0],
        ]
        + [AllGather.scratch(0, streams)[0]] * 4
        + zero_hops * 4
        + ReduceScatter.scratch(hops, streams, quarter, width)
        + GradReduce.scratch(seq_count, chunks, width, units),
        compiler_params=params(8),
    )(part, x, attn_gain, feed_gain, row_ids, col_ids, wq, wk, wv, wo, wg, wu, wd, cot)


def tail(
    grad_stu, filter_proj, lag_proj, conv, lag_stack, lag_masks, row_ids, ext_ids, base, x, gain, grad_one, gains, seq_count
):
    count, length_all, width = conv.shape
    streams, _, quarter, _ = x.shape
    length = length_all // streams
    lag_order, channels = lag_proj.shape[:2]
    wide = base.shape[2]
    blocks = length // LANES
    hops = seq_count - 1
    chunks = count + 1
    steps = seq_count * streams
    rows = width // seq_count
    gain_rows = 8

    def kernel(
        gs_ref, fp_ref, lp_ref, conv_ref, lag_ref, mask_ref, row_ref, ext_ref, base_ref, x_ref, gain_ref, one_ref, gains_ref,
        out, filter_out, lag_out, gain_out,
        strip, mask, cols, left, acc, terms, grad_conv, grads, lag_ext, total, grad_acc, gather_sem,
        gain_own, gain_near, gain_sum, gain_far, near_sem, far_sem, *scratch,
    ):
        s, t, y, c, core, far = place()
        p = lax.axis_index("dp")
        rs_scratch, gr_scratch = scratch[:6], scratch[6:]
        greet(seq_count, hops, wide=True, gains=True)

        def source(k):
            return grads.at[k]

        def result(k):
            return filter_out.at[k] if k < count else lag_out

        gr = GradReduce(seq_count, source, result, gr_scratch)
        rs = ReduceScatter(seq_count, hops, streams, lambda h, m: terms.at[h, m], rs_scratch)
        ag = AllGather(seq_count, 0, streams, out, gather_sem)

        early = min(2, count)

        @pl.loop(0, count)
        def _(k):
            grads[k] = dot_tn(conv_ref[k], gs_ref[...]).astype(BF)
            gr.start(k)
            product = dot_nt(gs_ref[...], fp_ref[k]).astype(BF)
            for m in range(streams):
                here = pl.ds(pl.multiple_of(k * length, LANES), length)
                grad_conv[m, here] = product[m * length : (m + 1) * length]

            @pl.when(k >= count - early)
            def _():
                gr.spread(k - (count - early))

        grads[count] = jnp.zeros_like(grads.at[count])
        for i in range(lag_order):
            grads[count, :, i * channels : (i + 1) * channels] = dot_tn(gs_ref[...], lag_ref[i]).astype(BF)
        gr.start(count)
        for m in range(streams):
            lag_ext[m] = jnp.zeros_like(lag_ext.at[m])
            for i in range(lag_order):
                term = dot_nt(gs_ref[m * length : (m + 1) * length], lp_ref[i]) * mask_ref[i, m]
                lag_ext[m, 7 - i : 7 - i + length] += term
        strips(base_ref, strip)
        turned = jnp.transpose(ext_ref[...].astype(F32))
        for j in range(steps):
            cols[j] = turned[:, j : j + 1]
        mine = pl.ds(pl.multiple_of(t * channels, LANES), channels)
        spread_at = {}
        collect_at = {}
        for k in range(early, chunks):
            if 2 * (k - early) < steps:
                spread_at[2 * (k - early)] = k
        for k in range(chunks):
            if 2 * k + 3 < steps and k < early + len(spread_at):
                collect_at[2 * k + 3] = k

        def step_of(i):
            return seq_count - 1 - i // streams, i - i // streams * streams

        @pl.loop(0, steps)
        def _(i):
            h, m = step_of(i)

            @pl.when(h <= s)
            def _():
                mask[...] = jnp.where(cols[h * streams + m] == row_ref[m].astype(F32), 1.0, 0.0).astype(BF)
                for k in range(count):
                    for a in range(blocks):
                        start = pl.multiple_of(LANES * (blocks * h + blocks - 1 - a), LANES)
                        down = slice(a * LANES, (a + 1) * LANES)
                        left[down, k * length : (k + 1) * length] = strip[k, :, pl.ds(start, length)] * mask[down]
                acc[...] = jnp.dot(left[...], grad_conv[m], preferred_element_type=F32)

                @pl.when(h == 0)
                def _():
                    acc[:, mine] += lag_ext[m, 8:]

                @pl.when(h == 1)
                def _():
                    acc[length - 8 :, mine] += lag_ext[m, :8]

                for quarter_y in range(2):
                    for quarter_c in range(2):
                        first = (2 * quarter_y + quarter_c) * quarter
                        terms[h, m, quarter_y, quarter_c] = acc[first : first + quarter].astype(BF)
                rs.start(h, m)

            @pl.when(i >= 1)
            def _():
                rs.middle(*step_of(i - 1))

            @pl.when((i >= 2) & (i < steps - streams + 2))
            def _():
                rs.hop(*step_of(i - 2))

            for step, k in spread_at.items():
                pl.when(i == step)(functools.partial(gr.spread, k))
            for step, k in collect_at.items():
                pl.when(i == step)(functools.partial(gr.collect, k, grad_acc))

        rs.middle(0, streams - 1)
        for k in range(early + len(spread_at), chunks):
            gr.spread(k)
        gain_own[...] = jnp.zeros_like(gain_own)
        for m in range(streams):
            rs.total(m, total)
            grad_in, gain_grad = norm_back(x_ref[m, t].astype(F32), gain_ref[...], total[...])
            out[0, m, t] = (one_ref[m] + grad_in).astype(BF)
            ag.start(m)
            gain_own[0:1] += gain_grad
        gain_own[1:3] = gains_ref[...]
        gain_near[t] = gain_own[...]

        def near_copy(j, slot):
            return remote(gain_own, gain_near.at[slot], near_sem.at[0, j], near_sem.at[1, slot], {"tensor": j})

        for j in range(4):
            pl.when(t != j)(lambda: near_copy(j, t).start())
        for m in range(streams):
            ag.pass_on(0, m)
        for k in range(len(collect_at), chunks):
            gr.collect(k, grad_acc)
        for j in range(4):
            pl.when(t != j)(lambda: near_copy(j, j).wait_recv())
        gain_sum[...] = gain_near[0] + gain_near[1] + gain_near[2] + gain_near[3]
        me = p * seq_count + s

        def far_copy(j, slot):
            d, q = j // seq_count, j % seq_count
            return remote(
                gain_sum.at[:, q * rows : (q + 1) * rows], gain_far.at[slot], far_sem.at[0, j], far_sem.at[1, slot],
                {"dp": d, "seq": q},
            )

        gain_far[me] = gain_sum[:, pl.ds(pl.multiple_of(s * rows, LANES), rows)]
        for j in range(2 * seq_count):
            pl.when(me != j)(lambda: far_copy(j, me).start())
        for m in range(streams):
            ag.finish(0, m)
        for k in range(chunks):
            gr.finish(k)
        for j in range(2 * seq_count):
            pl.when(me != j)(lambda: far_copy(j, j).wait_recv())
        gain_out[...] = functools.reduce(jnp.add, [gain_far[j] for j in range(2 * seq_count)])
        for j in range(4):
            pl.when(t != j)(lambda: near_copy(j, t).wait_send())
        for j in range(2 * seq_count):
            pl.when(me != j)(lambda: far_copy(j, me).wait_send())
        for k in range(chunks):
            gr.drain(k)
        rs.drain()
        ag.drain()

    return pl.pallas_call(
        kernel,
        name="tail",
        out_shape=(
            jax.ShapeDtypeStruct((1, streams, 4, quarter, width), BF),
            jax.ShapeDtypeStruct((count, rows, width), F32),
            jax.ShapeDtypeStruct((rows, width), F32),
            jax.ShapeDtypeStruct((gain_rows, rows), F32),
        ),
        in_specs=in_vmem(13),
        out_specs=tuple(in_vmem(4)),
        scratch_shapes=[
            pltpu.VMEM((count, LANES, wide), BF),
            pltpu.VMEM((length, length), BF),
            pltpu.VMEM((steps, length, 1), F32),
            pltpu.VMEM((length, count * length), BF),
            pltpu.VMEM((length, width), F32),
            pltpu.VMEM((seq_count, streams, 2, 2, quarter, width), BF),
            pltpu.VMEM((streams, count * length, width), BF),
            pltpu.VMEM((chunks, width, width), BF),
            pltpu.VMEM((streams, length + 8, channels), F32),
            pltpu.VMEM((quarter, width), F32),
            pltpu.VMEM((rows, width // 2), F32),
            AllGather.scratch(0, streams)[0],
            pltpu.VMEM((gain_rows, width), F32),
            pltpu.VMEM((4, gain_rows, width), F32),
            pltpu.VMEM((gain_rows, width), F32),
            pltpu.VMEM((2 * seq_count, gain_rows, rows), F32),
            pltpu.SemaphoreType.DMA((2, 4)),
            pltpu.SemaphoreType.DMA((2, 2 * seq_count)),
        ]
        + ReduceScatter.scratch(hops, streams, quarter, width)
        + GradReduce.scratch(seq_count, chunks, width, width),
        compiler_params=params(7),
    )(
        grad_stu, filter_proj, lag_proj, conv, lag_stack, lag_masks, row_ids, ext_ids, base, x, gain, grad_one, gains
    )


def gated_unit(gate_pre, up_pre):
    return jax.nn.gelu(gate_pre, approximate=True) * up_pre


def local(
    seq_count,
    tokens,
    document_index,
    filters,
    stu_gain,
    filter_proj,
    lag_proj,
    attention_gain,
    query_weight,
    key_weight,
    value_weight,
    output_weight,
    feed_gain,
    gate_weight,
    up_weight,
    down_weight,
    cotangent,
):
    streams, _, length, width = tokens.shape
    row_len = length * seq_count
    quarter = length // 4
    lag_order, channels = lag_proj.shape[:2]
    count = filters.shape[0]
    hops = WINDOW // length
    tensor_place = lax.axis_index("tensor")
    chan_start = tensor_place * channels

    def split(a):
        return a.reshape(a.shape[:-2] + (2, 2, quarter, width))

    def quarters(a):
        return a.reshape(a.shape[:-2] + (4, quarter, width))

    def whole(a):
        return a.reshape(a.shape[:-3] + (length, width))

    def row(gain):
        return gain.reshape(1, width)

    x = tokens[:, 0]
    grad_three = cotangent[:, 0]
    ids = document_index[:, 0]
    inputs = norm_of(x.astype(F32), stu_gain).astype(BF)
    id_tile = ids.reshape(streams * length // LANES, LANES)
    rows_ext, id_ext = gather_rows(quarters(inputs), id_tile, seq_count)
    rows_ext = whole(rows_ext)
    id_ext = id_ext.reshape(seq_count, streams, length)
    id_rows = id_ext[:, :, None, :]
    id_cols = id_ext[:, :, :, None]

    pad = jnp.zeros((count, 4 * LANES), filters.dtype)
    ahead = row_len - LANES
    base = jnp.concatenate(
        [
            jnp.flip(filters[:, : ahead + 1], axis=1),
            pad[:, : 4 * LANES],
            jnp.flip(filters[:, ahead + 1 :], axis=1),
        ],
        axis=1,
    ).astype(F32)[:, None]
    base_back = jnp.concatenate(
        [pad[:, : length - LANES], filters, pad[:, :LANES]], axis=1
    ).astype(F32)[:, None]
    conv = convolve(rows_ext, id_rows, id_cols[0], base, seq_count)

    chan_rows = lax.dynamic_slice_in_dim(rows_ext[:2], chan_start, channels, 3)
    joined = jnp.concatenate([chan_rows[1][:, length - lag_order :], chan_rows[0]], axis=1)
    joined_ids = jnp.concatenate([id_ext[1][:, length - lag_order :], ids], axis=1)
    masks = []
    lagged = []
    for step in range(1, lag_order + 1):
        low = lag_order - step
        masks.append((joined_ids[:, low : low + length] == ids)[:, :, None])
        lagged.append(jnp.where(masks[-1], joined[:, low : low + length], jnp.zeros((), BF)))
    lag_stack = jnp.stack(lagged)

    mixed = jnp.einsum("kmtd,kde->mte", conv, filter_proj, preferred_element_type=F32)
    mixed = mixed + jnp.einsum("imtc,ice->mte", lag_stack, lag_proj, preferred_element_type=F32)

    tokens_flat = streams * length
    cols = query_weight.shape[1]

    def answer(layer_output, input_gradient, gains, filter_grad, lag_grad, attn_grads, feed_grads):
        query_grad, key_grad, value_grad, output_grad = jnp.split(attn_grads, [cols, 2 * cols, 3 * cols], axis=1)
        gate_grad, up_grad, down_grad = feed_grads
        return (
            layer_output[:, None],
            input_gradient[:, None],
            gains[0],
            filter_grad,
            lag_grad[:, : lag_order * channels].T.reshape(lag_order, channels, -1),
            gains[1],
            query_grad,
            key_grad,
            value_grad,
            output_grad.T,
            gains[2],
            gate_grad,
            up_grad,
            down_grad.T,
        )

    if width // seq_count % LANES == 0:
        grad_stu, layer_output, grad_one, gain_grads, sums = middle(
            split(mixed.astype(BF))[None], quarters(x), row(attention_gain), row(feed_gain), id_rows[: hops + 1], id_cols[0],
            query_weight, key_weight, value_weight, output_weight, gate_weight, up_weight, down_weight, grad_three, seq_count,
        )
        input_gradient, filter_grad, lag_grad, gains = tail(
            grad_stu.reshape(tokens_flat, width), filter_proj, lag_proj, conv.reshape(count, tokens_flat, width),
            lag_stack.reshape(lag_order, tokens_flat, channels), jnp.stack(masks).astype(F32), id_rows[0],
            id_ext.reshape(seq_count * streams, length), base_back, quarters(x), row(stu_gain), grad_one, gain_grads, seq_count,
        )
        return answer(
            whole(layer_output)[0], whole(input_gradient)[0], gains, filter_grad, lag_grad, sums[3], (sums[0], sums[1], sums[2])
        )

    state = jax.ShapeDtypeStruct((streams, quarter, width), F32)
    gain_state = jax.ShapeDtypeStruct((1, width), F32)

    def finish_one(m, total, others, extra):
        x_ref, gain_ref = others
        hidden = x_ref[m, place()[1]].astype(F32) + total
        extra[0][m] = hidden
        return norm_of(hidden, gain_ref[...]).astype(BF)

    attn_ext, hidden_one = exchange(
        "exchange_one", 2, seq_count, [split(mixed.astype(BF))[None]], [quarters(x), row(attention_gain)], 0, hops,
        finish_one, [state],
    )
    attn_ext = whole(attn_ext)

    q, k, v, attended, lse, out_part = attend(
        attn_ext, id_rows[: hops + 1], id_cols[0], query_weight, key_weight, value_weight, output_weight
    )

    def finish_two(m, total, others, extra):
        hidden_ref, gain_ref = others
        hidden = hidden_ref[m] + total
        extra[0][m] = hidden
        return norm_of(hidden, gain_ref[...]).astype(BF)

    feed_in, hidden_two = exchange(
        "exchange_two", 3, seq_count, [split(out_part)[None]], [hidden_one, row(feed_gain)], 0, 0, finish_two, [state]
    )
    feed_in = whole(feed_in)[0].reshape(streams * length, width)
    flat_three = grad_three.reshape(streams * length, width)

    gate_pre = dot_nn(feed_in, gate_weight)
    up_pre = dot_nn(feed_in, up_weight)
    grad_inner = dot_nt(flat_three, down_weight)
    unit, pull = jax.vjp(gated_unit, gate_pre, up_pre)
    inner = unit.astype(BF)
    grad_gate, grad_up = pull(grad_inner)
    grad_gate = grad_gate.astype(BF)
    grad_up = grad_up.astype(BF)
    layer_part = dot_nn(inner, down_weight).astype(BF)
    feed_part = (dot_nt(grad_gate, gate_weight) + dot_nt(grad_up, up_weight)).astype(BF)

    def finish_three(m, total, others, extra):
        hidden_ref, gain_ref, cot_ref = others
        if m >= streams:
            return (hidden_ref[m - streams] + total).astype(BF)
        grad_in, gain_grad = norm_back(hidden_ref[m], gain_ref[...], total)
        grad_two = cot_ref[m, place()[1]].astype(F32) + grad_in
        extra[0][m] = grad_two
        extra[1][...] = gain_grad if m == 0 else extra[1][...] + gain_grad
        return grad_two.astype(BF)

    feed_grads = jnp.stack(
        [
            dot_tn(feed_in, grad_gate).astype(BF),
            dot_tn(feed_in, grad_up).astype(BF),
            dot_tn(flat_three, inner).astype(BF),
        ]
    )
    shape = (1, streams, length, width)
    both, grad_two, feed_gain_grad = exchange(
        "exchange_three", 4, seq_count, [split(feed_part.reshape(shape)), split(layer_part.reshape(shape))],
        [hidden_two, row(feed_gain), quarters(grad_three)], 0, 0, finish_three, [state, gain_state],
    )
    both = whole(both)[0]
    grad_att_out = both[:streams]
    layer_output = both[streams:]

    dq, dk, dv, attn_part = attend_back(
        q, k, v, lse, grad_att_out, id_rows[: hops + 1], id_cols[0], query_weight, key_weight, value_weight, output_weight
    )

    go = grad_att_out.reshape(tokens_flat, width)
    attn_grads = jnp.concatenate(
        [
            dot_tn(attn_ext[0].reshape(tokens_flat, width), dq.reshape(tokens_flat, -1)).astype(BF),
            dot_tn(attn_ext.reshape(-1, width), dk.reshape(-1, dk.shape[-1])).astype(BF),
            dot_tn(attn_ext.reshape(-1, width), dv.reshape(-1, dv.shape[-1])).astype(BF),
            dot_tn(go, attended.reshape(tokens_flat, -1)).astype(BF),
        ],
        axis=1,
    )

    def finish_four(m, total, others, extra):
        hidden_ref, gain_ref, grad_ref = others
        grad_in, gain_grad = norm_back(hidden_ref[m], gain_ref[...], total)
        grad_one = grad_ref[m] + grad_in
        extra[0][m] = grad_one
        extra[1][...] = gain_grad if m == 0 else extra[1][...] + gain_grad
        return grad_one.astype(BF)

    grad_stu, grad_one, attn_gain_grad = exchange(
        "exchange_four", 5, seq_count, [split(attn_part)], [hidden_one, row(attention_gain), grad_two], hops, 0,
        finish_four, [state, gain_state],
    )
    grad_stu = whole(grad_stu)[0]
    grad_conv = jnp.einsum("mte,kde->kmtd", grad_stu, filter_proj, preferred_element_type=F32).astype(BF)
    grad_lagged = jnp.einsum("mte,ice->imtc", grad_stu, lag_proj, preferred_element_type=F32)
    ext_grad = jnp.zeros((streams, 8 + length, channels), F32)
    for step in range(1, lag_order + 1):
        term = jnp.where(masks[step - 1], grad_lagged[step - 1], 0.0)
        ext_grad = ext_grad + jnp.pad(term, ((0, 0), (8 - step, step), (0, 0)))
    terms = convolve_back(
        grad_conv, id_rows[0], id_cols, base_back, ext_grad[:, 8:], ext_grad[:, :8], seq_count
    )

    def finish_five(m, total, others, extra):
        x_ref, gain_ref, grad_ref = others
        grad_in, gain_grad = norm_back(x_ref[m, place()[1]].astype(F32), gain_ref[...], total)
        extra[0][...] = gain_grad if m == 0 else extra[0][...] + gain_grad
        return (grad_ref[m] + grad_in).astype(BF)

    input_gradient, stu_gain_grad = exchange(
        "exchange_five", 6, seq_count, [split(terms)], [quarters(x), row(stu_gain), grad_one], seq_count - 1, 0,
        finish_five, [gain_state],
    )
    input_gradient = whole(input_gradient)[0]
    stu = grad_stu.reshape(tokens_flat, width)
    filter_part = jnp.einsum("kmtd,mte->kde", conv, grad_stu, preferred_element_type=F32).astype(BF)
    lag_part = jnp.concatenate(
        [dot_tn(stu, lag_stack[i].reshape(tokens_flat, channels)).astype(BF) for i in range(lag_order)], axis=1
    )
    feed_grads = lax.psum(
        lax.psum_scatter(feed_grads, "seq", scatter_dimension=1, tiled=True), "dp"
    ).astype(F32)
    attn_grads = lax.psum(lax.psum_scatter(attn_grads, "seq", scatter_dimension=0, tiled=True), "dp").astype(F32)
    filter_grad = lax.psum(
        lax.psum_scatter(filter_part, "seq", scatter_dimension=1, tiled=True), "dp"
    ).astype(F32)
    lag_grad = lax.psum(lax.psum_scatter(lag_part, "seq", scatter_dimension=0, tiled=True), "dp").astype(F32)
    gains = jnp.concatenate([stu_gain_grad, attn_gain_grad, feed_gain_grad], axis=0)
    gains = lax.psum(gains, ("dp", "seq", "tensor"))
    gain_width = width // seq_count
    gains = lax.dynamic_slice_in_dim(gains, lax.axis_index("seq") * gain_width, gain_width, 1)
    return answer(layer_output, input_gradient, gains, filter_grad, lag_grad, attn_grads, feed_grads)


def solution(mesh):
    return jax.shard_map(
        functools.partial(local, mesh.shape["seq"]),
        mesh=mesh,
        in_specs=(
            P(None, "dp", "seq", None),
            P(None, "dp", "seq"),
            P("tensor", None),
            P(),
            P("tensor", None, None),
            P(None, "tensor", None),
            P(),
            P(None, "tensor"),
            P(None, "tensor"),
            P(None, "tensor"),
            P("tensor", None),
            P(),
            P(None, "tensor"),
            P(None, "tensor"),
            P("tensor", None),
            P(None, "dp", "seq", None),
        ),
        out_specs=(
            P(None, "dp", "seq", None),
            P(None, "dp", "seq", None),
            P("seq"),
            P("tensor", "seq", None),
            P(None, "tensor", "seq"),
            P("seq"),
            P("seq", "tensor"),
            P("seq", "tensor"),
            P("seq", "tensor"),
            P("tensor", "seq"),
            P("seq"),
            P("seq", "tensor"),
            P("seq", "tensor"),
            P("tensor", "seq"),
        ),
        check_vma=False,
    )
```

```python
import functools

import jax
import jax.numpy as jnp
from jax import lax
from jax.experimental import pallas as pl
from jax.experimental.pallas import tpu as pltpu
from jax.sharding import PartitionSpec as P

HD = 64
WINDOW = 1024
EPSILON = 1e-05
LANES = 128
NEGATIVE = -1e30
MESH = pl.DeviceIdType.MESH
BF = jnp.bfloat16
F32 = jnp.float32
VMEM_LIMIT = 63 * 1024 * 1024


def place():
    s = lax.axis_index("seq")
    t = lax.axis_index("tensor")
    y = t // 2
    c = t - 2 * y
    return s, t, y, c, t + 1 - 2 * c, t + 2 - 4 * y


def when(condition, action):
    if condition is True:
        action()
    else:
        pl.when(condition)(action)


def remote(src, dst, send_sem, recv_sem, device):
    return pltpu.make_async_remote_copy(
        src_ref=src, dst_ref=dst, send_sem=send_sem, recv_sem=recv_sem, device_id=device, device_id_type=MESH
    )


def greet(seq_count, hops, wide=False, gains=False):
    s, t, y, c, core, far = place()
    barrier = pltpu.get_barrier_semaphore()

    def signal(device):
        pl.semaphore_signal(barrier, inc=1, device_id=device, device_id_type=MESH)

    signal({"tensor": core})
    signal({"tensor": far})
    if gains:
        signal({"tensor": 3 - t})
    if wide:
        p = lax.axis_index("dp")
        signal({"dp": 1 - p})
        for j in range(seq_count):

            @pl.when(s != j)
            def _():
                signal({"seq": j})
                if gains:
                    signal({"dp": 1 - p, "seq": j})

        peers = 2 + gains + 1 + (seq_count - 1) * (1 + gains)
    else:
        for h in range(1, hops + 1):
            for there, peer in ((s - h >= 0, s - h), (s + h < seq_count, s + h)):

                @pl.when(there)
                def _():
                    signal({"seq": peer})

        peers = 2 + jnp.minimum(s, hops) + jnp.minimum(seq_count - 1 - s, hops)
    pl.semaphore_wait(barrier, peers)


class ReduceScatter:
    def __init__(self, seq_count, hops, streams, part, scratch):
        self.seq_count, self.hops, self.streams, self.part = seq_count, hops, streams, part
        self.near, self.half, self.over, self.hop_out, self.hop_in, self.sem = scratch

    @staticmethod
    def scratch(hops, streams, rows, width):
        quarter = (hops + 1, streams, rows, width)
        over_seq = quarter if hops else (1, 1, 16, LANES)
        return [
            pltpu.VMEM((hops + 1, streams, 2, rows, width), BF),
            pltpu.VMEM(quarter, BF),
            pltpu.VMEM(quarter, BF),
            pltpu.VMEM(over_seq, BF),
            pltpu.VMEM(over_seq, BF),
            pltpu.SemaphoreType.DMA((6, hops + 1, streams)),
        ]

    def to_core(self, h, m):
        s, t, y, c, core, far = place()
        return remote(
            self.part(h, m).at[:, 1 - c], self.near.at[h, m], self.sem.at[0, h, m], self.sem.at[1, h, m], {"tensor": core}
        )

    def to_far(self, h, m):
        s, t, y, c, core, far = place()
        return remote(self.half.at[h, m], self.over.at[h, m], self.sem.at[2, h, m], self.sem.at[3, h, m], {"tensor": far})

    def to_hop(self, h, m, peer):
        return remote(
            self.hop_out.at[h, m], self.hop_in.at[h - 1, m], self.sem.at[4, h, m], self.sem.at[5, h - 1, m], {"seq": peer}
        )

    def add_hop(self, h, m, acc):
        s = lax.axis_index("seq")

        @pl.when(s + 1 < self.seq_count)
        def _():
            remote(
                self.hop_out.at[h, m], self.hop_in.at[h, m], self.sem.at[4, h, m], self.sem.at[5, h, m], {"seq": s + 1}
            ).wait_recv()
            acc[...] += self.hop_in[h, m].astype(F32)

    def there(self, h):
        return True if isinstance(h, int) and h == 0 else lax.axis_index("seq") - h >= 0

    def order(self):
        return [(h, m) for h in range(self.hops, -1, -1) for m in range(self.streams)]

    def start(self, h, m):
        when(self.there(h), lambda: self.to_core(h, m).start())

    def middle(self, h, m):
        s, t, y, c, core, far = place()

        def act():
            self.to_core(h, m).wait_recv()
            mine = self.part(h, m)[1 - y, c].astype(F32) + self.near[h, m, 1 - y].astype(F32)
            self.half[h, m] = mine.astype(BF)
            self.to_far(h, m).start()

        when(self.there(h), act)

    def own(self, h, m):
        s, t, y, c, core, far = place()
        self.to_far(h, m).wait_recv()
        return (
            self.part(h, m)[y, c].astype(F32) + self.near[h, m, y].astype(F32) + self.over[h, m].astype(F32)
        )

    def hop(self, h, m, acc):
        def act():
            acc[...] = self.own(h, m)
            if isinstance(h, int):
                if h < self.hops:
                    self.add_hop(h, m, acc)
            else:
                pl.when(h < self.hops)(lambda: self.add_hop(h, m, acc))
            self.hop_out[h, m] = acc[...].astype(BF)
            self.to_hop(h, m, lax.axis_index("seq") - 1).start()

        when(self.there(h), act)

    def total(self, m, acc):
        acc[...] = self.own(0, m)
        if self.hops:
            self.add_hop(0, m, acc)

    def drain(self):
        for h, m in self.order():

            def act():
                self.to_core(h, m).wait_send()
                self.to_far(h, m).wait_send()
                if h:
                    self.to_hop(h, m, lax.axis_index("seq") - 1).wait_send()

            when(self.there(h), act)


class AllGather:
    def __init__(self, seq_count, hops, streams, at, sem, first=0):
        self.seq_count, self.hops, self.streams, self.sem, self.first = seq_count, hops, streams, sem, first
        self.at = at if callable(at) else lambda h, m, quarter: at.at[h, m, quarter]

    @staticmethod
    def scratch(hops, streams):
        return [pltpu.SemaphoreType.DMA((8, hops + 1, streams))]

    def there(self, h):
        return True if h == 0 else lax.axis_index("seq") - h >= 0

    def copy(self, kind, h, m, quarter, device):
        ref = self.at(h, m, quarter)
        return remote(ref, ref, self.sem.at[2 * kind, h, m], self.sem.at[2 * kind + 1, h, m], device)

    def relay(self, h, m):
        s, t = lax.axis_index("seq"), place()[1]
        return remote(
            self.at(h, m, t), self.at(h + 1, m, t), self.sem.at[0, h, m], self.sem.at[1, h + 1, m], {"seq": s + 1}
        )

    def relays(self, h):
        s = lax.axis_index("seq")
        return (s - h >= 0) & (s + 1 < self.seq_count)

    def forward(self, h, m):
        if h < self.hops:
            pl.when(self.relays(h))(lambda: self.relay(h, m).start())

    def spread(self, h, m):
        s, t, y, c, core, far = place()
        self.copy(1, h, m, t, {"tensor": far}).start()
        self.copy(2, h, m, t, {"tensor": core}).start()

    def start(self, m):
        self.forward(0, m)
        if self.first == 0:
            self.spread(0, m)

    def arrive(self, h, m):
        @pl.when(self.there(h))
        def _():
            self.copy(0, h, m, place()[1], {"seq": lax.axis_index("seq") - 1}).wait_recv()

        self.forward(h, m)
        pl.when(self.there(h))(lambda: self.spread(h, m))

    def pass_on(self, h, m):
        s, t, y, c, core, far = place()

        def act():
            self.copy(1, h, m, far, {"tensor": far}).wait_recv()
            self.copy(3, h, m, far, {"tensor": core}).start()

        when(self.there(h), act)

    def finish(self, h, m):
        s, t, y, c, core, far = place()

        def act():
            self.copy(2, h, m, core, {"tensor": core}).wait_recv()
            self.copy(3, h, m, 3 - t, {"tensor": core}).wait_recv()

        when(self.there(h), act)

    def clear(self, h, m):
        @pl.when(lax.axis_index("seq") - h < 0)
        def _():
            for quarter in range(4):
                ref = self.at(h, m, quarter)
                ref[...] = jnp.zeros(ref.shape, ref.dtype)

    def drain(self):
        s, t, y, c, core, far = place()
        for m in range(self.streams):
            for h in range(self.hops):
                pl.when(self.relays(h))(functools.partial(lambda h, m: self.relay(h, m).wait_send(), h, m))
            for h in range(self.first, self.hops + 1):

                def act():
                    self.copy(1, h, m, t, {"tensor": far}).wait_send()
                    self.copy(2, h, m, t, {"tensor": core}).wait_send()
                    self.copy(3, h, m, far, {"tensor": core}).wait_send()

                when(self.there(h), act)


class GradReduce:
    def __init__(self, seq_count, source, result, scratch):
        self.seq_count, self.source, self.result = seq_count, source, result
        self.x_in, self.z_out, self.z_in, self.back_out, self.back_in, self.x_sem, self.z_sem, self.back_sem = scratch
        self.half = self.x_in.shape[2]
        self.rows = self.back_out.shape[1]

    @staticmethod
    def scratch(seq_count, chunks, depth, width):
        rows, half = depth // seq_count, width // 2
        return [
            pltpu.VMEM((chunks, depth, half), BF),
            pltpu.VMEM((chunks, depth, half), BF),
            pltpu.VMEM((chunks, seq_count, rows, half), BF),
            pltpu.VMEM((chunks, rows, half), BF),
            pltpu.VMEM((chunks, rows, half), BF),
            pltpu.SemaphoreType.DMA((2, chunks)),
            pltpu.SemaphoreType.DMA((2, chunks, seq_count)),
            pltpu.SemaphoreType.DMA((2, chunks)),
        ]

    def columns(self, p):
        return pl.ds(pl.multiple_of(p * self.half, LANES), self.half)

    def block(self, j):
        return pl.ds(pl.multiple_of(j * self.rows, 16), self.rows)

    def over(self, c):
        p = lax.axis_index("dp")
        return remote(
            self.source(c).at[:, self.columns(1 - p)], self.x_in.at[c], self.x_sem.at[0, c], self.x_sem.at[1, c], {"dp": 1 - p}
        )

    def row_copy(self, c, j, slot):
        return remote(
            self.z_out.at[c, self.block(j)], self.z_in.at[c, slot], self.z_sem.at[0, c, j], self.z_sem.at[1, c, slot], {"seq": j}
        )

    def back(self, c):
        p = lax.axis_index("dp")
        return remote(
            self.back_out.at[c], self.back_in.at[c], self.back_sem.at[0, c], self.back_sem.at[1, c], {"dp": 1 - p}
        )

    def others(self, action):
        for j in range(self.seq_count):
            pl.when(lax.axis_index("seq") != j)(functools.partial(action, j))

    def start(self, c):
        self.over(c).start()

    def spread(self, c):
        s, p = lax.axis_index("seq"), lax.axis_index("dp")
        self.over(c).wait_recv()
        mine = self.source(c)[:, self.columns(p)].astype(F32) + self.x_in[c].astype(F32)
        self.z_out[c] = mine.astype(BF)
        self.others(lambda j: self.row_copy(c, j, s).start())

    def collect(self, c, acc):
        s, p = lax.axis_index("seq"), lax.axis_index("dp")
        here = self.block(s)
        acc[...] = self.source(c)[here, self.columns(p)].astype(F32) + self.x_in[c, here].astype(F32)

        def add(j):
            self.row_copy(c, j, j).wait_recv()
            acc[...] += self.z_in[c, j].astype(F32)

        self.others(add)
        self.back_out[c] = acc[...].astype(BF)
        self.back(c).start()

    def finish(self, c):
        p = lax.axis_index("dp")
        self.back(c).wait_recv()
        self.result(c)[:, self.columns(p)] = self.back_out[c].astype(F32)
        self.result(c)[:, self.columns(1 - p)] = self.back_in[c].astype(F32)

    def drain(self, c):
        self.over(c).wait_send()
        self.others(lambda j: self.row_copy(c, j, lax.axis_index("seq")).wait_send())
        self.back(c).wait_send()


def params(cid=None):
    if cid is None:
        return pltpu.CompilerParams(vmem_limit_bytes=VMEM_LIMIT)
    return pltpu.CompilerParams(vmem_limit_bytes=VMEM_LIMIT, collective_id=cid, has_side_effects=True)


def in_vmem(count):
    return [pl.BlockSpec(memory_space=pltpu.VMEM)] * count


def gather_rows(inputs, ids, seq_count):
    streams, quarters, rows, width = inputs.shape
    hops = seq_count - 1

    def kernel(x_ref, id_ref, out, out_ids, sem, id_sem):
        s, t, y, c, core, far = place()
        greet(seq_count, hops)
        out[0] = x_ref[...]
        out_ids[0] = id_ref[...]
        ag = AllGather(seq_count, hops, streams, out, sem, first=1)

        def id_copy(h, peer):
            return remote(id_ref, out_ids.at[h], id_sem.at[0, h], id_sem.at[1, h], {"seq": peer})

        for h in range(1, hops + 1):

            @pl.when(s + h < seq_count)
            def _():
                id_copy(h, s + h).start()

        for m in range(streams):
            ag.start(m)
        for h in range(1, hops + 1):
            for m in range(streams):
                ag.clear(h, m)

            @pl.when(s - h < 0)
            def _():
                out_ids[h] = jnp.full(out_ids.shape[1:], -1, jnp.int32)

        for m in range(streams):
            for h in range(1, hops + 1):
                ag.arrive(h, m)
        for m in range(streams):
            for h in range(1, hops + 1):
                ag.pass_on(h, m)
        for h in range(1, hops + 1):
            for m in range(streams):
                ag.finish(h, m)

            @pl.when(s - h >= 0)
            def _():
                id_copy(h, s - h).wait_recv()

            @pl.when(s + h < seq_count)
            def _():
                id_copy(h, s + h).wait_send()

        ag.drain()

    return pl.pallas_call(
        kernel,
        name="gather_rows",
        out_shape=(
            jax.ShapeDtypeStruct((seq_count,) + inputs.shape, inputs.dtype),
            jax.ShapeDtypeStruct((seq_count,) + ids.shape, jnp.int32),
        ),
        in_specs=in_vmem(2),
        out_specs=tuple(in_vmem(2)),
        scratch_shapes=AllGather.scratch(hops, streams) + [pltpu.SemaphoreType.DMA((2, seq_count))],
        compiler_params=params(1),
    )(inputs, ids)


def exchange(name, cid, seq_count, parts, others, reduce_hops, gather_hops, finish, extra):
    per_part = parts[0].shape[1]
    rows, width = parts[0].shape[4:]
    streams = per_part * len(parts)
    hops = max(reduce_hops, gather_hops)

    def kernel(*refs):
        refs = list(refs)
        part_refs = [refs.pop(0) for _ in parts]
        other_refs = [refs.pop(0) for _ in others]
        out = refs.pop(0)
        extra_refs = [refs.pop(0) for _ in extra]
        acc = refs.pop(0)
        gather_sem = refs.pop(0)
        s, t, y, c, core, far = place()
        greet(seq_count, hops)
        rs = ReduceScatter(
            seq_count, reduce_hops, streams, lambda h, m: part_refs[m // per_part].at[h, m % per_part], refs
        )
        ag = AllGather(seq_count, gather_hops, streams, out, gather_sem)
        for h, m in rs.order():
            rs.start(h, m)
        for h in range(1, gather_hops + 1):
            for m in range(streams):
                ag.clear(h, m)
        for h, m in rs.order():
            rs.middle(h, m)
        for h, m in rs.order():
            if h:
                rs.hop(h, m, acc)
        for m in range(streams):
            rs.total(m, acc)
            out[0, m, t] = finish(m, acc[...], other_refs, extra_refs)
            ag.start(m)
        for m in range(streams):
            ag.pass_on(0, m)
            for h in range(1, gather_hops + 1):
                ag.arrive(h, m)
        for m in range(streams):
            for h in range(1, gather_hops + 1):
                ag.pass_on(h, m)
        for h in range(gather_hops + 1):
            for m in range(streams):
                ag.finish(h, m)
        rs.drain()
        ag.drain()

    return pl.pallas_call(
        kernel,
        name=name,
        out_shape=(jax.ShapeDtypeStruct((gather_hops + 1, streams, 4, rows, width), BF),) + tuple(extra),
        in_specs=in_vmem(len(parts) + len(others)),
        out_specs=tuple(in_vmem(1 + len(extra))),
        scratch_shapes=[pltpu.VMEM((rows, width), F32)]
        + AllGather.scratch(gather_hops, streams)
        + ReduceScatter.scratch(reduce_hops, streams, rows, width),
        compiler_params=params(cid),
    )(*parts, *others)


def norm_of(values, gain_row):
    inverse = lax.rsqrt(jnp.mean(values * values, axis=-1, keepdims=True) + EPSILON)
    return values * inverse * gain_row


def norm_back(values, gain_row, grad_out):
    inverse = lax.rsqrt(jnp.mean(values * values, axis=-1, keepdims=True) + EPSILON)
    scaled = grad_out * gain_row
    dot = jnp.mean(scaled * values, axis=-1, keepdims=True)
    grad_in = inverse * scaled - values * (inverse * inverse * inverse) * dot
    return grad_in, jnp.sum(grad_out * values * inverse, axis=0, keepdims=True)


def strips(base_ref, strip):
    @pl.loop(0, base_ref.shape[0])
    def _(k):
        row = jnp.broadcast_to(base_ref[k], strip.shape[1:])
        strip[k] = pltpu.roll(row, 0, 1, stride=1, stride_axis=0).astype(BF)


def convolve(rows, row_ids, col_ids, base, seq_count):
    _, streams, length, width = rows.shape
    count, _, wide = base.shape
    blocks = length // LANES
    at_once = seq_count <= 4

    def whole_kernel(x_ref, row_ref, col_ref, base_ref, out_ref, strip, mask, left):
        strips(base_ref, strip)

        @pl.loop(0, streams)
        def _(m):
            for h in range(seq_count):
                mask[:, h * length : (h + 1) * length] = jnp.where(col_ref[m] == row_ref[h, m], 1.0, 0.0).astype(BF)
            right = jnp.concatenate([x_ref[h, m] for h in range(seq_count)], axis=0)

            @pl.loop(0, count)
            def _(k):
                for a in range(blocks):
                    for h in range(seq_count):
                        start = LANES * (blocks * (seq_count - h) - 1 - a)
                        down, across = slice(a * LANES, (a + 1) * LANES), slice(h * length, (h + 1) * length)
                        left[down, across] = strip[k, :, start : start + length] * mask[down, across]
                out_ref[k, m] = jnp.dot(left[...], right, preferred_element_type=F32).astype(BF)

    def kernel(x_ref, row_ref, col_ref, base_ref, out_ref, strip, mask, acc):
        strips(base_ref, strip)
        s = lax.axis_index("seq")

        @pl.loop(0, streams)
        def _(m):
            acc[...] = jnp.zeros_like(acc)

            @pl.loop(0, s + 1)
            def _(h):
                mask[...] = jnp.where(col_ref[m] == row_ref[h, m], 1.0, 0.0).astype(BF)

                @pl.loop(0, count)
                def _(k):
                    pieces = []
                    for a in range(blocks):
                        start = pl.multiple_of(LANES * (blocks * (seq_count - h) - 1 - a), LANES)
                        pieces.append(strip[k, :, pl.ds(start, length)] * mask[a * LANES : (a + 1) * LANES])
                    acc[k] += jnp.dot(jnp.concatenate(pieces, axis=0), x_ref[h, m], preferred_element_type=F32)

            @pl.loop(0, count)
            def _(k):
                out_ref[k, m] = acc[k].astype(BF)

    span = seq_count * length if at_once else length
    return pl.pallas_call(
        whole_kernel if at_once else kernel,
        name="convolve",
        out_shape=jax.ShapeDtypeStruct((count, streams, length, width), BF),
        in_specs=in_vmem(4),
        out_specs=in_vmem(1)[0],
        scratch_shapes=[
            pltpu.VMEM((count, LANES, wide), BF),
            pltpu.VMEM((length, span), BF),
            pltpu.VMEM((length, span), BF) if at_once else pltpu.VMEM((count, length, width), F32),
        ],
        compiler_params=params(),
    )(rows, row_ids, col_ids, base)


def convolve_back(grads, row_ids, col_ids, base, own_lag, tail_lag, seq_count):
    count, streams, length, width = grads.shape
    wide = base.shape[2]
    blocks = length // LANES
    channels = own_lag.shape[2]
    tail_rows = tail_lag.shape[1]

    def kernel(g_ref, row_ref, col_ref, base_ref, own_ref, tail_ref, out_ref, strip, mask, acc):
        strips(base_ref, strip)
        s = lax.axis_index("seq")
        mine = pl.ds(pl.multiple_of(lax.axis_index("tensor") * channels, LANES), channels)

        @pl.loop(0, s + 1)
        def _(h):
            @pl.loop(0, streams)
            def _(m):
                mask[...] = jnp.where(col_ref[h, m] == row_ref[m], 1.0, 0.0).astype(BF)
                acc[...] = jnp.zeros_like(acc)

                @pl.when(h == 0)
                def _():
                    acc[:, mine] = own_ref[m]

                @pl.when(h == 1)
                def _():
                    acc[length - tail_rows :, mine] = tail_ref[m]

                @pl.loop(0, count)
                def _(k):
                    pieces = []
                    for a in range(blocks):
                        start = pl.multiple_of(LANES * (blocks * h + blocks - 1 - a), LANES)
                        pieces.append(strip[k, :, pl.ds(start, length)] * mask[a * LANES : (a + 1) * LANES])
                    acc[...] += jnp.dot(jnp.concatenate(pieces, axis=0), g_ref[k, m], preferred_element_type=F32)

                out_ref[h, m] = acc[...].astype(BF)

    return pl.pallas_call(
        kernel,
        name="convolve_back",
        out_shape=jax.ShapeDtypeStruct((seq_count, streams, length, width), BF),
        in_specs=in_vmem(6),
        out_specs=in_vmem(1)[0],
        scratch_shapes=[
            pltpu.VMEM((count, LANES, wide), BF),
            pltpu.VMEM((length, length), BF),
            pltpu.VMEM((length, width), F32),
        ],
        compiler_params=params(),
    )(grads, row_ids, col_ids, base, own_lag, tail_lag)


def dot_nn(a, b):
    return jnp.dot(a, b, preferred_element_type=F32)


def dot_nt(a, b):
    return lax.dot_general(a, b, (((1,), (1,)), ((), ())), preferred_element_type=F32)


def dot_tn(a, b):
    return lax.dot_general(a, b, (((0,), (0,)), ((), ())), preferred_element_type=F32)


def allowed_keys(query_ids, key_ids, first_row, distance):
    shape = (query_ids.shape[0], key_ids.shape[1])
    offset = lax.broadcasted_iota(jnp.int32, shape, 0) - lax.broadcasted_iota(jnp.int32, shape, 1) + (first_row + distance)
    return (query_ids == key_ids) & (offset >= 0) & (offset < WINDOW)


def one_head(block, head):
    lane = lax.broadcasted_iota(jnp.int32, block.shape, 1)
    return jnp.where((lane >= head * HD) & (lane < (head + 1) * HD), block, jnp.zeros_like(block))


def attend(rows, row_ids, col_ids, wq, wk, wv, wo):
    spans, streams, length, width = rows.shape
    cols = wq.shape[1]
    heads = cols // HD
    tile = min(256, length)
    scale = HD ** (-0.5)

    def kernel(x_ref, row_ref, col_ref, wq_ref, wk_ref, wv_ref, wo_ref, q_ref, k_ref, v_ref, a_ref, lse_ref, p_ref):
        @pl.loop(0, streams)
        def _(m):
            q_ref[m] = dot_nn(x_ref[0, m], wq_ref[...]).astype(BF)
            for h in range(spans):
                k_ref[h, m] = dot_nn(x_ref[h, m], wk_ref[...]).astype(BF)
                v_ref[h, m] = dot_nn(x_ref[h, m], wv_ref[...]).astype(BF)

            @pl.loop(0, length // tile)
            def _(i):
                first = pl.multiple_of(i * tile, tile)
                here = pl.ds(first, tile)
                masks = [allowed_keys(col_ref[m, here], row_ref[h, m], first, h * length) for h in range(spans)]
                block = q_ref[m, here]
                result = jnp.zeros((tile, cols), F32)
                for head in range(heads):
                    query = one_head(block, head)
                    scores = [
                        jnp.where(masks[h], dot_nt(query, k_ref[h, m]) * scale, NEGATIVE) for h in range(spans)
                    ]
                    peak = functools.reduce(jnp.maximum, [jnp.max(v, axis=-1, keepdims=True) for v in scores])
                    raised = [jnp.exp(v - peak) for v in scores]
                    total = sum([jnp.sum(v, axis=-1, keepdims=True) for v in raised])
                    inverse = 1.0 / total
                    mixed = sum([dot_nn((raised[h] * inverse).astype(BF), v_ref[h, m]) for h in range(spans)])
                    result = result + one_head(mixed, head)
                    lse_ref[m, head, here] = jnp.broadcast_to(peak + jnp.log(total), (tile, LANES))
                a_ref[m, here] = result.astype(BF)

            p_ref[m] = dot_nn(a_ref[m], wo_ref[...]).astype(BF)

    part = jax.ShapeDtypeStruct((streams, length, cols), BF)
    span = jax.ShapeDtypeStruct((spans, streams, length, cols), BF)
    return pl.pallas_call(
        kernel,
        name="attend",
        out_shape=(
            part,
            span,
            span,
            part,
            jax.ShapeDtypeStruct((streams, heads, length, LANES), F32),
            jax.ShapeDtypeStruct((streams, length, width), BF),
        ),
        in_specs=in_vmem(7),
        out_specs=tuple(in_vmem(6)),
        compiler_params=params(),
    )(rows, row_ids, col_ids, wq, wk, wv, wo)


def attend_back(q, k, v, lse, grad_out, row_ids, col_ids, wq, wk, wv, wo):
    spans, streams, length, cols = k.shape
    width = grad_out.shape[2]
    heads = cols // HD
    tile = min(256, length)
    scale = HD ** (-0.5)

    def kernel(
        q_ref, k_ref, v_ref, lse_ref, go_ref, row_ref, col_ref, wq_ref, wk_ref, wv_ref, wo_ref,
        dq_ref, dk_ref, dv_ref, p_ref, ga_ref, dk_acc, dv_acc,
    ):
        @pl.loop(0, streams)
        def _(m):
            ga_ref[...] = dot_nt(go_ref[m], wo_ref[...]).astype(BF)
            dk_acc[...] = jnp.zeros_like(dk_acc)
            dv_acc[...] = jnp.zeros_like(dv_acc)

            @pl.loop(0, length // tile)
            def _(i):
                first = pl.multiple_of(i * tile, tile)
                here = pl.ds(first, tile)
                masks = [allowed_keys(col_ref[m, here], row_ref[h, m], first, h * length) for h in range(spans)]
                block = q_ref[m, here]
                grad_block = ga_ref[here]
                result = jnp.zeros((tile, cols), F32)
                for head in range(heads):
                    query = one_head(block, head)
                    grad = one_head(grad_block, head)
                    level = lse_ref[m, head, here][:, :1]
                    prob = [
                        jnp.where(masks[h], jnp.exp(dot_nt(query, k_ref[h, m]) * scale - level), 0.0)
                        for h in range(spans)
                    ]
                    grad_prob = [dot_nt(grad, v_ref[h, m]) for h in range(spans)]
                    mean = sum([jnp.sum(p * g, axis=-1, keepdims=True) for p, g in zip(prob, grad_prob)])
                    grad_scores = [(p * (g - mean)).astype(BF) for p, g in zip(prob, grad_prob)]
                    for h in range(spans):
                        dv_acc[h] += dot_tn(prob[h].astype(BF), grad)
                        dk_acc[h] += dot_tn(grad_scores[h], query)
                    mixed = sum([dot_nn(grad_scores[h], k_ref[h, m]) for h in range(spans)])
                    result = result + one_head(mixed, head)
                dq_ref[m, here] = (result * scale).astype(BF)

            for h in range(spans):
                dk_ref[h, m] = (dk_acc[h] * scale).astype(BF)
                dv_ref[h, m] = dv_acc[h].astype(BF)
                back = dot_nt(dk_ref[h, m], wk_ref[...]) + dot_nt(dv_ref[h, m], wv_ref[...])
                if h == 0:
                    back = back + dot_nt(dq_ref[m], wq_ref[...])
                p_ref[h, m] = back.astype(BF)

    span = jax.ShapeDtypeStruct((spans, streams, length, cols), BF)
    return pl.pallas_call(
        kernel,
        name="attend_back",
        out_shape=(
            jax.ShapeDtypeStruct((streams, length, cols), BF),
            span,
            span,
            jax.ShapeDtypeStruct((spans, streams, length, width), BF),
        ),
        in_specs=in_vmem(11),
        out_specs=tuple(in_vmem(4)),
        scratch_shapes=[
            pltpu.VMEM((length, cols), BF),
            pltpu.VMEM((spans, length, cols), F32),
            pltpu.VMEM((spans, length, cols), F32),
        ],
        compiler_params=params(),
    )(q, k, v, lse, grad_out, row_ids, col_ids, wq, wk, wv, wo)


def unit_terms(gate_pre, up_pre, grad_inner):
    root = 0.7978845608028654
    square = gate_pre * gate_pre
    bend = jnp.tanh(root * (gate_pre + 0.044715 * (gate_pre * square)))
    half = 0.5 * (1.0 + bend)
    gelu = gate_pre * half
    slope = half + 0.5 * gate_pre * (1.0 - bend * bend) * (root * (1.0 + 3.0 * 0.044715 * square))
    return gelu * up_pre, grad_inner * up_pre * slope, grad_inner * gelu


def head(
    x, ids, stu_gain, filter_proj, lag_proj, base, base_back, attn_gain, feed_gain, wq, wk, wv, wo, wg, wu, wd, cot, seq_count
):
    streams, _, quarter, width = x.shape
    length = 4 * quarter
    hops = WINDOW // length
    spans = hops + 1
    count, _, wide = base.shape
    lag_order, channels = lag_proj.shape[:2]
    blocks = length // LANES
    id_rows_each = length // LANES
    cols, units = wq.shape[1], wg.shape[1]
    heads = cols // HD
    tile = 2 * quarter
    steps = 2 * streams
    scale = HD ** (-0.5)
    rows = width // seq_count
    chunks = 4
    assert streams == 2 and units == 4 * cols

    rows_of = pltpu.VMEM((streams, length, cols), BF)
    unit_rows = pltpu.VMEM((streams, length, units), BF)
    state = pltpu.VMEM((streams, quarter, width), F32)
    gathered = (1, streams, 4, quarter, width)
    split_part = pltpu.VMEM((1, streams, 2, 2, quarter, width), BF)
    zero_hops = ReduceScatter.scratch(0, streams, quarter, width)

    def kernel(
        x_ref, id_ref, sg_ref, fp_ref, lp_ref, base_ref, back_ref, ag_ref, fg_ref,
        wq_ref, wk_ref, wv_ref, wo_ref, wg_ref, wu_ref, wd_ref, cot_ref,
        stu_out, layer_out, one_out, gain_out, sum_out, lag_out, ids_out, conv_out, strip_out,
        rows_in, ids_in, cols_in, id_ext, lag_ext, part_ref, id_sem, strip_sem, conv_sem,
        attn_in, feed_in, grad_att, hid_one, hid_two, grad_two, grads, total, grad_acc,
        o_part, feed_part, layer_part, attn_part,
        sem_rows, sem_one, sem_two, sem_three, sem_layer, sem_five, *scratch,
    ):
        s, t, y, c, core, far = place()
        scratch = list(scratch)

        def take(count):
            taken = scratch[:count]
            del scratch[:count]
            return taken

        def reducer(ref, distance):
            return ReduceScatter(seq_count, distance, streams, lambda h, m: ref.at[h, m], take(6))

        rs_one, rs_two, rs_three, rs_layer = [reducer(r, 0) for r in (part_ref, o_part, feed_part, layer_part)]
        rs_four = reducer(attn_part, hops)
        gr = GradReduce(seq_count, lambda k: grads.at[k], lambda k: sum_out.at[k], take(8))
        ag_rows = AllGather(
            seq_count, seq_count - 1, streams, lambda h, m, q: rows_in.at[m, h, q], sem_rows, first=1
        )
        ag_one = AllGather(seq_count, hops, streams, attn_in, sem_one)
        ag_two = AllGather(seq_count, 0, streams, feed_in, sem_two)
        ag_three = AllGather(seq_count, 0, streams, grad_att, sem_three)
        ag_layer = AllGather(seq_count, 0, streams, layer_out, sem_layer)
        ag_five = AllGather(seq_count, 0, streams, stu_out, sem_five)

        def flat(value):
            return value.reshape(-1, value.shape[-1])

        def all_rows(ref, m):
            return flat(ref[0, m])

        def masks_of(m, here, first):
            return [
                allowed_keys(cols_in[m, here], ids_out[pl.ds(h * streams + m, 1)], first, h * length) for h in range(spans)
            ]

        def first_norm(m):
            rs_one.total(m, total)
            hidden = x_ref[m, t].astype(F32) + total[...]
            hid_one[m] = hidden
            attn_in[0, m, t] = norm_of(hidden, ag_ref[...]).astype(BF)
            ag_one.start(m)

        def after(i, step, *actions):
            @pl.when(i == step)
            def _():
                for action in actions:
                    action()

        def id_copy(h, peer):
            return remote(id_ref, ids_in.at[h], id_sem.at[0, h], id_sem.at[1, h], {"seq": peer})

        far_back = range(1, seq_count)

        def front(strip, left, mask, conv):
            for m in range(streams):
                rows_in[m, 0, t] = norm_of(x_ref[m, t].astype(F32), sg_ref[...]).astype(BF)
            greet(seq_count, 0, wide=True)
            for m in range(streams):
                ag_rows.start(m)
            for h in far_back:
                pl.when(s + h < seq_count)(functools.partial(lambda h: id_copy(h, s + h).start(), h))
            for m in range(streams):
                for q in range(4):

                    @pl.when(t != q)
                    def _():
                        rows_in[m, 0, q] = norm_of(x_ref[m, q].astype(F32), sg_ref[...]).astype(BF)

            for m in range(streams):
                for h in far_back:
                    ag_rows.clear(h, m)
                for h in range(1, spans):
                    ag_one.clear(h, m)
            ids_in[0] = id_ref[...]
            for h in far_back:

                @pl.when(s - h < 0)
                def _():
                    ids_in[h] = jnp.full(ids_in.shape[1:], -1, jnp.int32)

            strips(back_ref, strip)
            strip_copy = pltpu.make_async_copy(strip, strip_out, strip_sem)
            strip_copy.start()
            for h in far_back:
                ag_rows.arrive(h, 0)
            for h in far_back:
                pl.when(s - h >= 0)(functools.partial(lambda h: id_copy(h, s - h).wait_recv(), h))
            for h in range(seq_count):
                values = ids_in[h].astype(F32)
                for m in range(streams):
                    first = m * id_rows_each
                    ids_out[h * streams + m : h * streams + m + 1] = jnp.concatenate(
                        [values[first + r : first + r + 1] for r in range(id_rows_each)], axis=1
                    )
            turned = jnp.transpose(ids_out[...])
            for m in range(streams):
                cols_in[m] = turned[:, m : m + 1]
                id_ext[m, :8] = turned[length - 8 :, streams + m : streams + m + 1]
                id_ext[m, 8:] = turned[:, m : m + 1]
            strip_copy.wait()
            strips(base_ref, strip)
            for h in far_back:
                ag_rows.pass_on(h, 0)
            for h in far_back:
                ag_rows.arrive(h, 1)
            for h in far_back:
                ag_rows.finish(h, 0)
            mine = pl.ds(pl.multiple_of(t * channels, LANES), channels)

            def lags(m):
                own = rows_in[m, 0, :, :, mine].reshape(length, channels)
                lag_ext[:8] = rows_in[m, 1, 3, quarter - 8 :, mine].astype(F32)
                lag_ext[8:] = own.astype(F32)
                for i in range(lag_order):
                    same = id_ext[m, 7 - i : 7 - i + length] == cols_in[m]
                    lag_out[i, m] = jnp.where(same, lag_ext[7 - i : 7 - i + length], 0.0).astype(BF)

            def conv_copy(k, m):
                return pltpu.make_async_copy(
                    conv.at[k], conv_out.at[k, pl.ds(pl.multiple_of(m * length, LANES), length)], conv_sem.at[k]
                )

            lags(0)

            @pl.loop(0, streams * count)
            def _(j):
                m = j // count
                k = j - m * count

                @pl.when(k == 0)
                def _():
                    for h in range(seq_count):
                        mask[:, h * length : (h + 1) * length] = jnp.where(
                            cols_in[m] == ids_out[pl.ds(h * streams + m, 1)], 1.0, 0.0
                        ).astype(BF)

                for a in range(blocks):
                    for h in range(seq_count):
                        start = LANES * (blocks * (seq_count - h) - 1 - a)
                        down, across = slice(a * LANES, (a + 1) * LANES), slice(h * length, (h + 1) * length)
                        left[down, across] = strip[k, :, start : start + length] * mask[down, across]
                result = dot_nn(left[...], rows_in[m].reshape(seq_count * length, width)).astype(BF)
                pl.when(m > 0)(lambda: conv_copy(k, m - 1).wait())
                conv[k] = result
                conv_copy(k, m).start()

                @pl.when(k == count - 1)
                def _():
                    @pl.loop(0, 2)
                    def _(half):
                        here = pl.ds(pl.multiple_of(half * tile, tile), tile)
                        mixed = sum([dot_nn(conv[q, here], fp_ref[q]) for q in range(count)])
                        mixed = mixed + sum([dot_nn(lag_out[i, m, here], lp_ref[i]) for i in range(lag_order)])
                        part_ref[0, m, half] = mixed.astype(BF).reshape(2, quarter, width)

                after(j, 1, *[functools.partial(ag_rows.pass_on, h, 1) for h in far_back])
                after(
                    j,
                    count - 1,
                    lambda: rs_one.start(0, 0),
                    *[functools.partial(ag_rows.finish, h, 1) for h in far_back],
                    lambda: lags(1),
                )
                after(j, count, lambda: rs_one.middle(0, 0))
                after(j, count + 2, lambda: first_norm(0))
                after(j, count + 4, lambda: ag_one.pass_on(0, 0), lambda: ag_one.arrive(1, 0) if hops > 0 else None)

            rs_one.start(0, 1)
            for k in range(count):
                conv_copy(k, streams - 1).wait()

        pl.run_scoped(
            front,
            pltpu.VMEM((count, LANES, wide), BF),
            pltpu.VMEM((length, seq_count * length), BF),
            pltpu.VMEM((length, seq_count * length), BF),
            pltpu.VMEM((count, length, width), BF),
        )

        def attention_on(
            q_ref, k_ref, v_ref, a_ref, lse_ref, inner_ref, gg_ref, gu_ref, ga_ref, dk_acc, dv_acc, dq_ref, dkv_ref
        ):
            rs_one.middle(0, 1)
            for h in range(2, spans):
                ag_one.arrive(h, 0)
            for h in range(1, spans):
                ag_one.pass_on(h, 0)
            first_norm(1)
            for h in range(spans):
                ag_one.finish(h, 0)

            def split_step(i):
                m = i // 2
                return m, i - 2 * m

            @pl.loop(0, steps)
            def _(i):
                m, half = split_step(i)
                first = pl.multiple_of(half * tile, tile)
                here = pl.ds(first, tile)

                @pl.when(half == 0)
                def _():
                    own = flat(attn_in[0, m])
                    q_ref[m] = dot_nn(own, wq_ref[...]).astype(BF)
                    for h in range(spans):
                        block = flat(attn_in[h, m])
                        k_ref[h, m] = dot_nn(block, wk_ref[...]).astype(BF)
                        v_ref[h, m] = dot_nn(block, wv_ref[...]).astype(BF)

                masks = masks_of(m, here, first)
                block = q_ref[m, here]
                result = jnp.zeros((tile, cols), F32)
                for head in range(heads):
                    query = one_head(block, head)
                    scores = [jnp.where(masks[h], dot_nt(query, k_ref[h, m]) * scale, NEGATIVE) for h in range(spans)]
                    peak = functools.reduce(jnp.maximum, [jnp.max(v, axis=-1, keepdims=True) for v in scores])
                    raised = [jnp.exp(v - peak) for v in scores]
                    norm = sum([jnp.sum(v, axis=-1, keepdims=True) for v in raised])
                    inverse = 1.0 / norm
                    mixed = sum([dot_nn((raised[h] * inverse).astype(BF), v_ref[h, m]) for h in range(spans)])
                    result = result + one_head(mixed, head)
                    lse_ref[m, head, here] = jnp.broadcast_to(peak + jnp.log(norm), (tile, LANES))
                low = result.astype(BF)
                a_ref[m, here] = low
                o_part[0, m, half] = dot_nn(low, wo_ref[...]).astype(BF).reshape(2, quarter, width)
                after(i, 0, lambda: ag_one.pass_on(0, 1), *[functools.partial(ag_one.arrive, h, 1) for h in range(1, spans)])
                after(
                    i,
                    1,
                    lambda: rs_two.start(0, 0),
                    *[functools.partial(ag_one.pass_on, h, 1) for h in range(1, spans)],
                    *[functools.partial(ag_one.finish, h, 1) for h in range(spans)],
                )
                after(i, 2, lambda: rs_two.middle(0, 0))
                after(i, 3, lambda: rs_two.start(0, 1))

            def second_norm(m):
                rs_two.total(m, total)
                hidden = hid_one[m] + total[...]
                hid_two[m] = hidden
                feed_in[0, m, t] = norm_of(hidden, fg_ref[...]).astype(BF)
                ag_two.start(m)

            second_norm(0)
            rs_two.middle(0, 1)
            ag_two.pass_on(0, 0)
            second_norm(1)
            ag_two.finish(0, 0)

            @pl.loop(0, steps)
            def _(i):
                m, half = split_step(i)
                here = pl.ds(pl.multiple_of(half * tile, tile), tile)
                block = flat(feed_in[0, m, pl.ds(2 * half, 2)])
                inner, grad_gate, grad_up = unit_terms(
                    dot_nn(block, wg_ref[...]), dot_nn(block, wu_ref[...]), dot_nt(cot_ref[m, here], wd_ref[...])
                )
                inner, grad_gate, grad_up = inner.astype(BF), grad_gate.astype(BF), grad_up.astype(BF)
                inner_ref[m, here] = inner
                gg_ref[m, here] = grad_gate
                gu_ref[m, here] = grad_up
                back = dot_nt(grad_gate, wg_ref[...]) + dot_nt(grad_up, wu_ref[...])
                feed_part[0, m, half] = back.astype(BF).reshape(2, quarter, width)
                layer_part[0, m, half] = dot_nn(inner, wd_ref[...]).astype(BF).reshape(2, quarter, width)
                after(i, 0, lambda: ag_two.pass_on(0, 1))
                after(i, 1, lambda: rs_three.start(0, 0), lambda: ag_two.finish(0, 1))
                after(i, 2, lambda: rs_three.middle(0, 0))
                after(i, 3, lambda: rs_three.start(0, 1))

            def third_norm(m):
                rs_three.total(m, total)
                grad_in, gain_grad = norm_back(hid_two[m], fg_ref[...], total[...])
                value = cot_ref[m, pl.ds(pl.multiple_of(t * quarter, quarter), quarter)].astype(F32) + grad_in
                grad_two[m] = value
                gain_out[1:2] = gain_grad if m == 0 else gain_out[1:2] + gain_grad
                grad_att[0, m, t] = value.astype(BF)
                ag_three.start(m)

            third_norm(0)
            feed_all = flat(feed_in[0])
            grads[0] = dot_tn(feed_all, flat(gg_ref[...])).astype(BF)
            gr.start(0)
            rs_three.middle(0, 1)
            ag_three.pass_on(0, 0)
            grads[1] = dot_tn(feed_all, flat(gu_ref[...])).astype(BF)
            gr.start(1)
            third_norm(1)
            ag_three.finish(0, 0)
            grads[2] = dot_tn(flat(cot_ref[...]), flat(inner_ref[...])).astype(BF)
            gr.start(2)
            for m in range(streams):
                rs_layer.start(0, m)

            def layer_sum(m):
                rs_layer.total(m, total)
                layer_out[0, m, t] = (hid_two[m] + total[...]).astype(BF)
                ag_layer.start(m)

            @pl.loop(0, steps)
            def _(i):
                m, half = split_step(i)
                first = pl.multiple_of(half * tile, tile)
                here = pl.ds(first, tile)

                @pl.when(half == 0)
                def _():
                    ga_ref[...] = dot_nt(all_rows(grad_att, m), wo_ref[...]).astype(BF)
                    dk_acc[...] = jnp.zeros_like(dk_acc)
                    dv_acc[...] = jnp.zeros_like(dv_acc)

                masks = masks_of(m, here, first)
                block = q_ref[m, here]
                grad_block = ga_ref[here]
                result = jnp.zeros((tile, cols), F32)
                for head in range(heads):
                    query = one_head(block, head)
                    grad = one_head(grad_block, head)
                    level = lse_ref[m, head, here][:, :1]
                    prob = [
                        jnp.where(masks[h], jnp.exp(dot_nt(query, k_ref[h, m]) * scale - level), 0.0) for h in range(spans)
                    ]
                    grad_prob = [dot_nt(grad, v_ref[h, m]) for h in range(spans)]
                    mean = sum([jnp.sum(p * g, axis=-1, keepdims=True) for p, g in zip(prob, grad_prob)])
                    grad_scores = [(p * (g - mean)).astype(BF) for p, g in zip(prob, grad_prob)]
                    for h in range(spans):
                        dv_acc[h] += dot_tn(prob[h].astype(BF), grad)
                        dk_acc[h] += dot_tn(grad_scores[h], query)
                    mixed = sum([dot_nn(grad_scores[h], k_ref[h, m]) for h in range(spans)])
                    result = result + one_head(mixed, head)
                dq_ref[m, here] = (result * scale).astype(BF)

                @pl.when(half == 1)
                def _():
                    for h in range(hops, -1, -1):
                        grad_k = (dk_acc[h] * scale).astype(BF)
                        grad_v = dv_acc[h].astype(BF)
                        dkv_ref[h, m, :, :cols] = grad_k
                        dkv_ref[h, m, :, cols:] = grad_v
                        back = dot_nt(grad_k, wk_ref[...]) + dot_nt(grad_v, wv_ref[...])
                        if h == 0:
                            back = back + dot_nt(dq_ref[m], wq_ref[...])
                        attn_part[h, m] = back.astype(BF).reshape(2, 2, quarter, width)
                        rs_four.start(h, m)

                after(i, 0, lambda: ag_three.pass_on(0, 1), lambda: rs_layer.middle(0, 0), lambda: rs_layer.middle(0, 1))
                after(i, 1, lambda: ag_three.finish(0, 1), lambda: gr.spread(0), lambda: layer_sum(0), lambda: layer_sum(1))
                after(i, 2, *[functools.partial(rs_four.middle, h, 0) for h in range(hops, -1, -1)], lambda: gr.spread(1))
                after(i, 3, *[functools.partial(rs_four.hop, h, 0, total) for h in range(hops, 0, -1)], lambda: gr.spread(2))

            attn_all = attn_in[...].reshape(spans * streams * length, width)
            grads[3, :, cols : 3 * cols] = dot_tn(attn_all, flat(dkv_ref[...].reshape(-1, 2 * cols))).astype(BF)
            for h in range(hops, -1, -1):
                rs_four.middle(h, 1)
            grads[3, :, :cols] = dot_tn(flat(attn_in[0]), flat(dq_ref[...])).astype(BF)
            grads[3, :, 3 * cols :] = dot_tn(flat(grad_att[0]), flat(a_ref[...])).astype(BF)
            gr.start(3)
            for h in range(hops, 0, -1):
                rs_four.hop(h, 1, total)
            for m in range(streams):
                rs_four.total(m, total)
                grad_in, gain_grad = norm_back(hid_one[m], ag_ref[...], total[...])
                value = grad_two[m] + grad_in
                one_out[m] = value
                gain_out[0:1] = gain_grad if m == 0 else gain_out[0:1] + gain_grad
                stu_out[0, m, t] = value.astype(BF)
                ag_five.start(m)
                gr.collect(m, grad_acc)
                ag_layer.pass_on(0, m)
            gr.spread(3)
            for m in range(streams):
                ag_five.pass_on(0, m)
            gr.collect(2, grad_acc)
            for m in range(streams):
                ag_layer.finish(0, m)
            gr.collect(3, grad_acc)
            for m in range(streams):
                ag_five.finish(0, m)
            for k in range(chunks):
                gr.finish(k)
                gr.drain(k)
            for item in (rs_one, rs_two, rs_three, rs_layer, rs_four, ag_rows, ag_one, ag_two, ag_three, ag_layer, ag_five):
                item.drain()
            for h in far_back:
                pl.when(s + h < seq_count)(functools.partial(lambda h: id_copy(h, s + h).wait_send(), h))

        pl.run_scoped(
            attention_on,
            rows_of,
            pltpu.VMEM((spans, streams, length, cols), BF),
            pltpu.VMEM((spans, streams, length, cols), BF),
            rows_of,
            pltpu.VMEM((streams, heads, length, LANES), F32),
            unit_rows,
            unit_rows,
            unit_rows,
            pltpu.VMEM((length, cols), BF),
            pltpu.VMEM((spans, length, cols), F32),
            pltpu.VMEM((spans, length, cols), F32),
            rows_of,
            pltpu.VMEM((spans, streams, length, 2 * cols), BF),
        )

    anywhere = pl.BlockSpec(memory_space=pl.ANY)
    return pl.pallas_call(
        kernel,
        name="head",
        out_shape=(
            jax.ShapeDtypeStruct(gathered, BF),
            jax.ShapeDtypeStruct(gathered, BF),
            jax.ShapeDtypeStruct((streams, quarter, width), F32),
            jax.ShapeDtypeStruct((2, width), F32),
            jax.ShapeDtypeStruct((chunks, rows, units), F32),
            jax.ShapeDtypeStruct((lag_order, streams, length, channels), BF),
            jax.ShapeDtypeStruct((seq_count * streams, length), F32),
            jax.ShapeDtypeStruct((count, streams * length, width), BF),
            jax.ShapeDtypeStruct((count, LANES, wide), BF),
        ),
        in_specs=in_vmem(17),
        out_specs=tuple(in_vmem(7)) + (anywhere, anywhere),
        scratch_shapes=[
            pltpu.VMEM((streams, seq_count, 4, quarter, width), BF),
            pltpu.VMEM((seq_count,) + ids.shape, jnp.int32),
            pltpu.VMEM((streams, length, 1), F32),
            pltpu.VMEM((streams, length + 8, 1), F32),
            pltpu.VMEM((length + 8, channels), F32),
            split_part,
            pltpu.SemaphoreType.DMA((2, seq_count)),
            pltpu.SemaphoreType.DMA,
            pltpu.SemaphoreType.DMA((count,)),
            pltpu.VMEM((spans, streams, 4, quarter, width), BF),
            pltpu.VMEM(gathered, BF),
            pltpu.VMEM(gathered, BF),
            state,
            state,
            state,
            pltpu.VMEM((chunks, width, units), BF),
            pltpu.VMEM((quarter, width), F32),
            pltpu.VMEM((rows, units // 2), F32),
            split_part,
            split_part,
            split_part,
            pltpu.VMEM((spans, streams, 2, 2, quarter, width), BF),
            AllGather.scratch(seq_count - 1, streams)[0],
            AllGather.scratch(hops, streams)[0],
        ]
        + [AllGather.scratch(0, streams)[0]] * 4
        + zero_hops * 4
        + ReduceScatter.scratch(hops, streams, quarter, width)
        + GradReduce.scratch(seq_count, chunks, width, units),
        compiler_params=params(8),
    )(
        x, ids, stu_gain, filter_proj, lag_proj, base, base_back, attn_gain, feed_gain, wq, wk, wv, wo, wg, wu, wd, cot
    )


def tail(
    grad_stu, filter_proj, lag_proj, conv, lag_stack, ext_ids, strip_back, x, gain, grad_one, gains, seq_count
):
    count, length_all, width = conv.shape
    streams, _, quarter, _ = x.shape
    length = length_all // streams
    lag_order, channels = lag_proj.shape[:2]
    blocks = length // LANES
    hops = seq_count - 1
    chunks = count + 1
    steps = seq_count * streams
    rows = width // seq_count
    gain_rows = 8

    def kernel(
        gs_ref, fp_hbm, lp_ref, conv_hbm, lag_ref, ext_ref, strip_hbm, x_ref, gain_ref, one_ref, gains_ref,
        out, filter_out, lag_out, gain_out,
        conv_ref, fp_ref, strip, conv_sem, fp_sem, strip_sem, id_ext,
        mask, cols, left, acc, terms, grad_conv, grads, lag_ext, total, grad_acc, gather_sem,
        gain_own, gain_near, gain_sum, gain_far, near_sem, far_sem, *scratch,
    ):
        s, t, y, c, core, far = place()
        p = lax.axis_index("dp")
        rs_scratch, gr_scratch = scratch[:6], scratch[6:]

        def conv_copy(k):
            return pltpu.make_async_copy(conv_hbm.at[k], conv_ref.at[k], conv_sem.at[k])

        def fp_copy(k):
            return pltpu.make_async_copy(fp_hbm.at[k], fp_ref.at[k], fp_sem.at[k])

        strip_copy = pltpu.make_async_copy(strip_hbm, strip, strip_sem)
        for k in range(count):
            conv_copy(k).start()
            fp_copy(k).start()
        strip_copy.start()
        greet(seq_count, hops, wide=True, gains=True)

        def source(k):
            return grads.at[k]

        def result(k):
            return filter_out.at[k] if k < count else lag_out

        gr = GradReduce(seq_count, source, result, gr_scratch)
        rs = ReduceScatter(seq_count, hops, streams, lambda h, m: terms.at[h, m], rs_scratch)
        ag = AllGather(seq_count, 0, streams, out, gather_sem)

        early = min(2, count)

        @pl.loop(0, count)
        def _(k):
            conv_copy(k).wait()
            grads[k] = dot_tn(conv_ref[k], gs_ref[...]).astype(BF)
            gr.start(k)
            fp_copy(k).wait()
            product = dot_nt(gs_ref[...], fp_ref[k]).astype(BF)
            for m in range(streams):
                here = pl.ds(pl.multiple_of(k * length, LANES), length)
                grad_conv[m, here] = product[m * length : (m + 1) * length]

            @pl.when(k >= count - early)
            def _():
                gr.spread(k - (count - early))

        grads[count] = jnp.zeros_like(grads.at[count])
        for i in range(lag_order):
            grads[count, :, i * channels : (i + 1) * channels] = dot_tn(gs_ref[...], lag_ref[i]).astype(BF)
        gr.start(count)
        turned = jnp.transpose(ext_ref[...])
        for j in range(steps):
            cols[j] = turned[:, j : j + 1]
        for m in range(streams):
            lag_ext[m] = jnp.zeros_like(lag_ext.at[m])
            id_ext[:8] = turned[length - 8 :, streams + m : streams + m + 1]
            id_ext[8:] = turned[:, m : m + 1]
            for i in range(lag_order):
                term = dot_nt(gs_ref[m * length : (m + 1) * length], lp_ref[i])
                same = id_ext[7 - i : 7 - i + length] == cols[m]
                lag_ext[m, 7 - i : 7 - i + length] += jnp.where(same, term, 0.0)
        strip_copy.wait()
        mine = pl.ds(pl.multiple_of(t * channels, LANES), channels)
        spread_at = {}
        collect_at = {}
        for k in range(early, chunks):
            if 2 * (k - early) < steps:
                spread_at[2 * (k - early)] = k
        for k in range(chunks):
            if 2 * k + 3 < steps and k < early + len(spread_at):
                collect_at[2 * k + 3] = k

        def step_of(i):
            return seq_count - 1 - i // streams, i - i // streams * streams

        @pl.loop(0, steps)
        def _(i):
            h, m = step_of(i)

            @pl.when(h <= s)
            def _():
                mask[...] = jnp.where(cols[h * streams + m] == ext_ref[pl.ds(m, 1)], 1.0, 0.0).astype(BF)
                for k in range(count):
                    for a in range(blocks):
                        start = pl.multiple_of(LANES * (blocks * h + blocks - 1 - a), LANES)
                        down = slice(a * LANES, (a + 1) * LANES)
                        left[down, k * length : (k + 1) * length] = strip[k, :, pl.ds(start, length)] * mask[down]
                acc[...] = jnp.dot(left[...], grad_conv[m], preferred_element_type=F32)

                @pl.when(h == 0)
                def _():
                    acc[:, mine] += lag_ext[m, 8:]

                @pl.when(h == 1)
                def _():
                    acc[length - 8 :, mine] += lag_ext[m, :8]

                for quarter_y in range(2):
                    for quarter_c in range(2):
                        first = (2 * quarter_y + quarter_c) * quarter
                        terms[h, m, quarter_y, quarter_c] = acc[first : first + quarter].astype(BF)
                rs.start(h, m)

            @pl.when(i >= 1)
            def _():
                rs.middle(*step_of(i - 1))

            @pl.when((i >= 2) & (i < steps - streams + 2))
            def _():
                rs.hop(*step_of(i - 2), total)

            for step, k in spread_at.items():
                pl.when(i == step)(functools.partial(gr.spread, k))
            for step, k in collect_at.items():
                pl.when(i == step)(functools.partial(gr.collect, k, grad_acc))

        rs.middle(0, streams - 1)
        for k in range(early + len(spread_at), chunks):
            gr.spread(k)
        gain_own[...] = jnp.zeros_like(gain_own)
        for m in range(streams):
            rs.total(m, total)
            grad_in, gain_grad = norm_back(x_ref[m, t].astype(F32), gain_ref[...], total[...])
            out[0, m, t] = (one_ref[m] + grad_in).astype(BF)
            ag.start(m)
            gain_own[0:1] += gain_grad
        gain_own[1:3] = gains_ref[...]
        gain_near[t] = gain_own[...]

        def near_copy(j, slot):
            return remote(gain_own, gain_near.at[slot], near_sem.at[0, j], near_sem.at[1, slot], {"tensor": j})

        for j in range(4):
            pl.when(t != j)(lambda: near_copy(j, t).start())
        for m in range(streams):
            ag.pass_on(0, m)
        for k in range(len(collect_at), chunks):
            gr.collect(k, grad_acc)
        for j in range(4):
            pl.when(t != j)(lambda: near_copy(j, j).wait_recv())
        gain_sum[...] = gain_near[0] + gain_near[1] + gain_near[2] + gain_near[3]
        me = p * seq_count + s

        def far_copy(j, slot):
            d, q = j // seq_count, j % seq_count
            return remote(
                gain_sum.at[:, q * rows : (q + 1) * rows], gain_far.at[slot], far_sem.at[0, j], far_sem.at[1, slot],
                {"dp": d, "seq": q},
            )

        gain_far[me] = gain_sum[:, pl.ds(pl.multiple_of(s * rows, LANES), rows)]
        for j in range(2 * seq_count):
            pl.when(me != j)(lambda: far_copy(j, me).start())
        for m in range(streams):
            ag.finish(0, m)
        for k in range(chunks):
            gr.finish(k)
        for j in range(2 * seq_count):
            pl.when(me != j)(lambda: far_copy(j, j).wait_recv())
        gain_out[...] = functools.reduce(jnp.add, [gain_far[j] for j in range(2 * seq_count)])
        for j in range(4):
            pl.when(t != j)(lambda: near_copy(j, t).wait_send())
        for j in range(2 * seq_count):
            pl.when(me != j)(lambda: far_copy(j, me).wait_send())
        for k in range(chunks):
            gr.drain(k)
        rs.drain()
        ag.drain()

    anywhere = pl.BlockSpec(memory_space=pl.ANY)
    return pl.pallas_call(
        kernel,
        name="tail",
        out_shape=(
            jax.ShapeDtypeStruct((1, streams, 4, quarter, width), BF),
            jax.ShapeDtypeStruct((count, rows, width), F32),
            jax.ShapeDtypeStruct((rows, width), F32),
            jax.ShapeDtypeStruct((gain_rows, rows), F32),
        ),
        in_specs=[anywhere if i in (1, 3, 6) else spec for i, spec in enumerate(in_vmem(11))],
        out_specs=tuple(in_vmem(4)),
        scratch_shapes=[
            pltpu.VMEM(conv.shape, BF),
            pltpu.VMEM(filter_proj.shape, BF),
            pltpu.VMEM(strip_back.shape, BF),
            pltpu.SemaphoreType.DMA((count,)),
            pltpu.SemaphoreType.DMA((count,)),
            pltpu.SemaphoreType.DMA,
            pltpu.VMEM((length + 8, 1), F32),
            pltpu.VMEM((length, length), BF),
            pltpu.VMEM((steps, length, 1), F32),
            pltpu.VMEM((length, count * length), BF),
            pltpu.VMEM((length, width), F32),
            pltpu.VMEM((seq_count, streams, 2, 2, quarter, width), BF),
            pltpu.VMEM((streams, count * length, width), BF),
            pltpu.VMEM((chunks, width, width), BF),
            pltpu.VMEM((streams, length + 8, channels), F32),
            pltpu.VMEM((quarter, width), F32),
            pltpu.VMEM((rows, width // 2), F32),
            AllGather.scratch(0, streams)[0],
            pltpu.VMEM((gain_rows, width), F32),
            pltpu.VMEM((4, gain_rows, width), F32),
            pltpu.VMEM((gain_rows, width), F32),
            pltpu.VMEM((2 * seq_count, gain_rows, rows), F32),
            pltpu.SemaphoreType.DMA((2, 4)),
            pltpu.SemaphoreType.DMA((2, 2 * seq_count)),
        ]
        + ReduceScatter.scratch(hops, streams, quarter, width)
        + GradReduce.scratch(seq_count, chunks, width, width),
        compiler_params=params(7),
    )(
        grad_stu, filter_proj, lag_proj, conv, lag_stack, ext_ids, strip_back, x, gain, grad_one, gains
    )


def gated_unit(gate_pre, up_pre):
    return jax.nn.gelu(gate_pre, approximate=True) * up_pre


def local(
    seq_count,
    tokens,
    document_index,
    filters,
    stu_gain,
    filter_proj,
    lag_proj,
    attention_gain,
    query_weight,
    key_weight,
    value_weight,
    output_weight,
    feed_gain,
    gate_weight,
    up_weight,
    down_weight,
    cotangent,
):
    streams, _, length, width = tokens.shape
    row_len = length * seq_count
    quarter = length // 4
    lag_order, channels = lag_proj.shape[:2]
    count = filters.shape[0]
    hops = WINDOW // length
    tensor_place = lax.axis_index("tensor")
    chan_start = tensor_place * channels

    def split(a):
        return a.reshape(a.shape[:-2] + (2, 2, quarter, width))

    def quarters(a):
        return a.reshape(a.shape[:-2] + (4, quarter, width))

    def whole(a):
        return a.reshape(a.shape[:-3] + (length, width))

    def row(gain):
        return gain.reshape(1, width)

    x = tokens[:, 0]
    grad_three = cotangent[:, 0]
    ids = document_index[:, 0]
    id_tile = ids.reshape(streams * length // LANES, LANES)
    pad = jnp.zeros((count, 4 * LANES), filters.dtype)
    ahead = row_len - LANES
    base = jnp.concatenate(
        [
            jnp.flip(filters[:, : ahead + 1], axis=1),
            pad[:, : 4 * LANES],
            jnp.flip(filters[:, ahead + 1 :], axis=1),
        ],
        axis=1,
    ).astype(F32)[:, None]
    base_back = jnp.concatenate(
        [pad[:, : length - LANES], filters, pad[:, :LANES]], axis=1
    ).astype(F32)[:, None]

    tokens_flat = streams * length
    cols = query_weight.shape[1]

    def answer(layer_output, input_gradient, gains, filter_grad, lag_grad, attn_grads, feed_grads):
        query_grad, key_grad, value_grad, output_grad = jnp.split(attn_grads, [cols, 2 * cols, 3 * cols], axis=1)
        gate_grad, up_grad, down_grad = feed_grads
        return (
            layer_output[:, None],
            input_gradient[:, None],
            gains[0],
            filter_grad,
            lag_grad[:, : lag_order * channels].T.reshape(lag_order, channels, -1),
            gains[1],
            query_grad,
            key_grad,
            value_grad,
            output_grad.T,
            gains[2],
            gate_grad,
            up_grad,
            down_grad.T,
        )

    if width // seq_count % LANES == 0:
        grad_stu, layer_output, grad_one, gain_grads, sums, lag_stack, ext_ids, conv, strip_back = head(
            quarters(x), id_tile, row(stu_gain), filter_proj, lag_proj, base, base_back, row(attention_gain), row(feed_gain),
            query_weight, key_weight, value_weight, output_weight, gate_weight, up_weight, down_weight, grad_three, seq_count,
        )
        input_gradient, filter_grad, lag_grad, gains = tail(
            grad_stu.reshape(tokens_flat, width), filter_proj, lag_proj, conv,
            lag_stack.reshape(lag_order, tokens_flat, channels), ext_ids, strip_back, quarters(x), row(stu_gain), grad_one,
            gain_grads, seq_count,
        )
        return answer(
            whole(layer_output)[0], whole(input_gradient)[0], gains, filter_grad, lag_grad, sums[3], (sums[0], sums[1], sums[2])
        )

    inputs = norm_of(x.astype(F32), stu_gain).astype(BF)
    rows_ext, id_ext = gather_rows(quarters(inputs), id_tile, seq_count)
    rows_ext = whole(rows_ext)
    id_ext = id_ext.reshape(seq_count, streams, length)
    id_rows = id_ext[:, :, None, :]
    id_cols = id_ext[:, :, :, None]

    conv = convolve(rows_ext, id_rows, id_cols[0], base, seq_count)

    chan_rows = lax.dynamic_slice_in_dim(rows_ext[:2], chan_start, channels, 3)
    joined = jnp.concatenate([chan_rows[1][:, length - lag_order :], chan_rows[0]], axis=1)
    joined_ids = jnp.concatenate([id_ext[1][:, length - lag_order :], ids], axis=1)
    masks = []
    lagged = []
    for step in range(1, lag_order + 1):
        low = lag_order - step
        masks.append((joined_ids[:, low : low + length] == ids)[:, :, None])
        lagged.append(jnp.where(masks[-1], joined[:, low : low + length], jnp.zeros((), BF)))
    lag_stack = jnp.stack(lagged)

    mixed = jnp.einsum("kmtd,kde->mte", conv, filter_proj, preferred_element_type=F32)
    mixed = mixed + jnp.einsum("imtc,ice->mte", lag_stack, lag_proj, preferred_element_type=F32)

    state = jax.ShapeDtypeStruct((streams, quarter, width), F32)
    gain_state = jax.ShapeDtypeStruct((1, width), F32)

    def finish_one(m, total, others, extra):
        x_ref, gain_ref = others
        hidden = x_ref[m, place()[1]].astype(F32) + total
        extra[0][m] = hidden
        return norm_of(hidden, gain_ref[...]).astype(BF)

    attn_ext, hidden_one = exchange(
        "exchange_one", 2, seq_count, [split(mixed.astype(BF))[None]], [quarters(x), row(attention_gain)], 0, hops,
        finish_one, [state],
    )
    attn_ext = whole(attn_ext)

    q, k, v, attended, lse, out_part = attend(
        attn_ext, id_rows[: hops + 1], id_cols[0], query_weight, key_weight, value_weight, output_weight
    )

    def finish_two(m, total, others, extra):
        hidden_ref, gain_ref = others
        hidden = hidden_ref[m] + total
        extra[0][m] = hidden
        return norm_of(hidden, gain_ref[...]).astype(BF)

    feed_in, hidden_two = exchange(
        "exchange_two", 3, seq_count, [split(out_part)[None]], [hidden_one, row(feed_gain)], 0, 0, finish_two, [state]
    )
    feed_in = whole(feed_in)[0].reshape(streams * length, width)
    flat_three = grad_three.reshape(streams * length, width)

    gate_pre = dot_nn(feed_in, gate_weight)
    up_pre = dot_nn(feed_in, up_weight)
    grad_inner = dot_nt(flat_three, down_weight)
    unit, pull = jax.vjp(gated_unit, gate_pre, up_pre)
    inner = unit.astype(BF)
    grad_gate, grad_up = pull(grad_inner)
    grad_gate = grad_gate.astype(BF)
    grad_up = grad_up.astype(BF)
    layer_part = dot_nn(inner, down_weight).astype(BF)
    feed_part = (dot_nt(grad_gate, gate_weight) + dot_nt(grad_up, up_weight)).astype(BF)

    def finish_three(m, total, others, extra):
        hidden_ref, gain_ref, cot_ref = others
        if m >= streams:
            return (hidden_ref[m - streams] + total).astype(BF)
        grad_in, gain_grad = norm_back(hidden_ref[m], gain_ref[...], total)
        grad_two = cot_ref[m, place()[1]].astype(F32) + grad_in
        extra[0][m] = grad_two
        extra[1][...] = gain_grad if m == 0 else extra[1][...] + gain_grad
        return grad_two.astype(BF)

    feed_grads = jnp.stack(
        [
            dot_tn(feed_in, grad_gate).astype(BF),
            dot_tn(feed_in, grad_up).astype(BF),
            dot_tn(flat_three, inner).astype(BF),
        ]
    )
    shape = (1, streams, length, width)
    both, grad_two, feed_gain_grad = exchange(
        "exchange_three", 4, seq_count, [split(feed_part.reshape(shape)), split(layer_part.reshape(shape))],
        [hidden_two, row(feed_gain), quarters(grad_three)], 0, 0, finish_three, [state, gain_state],
    )
    both = whole(both)[0]
    grad_att_out = both[:streams]
    layer_output = both[streams:]

    dq, dk, dv, attn_part = attend_back(
        q, k, v, lse, grad_att_out, id_rows[: hops + 1], id_cols[0], query_weight, key_weight, value_weight, output_weight
    )

    go = grad_att_out.reshape(tokens_flat, width)
    attn_grads = jnp.concatenate(
        [
            dot_tn(attn_ext[0].reshape(tokens_flat, width), dq.reshape(tokens_flat, -1)).astype(BF),
            dot_tn(attn_ext.reshape(-1, width), dk.reshape(-1, dk.shape[-1])).astype(BF),
            dot_tn(attn_ext.reshape(-1, width), dv.reshape(-1, dv.shape[-1])).astype(BF),
            dot_tn(go, attended.reshape(tokens_flat, -1)).astype(BF),
        ],
        axis=1,
    )

    def finish_four(m, total, others, extra):
        hidden_ref, gain_ref, grad_ref = others
        grad_in, gain_grad = norm_back(hidden_ref[m], gain_ref[...], total)
        grad_one = grad_ref[m] + grad_in
        extra[0][m] = grad_one
        extra[1][...] = gain_grad if m == 0 else extra[1][...] + gain_grad
        return grad_one.astype(BF)

    grad_stu, grad_one, attn_gain_grad = exchange(
        "exchange_four", 5, seq_count, [split(attn_part)], [hidden_one, row(attention_gain), grad_two], hops, 0,
        finish_four, [state, gain_state],
    )
    grad_stu = whole(grad_stu)[0]
    grad_conv = jnp.einsum("mte,kde->kmtd", grad_stu, filter_proj, preferred_element_type=F32).astype(BF)
    grad_lagged = jnp.einsum("mte,ice->imtc", grad_stu, lag_proj, preferred_element_type=F32)
    ext_grad = jnp.zeros((streams, 8 + length, channels), F32)
    for step in range(1, lag_order + 1):
        term = jnp.where(masks[step - 1], grad_lagged[step - 1], 0.0)
        ext_grad = ext_grad + jnp.pad(term, ((0, 0), (8 - step, step), (0, 0)))
    terms = convolve_back(
        grad_conv, id_rows[0], id_cols, base_back, ext_grad[:, 8:], ext_grad[:, :8], seq_count
    )

    def finish_five(m, total, others, extra):
        x_ref, gain_ref, grad_ref = others
        grad_in, gain_grad = norm_back(x_ref[m, place()[1]].astype(F32), gain_ref[...], total)
        extra[0][...] = gain_grad if m == 0 else extra[0][...] + gain_grad
        return (grad_ref[m] + grad_in).astype(BF)

    input_gradient, stu_gain_grad = exchange(
        "exchange_five", 6, seq_count, [split(terms)], [quarters(x), row(stu_gain), grad_one], seq_count - 1, 0,
        finish_five, [gain_state],
    )
    input_gradient = whole(input_gradient)[0]
    stu = grad_stu.reshape(tokens_flat, width)
    filter_part = jnp.einsum("kmtd,mte->kde", conv, grad_stu, preferred_element_type=F32).astype(BF)
    lag_part = jnp.concatenate(
        [dot_tn(stu, lag_stack[i].reshape(tokens_flat, channels)).astype(BF) for i in range(lag_order)], axis=1
    )
    feed_grads = lax.psum(
        lax.psum_scatter(feed_grads, "seq", scatter_dimension=1, tiled=True), "dp"
    ).astype(F32)
    attn_grads = lax.psum(lax.psum_scatter(attn_grads, "seq", scatter_dimension=0, tiled=True), "dp").astype(F32)
    filter_grad = lax.psum(
        lax.psum_scatter(filter_part, "seq", scatter_dimension=1, tiled=True), "dp"
    ).astype(F32)
    lag_grad = lax.psum(lax.psum_scatter(lag_part, "seq", scatter_dimension=0, tiled=True), "dp").astype(F32)
    gains = jnp.concatenate([stu_gain_grad, attn_gain_grad, feed_gain_grad], axis=0)
    gains = lax.psum(gains, ("dp", "seq", "tensor"))
    gain_width = width // seq_count
    gains = lax.dynamic_slice_in_dim(gains, lax.axis_index("seq") * gain_width, gain_width, 1)
    return answer(layer_output, input_gradient, gains, filter_grad, lag_grad, attn_grads, feed_grads)


def solution(mesh):
    return jax.shard_map(
        functools.partial(local, mesh.shape["seq"]),
        mesh=mesh,
        in_specs=(
            P(None, "dp", "seq", None),
            P(None, "dp", "seq"),
            P("tensor", None),
            P(),
            P("tensor", None, None),
            P(None, "tensor", None),
            P(),
            P(None, "tensor"),
            P(None, "tensor"),
            P(None, "tensor"),
            P("tensor", None),
            P(),
            P(None, "tensor"),
            P(None, "tensor"),
            P("tensor", None),
            P(None, "dp", "seq", None),
        ),
        out_specs=(
            P(None, "dp", "seq", None),
            P(None, "dp", "seq", None),
            P("seq"),
            P("tensor", "seq", None),
            P(None, "tensor", "seq"),
            P("seq"),
            P("seq", "tensor"),
            P("seq", "tensor"),
            P("seq", "tensor"),
            P("tensor", "seq"),
            P("seq"),
            P("seq", "tensor"),
            P("seq", "tensor"),
            P("tensor", "seq"),
        ),
        check_vma=False,
    )
```

```python
import functools

import jax
import jax.numpy as jnp
from jax import lax
from jax.experimental import pallas as pl
from jax.experimental.pallas import tpu as pltpu
from jax.sharding import PartitionSpec as P

HD = 64
WINDOW = 1024
EPSILON = 1e-05
LANES = 128
NEGATIVE = -1e30
MESH = pl.DeviceIdType.MESH
BF = jnp.bfloat16
F32 = jnp.float32
VMEM_LIMIT = 63 * 1024 * 1024


def place():
    s = lax.axis_index("seq")
    t = lax.axis_index("tensor")
    y = t // 2
    c = t - 2 * y
    return s, t, y, c, t + 1 - 2 * c, t + 2 - 4 * y


def when(condition, action):
    if condition is True:
        action()
    else:
        pl.when(condition)(action)


def remote(src, dst, send_sem, recv_sem, device):
    return pltpu.make_async_remote_copy(
        src_ref=src, dst_ref=dst, send_sem=send_sem, recv_sem=recv_sem, device_id=device, device_id_type=MESH
    )


def greet(seq_count, hops, wide=False, gains=False):
    s, t, y, c, core, far = place()
    barrier = pltpu.get_barrier_semaphore()

    def signal(device):
        pl.semaphore_signal(barrier, inc=1, device_id=device, device_id_type=MESH)

    signal({"tensor": core})
    signal({"tensor": far})
    if gains:
        signal({"tensor": 3 - t})
    if wide:
        p = lax.axis_index("dp")
        signal({"dp": 1 - p})
        for j in range(seq_count):

            @pl.when(s != j)
            def _():
                signal({"seq": j})
                if gains:
                    signal({"dp": 1 - p, "seq": j})

        peers = 2 + gains + 1 + (seq_count - 1) * (1 + gains)
    else:
        for h in range(1, hops + 1):
            for there, peer in ((s - h >= 0, s - h), (s + h < seq_count, s + h)):

                @pl.when(there)
                def _():
                    signal({"seq": peer})

        peers = 2 + jnp.minimum(s, hops) + jnp.minimum(seq_count - 1 - s, hops)
    pl.semaphore_wait(barrier, peers)


class ReduceScatter:
    def __init__(self, seq_count, hops, streams, part, scratch):
        self.seq_count, self.hops, self.streams, self.part = seq_count, hops, streams, part
        self.near, self.half, self.over, self.hop_out, self.hop_in, self.sem = scratch

    @staticmethod
    def scratch(hops, streams, rows, width):
        quarter = (hops + 1, streams, rows, width)
        over_seq = quarter if hops else (1, 1, 16, LANES)
        return [
            pltpu.VMEM((hops + 1, streams, 2, rows, width), BF),
            pltpu.VMEM(quarter, BF),
            pltpu.VMEM(quarter, BF),
            pltpu.VMEM(over_seq, BF),
            pltpu.VMEM(over_seq, BF),
            pltpu.SemaphoreType.DMA((6, hops + 1, streams)),
        ]

    def to_core(self, h, m):
        s, t, y, c, core, far = place()
        return remote(
            self.part(h, m).at[:, 1 - c], self.near.at[h, m], self.sem.at[0, h, m], self.sem.at[1, h, m], {"tensor": core}
        )

    def to_far(self, h, m):
        s, t, y, c, core, far = place()
        return remote(self.half.at[h, m], self.over.at[h, m], self.sem.at[2, h, m], self.sem.at[3, h, m], {"tensor": far})

    def to_hop(self, h, m, peer):
        return remote(
            self.hop_out.at[h, m], self.hop_in.at[h - 1, m], self.sem.at[4, h, m], self.sem.at[5, h - 1, m], {"seq": peer}
        )

    def add_hop(self, h, m, acc):
        s = lax.axis_index("seq")

        @pl.when(s + 1 < self.seq_count)
        def _():
            remote(
                self.hop_out.at[h, m], self.hop_in.at[h, m], self.sem.at[4, h, m], self.sem.at[5, h, m], {"seq": s + 1}
            ).wait_recv()
            acc[...] += self.hop_in[h, m].astype(F32)

    def there(self, h):
        return True if isinstance(h, int) and h == 0 else lax.axis_index("seq") - h >= 0

    def order(self):
        return [(h, m) for h in range(self.hops, -1, -1) for m in range(self.streams)]

    def start(self, h, m):
        when(self.there(h), lambda: self.to_core(h, m).start())

    def middle(self, h, m):
        s, t, y, c, core, far = place()

        def act():
            self.to_core(h, m).wait_recv()
            mine = self.part(h, m)[1 - y, c].astype(F32) + self.near[h, m, 1 - y].astype(F32)
            self.half[h, m] = mine.astype(BF)
            self.to_far(h, m).start()

        when(self.there(h), act)

    def own(self, h, m):
        s, t, y, c, core, far = place()
        self.to_far(h, m).wait_recv()
        return (
            self.part(h, m)[y, c].astype(F32) + self.near[h, m, y].astype(F32) + self.over[h, m].astype(F32)
        )

    def hop(self, h, m, acc):
        def act():
            acc[...] = self.own(h, m)
            if isinstance(h, int):
                if h < self.hops:
                    self.add_hop(h, m, acc)
            else:
                pl.when(h < self.hops)(lambda: self.add_hop(h, m, acc))
            self.hop_out[h, m] = acc[...].astype(BF)
            self.to_hop(h, m, lax.axis_index("seq") - 1).start()

        when(self.there(h), act)

    def total(self, m, acc):
        acc[...] = self.own(0, m)
        if self.hops:
            self.add_hop(0, m, acc)

    def drain(self):
        for h, m in self.order():

            def act():
                self.to_core(h, m).wait_send()
                self.to_far(h, m).wait_send()
                if h:
                    self.to_hop(h, m, lax.axis_index("seq") - 1).wait_send()

            when(self.there(h), act)


class AllGather:
    def __init__(self, seq_count, hops, streams, at, sem, first=0):
        self.seq_count, self.hops, self.streams, self.sem, self.first = seq_count, hops, streams, sem, first
        self.at = at if callable(at) else lambda h, m, quarter: at.at[h, m, quarter]

    @staticmethod
    def scratch(hops, streams):
        return [pltpu.SemaphoreType.DMA((8, hops + 1, streams))]

    def there(self, h):
        return True if h == 0 else lax.axis_index("seq") - h >= 0

    def copy(self, kind, h, m, quarter, device):
        ref = self.at(h, m, quarter)
        return remote(ref, ref, self.sem.at[2 * kind, h, m], self.sem.at[2 * kind + 1, h, m], device)

    def relay(self, h, m):
        s, t = lax.axis_index("seq"), place()[1]
        return remote(
            self.at(h, m, t), self.at(h + 1, m, t), self.sem.at[0, h, m], self.sem.at[1, h + 1, m], {"seq": s + 1}
        )

    def relays(self, h):
        s = lax.axis_index("seq")
        return (s - h >= 0) & (s + 1 < self.seq_count)

    def forward(self, h, m):
        if h < self.hops:
            pl.when(self.relays(h))(lambda: self.relay(h, m).start())

    def spread(self, h, m):
        s, t, y, c, core, far = place()
        self.copy(1, h, m, t, {"tensor": far}).start()
        self.copy(2, h, m, t, {"tensor": core}).start()

    def start(self, m):
        self.forward(0, m)
        if self.first == 0:
            self.spread(0, m)

    def arrive(self, h, m):
        @pl.when(self.there(h))
        def _():
            self.copy(0, h, m, place()[1], {"seq": lax.axis_index("seq") - 1}).wait_recv()

        self.forward(h, m)
        pl.when(self.there(h))(lambda: self.spread(h, m))

    def pass_on(self, h, m):
        s, t, y, c, core, far = place()

        def act():
            self.copy(1, h, m, far, {"tensor": far}).wait_recv()
            self.copy(3, h, m, far, {"tensor": core}).start()

        when(self.there(h), act)

    def finish(self, h, m):
        s, t, y, c, core, far = place()

        def act():
            self.copy(2, h, m, core, {"tensor": core}).wait_recv()
            self.copy(3, h, m, 3 - t, {"tensor": core}).wait_recv()

        when(self.there(h), act)

    def clear(self, h, m):
        @pl.when(lax.axis_index("seq") - h < 0)
        def _():
            for quarter in range(4):
                ref = self.at(h, m, quarter)
                ref[...] = jnp.zeros(ref.shape, ref.dtype)

    def drain(self):
        s, t, y, c, core, far = place()
        for m in range(self.streams):
            for h in range(self.hops):
                pl.when(self.relays(h))(functools.partial(lambda h, m: self.relay(h, m).wait_send(), h, m))
            for h in range(self.first, self.hops + 1):

                def act():
                    self.copy(1, h, m, t, {"tensor": far}).wait_send()
                    self.copy(2, h, m, t, {"tensor": core}).wait_send()
                    self.copy(3, h, m, far, {"tensor": core}).wait_send()

                when(self.there(h), act)


class GradReduce:
    def __init__(self, seq_count, source, result, scratch):
        self.seq_count, self.source, self.result = seq_count, source, result
        self.x_in, self.z_out, self.z_in, self.back_out, self.back_in, self.x_sem, self.z_sem, self.back_sem = scratch
        self.half = self.x_in.shape[2]
        self.rows = self.back_out.shape[1]

    @staticmethod
    def scratch(seq_count, chunks, depth, width):
        rows, half = depth // seq_count, width // 2
        return [
            pltpu.VMEM((chunks, depth, half), BF),
            pltpu.VMEM((chunks, depth, half), BF),
            pltpu.VMEM((chunks, seq_count, rows, half), BF),
            pltpu.VMEM((chunks, rows, half), BF),
            pltpu.VMEM((chunks, rows, half), BF),
            pltpu.SemaphoreType.DMA((2, chunks)),
            pltpu.SemaphoreType.DMA((2, chunks, seq_count)),
            pltpu.SemaphoreType.DMA((2, chunks)),
        ]

    def columns(self, p):
        return pl.ds(pl.multiple_of(p * self.half, LANES), self.half)

    def block(self, j):
        return pl.ds(pl.multiple_of(j * self.rows, 16), self.rows)

    def over(self, c):
        p = lax.axis_index("dp")
        return remote(
            self.source(c).at[:, self.columns(1 - p)], self.x_in.at[c], self.x_sem.at[0, c], self.x_sem.at[1, c], {"dp": 1 - p}
        )

    def row_copy(self, c, j, slot):
        return remote(
            self.z_out.at[c, self.block(j)], self.z_in.at[c, slot], self.z_sem.at[0, c, j], self.z_sem.at[1, c, slot], {"seq": j}
        )

    def back(self, c):
        p = lax.axis_index("dp")
        return remote(
            self.back_out.at[c], self.back_in.at[c], self.back_sem.at[0, c], self.back_sem.at[1, c], {"dp": 1 - p}
        )

    def others(self, action):
        for j in range(self.seq_count):
            pl.when(lax.axis_index("seq") != j)(functools.partial(action, j))

    def start(self, c):
        self.over(c).start()

    def spread(self, c):
        s, p = lax.axis_index("seq"), lax.axis_index("dp")
        self.over(c).wait_recv()
        mine = self.source(c)[:, self.columns(p)].astype(F32) + self.x_in[c].astype(F32)
        self.z_out[c] = mine.astype(BF)
        self.others(lambda j: self.row_copy(c, j, s).start())

    def collect(self, c, acc):
        s, p = lax.axis_index("seq"), lax.axis_index("dp")
        here = self.block(s)
        acc[...] = self.source(c)[here, self.columns(p)].astype(F32) + self.x_in[c, here].astype(F32)

        def add(j):
            self.row_copy(c, j, j).wait_recv()
            acc[...] += self.z_in[c, j].astype(F32)

        self.others(add)
        self.back_out[c] = acc[...].astype(BF)
        self.back(c).start()

    def finish(self, c):
        p = lax.axis_index("dp")
        self.back(c).wait_recv()
        self.result(c)[:, self.columns(p)] = self.back_out[c]
        self.result(c)[:, self.columns(1 - p)] = self.back_in[c]

    def drain(self, c):
        self.over(c).wait_send()
        self.others(lambda j: self.row_copy(c, j, lax.axis_index("seq")).wait_send())
        self.back(c).wait_send()


def params(cid=None):
    if cid is None:
        return pltpu.CompilerParams(vmem_limit_bytes=VMEM_LIMIT)
    return pltpu.CompilerParams(vmem_limit_bytes=VMEM_LIMIT, collective_id=cid, has_side_effects=True)


def in_vmem(count):
    return [pl.BlockSpec(memory_space=pltpu.VMEM)] * count


def gather_rows(inputs, ids, seq_count):
    streams, quarters, rows, width = inputs.shape
    hops = seq_count - 1

    def kernel(x_ref, id_ref, out, out_ids, sem, id_sem):
        s, t, y, c, core, far = place()
        greet(seq_count, hops)
        out[0] = x_ref[...]
        out_ids[0] = id_ref[...]
        ag = AllGather(seq_count, hops, streams, out, sem, first=1)

        def id_copy(h, peer):
            return remote(id_ref, out_ids.at[h], id_sem.at[0, h], id_sem.at[1, h], {"seq": peer})

        for h in range(1, hops + 1):

            @pl.when(s + h < seq_count)
            def _():
                id_copy(h, s + h).start()

        for m in range(streams):
            ag.start(m)
        for h in range(1, hops + 1):
            for m in range(streams):
                ag.clear(h, m)

            @pl.when(s - h < 0)
            def _():
                out_ids[h] = jnp.full(out_ids.shape[1:], -1, jnp.int32)

        for m in range(streams):
            for h in range(1, hops + 1):
                ag.arrive(h, m)
        for m in range(streams):
            for h in range(1, hops + 1):
                ag.pass_on(h, m)
        for h in range(1, hops + 1):
            for m in range(streams):
                ag.finish(h, m)

            @pl.when(s - h >= 0)
            def _():
                id_copy(h, s - h).wait_recv()

            @pl.when(s + h < seq_count)
            def _():
                id_copy(h, s + h).wait_send()

        ag.drain()

    return pl.pallas_call(
        kernel,
        name="gather_rows",
        out_shape=(
            jax.ShapeDtypeStruct((seq_count,) + inputs.shape, inputs.dtype),
            jax.ShapeDtypeStruct((seq_count,) + ids.shape, jnp.int32),
        ),
        in_specs=in_vmem(2),
        out_specs=tuple(in_vmem(2)),
        scratch_shapes=AllGather.scratch(hops, streams) + [pltpu.SemaphoreType.DMA((2, seq_count))],
        compiler_params=params(1),
    )(inputs, ids)


def exchange(name, cid, seq_count, parts, others, reduce_hops, gather_hops, finish, extra):
    per_part = parts[0].shape[1]
    rows, width = parts[0].shape[4:]
    streams = per_part * len(parts)
    hops = max(reduce_hops, gather_hops)

    def kernel(*refs):
        refs = list(refs)
        part_refs = [refs.pop(0) for _ in parts]
        other_refs = [refs.pop(0) for _ in others]
        out = refs.pop(0)
        extra_refs = [refs.pop(0) for _ in extra]
        acc = refs.pop(0)
        gather_sem = refs.pop(0)
        s, t, y, c, core, far = place()
        greet(seq_count, hops)
        rs = ReduceScatter(
            seq_count, reduce_hops, streams, lambda h, m: part_refs[m // per_part].at[h, m % per_part], refs
        )
        ag = AllGather(seq_count, gather_hops, streams, out, gather_sem)
        for h, m in rs.order():
            rs.start(h, m)
        for h in range(1, gather_hops + 1):
            for m in range(streams):
                ag.clear(h, m)
        for h, m in rs.order():
            rs.middle(h, m)
        for h, m in rs.order():
            if h:
                rs.hop(h, m, acc)
        for m in range(streams):
            rs.total(m, acc)
            out[0, m, t] = finish(m, acc[...], other_refs, extra_refs)
            ag.start(m)
        for m in range(streams):
            ag.pass_on(0, m)
            for h in range(1, gather_hops + 1):
                ag.arrive(h, m)
        for m in range(streams):
            for h in range(1, gather_hops + 1):
                ag.pass_on(h, m)
        for h in range(gather_hops + 1):
            for m in range(streams):
                ag.finish(h, m)
        rs.drain()
        ag.drain()

    return pl.pallas_call(
        kernel,
        name=name,
        out_shape=(jax.ShapeDtypeStruct((gather_hops + 1, streams, 4, rows, width), BF),) + tuple(extra),
        in_specs=in_vmem(len(parts) + len(others)),
        out_specs=tuple(in_vmem(1 + len(extra))),
        scratch_shapes=[pltpu.VMEM((rows, width), F32)]
        + AllGather.scratch(gather_hops, streams)
        + ReduceScatter.scratch(reduce_hops, streams, rows, width),
        compiler_params=params(cid),
    )(*parts, *others)


def norm_of(values, gain_row):
    inverse = lax.rsqrt(jnp.mean(values * values, axis=-1, keepdims=True) + EPSILON)
    return values * inverse * gain_row


def norm_back(values, gain_row, grad_out):
    inverse = lax.rsqrt(jnp.mean(values * values, axis=-1, keepdims=True) + EPSILON)
    scaled = grad_out * gain_row
    dot = jnp.mean(scaled * values, axis=-1, keepdims=True)
    grad_in = inverse * scaled - values * (inverse * inverse * inverse) * dot
    return grad_in, jnp.sum(grad_out * values * inverse, axis=0, keepdims=True)


def strips(base_ref, strip):
    @pl.loop(0, base_ref.shape[0])
    def _(k):
        taps = base_ref[k] if len(base_ref.shape) == 3 else base_ref[pl.ds(k, 1)]
        row = jnp.broadcast_to(taps, strip.shape[1:])
        strip[k] = pltpu.roll(row, 0, 1, stride=1, stride_axis=0).astype(BF)


def lay_taps(taps_ref, base_ref, back):
    count, length = taps_ref.shape
    blocks = length // LANES
    base_ref[...] = jnp.zeros_like(base_ref)
    if back:
        base_ref[:, 3 * LANES : 3 * LANES + length] = taps_ref[...].astype(F32)
        return
    row = lax.broadcasted_iota(jnp.int32, (LANES, LANES), 0)
    lane = lax.broadcasted_iota(jnp.int32, (LANES, LANES), 1)
    turn = jnp.where(row + lane == LANES, 1.0, 0.0).astype(BF)
    first = lax.broadcasted_iota(jnp.int32, (count, LANES), 1) == 0
    turned = [dot_nn(taps_ref[:, j * LANES : (j + 1) * LANES], turn) for j in range(blocks)]
    for b in range(blocks):
        j = blocks - 1 - b
        below = turned[j - 1] if j else jnp.zeros((count, LANES), F32)
        taps = taps_ref[:, j * LANES : (j + 1) * LANES].astype(F32)
        base_ref[:, b * LANES : (b + 1) * LANES] = jnp.where(first, taps, below)
    base_ref[:, (blocks + 3) * LANES :] = turned[blocks - 1]


def convolve(rows, row_ids, col_ids, base, seq_count):
    _, streams, length, width = rows.shape
    count, _, wide = base.shape
    blocks = length // LANES
    at_once = seq_count <= 4

    def whole_kernel(x_ref, row_ref, col_ref, base_ref, out_ref, strip, mask, left):
        strips(base_ref, strip)

        @pl.loop(0, streams)
        def _(m):
            for h in range(seq_count):
                mask[:, h * length : (h + 1) * length] = jnp.where(col_ref[m] == row_ref[h, m], 1.0, 0.0).astype(BF)
            right = jnp.concatenate([x_ref[h, m] for h in range(seq_count)], axis=0)

            @pl.loop(0, count)
            def _(k):
                for a in range(blocks):
                    for h in range(seq_count):
                        start = LANES * (blocks * (seq_count - h) - 1 - a)
                        down, across = slice(a * LANES, (a + 1) * LANES), slice(h * length, (h + 1) * length)
                        left[down, across] = strip[k, :, start : start + length] * mask[down, across]
                out_ref[k, m] = jnp.dot(left[...], right, preferred_element_type=F32).astype(BF)

    def kernel(x_ref, row_ref, col_ref, base_ref, out_ref, strip, mask, acc):
        strips(base_ref, strip)
        s = lax.axis_index("seq")

        @pl.loop(0, streams)
        def _(m):
            acc[...] = jnp.zeros_like(acc)

            @pl.loop(0, s + 1)
            def _(h):
                mask[...] = jnp.where(col_ref[m] == row_ref[h, m], 1.0, 0.0).astype(BF)

                @pl.loop(0, count)
                def _(k):
                    pieces = []
                    for a in range(blocks):
                        start = pl.multiple_of(LANES * (blocks * (seq_count - h) - 1 - a), LANES)
                        pieces.append(strip[k, :, pl.ds(start, length)] * mask[a * LANES : (a + 1) * LANES])
                    acc[k] += jnp.dot(jnp.concatenate(pieces, axis=0), x_ref[h, m], preferred_element_type=F32)

            @pl.loop(0, count)
            def _(k):
                out_ref[k, m] = acc[k].astype(BF)

    span = seq_count * length if at_once else length
    return pl.pallas_call(
        whole_kernel if at_once else kernel,
        name="convolve",
        out_shape=jax.ShapeDtypeStruct((count, streams, length, width), BF),
        in_specs=in_vmem(4),
        out_specs=in_vmem(1)[0],
        scratch_shapes=[
            pltpu.VMEM((count, LANES, wide), BF),
            pltpu.VMEM((length, span), BF),
            pltpu.VMEM((length, span), BF) if at_once else pltpu.VMEM((count, length, width), F32),
        ],
        compiler_params=params(),
    )(rows, row_ids, col_ids, base)


def convolve_back(grads, row_ids, col_ids, base, own_lag, tail_lag, seq_count):
    count, streams, length, width = grads.shape
    wide = base.shape[2]
    blocks = length // LANES
    channels = own_lag.shape[2]
    tail_rows = tail_lag.shape[1]

    def kernel(g_ref, row_ref, col_ref, base_ref, own_ref, tail_ref, out_ref, strip, mask, acc):
        strips(base_ref, strip)
        s = lax.axis_index("seq")
        mine = pl.ds(pl.multiple_of(lax.axis_index("tensor") * channels, LANES), channels)

        @pl.loop(0, s + 1)
        def _(h):
            @pl.loop(0, streams)
            def _(m):
                mask[...] = jnp.where(col_ref[h, m] == row_ref[m], 1.0, 0.0).astype(BF)
                acc[...] = jnp.zeros_like(acc)

                @pl.when(h == 0)
                def _():
                    acc[:, mine] = own_ref[m]

                @pl.when(h == 1)
                def _():
                    acc[length - tail_rows :, mine] = tail_ref[m]

                @pl.loop(0, count)
                def _(k):
                    pieces = []
                    for a in range(blocks):
                        start = pl.multiple_of(LANES * (blocks * h + blocks - 1 - a), LANES)
                        pieces.append(strip[k, :, pl.ds(start, length)] * mask[a * LANES : (a + 1) * LANES])
                    acc[...] += jnp.dot(jnp.concatenate(pieces, axis=0), g_ref[k, m], preferred_element_type=F32)

                out_ref[h, m] = acc[...].astype(BF)

    return pl.pallas_call(
        kernel,
        name="convolve_back",
        out_shape=jax.ShapeDtypeStruct((seq_count, streams, length, width), BF),
        in_specs=in_vmem(6),
        out_specs=in_vmem(1)[0],
        scratch_shapes=[
            pltpu.VMEM((count, LANES, wide), BF),
            pltpu.VMEM((length, length), BF),
            pltpu.VMEM((length, width), F32),
        ],
        compiler_params=params(),
    )(grads, row_ids, col_ids, base, own_lag, tail_lag)


def dot_nn(a, b):
    return jnp.dot(a, b, preferred_element_type=F32)


def dot_nt(a, b):
    return lax.dot_general(a, b, (((1,), (1,)), ((), ())), preferred_element_type=F32)


def dot_tn(a, b):
    return lax.dot_general(a, b, (((0,), (0,)), ((), ())), preferred_element_type=F32)


def allowed_keys(query_ids, key_ids, first_row, distance):
    shape = (query_ids.shape[0], key_ids.shape[1])
    offset = lax.broadcasted_iota(jnp.int32, shape, 0) - lax.broadcasted_iota(jnp.int32, shape, 1) + (first_row + distance)
    return (query_ids == key_ids) & (offset >= 0) & (offset < WINDOW)


def one_head(block, head):
    lane = lax.broadcasted_iota(jnp.int32, block.shape, 1)
    return jnp.where((lane >= head * HD) & (lane < (head + 1) * HD), block, jnp.zeros_like(block))


def attend(rows, row_ids, col_ids, wq, wk, wv, wo):
    spans, streams, length, width = rows.shape
    cols = wq.shape[1]
    heads = cols // HD
    tile = min(256, length)
    scale = HD ** (-0.5)

    def kernel(x_ref, row_ref, col_ref, wq_ref, wk_ref, wv_ref, wo_ref, q_ref, k_ref, v_ref, a_ref, lse_ref, p_ref):
        @pl.loop(0, streams)
        def _(m):
            q_ref[m] = dot_nn(x_ref[0, m], wq_ref[...]).astype(BF)
            for h in range(spans):
                k_ref[h, m] = dot_nn(x_ref[h, m], wk_ref[...]).astype(BF)
                v_ref[h, m] = dot_nn(x_ref[h, m], wv_ref[...]).astype(BF)

            @pl.loop(0, length // tile)
            def _(i):
                first = pl.multiple_of(i * tile, tile)
                here = pl.ds(first, tile)
                masks = [allowed_keys(col_ref[m, here], row_ref[h, m], first, h * length) for h in range(spans)]
                block = q_ref[m, here]
                result = jnp.zeros((tile, cols), F32)
                for head in range(heads):
                    query = one_head(block, head)
                    scores = [
                        jnp.where(masks[h], dot_nt(query, k_ref[h, m]) * scale, NEGATIVE) for h in range(spans)
                    ]
                    peak = functools.reduce(jnp.maximum, [jnp.max(v, axis=-1, keepdims=True) for v in scores])
                    raised = [jnp.exp(v - peak) for v in scores]
                    total = sum([jnp.sum(v, axis=-1, keepdims=True) for v in raised])
                    inverse = 1.0 / total
                    mixed = sum([dot_nn((raised[h] * inverse).astype(BF), v_ref[h, m]) for h in range(spans)])
                    result = result + one_head(mixed, head)
                    lse_ref[m, head, here] = jnp.broadcast_to(peak + jnp.log(total), (tile, LANES))
                a_ref[m, here] = result.astype(BF)

            p_ref[m] = dot_nn(a_ref[m], wo_ref[...]).astype(BF)

    part = jax.ShapeDtypeStruct((streams, length, cols), BF)
    span = jax.ShapeDtypeStruct((spans, streams, length, cols), BF)
    return pl.pallas_call(
        kernel,
        name="attend",
        out_shape=(
            part,
            span,
            span,
            part,
            jax.ShapeDtypeStruct((streams, heads, length, LANES), F32),
            jax.ShapeDtypeStruct((streams, length, width), BF),
        ),
        in_specs=in_vmem(7),
        out_specs=tuple(in_vmem(6)),
        compiler_params=params(),
    )(rows, row_ids, col_ids, wq, wk, wv, wo)


def attend_back(q, k, v, lse, grad_out, row_ids, col_ids, wq, wk, wv, wo):
    spans, streams, length, cols = k.shape
    width = grad_out.shape[2]
    heads = cols // HD
    tile = min(256, length)
    scale = HD ** (-0.5)

    def kernel(
        q_ref, k_ref, v_ref, lse_ref, go_ref, row_ref, col_ref, wq_ref, wk_ref, wv_ref, wo_ref,
        dq_ref, dk_ref, dv_ref, p_ref, ga_ref, dk_acc, dv_acc,
    ):
        @pl.loop(0, streams)
        def _(m):
            ga_ref[...] = dot_nt(go_ref[m], wo_ref[...]).astype(BF)
            dk_acc[...] = jnp.zeros_like(dk_acc)
            dv_acc[...] = jnp.zeros_like(dv_acc)

            @pl.loop(0, length // tile)
            def _(i):
                first = pl.multiple_of(i * tile, tile)
                here = pl.ds(first, tile)
                masks = [allowed_keys(col_ref[m, here], row_ref[h, m], first, h * length) for h in range(spans)]
                block = q_ref[m, here]
                grad_block = ga_ref[here]
                result = jnp.zeros((tile, cols), F32)
                for head in range(heads):
                    query = one_head(block, head)
                    grad = one_head(grad_block, head)
                    level = lse_ref[m, head, here][:, :1]
                    prob = [
                        jnp.where(masks[h], jnp.exp(dot_nt(query, k_ref[h, m]) * scale - level), 0.0)
                        for h in range(spans)
                    ]
                    grad_prob = [dot_nt(grad, v_ref[h, m]) for h in range(spans)]
                    mean = sum([jnp.sum(p * g, axis=-1, keepdims=True) for p, g in zip(prob, grad_prob)])
                    grad_scores = [(p * (g - mean)).astype(BF) for p, g in zip(prob, grad_prob)]
                    for h in range(spans):
                        dv_acc[h] += dot_tn(prob[h].astype(BF), grad)
                        dk_acc[h] += dot_tn(grad_scores[h], query)
                    mixed = sum([dot_nn(grad_scores[h], k_ref[h, m]) for h in range(spans)])
                    result = result + one_head(mixed, head)
                dq_ref[m, here] = (result * scale).astype(BF)

            for h in range(spans):
                dk_ref[h, m] = (dk_acc[h] * scale).astype(BF)
                dv_ref[h, m] = dv_acc[h].astype(BF)
                back = dot_nt(dk_ref[h, m], wk_ref[...]) + dot_nt(dv_ref[h, m], wv_ref[...])
                if h == 0:
                    back = back + dot_nt(dq_ref[m], wq_ref[...])
                p_ref[h, m] = back.astype(BF)

    span = jax.ShapeDtypeStruct((spans, streams, length, cols), BF)
    return pl.pallas_call(
        kernel,
        name="attend_back",
        out_shape=(
            jax.ShapeDtypeStruct((streams, length, cols), BF),
            span,
            span,
            jax.ShapeDtypeStruct((spans, streams, length, width), BF),
        ),
        in_specs=in_vmem(11),
        out_specs=tuple(in_vmem(4)),
        scratch_shapes=[
            pltpu.VMEM((length, cols), BF),
            pltpu.VMEM((spans, length, cols), F32),
            pltpu.VMEM((spans, length, cols), F32),
        ],
        compiler_params=params(),
    )(q, k, v, lse, grad_out, row_ids, col_ids, wq, wk, wv, wo)


def unit_terms(gate_pre, up_pre, grad_inner):
    root = 0.7978845608028654
    square = gate_pre * gate_pre
    bend = jnp.tanh(root * (gate_pre + 0.044715 * (gate_pre * square)))
    half = 0.5 * (1.0 + bend)
    gelu = gate_pre * half
    slope = half + 0.5 * gate_pre * (1.0 - bend * bend) * (root * (1.0 + 3.0 * 0.044715 * square))
    return gelu * up_pre, grad_inner * up_pre * slope, grad_inner * gelu


def head(
    x, ids, stu_gain, filter_proj, lag_proj, filters, attn_gain, feed_gain, wq, wk, wv, wo, wg, wu, wd, cot, seq_count
):
    streams, _, quarter, width = x.shape
    length = 4 * quarter
    hops = WINDOW // length
    spans = hops + 1
    count, taps = filters.shape
    wide = taps + 4 * LANES
    lag_order, channels = lag_proj.shape[:2]
    blocks = length // LANES
    cols, units = wq.shape[1], wg.shape[1]
    heads = cols // HD
    tile = 2 * quarter
    steps = 2 * streams
    scale = HD ** (-0.5)
    rows = width // seq_count
    chunks = 4
    assert streams == 2 and units == 4 * cols

    rows_of = pltpu.VMEM((streams, length, cols), BF)
    unit_rows = pltpu.VMEM((streams, length, units), BF)
    state = pltpu.VMEM((streams, quarter, width), F32)
    gathered = (1, streams, 4, quarter, width)
    split_part = pltpu.VMEM((1, streams, 2, 2, quarter, width), BF)
    zero_hops = ReduceScatter.scratch(0, streams, quarter, width)

    def kernel(
        x_ref, id_ref, sg_ref, fp_hbm, lp_ref, taps_ref, ag_ref, fg_ref,
        wq_ref, wk_ref, wv_ref, wo_ref, wg_hbm, wu_hbm, wd_hbm, cot_hbm,
        stu_out, layer_out, one_out, gain_out, sum_out, lag_out, ids_out, conv_out, strip_out,
        fp_ref, wg_ref, wu_ref, wd_ref, cot_ref, load_sem, base_ref,
        rows_in, ids_in, cols_in, id_ext, lag_ext, part_ref, id_sem, strip_sem, conv_sem,
        attn_in, feed_in, grad_att, hid_one, hid_two, grad_two, grads, total, grad_acc,
        o_part, feed_part, layer_part, attn_part,
        sem_rows, sem_one, sem_two, sem_three, sem_layer, sem_five, *scratch,
    ):
        s, t, y, c, core, far = place()
        scratch = list(scratch)

        def take(count):
            taken = scratch[:count]
            del scratch[:count]
            return taken

        def reducer(ref, distance):
            return ReduceScatter(seq_count, distance, streams, lambda h, m: ref.at[h, m], take(6))

        rs_one, rs_two, rs_three, rs_layer = [reducer(r, 0) for r in (part_ref, o_part, feed_part, layer_part)]
        rs_four = reducer(attn_part, hops)
        gr = GradReduce(seq_count, lambda k: grads.at[k], lambda k: sum_out.at[k], take(8))
        ag_rows = AllGather(
            seq_count, seq_count - 1, streams, lambda h, m, q: rows_in.at[m, h, q], sem_rows, first=1
        )
        ag_one = AllGather(seq_count, hops, streams, attn_in, sem_one)
        ag_two = AllGather(seq_count, 0, streams, feed_in, sem_two)
        ag_three = AllGather(seq_count, 0, streams, grad_att, sem_three)
        ag_layer = AllGather(seq_count, 0, streams, layer_out, sem_layer)
        ag_five = AllGather(seq_count, 0, streams, stu_out, sem_five)

        def flat(value):
            return value.reshape(-1, value.shape[-1])

        def all_rows(ref, m):
            return flat(ref[0, m])

        def masks_of(m, here, first):
            return [
                allowed_keys(cols_in[m, here], ids_out[pl.ds(h * streams + m, 1)], first, h * length) for h in range(spans)
            ]

        def first_norm(m):
            rs_one.total(m, total)
            hidden = x_ref[m, t].astype(F32) + total[...]
            hid_one[m] = hidden
            attn_in[0, m, t] = norm_of(hidden, ag_ref[...]).astype(BF)
            ag_one.start(m)

        def after(i, step, *actions):
            @pl.when(i == step)
            def _():
                for action in actions:
                    action()

        def id_copy(h, peer):
            return remote(id_ref, ids_in.at[h], id_sem.at[0, h], id_sem.at[1, h], {"seq": peer})

        far_back = range(1, seq_count)

        pairs = ((fp_hbm, fp_ref), (wg_hbm, wg_ref), (wu_hbm, wu_ref), (wd_hbm, wd_ref), (cot_hbm, cot_ref))
        loads = [pltpu.make_async_copy(a, b, load_sem.at[i]) for i, (a, b) in enumerate(pairs)]
        for load in loads:
            load.start()

        def front(strip, left, mask, conv):
            for m in range(streams):
                rows_in[m, 0, t] = norm_of(x_ref[m, t].astype(F32), sg_ref[...]).astype(BF)
            greet(seq_count, 0, wide=True)
            for m in range(streams):
                ag_rows.start(m)
            for h in far_back:
                pl.when(s + h < seq_count)(functools.partial(lambda h: id_copy(h, s + h).start(), h))
            for m in range(streams):
                for q in range(4):

                    @pl.when(t != q)
                    def _():
                        rows_in[m, 0, q] = norm_of(x_ref[m, q].astype(F32), sg_ref[...]).astype(BF)

            for m in range(streams):
                for h in far_back:
                    ag_rows.clear(h, m)
                for h in range(1, spans):
                    ag_one.clear(h, m)
            ids_in[0] = id_ref[...]
            for h in far_back:

                @pl.when(s - h < 0)
                def _():
                    ids_in[h] = jnp.full(ids_in.shape[1:], -1, jnp.int32)

            lay_taps(taps_ref, base_ref, True)
            strips(base_ref, strip)
            strip_copy = pltpu.make_async_copy(strip, strip_out, strip_sem)
            strip_copy.start()
            for h in far_back:
                ag_rows.arrive(h, 0)
            for h in far_back:
                pl.when(s - h >= 0)(functools.partial(lambda h: id_copy(h, s - h).wait_recv(), h))
            for h in range(seq_count):
                for m in range(streams):
                    ids_out[h * streams + m : h * streams + m + 1] = ids_in[h, m].astype(F32)
            turned = jnp.transpose(ids_out[...])
            for m in range(streams):
                cols_in[m] = turned[:, m : m + 1]
                id_ext[m, :8] = turned[length - 8 :, streams + m : streams + m + 1]
                id_ext[m, 8:] = turned[:, m : m + 1]
            lay_taps(taps_ref, base_ref, False)
            strip_copy.wait()
            strips(base_ref, strip)
            for load in loads:
                load.wait()
            for h in far_back:
                ag_rows.pass_on(h, 0)
            for h in far_back:
                ag_rows.arrive(h, 1)
            for h in far_back:
                ag_rows.finish(h, 0)
            mine = pl.ds(pl.multiple_of(t * channels, LANES), channels)

            def lags(m):
                own = rows_in[m, 0, :, :, mine].reshape(length, channels)
                lag_ext[:8] = rows_in[m, 1, 3, quarter - 8 :, mine].astype(F32)
                lag_ext[8:] = own.astype(F32)
                for i in range(lag_order):
                    same = id_ext[m, 7 - i : 7 - i + length] == cols_in[m]
                    lag_out[i, m] = jnp.where(same, lag_ext[7 - i : 7 - i + length], 0.0).astype(BF)

            def conv_copy(k, m):
                return pltpu.make_async_copy(
                    conv.at[k], conv_out.at[k, pl.ds(pl.multiple_of(m * length, LANES), length)], conv_sem.at[k]
                )

            lags(0)

            @pl.loop(0, streams * count)
            def _(j):
                m = j // count
                k = j - m * count

                @pl.when(k == 0)
                def _():
                    for h in range(seq_count):
                        mask[:, h * length : (h + 1) * length] = jnp.where(
                            cols_in[m] == ids_out[pl.ds(h * streams + m, 1)], 1.0, 0.0
                        ).astype(BF)

                for a in range(blocks):
                    for h in range(seq_count):
                        start = LANES * (blocks * (seq_count - h) - 1 - a)
                        down, across = slice(a * LANES, (a + 1) * LANES), slice(h * length, (h + 1) * length)
                        left[down, across] = strip[k, :, start : start + length] * mask[down, across]
                result = dot_nn(left[...], rows_in[m].reshape(seq_count * length, width)).astype(BF)
                pl.when(m > 0)(lambda: conv_copy(k, m - 1).wait())
                conv[k] = result
                conv_copy(k, m).start()

                @pl.when(k == count - 1)
                def _():
                    @pl.loop(0, 2)
                    def _(half):
                        here = pl.ds(pl.multiple_of(half * tile, tile), tile)
                        mixed = sum([dot_nn(conv[q, here], fp_ref[q]) for q in range(count)])
                        mixed = mixed + sum([dot_nn(lag_out[i, m, here], lp_ref[i]) for i in range(lag_order)])
                        part_ref[0, m, half] = mixed.astype(BF).reshape(2, quarter, width)

                after(j, 1, *[functools.partial(ag_rows.pass_on, h, 1) for h in far_back])
                after(
                    j,
                    count - 1,
                    lambda: rs_one.start(0, 0),
                    *[functools.partial(ag_rows.finish, h, 1) for h in far_back],
                    lambda: lags(1),
                )
                after(j, count, lambda: rs_one.middle(0, 0))
                after(j, count + 2, lambda: first_norm(0))
                after(j, count + 4, lambda: ag_one.pass_on(0, 0), lambda: ag_one.arrive(1, 0) if hops > 0 else None)

            rs_one.start(0, 1)
            for k in range(count):
                conv_copy(k, streams - 1).wait()

        pl.run_scoped(
            front,
            pltpu.VMEM((count, LANES, wide), BF),
            pltpu.VMEM((length, seq_count * length), BF),
            pltpu.VMEM((length, seq_count * length), BF),
            pltpu.VMEM((count, length, width), BF),
        )

        def attention_on(
            q_ref, k_ref, v_ref, a_ref, lse_ref, inner_ref, gg_ref, gu_ref, ga_ref, dk_acc, dv_acc, dq_ref, dkv_ref
        ):
            rs_one.middle(0, 1)
            for h in range(2, spans):
                ag_one.arrive(h, 0)
            for h in range(1, spans):
                ag_one.pass_on(h, 0)
            first_norm(1)
            for h in range(spans):
                ag_one.finish(h, 0)

            def split_step(i):
                m = i // 2
                return m, i - 2 * m

            @pl.loop(0, steps)
            def _(i):
                m, half = split_step(i)
                first = pl.multiple_of(half * tile, tile)
                here = pl.ds(first, tile)

                @pl.when(half == 0)
                def _():
                    own = flat(attn_in[0, m])
                    q_ref[m] = dot_nn(own, wq_ref[...]).astype(BF)
                    for h in range(spans):
                        block = flat(attn_in[h, m])
                        k_ref[h, m] = dot_nn(block, wk_ref[...]).astype(BF)
                        v_ref[h, m] = dot_nn(block, wv_ref[...]).astype(BF)

                masks = masks_of(m, here, first)
                block = q_ref[m, here]
                result = jnp.zeros((tile, cols), F32)
                for head in range(heads):
                    query = one_head(block, head)
                    scores = [jnp.where(masks[h], dot_nt(query, k_ref[h, m]) * scale, NEGATIVE) for h in range(spans)]
                    peak = functools.reduce(jnp.maximum, [jnp.max(v, axis=-1, keepdims=True) for v in scores])
                    raised = [jnp.exp(v - peak) for v in scores]
                    norm = sum([jnp.sum(v, axis=-1, keepdims=True) for v in raised])
                    inverse = 1.0 / norm
                    mixed = sum([dot_nn((raised[h] * inverse).astype(BF), v_ref[h, m]) for h in range(spans)])
                    result = result + one_head(mixed, head)
                    lse_ref[m, head, here] = jnp.broadcast_to(peak + jnp.log(norm), (tile, LANES))
                low = result.astype(BF)
                a_ref[m, here] = low
                o_part[0, m, half] = dot_nn(low, wo_ref[...]).astype(BF).reshape(2, quarter, width)
                after(i, 0, lambda: ag_one.pass_on(0, 1), *[functools.partial(ag_one.arrive, h, 1) for h in range(1, spans)])
                after(
                    i,
                    1,
                    lambda: rs_two.start(0, 0),
                    *[functools.partial(ag_one.pass_on, h, 1) for h in range(1, spans)],
                    *[functools.partial(ag_one.finish, h, 1) for h in range(spans)],
                )
                after(i, 2, lambda: rs_two.middle(0, 0))
                after(i, 3, lambda: rs_two.start(0, 1))

            def second_norm(m):
                rs_two.total(m, total)
                hidden = hid_one[m] + total[...]
                hid_two[m] = hidden
                feed_in[0, m, t] = norm_of(hidden, fg_ref[...]).astype(BF)
                ag_two.start(m)

            second_norm(0)
            rs_two.middle(0, 1)
            ag_two.pass_on(0, 0)
            ag_two.finish(0, 0)

            @pl.loop(0, steps)
            def _(i):
                m, half = split_step(i)
                here = pl.ds(pl.multiple_of(half * tile, tile), tile)
                block = flat(feed_in[0, m, pl.ds(2 * half, 2)])
                inner, grad_gate, grad_up = unit_terms(
                    dot_nn(block, wg_ref[...]), dot_nn(block, wu_ref[...]), dot_nt(cot_ref[m, here], wd_ref[...])
                )
                inner, grad_gate, grad_up = inner.astype(BF), grad_gate.astype(BF), grad_up.astype(BF)
                inner_ref[m, here] = inner
                gg_ref[m, here] = grad_gate
                gu_ref[m, here] = grad_up
                back = dot_nt(grad_gate, wg_ref[...]) + dot_nt(grad_up, wu_ref[...])
                feed_part[0, m, half] = back.astype(BF).reshape(2, quarter, width)
                layer_part[0, m, half] = dot_nn(inner, wd_ref[...]).astype(BF).reshape(2, quarter, width)
                after(i, 0, lambda: second_norm(1))
                after(
                    i,
                    1,
                    lambda: rs_three.start(0, 0),
                    lambda: ag_two.pass_on(0, 1),
                    lambda: rs_three.middle(0, 0),
                    lambda: ag_two.finish(0, 1),
                )
                after(i, 3, lambda: rs_three.start(0, 1))

            def third_norm(m):
                rs_three.total(m, total)
                grad_in, gain_grad = norm_back(hid_two[m], fg_ref[...], total[...])
                value = cot_ref[m, pl.ds(pl.multiple_of(t * quarter, quarter), quarter)].astype(F32) + grad_in
                grad_two[m] = value
                gain_out[1:2] = gain_grad if m == 0 else gain_out[1:2] + gain_grad
                grad_att[0, m, t] = value.astype(BF)
                ag_three.start(m)

            third_norm(0)
            feed_all = flat(feed_in[0])
            grads[0] = dot_tn(feed_all, flat(gg_ref[...])).astype(BF)
            gr.start(0)
            rs_three.middle(0, 1)
            grads[1] = dot_tn(feed_all, flat(gu_ref[...])).astype(BF)
            gr.start(1)
            grads[2] = dot_tn(flat(cot_ref[...]), flat(inner_ref[...])).astype(BF)
            gr.start(2)
            ag_three.pass_on(0, 0)
            ag_three.finish(0, 0)
            for m in range(streams):
                rs_layer.start(0, m)

            def layer_sum(m):
                rs_layer.total(m, total)
                layer_out[0, m, t] = (hid_two[m] + total[...]).astype(BF)
                ag_layer.start(m)

            @pl.loop(0, steps)
            def _(i):
                m, half = split_step(i)
                first = pl.multiple_of(half * tile, tile)
                here = pl.ds(first, tile)

                @pl.when(half == 0)
                def _():
                    ga_ref[...] = dot_nt(all_rows(grad_att, m), wo_ref[...]).astype(BF)
                    dk_acc[...] = jnp.zeros_like(dk_acc)
                    dv_acc[...] = jnp.zeros_like(dv_acc)

                masks = masks_of(m, here, first)
                block = q_ref[m, here]
                grad_block = ga_ref[here]
                result = jnp.zeros((tile, cols), F32)
                for head in range(heads):
                    query = one_head(block, head)
                    grad = one_head(grad_block, head)
                    level = lse_ref[m, head, here][:, :1]
                    prob = [
                        jnp.where(masks[h], jnp.exp(dot_nt(query, k_ref[h, m]) * scale - level), 0.0) for h in range(spans)
                    ]
                    grad_prob = [dot_nt(grad, v_ref[h, m]) for h in range(spans)]
                    mean = sum([jnp.sum(p * g, axis=-1, keepdims=True) for p, g in zip(prob, grad_prob)])
                    grad_scores = [(p * (g - mean)).astype(BF) for p, g in zip(prob, grad_prob)]
                    for h in range(spans):
                        dv_acc[h] += dot_tn(prob[h].astype(BF), grad)
                        dk_acc[h] += dot_tn(grad_scores[h], query)
                    mixed = sum([dot_nn(grad_scores[h], k_ref[h, m]) for h in range(spans)])
                    result = result + one_head(mixed, head)
                dq_ref[m, here] = (result * scale).astype(BF)

                @pl.when(half == 1)
                def _():
                    for h in range(hops, -1, -1):
                        grad_k = (dk_acc[h] * scale).astype(BF)
                        grad_v = dv_acc[h].astype(BF)
                        dkv_ref[h, m, :, :cols] = grad_k
                        dkv_ref[h, m, :, cols:] = grad_v
                        back = dot_nt(grad_k, wk_ref[...]) + dot_nt(grad_v, wv_ref[...])
                        if h == 0:
                            back = back + dot_nt(dq_ref[m], wq_ref[...])
                        attn_part[h, m] = back.astype(BF).reshape(2, 2, quarter, width)
                        rs_four.start(h, m)

                after(i, 0, lambda: third_norm(1), lambda: rs_layer.middle(0, 0), lambda: rs_layer.middle(0, 1))
                after(i, 1, lambda: gr.spread(0), lambda: ag_three.pass_on(0, 1), lambda: ag_three.finish(0, 1))
                after(i, 2, *[functools.partial(rs_four.middle, h, 0) for h in range(hops, -1, -1)], lambda: gr.spread(1))
                after(
                    i,
                    3,
                    *[functools.partial(rs_four.hop, h, 0, total) for h in range(hops, 0, -1)],
                    lambda: gr.spread(2),
                    lambda: layer_sum(0),
                    lambda: layer_sum(1),
                )

            attn_all = attn_in[...].reshape(spans * streams * length, width)
            grads[3, :, cols : 3 * cols] = dot_tn(attn_all, flat(dkv_ref[...].reshape(-1, 2 * cols))).astype(BF)
            for h in range(hops, -1, -1):
                rs_four.middle(h, 1)
            grads[3, :, :cols] = dot_tn(flat(attn_in[0]), flat(dq_ref[...])).astype(BF)
            grads[3, :, 3 * cols :] = dot_tn(flat(grad_att[0]), flat(a_ref[...])).astype(BF)
            gr.start(3)

            def fourth_norm(m):
                rs_four.total(m, total)
                grad_in, gain_grad = norm_back(hid_one[m], ag_ref[...], total[...])
                value = grad_two[m] + grad_in
                one_out[m] = value
                gain_out[0:1] = gain_grad if m == 0 else gain_out[0:1] + gain_grad
                stu_out[0, m, t] = value.astype(BF)
                ag_five.start(m)

            fourth_norm(0)
            for h in range(hops, 0, -1):
                rs_four.hop(h, 1, total)
            gr.spread(3)
            gr.collect(0, grad_acc)
            fourth_norm(1)
            for m in range(streams):
                ag_five.pass_on(0, m)
            for m in range(streams):
                ag_layer.pass_on(0, m)
            gr.collect(1, grad_acc)
            gr.collect(2, grad_acc)
            for m in range(streams):
                ag_five.finish(0, m)
            gr.collect(3, grad_acc)
            for m in range(streams):
                ag_layer.finish(0, m)
            for k in range(chunks):
                gr.finish(k)
                gr.drain(k)
            for item in (rs_one, rs_two, rs_three, rs_layer, rs_four, ag_rows, ag_one, ag_two, ag_three, ag_layer, ag_five):
                item.drain()
            for h in far_back:
                pl.when(s + h < seq_count)(functools.partial(lambda h: id_copy(h, s + h).wait_send(), h))

        pl.run_scoped(
            attention_on,
            rows_of,
            pltpu.VMEM((spans, streams, length, cols), BF),
            pltpu.VMEM((spans, streams, length, cols), BF),
            rows_of,
            pltpu.VMEM((streams, heads, length, LANES), F32),
            unit_rows,
            unit_rows,
            unit_rows,
            pltpu.VMEM((length, cols), BF),
            pltpu.VMEM((spans, length, cols), F32),
            pltpu.VMEM((spans, length, cols), F32),
            rows_of,
            pltpu.VMEM((spans, streams, length, 2 * cols), BF),
        )

    anywhere = pl.BlockSpec(memory_space=pl.ANY)
    return pl.pallas_call(
        kernel,
        name="head",
        out_shape=(
            jax.ShapeDtypeStruct(gathered, BF),
            jax.ShapeDtypeStruct(gathered, BF),
            jax.ShapeDtypeStruct((streams, quarter, width), F32),
            jax.ShapeDtypeStruct((2, width), F32),
            jax.ShapeDtypeStruct((chunks, rows, units), BF),
            jax.ShapeDtypeStruct((lag_order, streams, length, channels), BF),
            jax.ShapeDtypeStruct((seq_count * streams, length), F32),
            jax.ShapeDtypeStruct((count, streams * length, width), BF),
            jax.ShapeDtypeStruct((count, LANES, wide), BF),
        ),
        in_specs=[anywhere if i in (3, 12, 13, 14, 15) else spec for i, spec in enumerate(in_vmem(16))],
        out_specs=tuple(in_vmem(7)) + (anywhere, anywhere),
        scratch_shapes=[
            pltpu.VMEM(filter_proj.shape, BF),
            pltpu.VMEM(wg.shape, BF),
            pltpu.VMEM(wu.shape, BF),
            pltpu.VMEM(wd.shape, BF),
            pltpu.VMEM(cot.shape, BF),
            pltpu.SemaphoreType.DMA((5,)),
            pltpu.VMEM((count, wide), F32),
            pltpu.VMEM((streams, seq_count, 4, quarter, width), BF),
            pltpu.VMEM((seq_count,) + ids.shape, jnp.int32),
            pltpu.VMEM((streams, length, 1), F32),
            pltpu.VMEM((streams, length + 8, 1), F32),
            pltpu.VMEM((length + 8, channels), F32),
            split_part,
            pltpu.SemaphoreType.DMA((2, seq_count)),
            pltpu.SemaphoreType.DMA,
            pltpu.SemaphoreType.DMA((count,)),
            pltpu.VMEM((spans, streams, 4, quarter, width), BF),
            pltpu.VMEM(gathered, BF),
            pltpu.VMEM(gathered, BF),
            state,
            state,
            state,
            pltpu.VMEM((chunks, width, units), BF),
            pltpu.VMEM((quarter, width), F32),
            pltpu.VMEM((rows, units // 2), F32),
            split_part,
            split_part,
            split_part,
            pltpu.VMEM((spans, streams, 2, 2, quarter, width), BF),
            AllGather.scratch(seq_count - 1, streams)[0],
            AllGather.scratch(hops, streams)[0],
        ]
        + [AllGather.scratch(0, streams)[0]] * 4
        + zero_hops * 4
        + ReduceScatter.scratch(hops, streams, quarter, width)
        + GradReduce.scratch(seq_count, chunks, width, units),
        compiler_params=params(8),
    )(
        x, ids, stu_gain, filter_proj, lag_proj, filters, attn_gain, feed_gain, wq, wk, wv, wo, wg, wu, wd, cot
    )


def tail(
    grad_stu, filter_proj, lag_proj, conv, lag_stack, ext_ids, strip_back, x, gain, grad_one, gains, seq_count
):
    count, length_all, width = conv.shape
    streams, _, quarter, _ = x.shape
    length = length_all // streams
    lag_order, channels = lag_proj.shape[:2]
    blocks = length // LANES
    hops = seq_count - 1
    chunks = count + 1
    steps = seq_count * streams
    rows = width // seq_count
    gain_rows = 8

    def kernel(
        gs_ref, fp_hbm, lp_ref, conv_hbm, lag_ref, ext_ref, strip_hbm, x_hbm, gain_ref, one_ref, gains_ref,
        out, filter_out, lag_out, gain_out,
        conv_ref, fp_ref, strip, x_own, conv_sem, fp_sem, strip_sem, x_sem, id_ext,
        mask, cols, left, acc, terms, grad_conv, grads, lag_ext, total, grad_acc, gather_sem,
        gain_own, gain_near, gain_sum, gain_far, near_sem, far_sem, *scratch,
    ):
        s, t, y, c, core, far = place()
        p = lax.axis_index("dp")
        rs_scratch, gr_scratch = scratch[:6], scratch[6:]

        def conv_copy(k):
            return pltpu.make_async_copy(conv_hbm.at[k], conv_ref.at[k], conv_sem.at[k])

        def fp_copy(k):
            return pltpu.make_async_copy(fp_hbm.at[k], fp_ref.at[k], fp_sem.at[k])

        strip_copy = pltpu.make_async_copy(strip_hbm, strip, strip_sem)
        for k in range(count):
            conv_copy(k).start()
            fp_copy(k).start()
        strip_copy.start()
        x_copy = pltpu.make_async_copy(x_hbm.at[:, t], x_own, x_sem)
        x_copy.start()
        greet(seq_count, hops, wide=True, gains=True)

        def source(k):
            return grads.at[k]

        def result(k):
            return filter_out.at[k] if k < count else lag_out

        gr = GradReduce(seq_count, source, result, gr_scratch)
        rs = ReduceScatter(seq_count, hops, streams, lambda h, m: terms.at[h, m], rs_scratch)
        ag = AllGather(seq_count, 0, streams, out, gather_sem)

        @pl.loop(0, count)
        def _(k):
            conv_copy(k).wait()
            grads[k] = dot_tn(conv_ref[k], gs_ref[...]).astype(BF)
            gr.start(k)
            fp_copy(k).wait()
            product = dot_nt(gs_ref[...], fp_ref[k]).astype(BF)
            for m in range(streams):
                here = pl.ds(pl.multiple_of(k * length, LANES), length)
                grad_conv[m, here] = product[m * length : (m + 1) * length]

        grads[count] = jnp.zeros_like(grads.at[count])
        for i in range(lag_order):
            grads[count, :, i * channels : (i + 1) * channels] = dot_tn(gs_ref[...], lag_ref[i]).astype(BF)
        gr.start(count)
        turned = jnp.transpose(ext_ref[...])
        for j in range(steps):
            cols[j] = turned[:, j : j + 1]
        for m in range(streams):
            lag_ext[m] = jnp.zeros_like(lag_ext.at[m])
            id_ext[:8] = turned[length - 8 :, streams + m : streams + m + 1]
            id_ext[8:] = turned[:, m : m + 1]
            for i in range(lag_order):
                term = dot_nt(gs_ref[m * length : (m + 1) * length], lp_ref[i])
                same = id_ext[7 - i : 7 - i + length] == cols[m]
                lag_ext[m, 7 - i : 7 - i + length] += jnp.where(same, term, 0.0)
        strip_copy.wait()
        x_copy.wait()
        mine = pl.ds(pl.multiple_of(t * channels, LANES), channels)
        spread_at = {0: 0, 1: 1, 4: 2, 6: 3} if steps == 8 and chunks >= 7 else {}
        collect_at = {5: 0, 7: 1} if spread_at else {}

        def step_of(i):
            return seq_count - 1 - i // streams, i - i // streams * streams

        @pl.loop(0, steps)
        def _(i):
            h, m = step_of(i)

            @pl.when(h <= s)
            def _():
                mask[...] = jnp.where(cols[h * streams + m] == ext_ref[pl.ds(m, 1)], 1.0, 0.0).astype(BF)
                for k in range(count):
                    for a in range(blocks):
                        start = pl.multiple_of(LANES * (blocks * h + blocks - 1 - a), LANES)
                        down = slice(a * LANES, (a + 1) * LANES)
                        left[down, k * length : (k + 1) * length] = strip[k, :, pl.ds(start, length)] * mask[down]
                acc[...] = jnp.dot(left[...], grad_conv[m], preferred_element_type=F32)

                @pl.when(h == 0)
                def _():
                    acc[:, mine] += lag_ext[m, 8:]

                @pl.when(h == 1)
                def _():
                    acc[length - 8 :, mine] += lag_ext[m, :8]

                for quarter_y in range(2):
                    for quarter_c in range(2):
                        first = (2 * quarter_y + quarter_c) * quarter
                        terms[h, m, quarter_y, quarter_c] = acc[first : first + quarter].astype(BF)
                rs.start(h, m)

            @pl.when(i >= 1)
            def _():
                rs.middle(*step_of(i - 1))

            @pl.when((i >= 2) & (i < steps - streams + 2))
            def _():
                rs.hop(*step_of(i - 2), total)

            for step, k in spread_at.items():
                pl.when(i == step)(functools.partial(gr.spread, k))
            for step, k in collect_at.items():
                pl.when(i == step)(functools.partial(gr.collect, k, grad_acc))

        rs.middle(0, streams - 1)
        waiting = list(range(len(spread_at), chunks))
        gathered = list(range(len(collect_at), chunks))

        def next_spread():
            if waiting:
                gr.spread(waiting.pop(0))

        gain_own[...] = jnp.zeros_like(gain_own)
        for m in range(streams):
            rs.total(m, total)
            grad_in, gain_grad = norm_back(x_own[m].astype(F32), gain_ref[...], total[...])
            out[0, m, t] = (one_ref[m] + grad_in).astype(BF)
            ag.start(m)
            gain_own[0:1] += gain_grad
            next_spread()
        gain_own[1:3] = gains_ref[...]
        gain_near[t] = gain_own[...]

        def near_copy(j, slot):
            return remote(gain_own, gain_near.at[slot], near_sem.at[0, j], near_sem.at[1, slot], {"tensor": j})

        for j in range(4):
            pl.when(t != j)(functools.partial(lambda j: near_copy(j, t).start(), j))
        while len(gathered) > 3 and chunks - len(gathered) < chunks - len(waiting):
            gr.collect(gathered.pop(0), grad_acc)
        for m in range(streams):
            ag.pass_on(0, m)
        for j in range(4):
            pl.when(t != j)(functools.partial(lambda j: near_copy(j, j).wait_recv(), j))
        gain_sum[...] = gain_near[0] + gain_near[1] + gain_near[2] + gain_near[3]
        me = p * seq_count + s

        def far_copy(j, slot):
            d, q = j // seq_count, j % seq_count
            return remote(
                gain_sum.at[:, q * rows : (q + 1) * rows], gain_far.at[slot], far_sem.at[0, j], far_sem.at[1, slot],
                {"dp": d, "seq": q},
            )

        gain_far[me] = gain_sum[:, pl.ds(pl.multiple_of(s * rows, LANES), rows)]
        for j in range(2 * seq_count):
            pl.when(me != j)(lambda: far_copy(j, me).start())
        while waiting:
            next_spread()
        for m in range(streams):
            ag.finish(0, m)
        while gathered:
            gr.collect(gathered.pop(0), grad_acc)
        for j in range(2 * seq_count):
            pl.when(me != j)(lambda: far_copy(j, j).wait_recv())
        gain_out[...] = functools.reduce(jnp.add, [gain_far[j] for j in range(2 * seq_count)])
        for k in range(chunks):
            gr.finish(k)
        for j in range(4):
            pl.when(t != j)(lambda: near_copy(j, t).wait_send())
        for j in range(2 * seq_count):
            pl.when(me != j)(lambda: far_copy(j, me).wait_send())
        for k in range(chunks):
            gr.drain(k)
        rs.drain()
        ag.drain()

    anywhere = pl.BlockSpec(memory_space=pl.ANY)
    return pl.pallas_call(
        kernel,
        name="tail",
        out_shape=(
            jax.ShapeDtypeStruct((1, streams, 4, quarter, width), BF),
            jax.ShapeDtypeStruct((count, rows, width), BF),
            jax.ShapeDtypeStruct((rows, width), BF),
            jax.ShapeDtypeStruct((gain_rows, rows), F32),
        ),
        in_specs=[anywhere if i in (1, 3, 6, 7) else spec for i, spec in enumerate(in_vmem(11))],
        out_specs=tuple(in_vmem(4)),
        scratch_shapes=[
            pltpu.VMEM(conv.shape, BF),
            pltpu.VMEM(filter_proj.shape, BF),
            pltpu.VMEM(strip_back.shape, BF),
            pltpu.VMEM((streams, quarter, width), BF),
            pltpu.SemaphoreType.DMA((count,)),
            pltpu.SemaphoreType.DMA((count,)),
            pltpu.SemaphoreType.DMA,
            pltpu.SemaphoreType.DMA,
            pltpu.VMEM((length + 8, 1), F32),
            pltpu.VMEM((length, length), BF),
            pltpu.VMEM((steps, length, 1), F32),
            pltpu.VMEM((length, count * length), BF),
            pltpu.VMEM((length, width), F32),
            pltpu.VMEM((seq_count, streams, 2, 2, quarter, width), BF),
            pltpu.VMEM((streams, count * length, width), BF),
            pltpu.VMEM((chunks, width, width), BF),
            pltpu.VMEM((streams, length + 8, channels), F32),
            pltpu.VMEM((quarter, width), F32),
            pltpu.VMEM((rows, width // 2), F32),
            AllGather.scratch(0, streams)[0],
            pltpu.VMEM((gain_rows, width), F32),
            pltpu.VMEM((4, gain_rows, width), F32),
            pltpu.VMEM((gain_rows, width), F32),
            pltpu.VMEM((2 * seq_count, gain_rows, rows), F32),
            pltpu.SemaphoreType.DMA((2, 4)),
            pltpu.SemaphoreType.DMA((2, 2 * seq_count)),
        ]
        + ReduceScatter.scratch(hops, streams, quarter, width)
        + GradReduce.scratch(seq_count, chunks, width, width),
        compiler_params=params(7),
    )(
        grad_stu, filter_proj, lag_proj, conv, lag_stack, ext_ids, strip_back, x, gain, grad_one, gains
    )


def write_out(layer_output, input_gradient, gains, filter_grad, lag_grad, sums, lag_order, channels, cols):
    _, streams, _, quarter, width = layer_output.shape
    rows, units = sums.shape[1:]
    count = filter_grad.shape[0]

    def kernel(
        layer_ref, input_ref, gains_ref, filter_ref, lag_ref, sums_ref,
        layer_out, input_out, stu_out, filter_out, lag_out, attn_out, q_out, k_out, v_out, o_out, feed_out, gate_out, up_out,
        down_out,
    ):
        layer_out[...] = layer_ref[0].reshape(streams, 1, 4 * quarter, width)
        input_out[...] = input_ref[0].reshape(streams, 1, 4 * quarter, width)
        filter_out[...] = filter_ref[...].astype(F32)
        for i, ref in enumerate((stu_out, attn_out, feed_out)):
            ref[...] = gains_ref[i : i + 1]
        for i in range(lag_order):
            lag_out[i] = jnp.transpose(lag_ref[:, i * channels : (i + 1) * channels].astype(F32))
        for i, ref in enumerate((q_out, k_out, v_out)):
            ref[...] = sums_ref[3, :, i * cols : (i + 1) * cols].astype(F32)
        o_out[...] = jnp.transpose(sums_ref[3, :, 3 * cols :].astype(F32))
        gate_out[...] = sums_ref[0].astype(F32)
        up_out[...] = sums_ref[1].astype(F32)
        down_out[...] = jnp.transpose(sums_ref[2].astype(F32))

    def out(*shape, kind=F32):
        return jax.ShapeDtypeStruct(shape, kind)

    shapes = (
        out(streams, 1, 4 * quarter, width, kind=BF),
        out(streams, 1, 4 * quarter, width, kind=BF),
        out(1, rows),
        out(count, rows, width),
        out(lag_order, channels, rows),
        out(1, rows),
        out(rows, cols),
        out(rows, cols),
        out(rows, cols),
        out(cols, rows),
        out(1, rows),
        out(rows, units),
        out(rows, units),
        out(units, rows),
    )
    results = pl.pallas_call(
        kernel,
        name="write_out",
        out_shape=shapes,
        in_specs=in_vmem(6),
        out_specs=tuple(in_vmem(len(shapes))),
        compiler_params=params(),
    )(layer_output, input_gradient, gains, filter_grad, lag_grad, sums)
    return tuple(r.reshape(rows) if r.shape == (1, rows) else r for r in results)


def gated_unit(gate_pre, up_pre):
    return jax.nn.gelu(gate_pre, approximate=True) * up_pre


def local(
    seq_count,
    tokens,
    document_index,
    filters,
    stu_gain,
    filter_proj,
    lag_proj,
    attention_gain,
    query_weight,
    key_weight,
    value_weight,
    output_weight,
    feed_gain,
    gate_weight,
    up_weight,
    down_weight,
    cotangent,
):
    streams, _, length, width = tokens.shape
    row_len = length * seq_count
    quarter = length // 4
    lag_order, channels = lag_proj.shape[:2]
    count = filters.shape[0]
    hops = WINDOW // length
    tensor_place = lax.axis_index("tensor")
    chan_start = tensor_place * channels

    def split(a):
        return a.reshape(a.shape[:-2] + (2, 2, quarter, width))

    def quarters(a):
        return a.reshape(a.shape[:-2] + (4, quarter, width))

    def whole(a):
        return a.reshape(a.shape[:-3] + (length, width))

    def row(gain):
        return gain.reshape(1, width)

    if width // seq_count % LANES == 0:
        rows = tokens.reshape(streams, 4, quarter, width)
        grad_stu, layer_output, grad_one, gain_grads, sums, lag_stack, ext_ids, conv, strip_back = head(
            rows, document_index, row(stu_gain), filter_proj, lag_proj, filters, row(attention_gain), row(feed_gain),
            query_weight, key_weight, value_weight, output_weight, gate_weight, up_weight, down_weight,
            cotangent.reshape(streams, length, width), seq_count,
        )
        input_gradient, filter_grad, lag_grad, gains = tail(
            grad_stu.reshape(streams * length, width), filter_proj, lag_proj, conv,
            lag_stack.reshape(lag_order, streams * length, channels), ext_ids, strip_back, rows, row(stu_gain), grad_one,
            gain_grads, seq_count,
        )
        return write_out(
            layer_output, input_gradient, gains, filter_grad, lag_grad, sums, lag_order, channels, query_weight.shape[1]
        )

    x = tokens[:, 0]
    grad_three = cotangent[:, 0]
    ids = document_index[:, 0]
    id_tile = ids.reshape(streams * length // LANES, LANES)
    pad = jnp.zeros((count, 4 * LANES), filters.dtype)
    ahead = row_len - LANES
    base = jnp.concatenate(
        [
            jnp.flip(filters[:, : ahead + 1], axis=1),
            pad[:, : 4 * LANES],
            jnp.flip(filters[:, ahead + 1 :], axis=1),
        ],
        axis=1,
    ).astype(F32)[:, None]
    base_back = jnp.concatenate(
        [pad[:, : length - LANES], filters, pad[:, :LANES]], axis=1
    ).astype(F32)[:, None]

    tokens_flat = streams * length
    cols = query_weight.shape[1]

    def answer(layer_output, input_gradient, gains, filter_grad, lag_grad, attn_grads, feed_grads):
        query_grad, key_grad, value_grad, output_grad = jnp.split(attn_grads, [cols, 2 * cols, 3 * cols], axis=1)
        gate_grad, up_grad, down_grad = feed_grads
        return (
            layer_output[:, None],
            input_gradient[:, None],
            gains[0],
            filter_grad,
            lag_grad[:, : lag_order * channels].T.reshape(lag_order, channels, -1),
            gains[1],
            query_grad,
            key_grad,
            value_grad,
            output_grad.T,
            gains[2],
            gate_grad,
            up_grad,
            down_grad.T,
        )

    inputs = norm_of(x.astype(F32), stu_gain).astype(BF)
    rows_ext, id_ext = gather_rows(quarters(inputs), id_tile, seq_count)
    rows_ext = whole(rows_ext)
    id_ext = id_ext.reshape(seq_count, streams, length)
    id_rows = id_ext[:, :, None, :]
    id_cols = id_ext[:, :, :, None]

    conv = convolve(rows_ext, id_rows, id_cols[0], base, seq_count)

    chan_rows = lax.dynamic_slice_in_dim(rows_ext[:2], chan_start, channels, 3)
    joined = jnp.concatenate([chan_rows[1][:, length - lag_order :], chan_rows[0]], axis=1)
    joined_ids = jnp.concatenate([id_ext[1][:, length - lag_order :], ids], axis=1)
    masks = []
    lagged = []
    for step in range(1, lag_order + 1):
        low = lag_order - step
        masks.append((joined_ids[:, low : low + length] == ids)[:, :, None])
        lagged.append(jnp.where(masks[-1], joined[:, low : low + length], jnp.zeros((), BF)))
    lag_stack = jnp.stack(lagged)

    mixed = jnp.einsum("kmtd,kde->mte", conv, filter_proj, preferred_element_type=F32)
    mixed = mixed + jnp.einsum("imtc,ice->mte", lag_stack, lag_proj, preferred_element_type=F32)

    state = jax.ShapeDtypeStruct((streams, quarter, width), F32)
    gain_state = jax.ShapeDtypeStruct((1, width), F32)

    def finish_one(m, total, others, extra):
        x_ref, gain_ref = others
        hidden = x_ref[m, place()[1]].astype(F32) + total
        extra[0][m] = hidden
        return norm_of(hidden, gain_ref[...]).astype(BF)

    attn_ext, hidden_one = exchange(
        "exchange_one", 2, seq_count, [split(mixed.astype(BF))[None]], [quarters(x), row(attention_gain)], 0, hops,
        finish_one, [state],
    )
    attn_ext = whole(attn_ext)

    q, k, v, attended, lse, out_part = attend(
        attn_ext, id_rows[: hops + 1], id_cols[0], query_weight, key_weight, value_weight, output_weight
    )

    def finish_two(m, total, others, extra):
        hidden_ref, gain_ref = others
        hidden = hidden_ref[m] + total
        extra[0][m] = hidden
        return norm_of(hidden, gain_ref[...]).astype(BF)

    feed_in, hidden_two = exchange(
        "exchange_two", 3, seq_count, [split(out_part)[None]], [hidden_one, row(feed_gain)], 0, 0, finish_two, [state]
    )
    feed_in = whole(feed_in)[0].reshape(streams * length, width)
    flat_three = grad_three.reshape(streams * length, width)

    gate_pre = dot_nn(feed_in, gate_weight)
    up_pre = dot_nn(feed_in, up_weight)
    grad_inner = dot_nt(flat_three, down_weight)
    unit, pull = jax.vjp(gated_unit, gate_pre, up_pre)
    inner = unit.astype(BF)
    grad_gate, grad_up = pull(grad_inner)
    grad_gate = grad_gate.astype(BF)
    grad_up = grad_up.astype(BF)
    layer_part = dot_nn(inner, down_weight).astype(BF)
    feed_part = (dot_nt(grad_gate, gate_weight) + dot_nt(grad_up, up_weight)).astype(BF)

    def finish_three(m, total, others, extra):
        hidden_ref, gain_ref, cot_ref = others
        if m >= streams:
            return (hidden_ref[m - streams] + total).astype(BF)
        grad_in, gain_grad = norm_back(hidden_ref[m], gain_ref[...], total)
        grad_two = cot_ref[m, place()[1]].astype(F32) + grad_in
        extra[0][m] = grad_two
        extra[1][...] = gain_grad if m == 0 else extra[1][...] + gain_grad
        return grad_two.astype(BF)

    feed_grads = jnp.stack(
        [
            dot_tn(feed_in, grad_gate).astype(BF),
            dot_tn(feed_in, grad_up).astype(BF),
            dot_tn(flat_three, inner).astype(BF),
        ]
    )
    shape = (1, streams, length, width)
    both, grad_two, feed_gain_grad = exchange(
        "exchange_three", 4, seq_count, [split(feed_part.reshape(shape)), split(layer_part.reshape(shape))],
        [hidden_two, row(feed_gain), quarters(grad_three)], 0, 0, finish_three, [state, gain_state],
    )
    both = whole(both)[0]
    grad_att_out = both[:streams]
    layer_output = both[streams:]

    dq, dk, dv, attn_part = attend_back(
        q, k, v, lse, grad_att_out, id_rows[: hops + 1], id_cols[0], query_weight, key_weight, value_weight, output_weight
    )

    go = grad_att_out.reshape(tokens_flat, width)
    attn_grads = jnp.concatenate(
        [
            dot_tn(attn_ext[0].reshape(tokens_flat, width), dq.reshape(tokens_flat, -1)).astype(BF),
            dot_tn(attn_ext.reshape(-1, width), dk.reshape(-1, dk.shape[-1])).astype(BF),
            dot_tn(attn_ext.reshape(-1, width), dv.reshape(-1, dv.shape[-1])).astype(BF),
            dot_tn(go, attended.reshape(tokens_flat, -1)).astype(BF),
        ],
        axis=1,
    )

    def finish_four(m, total, others, extra):
        hidden_ref, gain_ref, grad_ref = others
        grad_in, gain_grad = norm_back(hidden_ref[m], gain_ref[...], total)
        grad_one = grad_ref[m] + grad_in
        extra[0][m] = grad_one
        extra[1][...] = gain_grad if m == 0 else extra[1][...] + gain_grad
        return grad_one.astype(BF)

    grad_stu, grad_one, attn_gain_grad = exchange(
        "exchange_four", 5, seq_count, [split(attn_part)], [hidden_one, row(attention_gain), grad_two], hops, 0,
        finish_four, [state, gain_state],
    )
    grad_stu = whole(grad_stu)[0]
    grad_conv = jnp.einsum("mte,kde->kmtd", grad_stu, filter_proj, preferred_element_type=F32).astype(BF)
    grad_lagged = jnp.einsum("mte,ice->imtc", grad_stu, lag_proj, preferred_element_type=F32)
    ext_grad = jnp.zeros((streams, 8 + length, channels), F32)
    for step in range(1, lag_order + 1):
        term = jnp.where(masks[step - 1], grad_lagged[step - 1], 0.0)
        ext_grad = ext_grad + jnp.pad(term, ((0, 0), (8 - step, step), (0, 0)))
    terms = convolve_back(
        grad_conv, id_rows[0], id_cols, base_back, ext_grad[:, 8:], ext_grad[:, :8], seq_count
    )

    def finish_five(m, total, others, extra):
        x_ref, gain_ref, grad_ref = others
        grad_in, gain_grad = norm_back(x_ref[m, place()[1]].astype(F32), gain_ref[...], total)
        extra[0][...] = gain_grad if m == 0 else extra[0][...] + gain_grad
        return (grad_ref[m] + grad_in).astype(BF)

    input_gradient, stu_gain_grad = exchange(
        "exchange_five", 6, seq_count, [split(terms)], [quarters(x), row(stu_gain), grad_one], seq_count - 1, 0,
        finish_five, [gain_state],
    )
    input_gradient = whole(input_gradient)[0]
    stu = grad_stu.reshape(tokens_flat, width)
    filter_part = jnp.einsum("kmtd,mte->kde", conv, grad_stu, preferred_element_type=F32).astype(BF)
    lag_part = jnp.concatenate(
        [dot_tn(stu, lag_stack[i].reshape(tokens_flat, channels)).astype(BF) for i in range(lag_order)], axis=1
    )
    feed_grads = lax.psum(
        lax.psum_scatter(feed_grads, "seq", scatter_dimension=1, tiled=True), "dp"
    ).astype(F32)
    attn_grads = lax.psum(lax.psum_scatter(attn_grads, "seq", scatter_dimension=0, tiled=True), "dp").astype(F32)
    filter_grad = lax.psum(
        lax.psum_scatter(filter_part, "seq", scatter_dimension=1, tiled=True), "dp"
    ).astype(F32)
    lag_grad = lax.psum(lax.psum_scatter(lag_part, "seq", scatter_dimension=0, tiled=True), "dp").astype(F32)
    gains = jnp.concatenate([stu_gain_grad, attn_gain_grad, feed_gain_grad], axis=0)
    gains = lax.psum(gains, ("dp", "seq", "tensor"))
    gain_width = width // seq_count
    gains = lax.dynamic_slice_in_dim(gains, lax.axis_index("seq") * gain_width, gain_width, 1)
    return answer(layer_output, input_gradient, gains, filter_grad, lag_grad, attn_grads, feed_grads)


def solution(mesh):
    return jax.shard_map(
        functools.partial(local, mesh.shape["seq"]),
        mesh=mesh,
        in_specs=(
            P(None, "dp", "seq", None),
            P(None, "dp", "seq"),
            P("tensor", None),
            P(),
            P("tensor", None, None),
            P(None, "tensor", None),
            P(),
            P(None, "tensor"),
            P(None, "tensor"),
            P(None, "tensor"),
            P("tensor", None),
            P(),
            P(None, "tensor"),
            P(None, "tensor"),
            P("tensor", None),
            P(None, "dp", "seq", None),
        ),
        out_specs=(
            P(None, "dp", "seq", None),
            P(None, "dp", "seq", None),
            P("seq"),
            P("tensor", "seq", None),
            P(None, "tensor", "seq"),
            P("seq"),
            P("seq", "tensor"),
            P("seq", "tensor"),
            P("seq", "tensor"),
            P("tensor", "seq"),
            P("seq"),
            P("seq", "tensor"),
            P("seq", "tensor"),
            P("tensor", "seq"),
        ),
        check_vma=False,
    )
```

```python
import functools

import jax
import jax.numpy as jnp
from jax import lax
from jax.experimental import pallas as pl
from jax.experimental.pallas import tpu as pltpu
from jax.sharding import PartitionSpec as P

HD = 64
WINDOW = 1024
EPSILON = 1e-05
LANES = 128
NEGATIVE = -1e30
MESH = pl.DeviceIdType.MESH
BF = jnp.bfloat16
F32 = jnp.float32
VMEM_LIMIT = 63 * 1024 * 1024


def place():
    s = lax.axis_index("seq")
    t = lax.axis_index("tensor")
    y = t // 2
    c = t - 2 * y
    return s, t, y, c, t + 1 - 2 * c, t + 2 - 4 * y


def when(condition, action):
    if condition is True:
        action()
    else:
        pl.when(condition)(action)


def remote(src, dst, send_sem, recv_sem, device):
    return pltpu.make_async_remote_copy(
        src_ref=src, dst_ref=dst, send_sem=send_sem, recv_sem=recv_sem, device_id=device, device_id_type=MESH
    )


def greet(seq_count, hops, wide=False, gains=False):
    s, t, y, c, core, far = place()
    barrier = pltpu.get_barrier_semaphore()

    def signal(device):
        pl.semaphore_signal(barrier, inc=1, device_id=device, device_id_type=MESH)

    signal({"tensor": core})
    signal({"tensor": far})
    if gains:
        signal({"tensor": 3 - t})
    if wide:
        p = lax.axis_index("dp")
        signal({"dp": 1 - p})
        for j in range(seq_count):

            @pl.when(s != j)
            def _():
                signal({"seq": j})
                if gains:
                    signal({"dp": 1 - p, "seq": j})

        peers = 2 + gains + 1 + (seq_count - 1) * (1 + gains)
    else:
        for h in range(1, hops + 1):
            for there, peer in ((s - h >= 0, s - h), (s + h < seq_count, s + h)):

                @pl.when(there)
                def _():
                    signal({"seq": peer})

        peers = 2 + jnp.minimum(s, hops) + jnp.minimum(seq_count - 1 - s, hops)
    pl.semaphore_wait(barrier, peers)


class ReduceScatter:
    def __init__(self, seq_count, hops, streams, part, scratch):
        self.seq_count, self.hops, self.streams, self.part = seq_count, hops, streams, part
        self.near, self.half, self.over, self.hop_out, self.hop_in, self.sem = scratch
        self.pieces, self.rows = self.half.shape[2:4]

    @staticmethod
    def scratch(hops, streams, rows, width, pieces=1):
        quarter = (hops + 1, streams, pieces, rows // pieces, width)
        over_seq = quarter if hops else (1, 1, 1, 16, LANES)
        return [
            pltpu.VMEM((hops + 1, streams, pieces, 2, rows // pieces, width), BF),
            pltpu.VMEM(quarter, BF),
            pltpu.VMEM(quarter, BF),
            pltpu.VMEM(over_seq, BF),
            pltpu.VMEM(over_seq, BF),
            pltpu.SemaphoreType.DMA((6, hops + 1, streams, pieces)),
        ]

    def span(self, n):
        return slice(n * self.rows, (n + 1) * self.rows)

    def move(self, kind, source, target, h, m, n, device, at=None):
        at = h if at is None else at
        return remote(source, target, self.sem.at[2 * kind, h, m, n], self.sem.at[2 * kind + 1, at, m, n], device)

    def to_core(self, h, m, n):
        s, t, y, c, core, far = place()
        source = self.part(h, m).at[:, 1 - c, pl.ds(n * self.rows, self.rows)]
        return self.move(0, source, self.near.at[h, m, n], h, m, n, {"tensor": core})

    def to_far(self, h, m, n):
        far = place()[5]
        return self.move(1, self.half.at[h, m, n], self.over.at[h, m, n], h, m, n, {"tensor": far})

    def to_hop(self, h, m, n):
        peer = {"seq": lax.axis_index("seq") - 1}
        return self.move(2, self.hop_out.at[h, m, n], self.hop_in.at[h - 1, m, n], h, m, n, peer, at=h - 1)

    def add_hop(self, h, m, acc):
        s = lax.axis_index("seq")

        @pl.when(s + 1 < self.seq_count)
        def _():
            for n in range(self.pieces):
                ref = self.hop_in.at[h, m, n]
                self.move(2, self.hop_out.at[h, m, n], ref, h, m, n, {"seq": s + 1}).wait_recv()
                acc[self.span(n)] += self.hop_in[h, m, n].astype(F32)

    def there(self, h):
        return True if isinstance(h, int) and h == 0 else lax.axis_index("seq") - h >= 0

    def order(self):
        return [(h, m) for h in range(self.hops, -1, -1) for m in range(self.streams)]

    def start(self, h, m):
        def act():
            for n in range(self.pieces):
                self.to_core(h, m, n).start()

        when(self.there(h), act)

    def middle(self, h, m):
        s, t, y, c, core, far = place()

        def act():
            for n in range(self.pieces):
                self.to_core(h, m, n).wait_recv()
                mine = self.part(h, m)[1 - y, c, self.span(n)].astype(F32) + self.near[h, m, n, 1 - y].astype(F32)
                self.half[h, m, n] = mine.astype(BF)
                self.to_far(h, m, n).start()

        when(self.there(h), act)

    def own(self, h, m, acc):
        s, t, y, c, core, far = place()
        for n in range(self.pieces):
            self.to_far(h, m, n).wait_recv()
            mine = self.part(h, m)[y, c, self.span(n)].astype(F32) + self.near[h, m, n, y].astype(F32)
            acc[self.span(n)] = mine + self.over[h, m, n].astype(F32)

    def hop(self, h, m, acc):
        def act():
            self.own(h, m, acc)
            if isinstance(h, int):
                if h < self.hops:
                    self.add_hop(h, m, acc)
            else:
                pl.when(h < self.hops)(lambda: self.add_hop(h, m, acc))
            for n in range(self.pieces):
                self.hop_out[h, m, n] = acc[self.span(n)].astype(BF)
                self.to_hop(h, m, n).start()

        when(self.there(h), act)

    def total(self, m, acc):
        self.own(0, m, acc)
        if self.hops:
            self.add_hop(0, m, acc)

    def drain(self):
        for h, m in self.order():

            def act():
                for n in range(self.pieces):
                    self.to_core(h, m, n).wait_send()
                    self.to_far(h, m, n).wait_send()
                    if h:
                        self.to_hop(h, m, n).wait_send()

            when(self.there(h), act)


class AllGather:
    def __init__(self, seq_count, hops, streams, at, sem, first=0):
        self.seq_count, self.hops, self.streams, self.sem, self.first = seq_count, hops, streams, sem, first
        self.at = at if callable(at) else lambda h, m, quarter: at.at[h, m, quarter]
        self.pieces = sem.shape[3]

    @staticmethod
    def scratch(hops, streams, pieces=1):
        return [pltpu.SemaphoreType.DMA((8, hops + 1, streams, pieces))]

    def there(self, h):
        return True if h == 0 else lax.axis_index("seq") - h >= 0

    def piece(self, h, m, quarter, n):
        ref = self.at(h, m, quarter)
        rows = ref.shape[0] // self.pieces
        return ref.at[pl.ds(n * rows, rows)]

    def copy(self, kind, h, m, quarter, n, device):
        ref = self.piece(h, m, quarter, n)
        return remote(ref, ref, self.sem.at[2 * kind, h, m, n], self.sem.at[2 * kind + 1, h, m, n], device)

    def relay(self, h, m, n):
        s, t = lax.axis_index("seq"), place()[1]
        return remote(
            self.piece(h, m, t, n),
            self.piece(h + 1, m, t, n),
            self.sem.at[0, h, m, n],
            self.sem.at[1, h + 1, m, n],
            {"seq": s + 1},
        )

    def relays(self, h):
        s = lax.axis_index("seq")
        return (s - h >= 0) & (s + 1 < self.seq_count)

    def forward(self, h, m, n):
        if h < self.hops:
            pl.when(self.relays(h))(lambda: self.relay(h, m, n).start())

    def spread(self, h, m, n):
        s, t, y, c, core, far = place()
        self.copy(1, h, m, t, n, {"tensor": far}).start()
        self.copy(2, h, m, t, n, {"tensor": core}).start()

    def start(self, m):
        for n in range(self.pieces):
            self.forward(0, m, n)
            if self.first == 0:
                self.spread(0, m, n)

    def arrive(self, h, m):
        @pl.when(self.there(h))
        def _():
            for n in range(self.pieces):
                self.copy(0, h, m, place()[1], n, {"seq": lax.axis_index("seq") - 1}).wait_recv()
                self.forward(h, m, n)
                self.spread(h, m, n)

    def pass_on(self, h, m):
        s, t, y, c, core, far = place()

        def act():
            for n in range(self.pieces):
                self.copy(1, h, m, far, n, {"tensor": far}).wait_recv()
                self.copy(3, h, m, far, n, {"tensor": core}).start()

        when(self.there(h), act)

    def finish(self, h, m):
        s, t, y, c, core, far = place()

        def act():
            for n in range(self.pieces):
                self.copy(2, h, m, core, n, {"tensor": core}).wait_recv()
                self.copy(3, h, m, 3 - t, n, {"tensor": core}).wait_recv()

        when(self.there(h), act)

    def clear(self, h, m):
        @pl.when(lax.axis_index("seq") - h < 0)
        def _():
            for quarter in range(4):
                ref = self.at(h, m, quarter)
                ref[...] = jnp.zeros(ref.shape, ref.dtype)

    def drain(self):
        s, t, y, c, core, far = place()
        for m in range(self.streams):
            for n in range(self.pieces):
                for h in range(self.hops):
                    pl.when(self.relays(h))(functools.partial(lambda h, m, n: self.relay(h, m, n).wait_send(), h, m, n))
                for h in range(self.first, self.hops + 1):

                    def act():
                        self.copy(1, h, m, t, n, {"tensor": far}).wait_send()
                        self.copy(2, h, m, t, n, {"tensor": core}).wait_send()
                        self.copy(3, h, m, far, n, {"tensor": core}).wait_send()

                    when(self.there(h), act)


class GradReduce:
    def __init__(self, seq_count, source, result, scratch):
        self.seq_count, self.source, self.result = seq_count, source, result
        self.x_in, self.z_out, self.z_in, self.back_out, self.back_in, self.x_sem, self.z_sem, self.back_sem = scratch
        self.half = self.x_in.shape[2]
        self.rows = self.back_out.shape[1]

    @staticmethod
    def scratch(seq_count, chunks, depth, width):
        rows, half = depth // seq_count, width // 2
        return [
            pltpu.VMEM((chunks, depth, half), BF),
            pltpu.VMEM((chunks, depth, half), BF),
            pltpu.VMEM((chunks, seq_count, rows, half), BF),
            pltpu.VMEM((chunks, rows, half), BF),
            pltpu.VMEM((chunks, rows, half), BF),
            pltpu.SemaphoreType.DMA((2, chunks)),
            pltpu.SemaphoreType.DMA((2, chunks, seq_count)),
            pltpu.SemaphoreType.DMA((2, chunks)),
        ]

    def columns(self, p):
        return pl.ds(pl.multiple_of(p * self.half, LANES), self.half)

    def block(self, j):
        return pl.ds(pl.multiple_of(j * self.rows, 16), self.rows)

    def over(self, c):
        p = lax.axis_index("dp")
        return remote(
            self.source(c).at[:, self.columns(1 - p)], self.x_in.at[c], self.x_sem.at[0, c], self.x_sem.at[1, c], {"dp": 1 - p}
        )

    def row_copy(self, c, j, slot):
        return remote(
            self.z_out.at[c, self.block(j)], self.z_in.at[c, slot], self.z_sem.at[0, c, j], self.z_sem.at[1, c, slot], {"seq": j}
        )

    def back(self, c):
        p = lax.axis_index("dp")
        return remote(
            self.back_out.at[c], self.back_in.at[c], self.back_sem.at[0, c], self.back_sem.at[1, c], {"dp": 1 - p}
        )

    def others(self, action):
        for j in range(self.seq_count):
            pl.when(lax.axis_index("seq") != j)(functools.partial(action, j))

    def start(self, c):
        self.over(c).start()

    def spread(self, c):
        s, p = lax.axis_index("seq"), lax.axis_index("dp")
        self.over(c).wait_recv()
        mine = self.source(c)[:, self.columns(p)].astype(F32) + self.x_in[c].astype(F32)
        self.z_out[c] = mine.astype(BF)
        self.others(lambda j: self.row_copy(c, j, s).start())

    def collect(self, c, acc):
        s, p = lax.axis_index("seq"), lax.axis_index("dp")
        here = self.block(s)
        acc[...] = self.source(c)[here, self.columns(p)].astype(F32) + self.x_in[c, here].astype(F32)

        def add(j):
            self.row_copy(c, j, j).wait_recv()
            acc[...] += self.z_in[c, j].astype(F32)

        self.others(add)
        self.back_out[c] = acc[...].astype(BF)
        self.back(c).start()

    def finish(self, c):
        p = lax.axis_index("dp")
        self.back(c).wait_recv()
        self.result(c)[:, self.columns(p)] = self.back_out[c]
        self.result(c)[:, self.columns(1 - p)] = self.back_in[c]

    def drain(self, c):
        self.over(c).wait_send()
        self.others(lambda j: self.row_copy(c, j, lax.axis_index("seq")).wait_send())
        self.back(c).wait_send()


def params(cid=None):
    if cid is None:
        return pltpu.CompilerParams(vmem_limit_bytes=VMEM_LIMIT)
    return pltpu.CompilerParams(vmem_limit_bytes=VMEM_LIMIT, collective_id=cid, has_side_effects=True)


def in_vmem(count):
    return [pl.BlockSpec(memory_space=pltpu.VMEM)] * count


def gather_rows(inputs, ids, seq_count):
    streams, quarters, rows, width = inputs.shape
    hops = seq_count - 1

    def kernel(x_ref, id_ref, out, out_ids, sem, id_sem):
        s, t, y, c, core, far = place()
        greet(seq_count, hops)
        out[0] = x_ref[...]
        out_ids[0] = id_ref[...]
        ag = AllGather(seq_count, hops, streams, out, sem, first=1)

        def id_copy(h, peer):
            return remote(id_ref, out_ids.at[h], id_sem.at[0, h], id_sem.at[1, h], {"seq": peer})

        for h in range(1, hops + 1):

            @pl.when(s + h < seq_count)
            def _():
                id_copy(h, s + h).start()

        for m in range(streams):
            ag.start(m)
        for h in range(1, hops + 1):
            for m in range(streams):
                ag.clear(h, m)

            @pl.when(s - h < 0)
            def _():
                out_ids[h] = jnp.full(out_ids.shape[1:], -1, jnp.int32)

        for m in range(streams):
            for h in range(1, hops + 1):
                ag.arrive(h, m)
        for m in range(streams):
            for h in range(1, hops + 1):
                ag.pass_on(h, m)
        for h in range(1, hops + 1):
            for m in range(streams):
                ag.finish(h, m)

            @pl.when(s - h >= 0)
            def _():
                id_copy(h, s - h).wait_recv()

            @pl.when(s + h < seq_count)
            def _():
                id_copy(h, s + h).wait_send()

        ag.drain()

    return pl.pallas_call(
        kernel,
        name="gather_rows",
        out_shape=(
            jax.ShapeDtypeStruct((seq_count,) + inputs.shape, inputs.dtype),
            jax.ShapeDtypeStruct((seq_count,) + ids.shape, jnp.int32),
        ),
        in_specs=in_vmem(2),
        out_specs=tuple(in_vmem(2)),
        scratch_shapes=AllGather.scratch(hops, streams) + [pltpu.SemaphoreType.DMA((2, seq_count))],
        compiler_params=params(1),
    )(inputs, ids)


def exchange(name, cid, seq_count, parts, others, reduce_hops, gather_hops, finish, extra):
    per_part = parts[0].shape[1]
    rows, width = parts[0].shape[4:]
    streams = per_part * len(parts)
    hops = max(reduce_hops, gather_hops)

    def kernel(*refs):
        refs = list(refs)
        part_refs = [refs.pop(0) for _ in parts]
        other_refs = [refs.pop(0) for _ in others]
        out = refs.pop(0)
        extra_refs = [refs.pop(0) for _ in extra]
        acc = refs.pop(0)
        gather_sem = refs.pop(0)
        s, t, y, c, core, far = place()
        greet(seq_count, hops)
        rs = ReduceScatter(
            seq_count, reduce_hops, streams, lambda h, m: part_refs[m // per_part].at[h, m % per_part], refs
        )
        ag = AllGather(seq_count, gather_hops, streams, out, gather_sem)
        for h, m in rs.order():
            rs.start(h, m)
        for h in range(1, gather_hops + 1):
            for m in range(streams):
                ag.clear(h, m)
        for h, m in rs.order():
            rs.middle(h, m)
        for h, m in rs.order():
            if h:
                rs.hop(h, m, acc)
        for m in range(streams):
            rs.total(m, acc)
            out[0, m, t] = finish(m, acc[...], other_refs, extra_refs)
            ag.start(m)
        for m in range(streams):
            ag.pass_on(0, m)
            for h in range(1, gather_hops + 1):
                ag.arrive(h, m)
        for m in range(streams):
            for h in range(1, gather_hops + 1):
                ag.pass_on(h, m)
        for h in range(gather_hops + 1):
            for m in range(streams):
                ag.finish(h, m)
        rs.drain()
        ag.drain()

    return pl.pallas_call(
        kernel,
        name=name,
        out_shape=(jax.ShapeDtypeStruct((gather_hops + 1, streams, 4, rows, width), BF),) + tuple(extra),
        in_specs=in_vmem(len(parts) + len(others)),
        out_specs=tuple(in_vmem(1 + len(extra))),
        scratch_shapes=[pltpu.VMEM((rows, width), F32)]
        + AllGather.scratch(gather_hops, streams)
        + ReduceScatter.scratch(reduce_hops, streams, rows, width),
        compiler_params=params(cid),
    )(*parts, *others)


def norm_of(values, gain_row):
    inverse = lax.rsqrt(jnp.mean(values * values, axis=-1, keepdims=True) + EPSILON)
    return values * inverse * gain_row


def norm_back(values, gain_row, grad_out):
    inverse = lax.rsqrt(jnp.mean(values * values, axis=-1, keepdims=True) + EPSILON)
    scaled = grad_out * gain_row
    dot = jnp.mean(scaled * values, axis=-1, keepdims=True)
    grad_in = inverse * scaled - values * (inverse * inverse * inverse) * dot
    return grad_in, jnp.sum(grad_out * values * inverse, axis=0, keepdims=True)


def strips(base_ref, strip):
    @pl.loop(0, base_ref.shape[0])
    def _(k):
        taps = base_ref[k] if len(base_ref.shape) == 3 else base_ref[pl.ds(k, 1)]
        row = jnp.broadcast_to(taps, strip.shape[1:])
        strip[k] = pltpu.roll(row, 0, 1, stride=1, stride_axis=0).astype(BF)


def lay_taps(taps_ref, base_ref, back):
    count, length = taps_ref.shape
    blocks = length // LANES
    base_ref[...] = jnp.zeros_like(base_ref)
    if back:
        base_ref[:, 3 * LANES : 3 * LANES + length] = taps_ref[...].astype(F32)
        return
    row = lax.broadcasted_iota(jnp.int32, (LANES, LANES), 0)
    lane = lax.broadcasted_iota(jnp.int32, (LANES, LANES), 1)
    turn = jnp.where(row + lane == LANES, 1.0, 0.0).astype(BF)
    first = lax.broadcasted_iota(jnp.int32, (count, LANES), 1) == 0
    turned = [dot_nn(taps_ref[:, j * LANES : (j + 1) * LANES], turn) for j in range(blocks)]
    for b in range(blocks):
        j = blocks - 1 - b
        below = turned[j - 1] if j else jnp.zeros((count, LANES), F32)
        taps = taps_ref[:, j * LANES : (j + 1) * LANES].astype(F32)
        base_ref[:, b * LANES : (b + 1) * LANES] = jnp.where(first, taps, below)
    base_ref[:, (blocks + 3) * LANES :] = turned[blocks - 1]


def convolve(rows, row_ids, col_ids, base, seq_count):
    _, streams, length, width = rows.shape
    count, _, wide = base.shape
    blocks = length // LANES
    at_once = seq_count <= 4

    def whole_kernel(x_ref, row_ref, col_ref, base_ref, out_ref, strip, mask, left):
        strips(base_ref, strip)

        @pl.loop(0, streams)
        def _(m):
            for h in range(seq_count):
                mask[:, h * length : (h + 1) * length] = jnp.where(col_ref[m] == row_ref[h, m], 1.0, 0.0).astype(BF)
            right = jnp.concatenate([x_ref[h, m] for h in range(seq_count)], axis=0)

            @pl.loop(0, count)
            def _(k):
                for a in range(blocks):
                    for h in range(seq_count):
                        start = LANES * (blocks * (seq_count - h) - 1 - a)
                        down, across = slice(a * LANES, (a + 1) * LANES), slice(h * length, (h + 1) * length)
                        left[down, across] = strip[k, :, start : start + length] * mask[down, across]
                out_ref[k, m] = jnp.dot(left[...], right, preferred_element_type=F32).astype(BF)

    def kernel(x_ref, row_ref, col_ref, base_ref, out_ref, strip, mask, acc):
        strips(base_ref, strip)
        s = lax.axis_index("seq")

        @pl.loop(0, streams)
        def _(m):
            acc[...] = jnp.zeros_like(acc)

            @pl.loop(0, s + 1)
            def _(h):
                mask[...] = jnp.where(col_ref[m] == row_ref[h, m], 1.0, 0.0).astype(BF)

                @pl.loop(0, count)
                def _(k):
                    pieces = []
                    for a in range(blocks):
                        start = pl.multiple_of(LANES * (blocks * (seq_count - h) - 1 - a), LANES)
                        pieces.append(strip[k, :, pl.ds(start, length)] * mask[a * LANES : (a + 1) * LANES])
                    acc[k] += jnp.dot(jnp.concatenate(pieces, axis=0), x_ref[h, m], preferred_element_type=F32)

            @pl.loop(0, count)
            def _(k):
                out_ref[k, m] = acc[k].astype(BF)

    span = seq_count * length if at_once else length
    return pl.pallas_call(
        whole_kernel if at_once else kernel,
        name="convolve",
        out_shape=jax.ShapeDtypeStruct((count, streams, length, width), BF),
        in_specs=in_vmem(4),
        out_specs=in_vmem(1)[0],
        scratch_shapes=[
            pltpu.VMEM((count, LANES, wide), BF),
            pltpu.VMEM((length, span), BF),
            pltpu.VMEM((length, span), BF) if at_once else pltpu.VMEM((count, length, width), F32),
        ],
        compiler_params=params(),
    )(rows, row_ids, col_ids, base)


def convolve_back(grads, row_ids, col_ids, base, own_lag, tail_lag, seq_count):
    count, streams, length, width = grads.shape
    wide = base.shape[2]
    blocks = length // LANES
    channels = own_lag.shape[2]
    tail_rows = tail_lag.shape[1]

    def kernel(g_ref, row_ref, col_ref, base_ref, own_ref, tail_ref, out_ref, strip, mask, acc):
        strips(base_ref, strip)
        s = lax.axis_index("seq")
        mine = pl.ds(pl.multiple_of(lax.axis_index("tensor") * channels, LANES), channels)

        @pl.loop(0, s + 1)
        def _(h):
            @pl.loop(0, streams)
            def _(m):
                mask[...] = jnp.where(col_ref[h, m] == row_ref[m], 1.0, 0.0).astype(BF)
                acc[...] = jnp.zeros_like(acc)

                @pl.when(h == 0)
                def _():
                    acc[:, mine] = own_ref[m]

                @pl.when(h == 1)
                def _():
                    acc[length - tail_rows :, mine] = tail_ref[m]

                @pl.loop(0, count)
                def _(k):
                    pieces = []
                    for a in range(blocks):
                        start = pl.multiple_of(LANES * (blocks * h + blocks - 1 - a), LANES)
                        pieces.append(strip[k, :, pl.ds(start, length)] * mask[a * LANES : (a + 1) * LANES])
                    acc[...] += jnp.dot(jnp.concatenate(pieces, axis=0), g_ref[k, m], preferred_element_type=F32)

                out_ref[h, m] = acc[...].astype(BF)

    return pl.pallas_call(
        kernel,
        name="convolve_back",
        out_shape=jax.ShapeDtypeStruct((seq_count, streams, length, width), BF),
        in_specs=in_vmem(6),
        out_specs=in_vmem(1)[0],
        scratch_shapes=[
            pltpu.VMEM((count, LANES, wide), BF),
            pltpu.VMEM((length, length), BF),
            pltpu.VMEM((length, width), F32),
        ],
        compiler_params=params(),
    )(grads, row_ids, col_ids, base, own_lag, tail_lag)


def dot_nn(a, b):
    return jnp.dot(a, b, preferred_element_type=F32)


def dot_nt(a, b):
    return lax.dot_general(a, b, (((1,), (1,)), ((), ())), preferred_element_type=F32)


def dot_tn(a, b):
    return lax.dot_general(a, b, (((0,), (0,)), ((), ())), preferred_element_type=F32)


def allowed_keys(query_ids, key_ids, first_row, distance):
    shape = (query_ids.shape[0], key_ids.shape[1])
    offset = lax.broadcasted_iota(jnp.int32, shape, 0) - lax.broadcasted_iota(jnp.int32, shape, 1) + (first_row + distance)
    return (query_ids == key_ids) & (offset >= 0) & (offset < WINDOW)


def one_head(block, head):
    lane = lax.broadcasted_iota(jnp.int32, block.shape, 1)
    return jnp.where((lane >= head * HD) & (lane < (head + 1) * HD), block, jnp.zeros_like(block))


def attend(rows, row_ids, col_ids, wq, wk, wv, wo):
    spans, streams, length, width = rows.shape
    cols = wq.shape[1]
    heads = cols // HD
    tile = min(256, length)
    scale = HD ** (-0.5)

    def kernel(x_ref, row_ref, col_ref, wq_ref, wk_ref, wv_ref, wo_ref, q_ref, k_ref, v_ref, a_ref, lse_ref, p_ref):
        @pl.loop(0, streams)
        def _(m):
            q_ref[m] = dot_nn(x_ref[0, m], wq_ref[...]).astype(BF)
            for h in range(spans):
                k_ref[h, m] = dot_nn(x_ref[h, m], wk_ref[...]).astype(BF)
                v_ref[h, m] = dot_nn(x_ref[h, m], wv_ref[...]).astype(BF)

            @pl.loop(0, length // tile)
            def _(i):
                first = pl.multiple_of(i * tile, tile)
                here = pl.ds(first, tile)
                masks = [allowed_keys(col_ref[m, here], row_ref[h, m], first, h * length) for h in range(spans)]
                block = q_ref[m, here]
                result = jnp.zeros((tile, cols), F32)
                for head in range(heads):
                    query = one_head(block, head)
                    scores = [
                        jnp.where(masks[h], dot_nt(query, k_ref[h, m]) * scale, NEGATIVE) for h in range(spans)
                    ]
                    peak = functools.reduce(jnp.maximum, [jnp.max(v, axis=-1, keepdims=True) for v in scores])
                    raised = [jnp.exp(v - peak) for v in scores]
                    total = sum([jnp.sum(v, axis=-1, keepdims=True) for v in raised])
                    inverse = 1.0 / total
                    mixed = sum([dot_nn((raised[h] * inverse).astype(BF), v_ref[h, m]) for h in range(spans)])
                    result = result + one_head(mixed, head)
                    lse_ref[m, head, here] = jnp.broadcast_to(peak + jnp.log(total), (tile, LANES))
                a_ref[m, here] = result.astype(BF)

            p_ref[m] = dot_nn(a_ref[m], wo_ref[...]).astype(BF)

    part = jax.ShapeDtypeStruct((streams, length, cols), BF)
    span = jax.ShapeDtypeStruct((spans, streams, length, cols), BF)
    return pl.pallas_call(
        kernel,
        name="attend",
        out_shape=(
            part,
            span,
            span,
            part,
            jax.ShapeDtypeStruct((streams, heads, length, LANES), F32),
            jax.ShapeDtypeStruct((streams, length, width), BF),
        ),
        in_specs=in_vmem(7),
        out_specs=tuple(in_vmem(6)),
        compiler_params=params(),
    )(rows, row_ids, col_ids, wq, wk, wv, wo)


def attend_back(q, k, v, lse, grad_out, row_ids, col_ids, wq, wk, wv, wo):
    spans, streams, length, cols = k.shape
    width = grad_out.shape[2]
    heads = cols // HD
    tile = min(256, length)
    scale = HD ** (-0.5)

    def kernel(
        q_ref, k_ref, v_ref, lse_ref, go_ref, row_ref, col_ref, wq_ref, wk_ref, wv_ref, wo_ref,
        dq_ref, dk_ref, dv_ref, p_ref, ga_ref, dk_acc, dv_acc,
    ):
        @pl.loop(0, streams)
        def _(m):
            ga_ref[...] = dot_nt(go_ref[m], wo_ref[...]).astype(BF)
            dk_acc[...] = jnp.zeros_like(dk_acc)
            dv_acc[...] = jnp.zeros_like(dv_acc)

            @pl.loop(0, length // tile)
            def _(i):
                first = pl.multiple_of(i * tile, tile)
                here = pl.ds(first, tile)
                masks = [allowed_keys(col_ref[m, here], row_ref[h, m], first, h * length) for h in range(spans)]
                block = q_ref[m, here]
                grad_block = ga_ref[here]
                result = jnp.zeros((tile, cols), F32)
                for head in range(heads):
                    query = one_head(block, head)
                    grad = one_head(grad_block, head)
                    level = lse_ref[m, head, here][:, :1]
                    prob = [
                        jnp.where(masks[h], jnp.exp(dot_nt(query, k_ref[h, m]) * scale - level), 0.0)
                        for h in range(spans)
                    ]
                    grad_prob = [dot_nt(grad, v_ref[h, m]) for h in range(spans)]
                    mean = sum([jnp.sum(p * g, axis=-1, keepdims=True) for p, g in zip(prob, grad_prob)])
                    grad_scores = [(p * (g - mean)).astype(BF) for p, g in zip(prob, grad_prob)]
                    for h in range(spans):
                        dv_acc[h] += dot_tn(prob[h].astype(BF), grad)
                        dk_acc[h] += dot_tn(grad_scores[h], query)
                    mixed = sum([dot_nn(grad_scores[h], k_ref[h, m]) for h in range(spans)])
                    result = result + one_head(mixed, head)
                dq_ref[m, here] = (result * scale).astype(BF)

            for h in range(spans):
                dk_ref[h, m] = (dk_acc[h] * scale).astype(BF)
                dv_ref[h, m] = dv_acc[h].astype(BF)
                back = dot_nt(dk_ref[h, m], wk_ref[...]) + dot_nt(dv_ref[h, m], wv_ref[...])
                if h == 0:
                    back = back + dot_nt(dq_ref[m], wq_ref[...])
                p_ref[h, m] = back.astype(BF)

    span = jax.ShapeDtypeStruct((spans, streams, length, cols), BF)
    return pl.pallas_call(
        kernel,
        name="attend_back",
        out_shape=(
            jax.ShapeDtypeStruct((streams, length, cols), BF),
            span,
            span,
            jax.ShapeDtypeStruct((spans, streams, length, width), BF),
        ),
        in_specs=in_vmem(11),
        out_specs=tuple(in_vmem(4)),
        scratch_shapes=[
            pltpu.VMEM((length, cols), BF),
            pltpu.VMEM((spans, length, cols), F32),
            pltpu.VMEM((spans, length, cols), F32),
        ],
        compiler_params=params(),
    )(q, k, v, lse, grad_out, row_ids, col_ids, wq, wk, wv, wo)


def unit_terms(gate_pre, up_pre, grad_inner):
    root = 0.7978845608028654
    square = gate_pre * gate_pre
    bend = jnp.tanh(root * (gate_pre + 0.044715 * (gate_pre * square)))
    half = 0.5 * (1.0 + bend)
    gelu = gate_pre * half
    slope = half + 0.5 * gate_pre * (1.0 - bend * bend) * (root * (1.0 + 3.0 * 0.044715 * square))
    return gelu * up_pre, grad_inner * up_pre * slope, grad_inner * gelu


def head(
    x, ids, stu_gain, filter_proj, lag_proj, filters, attn_gain, feed_gain, wq, wk, wv, wo, wg, wu, wd, cot, seq_count
):
    streams, _, quarter, width = x.shape
    length = 4 * quarter
    hops = WINDOW // length
    spans = hops + 1
    count, taps = filters.shape
    wide = taps + 4 * LANES
    lag_order, channels = lag_proj.shape[:2]
    blocks = length // LANES
    reach = taps * 5 // 8
    window = reach + 2 * quarter
    own = 4 * (seq_count - 1)
    assert reach % (2 * quarter) == 0 and window <= taps
    cols, units = wq.shape[1], wg.shape[1]
    heads = cols // HD
    tile = 2 * quarter
    steps = 2 * streams
    scale = HD ** (-0.5)
    rows = width // seq_count
    chunks = 4
    assert streams == 2 and units == 4 * cols

    rows_of = pltpu.VMEM((streams, length, cols), BF)
    unit_rows = pltpu.VMEM((streams, length, units), BF)
    state = pltpu.VMEM((streams, quarter, width), F32)
    gathered = (1, streams, 4, quarter, width)
    split_part = pltpu.VMEM((1, streams, 2, 2, quarter, width), BF)
    pieces = 2
    zero_hops = ReduceScatter.scratch(0, streams, quarter, width, pieces)

    def kernel(
        x_ref, id_ref, sg_ref, fp_hbm, lp_ref, taps_ref, ag_ref, fg_ref,
        wq_ref, wk_ref, wv_ref, wo_ref, wg_hbm, wu_hbm, wd_hbm, cot_hbm,
        stu_out, layer_out, one_out, gain_out, sum_out, lag_out, ids_out, conv_out, strip_out,
        fp_ref, wg_ref, wu_ref, wd_ref, cot_ref, load_sem, base_ref, ids_row,
        rows_in, ids_in, cols_in, id_ext, lag_ext, part_ref, id_sem, strip_sem, conv_sem,
        attn_in, feed_in, grad_att, hid_one, hid_two, grad_two, grads, total, grad_acc,
        o_part, feed_part, layer_part, attn_part,
        sem_rows, sem_one, sem_two, sem_three, sem_layer, sem_five, *scratch,
    ):
        s, t, y, c, core, far = place()
        scratch = list(scratch)

        def take(count):
            taken = scratch[:count]
            del scratch[:count]
            return taken

        def reducer(ref, distance):
            return ReduceScatter(seq_count, distance, streams, lambda h, m: ref.at[h, m], take(6))

        rs_one, rs_two, rs_three, rs_layer = [reducer(r, 0) for r in (part_ref, o_part, feed_part, layer_part)]
        rs_four = reducer(attn_part, hops)
        gr = GradReduce(seq_count, lambda k: grads.at[k], lambda k: sum_out.at[k], take(8))
        ag_rows = AllGather(
            seq_count,
            seq_count - 1,
            streams,
            lambda h, m, q: rows_in.at[m, 4 * (seq_count - 1 - h) + q],
            sem_rows,
            first=1,
        )
        ag_one = AllGather(seq_count, hops, streams, attn_in, sem_one)
        ag_two = AllGather(seq_count, 0, streams, feed_in, sem_two)
        ag_three = AllGather(seq_count, 0, streams, grad_att, sem_three)
        ag_layer = AllGather(seq_count, 0, streams, layer_out, sem_layer)
        ag_five = AllGather(seq_count, 0, streams, stu_out, sem_five)

        def flat(value):
            return value.reshape(-1, value.shape[-1])

        def all_rows(ref, m):
            return flat(ref[0, m])

        def masks_of(m, here, first):
            return [
                allowed_keys(cols_in[m, here], ids_out[pl.ds(h * streams + m, 1)], first, h * length) for h in range(spans)
            ]

        def first_norm(m):
            rs_one.total(m, total)
            hidden = x_ref[m, t].astype(F32) + total[...]
            hid_one[m] = hidden
            attn_in[0, m, t] = norm_of(hidden, ag_ref[...]).astype(BF)
            ag_one.start(m)

        def after(i, step, *actions):
            @pl.when(i == step)
            def _():
                for action in actions:
                    action()

        def id_copy(h, peer):
            return remote(id_ref, ids_in.at[h], id_sem.at[0, h], id_sem.at[1, h], {"seq": peer})

        far_back = range(1, seq_count)

        pairs = ((fp_hbm, fp_ref), (wg_hbm, wg_ref), (wu_hbm, wu_ref), (wd_hbm, wd_ref), (cot_hbm, cot_ref))
        loads = [pltpu.make_async_copy(a, b, load_sem.at[i]) for i, (a, b) in enumerate(pairs)]
        for load in loads:
            load.start()

        def front(strip, left, mask, conv):
            for m in range(streams):
                rows_in[m, own + t] = norm_of(x_ref[m, t].astype(F32), sg_ref[...]).astype(BF)
            greet(seq_count, 0, wide=True)
            for m in range(streams):
                ag_rows.start(m)
            for h in far_back:
                pl.when(s + h < seq_count)(functools.partial(lambda h: id_copy(h, s + h).start(), h))
            for m in range(streams):
                for q in range(4):

                    @pl.when(t != q)
                    def _():
                        rows_in[m, own + q] = norm_of(x_ref[m, q].astype(F32), sg_ref[...]).astype(BF)

            for m in range(streams):
                for h in far_back:
                    ag_rows.clear(h, m)
                for h in range(1, spans):
                    ag_one.clear(h, m)
            ids_in[0] = id_ref[...]
            for h in far_back:

                @pl.when(s - h < 0)
                def _():
                    ids_in[h] = jnp.full(ids_in.shape[1:], -1, jnp.int32)

            lay_taps(taps_ref, base_ref, True)
            strips(base_ref, strip)
            strip_copy = pltpu.make_async_copy(strip, strip_out, strip_sem)
            strip_copy.start()
            ag_rows.arrive(1, 0)
            ag_rows.arrive(2, 0)
            for h in far_back:
                pl.when(s - h >= 0)(functools.partial(lambda h: id_copy(h, s - h).wait_recv(), h))
            for h in range(seq_count):
                for m in range(streams):
                    ids_out[h * streams + m : h * streams + m + 1] = ids_in[h, m].astype(F32)
                    start = (seq_count - 1 - h) * length
                    ids_row[m : m + 1, start : start + length] = ids_in[h, m].astype(F32)
            turned = jnp.transpose(ids_out[...])
            for m in range(streams):
                cols_in[m] = turned[:, m : m + 1]
                id_ext[m, :8] = turned[length - 8 :, streams + m : streams + m + 1]
                id_ext[m, 8:] = turned[:, m : m + 1]
            lay_taps(taps_ref, base_ref, False)
            strip_copy.wait()
            strips(base_ref, strip)
            for load in loads:
                load.wait()
            ag_rows.pass_on(1, 0)
            ag_rows.arrive(3, 0)
            ag_rows.pass_on(2, 0)
            ag_rows.finish(1, 0)
            ag_rows.finish(2, 0)
            mine = pl.ds(pl.multiple_of(t * channels, LANES), channels)

            def lags(m):
                lag_ext[:8] = rows_in[m, own - 1, quarter - 8 :, mine].astype(F32)
                lag_ext[8:] = rows_in[m, own : own + 4, :, mine].reshape(length, channels).astype(F32)
                for i in range(lag_order):
                    same = id_ext[m, 7 - i : 7 - i + length] == cols_in[m]
                    lag_out[i, m] = jnp.where(same, lag_ext[7 - i : 7 - i + length], 0.0).astype(BF)

            def conv_copy(k, m, half):
                first = pl.multiple_of(half * tile, tile)
                return pltpu.make_async_copy(
                    conv.at[k, pl.ds(first, tile)],
                    conv_out.at[k, pl.ds(pl.multiple_of(m * length + first, tile), tile)],
                    conv_sem.at[k, half],
                )

            lags(0)
            per = 2 * count

            @pl.loop(0, streams * per)
            def _(j):
                m = j // per
                half = 1 - (j - m * per) // count
                k = j - m * per - (1 - half) * count
                first = pl.multiple_of(half * tile, tile)
                here = pl.ds(first, tile)
                offset = taps - length - reach

                @pl.when(k == 0)
                def _():
                    ids_there = ids_row[pl.ds(m, 1), pl.ds(pl.multiple_of(offset + first, tile), window)]
                    mask[...] = jnp.where(cols_in[m, here] == ids_there, 1.0, 0.0).astype(BF)

                for a in range(2 * quarter // LANES):
                    start = taps - LANES - reach - a * LANES
                    down = slice(a * LANES, (a + 1) * LANES)
                    left[down] = strip[k, :, start : start + window] * mask[down]
                right = rows_in[m, pl.ds(offset // quarter + 2 * half, window // quarter)].reshape(window, width)
                result = dot_nn(left[...], right).astype(BF)
                pl.when(m > 0)(lambda: conv_copy(k, m - 1, half).wait())
                conv[k, here] = result
                conv_copy(k, m, half).start()

                @pl.when(k == count - 1)
                def _():
                    mixed = sum([dot_nn(conv[q, here], fp_ref[q]) for q in range(count)])
                    mixed = mixed + sum([dot_nn(lag_out[i, m, here], lp_ref[i]) for i in range(lag_order)])
                    part_ref[0, m, half] = mixed.astype(BF).reshape(2, quarter, width)

                after(j, 0, lambda: ag_rows.arrive(1, 1))
                after(j, 1, lambda: ag_rows.pass_on(3, 0), lambda: ag_rows.arrive(2, 1))
                after(j, 3, lambda: ag_rows.arrive(3, 1), lambda: ag_rows.pass_on(1, 1))
                after(j, count - 1, lambda: ag_rows.finish(3, 0), lambda: ag_rows.pass_on(2, 1))
                after(j, count + 1, lambda: ag_rows.pass_on(3, 1))
                after(
                    j,
                    per - 1,
                    lambda: rs_one.start(0, 0),
                    *[functools.partial(ag_rows.finish, h, 1) for h in far_back],
                    lambda: lags(1),
                )
                after(j, per + 1, lambda: rs_one.middle(0, 0))
                after(j, per + 8, lambda: first_norm(0))

            rs_one.start(0, 1)
            for k in range(count):
                for half in range(2):
                    conv_copy(k, streams - 1, half).wait()

        pl.run_scoped(
            front,
            pltpu.VMEM((count, LANES, wide), BF),
            pltpu.VMEM((tile, window), BF),
            pltpu.VMEM((tile, window), BF),
            pltpu.VMEM((count, length, width), BF),
        )

        def attention_on(
            q_ref, k_ref, v_ref, a_ref, lse_ref, inner_ref, gg_ref, gu_ref, ga_ref, dk_acc, dv_acc, dq_ref, dkv_ref
        ):
            ag_one.pass_on(0, 0)
            rs_one.middle(0, 1)
            for h in range(1, spans):
                ag_one.arrive(h, 0)
            first_norm(1)
            for h in range(1, spans):
                ag_one.pass_on(h, 0)
            for h in range(spans):
                ag_one.finish(h, 0)

            def split_step(i):
                m = i // 2
                return m, i - 2 * m

            @pl.loop(0, steps)
            def _(i):
                m, half = split_step(i)
                first = pl.multiple_of(half * tile, tile)
                here = pl.ds(first, tile)

                @pl.when(half == 0)
                def _():
                    own = flat(attn_in[0, m])
                    q_ref[m] = dot_nn(own, wq_ref[...]).astype(BF)
                    for h in range(spans):
                        block = flat(attn_in[h, m])
                        k_ref[h, m] = dot_nn(block, wk_ref[...]).astype(BF)
                        v_ref[h, m] = dot_nn(block, wv_ref[...]).astype(BF)

                masks = masks_of(m, here, first)
                block = q_ref[m, here]
                result = jnp.zeros((tile, cols), F32)
                for head in range(heads):
                    query = one_head(block, head)
                    scores = [jnp.where(masks[h], dot_nt(query, k_ref[h, m]) * scale, NEGATIVE) for h in range(spans)]
                    peak = functools.reduce(jnp.maximum, [jnp.max(v, axis=-1, keepdims=True) for v in scores])
                    raised = [jnp.exp(v - peak) for v in scores]
                    norm = sum([jnp.sum(v, axis=-1, keepdims=True) for v in raised])
                    inverse = 1.0 / norm
                    mixed = sum([dot_nn((raised[h] * inverse).astype(BF), v_ref[h, m]) for h in range(spans)])
                    result = result + one_head(mixed, head)
                    lse_ref[m, head, here] = jnp.broadcast_to(peak + jnp.log(norm), (tile, LANES))
                low = result.astype(BF)
                a_ref[m, here] = low
                o_part[0, m, half] = dot_nn(low, wo_ref[...]).astype(BF).reshape(2, quarter, width)
                after(i, 0, lambda: ag_one.pass_on(0, 1), *[functools.partial(ag_one.arrive, h, 1) for h in range(1, spans)])
                after(
                    i,
                    1,
                    lambda: rs_two.start(0, 0),
                    *[functools.partial(ag_one.pass_on, h, 1) for h in range(1, spans)],
                    *[functools.partial(ag_one.finish, h, 1) for h in range(spans)],
                )
                after(i, 2, lambda: rs_two.middle(0, 0))
                after(i, 3, lambda: rs_two.start(0, 1))

            def second_norm(m):
                rs_two.total(m, total)
                hidden = hid_one[m] + total[...]
                hid_two[m] = hidden
                feed_in[0, m, t] = norm_of(hidden, fg_ref[...]).astype(BF)
                ag_two.start(m)

            second_norm(0)
            rs_two.middle(0, 1)
            ag_two.pass_on(0, 0)
            ag_two.finish(0, 0)

            @pl.loop(0, steps)
            def _(i):
                m, half = split_step(i)
                here = pl.ds(pl.multiple_of(half * tile, tile), tile)
                block = flat(feed_in[0, m, pl.ds(2 * half, 2)])
                inner, grad_gate, grad_up = unit_terms(
                    dot_nn(block, wg_ref[...]), dot_nn(block, wu_ref[...]), dot_nt(cot_ref[m, here], wd_ref[...])
                )
                inner, grad_gate, grad_up = inner.astype(BF), grad_gate.astype(BF), grad_up.astype(BF)
                inner_ref[m, here] = inner
                gg_ref[m, here] = grad_gate
                gu_ref[m, here] = grad_up
                back = dot_nt(grad_gate, wg_ref[...]) + dot_nt(grad_up, wu_ref[...])
                feed_part[0, m, half] = back.astype(BF).reshape(2, quarter, width)
                layer_part[0, m, half] = dot_nn(inner, wd_ref[...]).astype(BF).reshape(2, quarter, width)
                after(i, 0, lambda: second_norm(1))
                after(
                    i,
                    1,
                    lambda: rs_three.start(0, 0),
                    lambda: ag_two.pass_on(0, 1),
                    lambda: rs_three.middle(0, 0),
                    lambda: ag_two.finish(0, 1),
                )
                after(i, 3, lambda: rs_three.start(0, 1))

            def third_norm(m):
                rs_three.total(m, total)
                grad_in, gain_grad = norm_back(hid_two[m], fg_ref[...], total[...])
                value = cot_ref[m, pl.ds(pl.multiple_of(t * quarter, quarter), quarter)].astype(F32) + grad_in
                grad_two[m] = value
                gain_out[1:2] = gain_grad if m == 0 else gain_out[1:2] + gain_grad
                grad_att[0, m, t] = value.astype(BF)
                ag_three.start(m)

            third_norm(0)
            feed_all = flat(feed_in[0])
            grads[0] = dot_tn(feed_all, flat(gg_ref[...])).astype(BF)
            gr.start(0)
            rs_three.middle(0, 1)
            grads[1] = dot_tn(feed_all, flat(gu_ref[...])).astype(BF)
            gr.start(1)
            grads[2] = dot_tn(flat(cot_ref[...]), flat(inner_ref[...])).astype(BF)
            gr.start(2)
            ag_three.pass_on(0, 0)
            ag_three.finish(0, 0)
            for m in range(streams):
                rs_layer.start(0, m)

            def layer_sum(m):
                rs_layer.total(m, total)
                layer_out[0, m, t] = (hid_two[m] + total[...]).astype(BF)
                ag_layer.start(m)

            @pl.loop(0, steps)
            def _(i):
                m, half = split_step(i)
                first = pl.multiple_of(half * tile, tile)
                here = pl.ds(first, tile)

                @pl.when(half == 0)
                def _():
                    ga_ref[...] = dot_nt(all_rows(grad_att, m), wo_ref[...]).astype(BF)
                    dk_acc[...] = jnp.zeros_like(dk_acc)
                    dv_acc[...] = jnp.zeros_like(dv_acc)

                masks = masks_of(m, here, first)
                block = q_ref[m, here]
                grad_block = ga_ref[here]
                result = jnp.zeros((tile, cols), F32)
                for head in range(heads):
                    query = one_head(block, head)
                    grad = one_head(grad_block, head)
                    level = lse_ref[m, head, here][:, :1]
                    prob = [
                        jnp.where(masks[h], jnp.exp(dot_nt(query, k_ref[h, m]) * scale - level), 0.0) for h in range(spans)
                    ]
                    grad_prob = [dot_nt(grad, v_ref[h, m]) for h in range(spans)]
                    mean = sum([jnp.sum(p * g, axis=-1, keepdims=True) for p, g in zip(prob, grad_prob)])
                    grad_scores = [(p * (g - mean)).astype(BF) for p, g in zip(prob, grad_prob)]
                    for h in range(spans):
                        dv_acc[h] += dot_tn(prob[h].astype(BF), grad)
                        dk_acc[h] += dot_tn(grad_scores[h], query)
                    mixed = sum([dot_nn(grad_scores[h], k_ref[h, m]) for h in range(spans)])
                    result = result + one_head(mixed, head)
                dq_ref[m, here] = (result * scale).astype(BF)

                @pl.when(half == 1)
                def _():
                    for h in range(hops, -1, -1):
                        grad_k = (dk_acc[h] * scale).astype(BF)
                        grad_v = dv_acc[h].astype(BF)
                        dkv_ref[h, m, :, :cols] = grad_k
                        dkv_ref[h, m, :, cols:] = grad_v
                        back = dot_nt(grad_k, wk_ref[...]) + dot_nt(grad_v, wv_ref[...])
                        if h == 0:
                            back = back + dot_nt(dq_ref[m], wq_ref[...])
                        attn_part[h, m] = back.astype(BF).reshape(2, 2, quarter, width)
                        rs_four.start(h, m)

                after(i, 0, lambda: third_norm(1), lambda: rs_layer.middle(0, 0), lambda: rs_layer.middle(0, 1))
                after(i, 1, lambda: gr.spread(0), lambda: ag_three.pass_on(0, 1), lambda: ag_three.finish(0, 1))
                after(i, 2, *[functools.partial(rs_four.middle, h, 0) for h in range(hops, -1, -1)], lambda: gr.spread(1))
                after(
                    i,
                    3,
                    *[functools.partial(rs_four.hop, h, 0, total) for h in range(hops, 0, -1)],
                    lambda: gr.spread(2),
                    lambda: layer_sum(0),
                    lambda: layer_sum(1),
                )

            attn_all = attn_in[...].reshape(spans * streams * length, width)
            grads[3, :, cols : 3 * cols] = dot_tn(attn_all, flat(dkv_ref[...].reshape(-1, 2 * cols))).astype(BF)
            for h in range(hops, -1, -1):
                rs_four.middle(h, 1)
            grads[3, :, :cols] = dot_tn(flat(attn_in[0]), flat(dq_ref[...])).astype(BF)
            grads[3, :, 3 * cols :] = dot_tn(flat(grad_att[0]), flat(a_ref[...])).astype(BF)
            gr.start(3)

            def fourth_norm(m):
                rs_four.total(m, total)
                grad_in, gain_grad = norm_back(hid_one[m], ag_ref[...], total[...])
                value = grad_two[m] + grad_in
                one_out[m] = value
                gain_out[0:1] = gain_grad if m == 0 else gain_out[0:1] + gain_grad
                stu_out[0, m, t] = value.astype(BF)
                ag_five.start(m)

            fourth_norm(0)
            for h in range(hops, 0, -1):
                rs_four.hop(h, 1, total)
            gr.spread(3)
            gr.collect(0, grad_acc)
            fourth_norm(1)
            for m in range(streams):
                ag_five.pass_on(0, m)
            for m in range(streams):
                ag_layer.pass_on(0, m)
            gr.collect(1, grad_acc)
            gr.collect(2, grad_acc)
            for m in range(streams):
                ag_five.finish(0, m)
            gr.collect(3, grad_acc)
            for m in range(streams):
                ag_layer.finish(0, m)
            for k in range(chunks):
                gr.finish(k)
                gr.drain(k)
            for item in (rs_one, rs_two, rs_three, rs_layer, rs_four, ag_rows, ag_one, ag_two, ag_three, ag_layer, ag_five):
                item.drain()
            for h in far_back:
                pl.when(s + h < seq_count)(functools.partial(lambda h: id_copy(h, s + h).wait_send(), h))

        pl.run_scoped(
            attention_on,
            rows_of,
            pltpu.VMEM((spans, streams, length, cols), BF),
            pltpu.VMEM((spans, streams, length, cols), BF),
            rows_of,
            pltpu.VMEM((streams, heads, length, LANES), F32),
            unit_rows,
            unit_rows,
            unit_rows,
            pltpu.VMEM((length, cols), BF),
            pltpu.VMEM((spans, length, cols), F32),
            pltpu.VMEM((spans, length, cols), F32),
            rows_of,
            pltpu.VMEM((spans, streams, length, 2 * cols), BF),
        )

    anywhere = pl.BlockSpec(memory_space=pl.ANY)
    return pl.pallas_call(
        kernel,
        name="head",
        out_shape=(
            jax.ShapeDtypeStruct(gathered, BF),
            jax.ShapeDtypeStruct(gathered, BF),
            jax.ShapeDtypeStruct((streams, quarter, width), F32),
            jax.ShapeDtypeStruct((2, width), F32),
            jax.ShapeDtypeStruct((chunks, rows, units), BF),
            jax.ShapeDtypeStruct((lag_order, streams, length, channels), BF),
            jax.ShapeDtypeStruct((seq_count * streams, length), F32),
            jax.ShapeDtypeStruct((count, streams * length, width), BF),
            jax.ShapeDtypeStruct((count, LANES, wide), BF),
        ),
        in_specs=[anywhere if i in (3, 12, 13, 14, 15) else spec for i, spec in enumerate(in_vmem(16))],
        out_specs=tuple(in_vmem(7)) + (anywhere, anywhere),
        scratch_shapes=[
            pltpu.VMEM(filter_proj.shape, BF),
            pltpu.VMEM(wg.shape, BF),
            pltpu.VMEM(wu.shape, BF),
            pltpu.VMEM(wd.shape, BF),
            pltpu.VMEM(cot.shape, BF),
            pltpu.SemaphoreType.DMA((5,)),
            pltpu.VMEM((count, wide), F32),
            pltpu.VMEM((streams, taps), F32),
            pltpu.VMEM((streams, 4 * seq_count, quarter, width), BF),
            pltpu.VMEM((seq_count,) + ids.shape, jnp.int32),
            pltpu.VMEM((streams, length, 1), F32),
            pltpu.VMEM((streams, length + 8, 1), F32),
            pltpu.VMEM((length + 8, channels), F32),
            split_part,
            pltpu.SemaphoreType.DMA((2, seq_count)),
            pltpu.SemaphoreType.DMA,
            pltpu.SemaphoreType.DMA((count, 2)),
            pltpu.VMEM((spans, streams, 4, quarter, width), BF),
            pltpu.VMEM(gathered, BF),
            pltpu.VMEM(gathered, BF),
            state,
            state,
            state,
            pltpu.VMEM((chunks, width, units), BF),
            pltpu.VMEM((quarter, width), F32),
            pltpu.VMEM((rows, units // 2), F32),
            split_part,
            split_part,
            split_part,
            pltpu.VMEM((spans, streams, 2, 2, quarter, width), BF),
            AllGather.scratch(seq_count - 1, streams, pieces)[0],
            AllGather.scratch(hops, streams, pieces)[0],
        ]
        + [AllGather.scratch(0, streams, pieces)[0]] * 4
        + zero_hops * 4
        + ReduceScatter.scratch(hops, streams, quarter, width, pieces)
        + GradReduce.scratch(seq_count, chunks, width, units),
        compiler_params=params(8),
    )(
        x, ids, stu_gain, filter_proj, lag_proj, filters, attn_gain, feed_gain, wq, wk, wv, wo, wg, wu, wd, cot
    )


def tail(
    grad_stu, filter_proj, lag_proj, conv, lag_stack, ext_ids, strip_back, x, gain, grad_one, gains, seq_count
):
    count, length_all, width = conv.shape
    streams, _, quarter, _ = x.shape
    length = length_all // streams
    lag_order, channels = lag_proj.shape[:2]
    blocks = length // LANES
    hops = seq_count - 1
    chunks = count + 1
    steps = seq_count * streams
    rows = width // seq_count
    gain_rows = 8

    def kernel(
        gs_ref, fp_hbm, lp_ref, conv_hbm, lag_ref, ext_ref, strip_hbm, x_hbm, gain_ref, one_ref, gains_ref,
        out, filter_out, lag_out, gain_out,
        conv_ref, fp_ref, strip, x_own, conv_sem, fp_sem, strip_sem, x_sem, id_ext,
        mask, cols, left, acc, terms, grad_conv, grads, lag_ext, total, grad_acc, gather_sem,
        gain_own, gain_near, gain_sum, gain_far, near_sem, far_sem, *scratch,
    ):
        s, t, y, c, core, far = place()
        p = lax.axis_index("dp")
        rs_scratch, gr_scratch = scratch[:6], scratch[6:]

        def conv_copy(k):
            return pltpu.make_async_copy(conv_hbm.at[k], conv_ref.at[k], conv_sem.at[k])

        def fp_copy(k):
            return pltpu.make_async_copy(fp_hbm.at[k], fp_ref.at[k], fp_sem.at[k])

        strip_copy = pltpu.make_async_copy(strip_hbm, strip, strip_sem)
        for k in range(count):
            conv_copy(k).start()
            fp_copy(k).start()
        strip_copy.start()
        x_copy = pltpu.make_async_copy(x_hbm.at[:, t], x_own, x_sem)
        x_copy.start()
        greet(seq_count, hops, wide=True, gains=True)

        def source(k):
            return grads.at[k]

        def result(k):
            return filter_out.at[k] if k < count else lag_out

        gr = GradReduce(seq_count, source, result, gr_scratch)
        rs = ReduceScatter(seq_count, hops, streams, lambda h, m: terms.at[h, m], rs_scratch)
        ag = AllGather(seq_count, 0, streams, out, gather_sem)

        @pl.loop(0, count)
        def _(k):
            conv_copy(k).wait()
            grads[k] = dot_tn(conv_ref[k], gs_ref[...]).astype(BF)
            gr.start(k)
            fp_copy(k).wait()
            product = dot_nt(gs_ref[...], fp_ref[k]).astype(BF)
            for m in range(streams):
                here = pl.ds(pl.multiple_of(k * length, LANES), length)
                grad_conv[m, here] = product[m * length : (m + 1) * length]

        grads[count] = jnp.zeros_like(grads.at[count])
        for i in range(lag_order):
            grads[count, :, i * channels : (i + 1) * channels] = dot_tn(gs_ref[...], lag_ref[i]).astype(BF)
        gr.start(count)
        turned = jnp.transpose(ext_ref[...])
        for j in range(steps):
            cols[j] = turned[:, j : j + 1]
        for m in range(streams):
            lag_ext[m] = jnp.zeros_like(lag_ext.at[m])
            id_ext[:8] = turned[length - 8 :, streams + m : streams + m + 1]
            id_ext[8:] = turned[:, m : m + 1]
            for i in range(lag_order):
                term = dot_nt(gs_ref[m * length : (m + 1) * length], lp_ref[i])
                same = id_ext[7 - i : 7 - i + length] == cols[m]
                lag_ext[m, 7 - i : 7 - i + length] += jnp.where(same, term, 0.0)
        strip_copy.wait()
        x_copy.wait()
        mine = pl.ds(pl.multiple_of(t * channels, LANES), channels)
        spread_at = {0: 0, 1: 1, 4: 2, 6: 3} if steps == 8 and chunks >= 7 else {}
        collect_at = {5: 0, 7: 1} if spread_at else {}

        def step_of(i):
            return seq_count - 1 - i // streams, i - i // streams * streams

        @pl.loop(0, steps)
        def _(i):
            h, m = step_of(i)

            @pl.when(h <= s)
            def _():
                mask[...] = jnp.where(cols[h * streams + m] == ext_ref[pl.ds(m, 1)], 1.0, 0.0).astype(BF)
                for k in range(count):
                    for a in range(blocks):
                        start = pl.multiple_of(LANES * (blocks * h + blocks - 1 - a), LANES)
                        down = slice(a * LANES, (a + 1) * LANES)
                        left[down, k * length : (k + 1) * length] = strip[k, :, pl.ds(start, length)] * mask[down]
                acc[...] = jnp.dot(left[...], grad_conv[m], preferred_element_type=F32)

                @pl.when(h == 0)
                def _():
                    acc[:, mine] += lag_ext[m, 8:]

                @pl.when(h == 1)
                def _():
                    acc[length - 8 :, mine] += lag_ext[m, :8]

                for quarter_y in range(2):
                    for quarter_c in range(2):
                        first = (2 * quarter_y + quarter_c) * quarter
                        terms[h, m, quarter_y, quarter_c] = acc[first : first + quarter].astype(BF)
                rs.start(h, m)

            @pl.when(i >= 1)
            def _():
                rs.middle(*step_of(i - 1))

            @pl.when((i >= 2) & (i < steps - streams + 2))
            def _():
                rs.hop(*step_of(i - 2), total)

            for step, k in spread_at.items():
                pl.when(i == step)(functools.partial(gr.spread, k))
            for step, k in collect_at.items():
                pl.when(i == step)(functools.partial(gr.collect, k, grad_acc))

        rs.middle(0, streams - 1)
        waiting = list(range(len(spread_at), chunks))
        gathered = list(range(len(collect_at), chunks))

        def next_spread():
            if waiting:
                gr.spread(waiting.pop(0))

        next_spread()
        next_spread()
        gain_own[...] = jnp.zeros_like(gain_own)
        for m in range(streams):
            rs.total(m, total)
            grad_in, gain_grad = norm_back(x_own[m].astype(F32), gain_ref[...], total[...])
            out[0, m, t] = (one_ref[m] + grad_in).astype(BF)
            ag.start(m)
            gain_own[0:1] += gain_grad
        next_spread()
        gain_own[1:3] = gains_ref[...]
        gain_near[t] = gain_own[...]

        def near_copy(j, slot):
            return remote(gain_own, gain_near.at[slot], near_sem.at[0, j], near_sem.at[1, slot], {"tensor": j})

        for j in range(4):
            pl.when(t != j)(functools.partial(lambda j: near_copy(j, t).start(), j))
        while len(gathered) > 3 and chunks - len(gathered) < chunks - len(waiting):
            gr.collect(gathered.pop(0), grad_acc)
        for m in range(streams):
            ag.pass_on(0, m)
        for j in range(4):
            pl.when(t != j)(functools.partial(lambda j: near_copy(j, j).wait_recv(), j))
        gain_sum[...] = gain_near[0] + gain_near[1] + gain_near[2] + gain_near[3]
        me = p * seq_count + s

        def far_copy(j, slot):
            d, q = j // seq_count, j % seq_count
            return remote(
                gain_sum.at[:, q * rows : (q + 1) * rows], gain_far.at[slot], far_sem.at[0, j], far_sem.at[1, slot],
                {"dp": d, "seq": q},
            )

        gain_far[me] = gain_sum[:, pl.ds(pl.multiple_of(s * rows, LANES), rows)]
        for j in range(2 * seq_count):
            pl.when(me != j)(lambda: far_copy(j, me).start())
        while waiting:
            next_spread()
        for m in range(streams):
            ag.finish(0, m)
        while gathered:
            gr.collect(gathered.pop(0), grad_acc)
        for j in range(2 * seq_count):
            pl.when(me != j)(lambda: far_copy(j, j).wait_recv())
        gain_out[...] = functools.reduce(jnp.add, [gain_far[j] for j in range(2 * seq_count)])
        for k in range(chunks):
            gr.finish(k)
        for j in range(4):
            pl.when(t != j)(lambda: near_copy(j, t).wait_send())
        for j in range(2 * seq_count):
            pl.when(me != j)(lambda: far_copy(j, me).wait_send())
        for k in range(chunks):
            gr.drain(k)
        rs.drain()
        ag.drain()

    anywhere = pl.BlockSpec(memory_space=pl.ANY)
    return pl.pallas_call(
        kernel,
        name="tail",
        out_shape=(
            jax.ShapeDtypeStruct((1, streams, 4, quarter, width), BF),
            jax.ShapeDtypeStruct((count, rows, width), BF),
            jax.ShapeDtypeStruct((rows, width), BF),
            jax.ShapeDtypeStruct((gain_rows, rows), F32),
        ),
        in_specs=[anywhere if i in (1, 3, 6, 7) else spec for i, spec in enumerate(in_vmem(11))],
        out_specs=tuple(in_vmem(4)),
        scratch_shapes=[
            pltpu.VMEM(conv.shape, BF),
            pltpu.VMEM(filter_proj.shape, BF),
            pltpu.VMEM(strip_back.shape, BF),
            pltpu.VMEM((streams, quarter, width), BF),
            pltpu.SemaphoreType.DMA((count,)),
            pltpu.SemaphoreType.DMA((count,)),
            pltpu.SemaphoreType.DMA,
            pltpu.SemaphoreType.DMA,
            pltpu.VMEM((length + 8, 1), F32),
            pltpu.VMEM((length, length), BF),
            pltpu.VMEM((steps, length, 1), F32),
            pltpu.VMEM((length, count * length), BF),
            pltpu.VMEM((length, width), F32),
            pltpu.VMEM((seq_count, streams, 2, 2, quarter, width), BF),
            pltpu.VMEM((streams, count * length, width), BF),
            pltpu.VMEM((chunks, width, width), BF),
            pltpu.VMEM((streams, length + 8, channels), F32),
            pltpu.VMEM((quarter, width), F32),
            pltpu.VMEM((rows, width // 2), F32),
            AllGather.scratch(0, streams)[0],
            pltpu.VMEM((gain_rows, width), F32),
            pltpu.VMEM((4, gain_rows, width), F32),
            pltpu.VMEM((gain_rows, width), F32),
            pltpu.VMEM((2 * seq_count, gain_rows, rows), F32),
            pltpu.SemaphoreType.DMA((2, 4)),
            pltpu.SemaphoreType.DMA((2, 2 * seq_count)),
        ]
        + ReduceScatter.scratch(hops, streams, quarter, width)
        + GradReduce.scratch(seq_count, chunks, width, width),
        compiler_params=params(7),
    )(
        grad_stu, filter_proj, lag_proj, conv, lag_stack, ext_ids, strip_back, x, gain, grad_one, gains
    )


def write_out(layer_output, input_gradient, gains, filter_grad, lag_grad, sums, lag_order, channels, cols):
    _, streams, _, quarter, width = layer_output.shape
    rows, units = sums.shape[1:]
    count = filter_grad.shape[0]

    def kernel(
        layer_ref, input_ref, gains_ref, filter_ref, lag_ref, sums_ref,
        layer_out, input_out, stu_out, filter_out, lag_out, attn_out, q_out, k_out, v_out, o_out, feed_out, gate_out, up_out,
        down_out,
    ):
        layer_out[...] = layer_ref[0].reshape(streams, 1, 4 * quarter, width)
        input_out[...] = input_ref[0].reshape(streams, 1, 4 * quarter, width)
        filter_out[...] = filter_ref[...].astype(F32)
        for i, ref in enumerate((stu_out, attn_out, feed_out)):
            ref[...] = gains_ref[i : i + 1]
        for i in range(lag_order):
            lag_out[i] = jnp.transpose(lag_ref[:, i * channels : (i + 1) * channels].astype(F32))
        for i, ref in enumerate((q_out, k_out, v_out)):
            ref[...] = sums_ref[3, :, i * cols : (i + 1) * cols].astype(F32)
        o_out[...] = jnp.transpose(sums_ref[3, :, 3 * cols :].astype(F32))
        gate_out[...] = sums_ref[0].astype(F32)
        up_out[...] = sums_ref[1].astype(F32)
        down_out[...] = jnp.transpose(sums_ref[2].astype(F32))

    def out(*shape, kind=F32):
        return jax.ShapeDtypeStruct(shape, kind)

    shapes = (
        out(streams, 1, 4 * quarter, width, kind=BF),
        out(streams, 1, 4 * quarter, width, kind=BF),
        out(1, rows),
        out(count, rows, width),
        out(lag_order, channels, rows),
        out(1, rows),
        out(rows, cols),
        out(rows, cols),
        out(rows, cols),
        out(cols, rows),
        out(1, rows),
        out(rows, units),
        out(rows, units),
        out(units, rows),
    )
    results = pl.pallas_call(
        kernel,
        name="write_out",
        out_shape=shapes,
        in_specs=in_vmem(6),
        out_specs=tuple(in_vmem(len(shapes))),
        compiler_params=params(),
    )(layer_output, input_gradient, gains, filter_grad, lag_grad, sums)
    return tuple(r.reshape(rows) if r.shape == (1, rows) else r for r in results)


def gated_unit(gate_pre, up_pre):
    return jax.nn.gelu(gate_pre, approximate=True) * up_pre


def local(
    seq_count,
    tokens,
    document_index,
    filters,
    stu_gain,
    filter_proj,
    lag_proj,
    attention_gain,
    query_weight,
    key_weight,
    value_weight,
    output_weight,
    feed_gain,
    gate_weight,
    up_weight,
    down_weight,
    cotangent,
):
    streams, _, length, width = tokens.shape
    row_len = length * seq_count
    quarter = length // 4
    lag_order, channels = lag_proj.shape[:2]
    count = filters.shape[0]
    hops = WINDOW // length
    tensor_place = lax.axis_index("tensor")
    chan_start = tensor_place * channels

    def split(a):
        return a.reshape(a.shape[:-2] + (2, 2, quarter, width))

    def quarters(a):
        return a.reshape(a.shape[:-2] + (4, quarter, width))

    def whole(a):
        return a.reshape(a.shape[:-3] + (length, width))

    def row(gain):
        return gain.reshape(1, width)

    if width // seq_count % LANES == 0:
        rows = tokens.reshape(streams, 4, quarter, width)
        grad_stu, layer_output, grad_one, gain_grads, sums, lag_stack, ext_ids, conv, strip_back = head(
            rows, document_index, row(stu_gain), filter_proj, lag_proj, filters, row(attention_gain), row(feed_gain),
            query_weight, key_weight, value_weight, output_weight, gate_weight, up_weight, down_weight,
            cotangent.reshape(streams, length, width), seq_count,
        )
        input_gradient, filter_grad, lag_grad, gains = tail(
            grad_stu.reshape(streams * length, width), filter_proj, lag_proj, conv,
            lag_stack.reshape(lag_order, streams * length, channels), ext_ids, strip_back, rows, row(stu_gain), grad_one,
            gain_grads, seq_count,
        )
        return write_out(
            layer_output, input_gradient, gains, filter_grad, lag_grad, sums, lag_order, channels, query_weight.shape[1]
        )

    x = tokens[:, 0]
    grad_three = cotangent[:, 0]
    ids = document_index[:, 0]
    id_tile = ids.reshape(streams * length // LANES, LANES)
    pad = jnp.zeros((count, 4 * LANES), filters.dtype)
    ahead = row_len - LANES
    base = jnp.concatenate(
        [
            jnp.flip(filters[:, : ahead + 1], axis=1),
            pad[:, : 4 * LANES],
            jnp.flip(filters[:, ahead + 1 :], axis=1),
        ],
        axis=1,
    ).astype(F32)[:, None]
    base_back = jnp.concatenate(
        [pad[:, : length - LANES], filters, pad[:, :LANES]], axis=1
    ).astype(F32)[:, None]

    tokens_flat = streams * length
    cols = query_weight.shape[1]

    def answer(layer_output, input_gradient, gains, filter_grad, lag_grad, attn_grads, feed_grads):
        query_grad, key_grad, value_grad, output_grad = jnp.split(attn_grads, [cols, 2 * cols, 3 * cols], axis=1)
        gate_grad, up_grad, down_grad = feed_grads
        return (
            layer_output[:, None],
            input_gradient[:, None],
            gains[0],
            filter_grad,
            lag_grad[:, : lag_order * channels].T.reshape(lag_order, channels, -1),
            gains[1],
            query_grad,
            key_grad,
            value_grad,
            output_grad.T,
            gains[2],
            gate_grad,
            up_grad,
            down_grad.T,
        )

    inputs = norm_of(x.astype(F32), stu_gain).astype(BF)
    rows_ext, id_ext = gather_rows(quarters(inputs), id_tile, seq_count)
    rows_ext = whole(rows_ext)
    id_ext = id_ext.reshape(seq_count, streams, length)
    id_rows = id_ext[:, :, None, :]
    id_cols = id_ext[:, :, :, None]

    conv = convolve(rows_ext, id_rows, id_cols[0], base, seq_count)

    chan_rows = lax.dynamic_slice_in_dim(rows_ext[:2], chan_start, channels, 3)
    joined = jnp.concatenate([chan_rows[1][:, length - lag_order :], chan_rows[0]], axis=1)
    joined_ids = jnp.concatenate([id_ext[1][:, length - lag_order :], ids], axis=1)
    masks = []
    lagged = []
    for step in range(1, lag_order + 1):
        low = lag_order - step
        masks.append((joined_ids[:, low : low + length] == ids)[:, :, None])
        lagged.append(jnp.where(masks[-1], joined[:, low : low + length], jnp.zeros((), BF)))
    lag_stack = jnp.stack(lagged)

    mixed = jnp.einsum("kmtd,kde->mte", conv, filter_proj, preferred_element_type=F32)
    mixed = mixed + jnp.einsum("imtc,ice->mte", lag_stack, lag_proj, preferred_element_type=F32)

    state = jax.ShapeDtypeStruct((streams, quarter, width), F32)
    gain_state = jax.ShapeDtypeStruct((1, width), F32)

    def finish_one(m, total, others, extra):
        x_ref, gain_ref = others
        hidden = x_ref[m, place()[1]].astype(F32) + total
        extra[0][m] = hidden
        return norm_of(hidden, gain_ref[...]).astype(BF)

    attn_ext, hidden_one = exchange(
        "exchange_one", 2, seq_count, [split(mixed.astype(BF))[None]], [quarters(x), row(attention_gain)], 0, hops,
        finish_one, [state],
    )
    attn_ext = whole(attn_ext)

    q, k, v, attended, lse, out_part = attend(
        attn_ext, id_rows[: hops + 1], id_cols[0], query_weight, key_weight, value_weight, output_weight
    )

    def finish_two(m, total, others, extra):
        hidden_ref, gain_ref = others
        hidden = hidden_ref[m] + total
        extra[0][m] = hidden
        return norm_of(hidden, gain_ref[...]).astype(BF)

    feed_in, hidden_two = exchange(
        "exchange_two", 3, seq_count, [split(out_part)[None]], [hidden_one, row(feed_gain)], 0, 0, finish_two, [state]
    )
    feed_in = whole(feed_in)[0].reshape(streams * length, width)
    flat_three = grad_three.reshape(streams * length, width)

    gate_pre = dot_nn(feed_in, gate_weight)
    up_pre = dot_nn(feed_in, up_weight)
    grad_inner = dot_nt(flat_three, down_weight)
    unit, pull = jax.vjp(gated_unit, gate_pre, up_pre)
    inner = unit.astype(BF)
    grad_gate, grad_up = pull(grad_inner)
    grad_gate = grad_gate.astype(BF)
    grad_up = grad_up.astype(BF)
    layer_part = dot_nn(inner, down_weight).astype(BF)
    feed_part = (dot_nt(grad_gate, gate_weight) + dot_nt(grad_up, up_weight)).astype(BF)

    def finish_three(m, total, others, extra):
        hidden_ref, gain_ref, cot_ref = others
        if m >= streams:
            return (hidden_ref[m - streams] + total).astype(BF)
        grad_in, gain_grad = norm_back(hidden_ref[m], gain_ref[...], total)
        grad_two = cot_ref[m, place()[1]].astype(F32) + grad_in
        extra[0][m] = grad_two
        extra[1][...] = gain_grad if m == 0 else extra[1][...] + gain_grad
        return grad_two.astype(BF)

    feed_grads = jnp.stack(
        [
            dot_tn(feed_in, grad_gate).astype(BF),
            dot_tn(feed_in, grad_up).astype(BF),
            dot_tn(flat_three, inner).astype(BF),
        ]
    )
    shape = (1, streams, length, width)
    both, grad_two, feed_gain_grad = exchange(
        "exchange_three", 4, seq_count, [split(feed_part.reshape(shape)), split(layer_part.reshape(shape))],
        [hidden_two, row(feed_gain), quarters(grad_three)], 0, 0, finish_three, [state, gain_state],
    )
    both = whole(both)[0]
    grad_att_out = both[:streams]
    layer_output = both[streams:]

    dq, dk, dv, attn_part = attend_back(
        q, k, v, lse, grad_att_out, id_rows[: hops + 1], id_cols[0], query_weight, key_weight, value_weight, output_weight
    )

    go = grad_att_out.reshape(tokens_flat, width)
    attn_grads = jnp.concatenate(
        [
            dot_tn(attn_ext[0].reshape(tokens_flat, width), dq.reshape(tokens_flat, -1)).astype(BF),
            dot_tn(attn_ext.reshape(-1, width), dk.reshape(-1, dk.shape[-1])).astype(BF),
            dot_tn(attn_ext.reshape(-1, width), dv.reshape(-1, dv.shape[-1])).astype(BF),
            dot_tn(go, attended.reshape(tokens_flat, -1)).astype(BF),
        ],
        axis=1,
    )

    def finish_four(m, total, others, extra):
        hidden_ref, gain_ref, grad_ref = others
        grad_in, gain_grad = norm_back(hidden_ref[m], gain_ref[...], total)
        grad_one = grad_ref[m] + grad_in
        extra[0][m] = grad_one
        extra[1][...] = gain_grad if m == 0 else extra[1][...] + gain_grad
        return grad_one.astype(BF)

    grad_stu, grad_one, attn_gain_grad = exchange(
        "exchange_four", 5, seq_count, [split(attn_part)], [hidden_one, row(attention_gain), grad_two], hops, 0,
        finish_four, [state, gain_state],
    )
    grad_stu = whole(grad_stu)[0]
    grad_conv = jnp.einsum("mte,kde->kmtd", grad_stu, filter_proj, preferred_element_type=F32).astype(BF)
    grad_lagged = jnp.einsum("mte,ice->imtc", grad_stu, lag_proj, preferred_element_type=F32)
    ext_grad = jnp.zeros((streams, 8 + length, channels), F32)
    for step in range(1, lag_order + 1):
        term = jnp.where(masks[step - 1], grad_lagged[step - 1], 0.0)
        ext_grad = ext_grad + jnp.pad(term, ((0, 0), (8 - step, step), (0, 0)))
    terms = convolve_back(
        grad_conv, id_rows[0], id_cols, base_back, ext_grad[:, 8:], ext_grad[:, :8], seq_count
    )

    def finish_five(m, total, others, extra):
        x_ref, gain_ref, grad_ref = others
        grad_in, gain_grad = norm_back(x_ref[m, place()[1]].astype(F32), gain_ref[...], total)
        extra[0][...] = gain_grad if m == 0 else extra[0][...] + gain_grad
        return (grad_ref[m] + grad_in).astype(BF)

    input_gradient, stu_gain_grad = exchange(
        "exchange_five", 6, seq_count, [split(terms)], [quarters(x), row(stu_gain), grad_one], seq_count - 1, 0,
        finish_five, [gain_state],
    )
    input_gradient = whole(input_gradient)[0]
    stu = grad_stu.reshape(tokens_flat, width)
    filter_part = jnp.einsum("kmtd,mte->kde", conv, grad_stu, preferred_element_type=F32).astype(BF)
    lag_part = jnp.concatenate(
        [dot_tn(stu, lag_stack[i].reshape(tokens_flat, channels)).astype(BF) for i in range(lag_order)], axis=1
    )
    feed_grads = lax.psum(
        lax.psum_scatter(feed_grads, "seq", scatter_dimension=1, tiled=True), "dp"
    ).astype(F32)
    attn_grads = lax.psum(lax.psum_scatter(attn_grads, "seq", scatter_dimension=0, tiled=True), "dp").astype(F32)
    filter_grad = lax.psum(
        lax.psum_scatter(filter_part, "seq", scatter_dimension=1, tiled=True), "dp"
    ).astype(F32)
    lag_grad = lax.psum(lax.psum_scatter(lag_part, "seq", scatter_dimension=0, tiled=True), "dp").astype(F32)
    gains = jnp.concatenate([stu_gain_grad, attn_gain_grad, feed_gain_grad], axis=0)
    gains = lax.psum(gains, ("dp", "seq", "tensor"))
    gain_width = width // seq_count
    gains = lax.dynamic_slice_in_dim(gains, lax.axis_index("seq") * gain_width, gain_width, 1)
    return answer(layer_output, input_gradient, gains, filter_grad, lag_grad, attn_grads, feed_grads)


def solution(mesh):
    return jax.shard_map(
        functools.partial(local, mesh.shape["seq"]),
        mesh=mesh,
        in_specs=(
            P(None, "dp", "seq", None),
            P(None, "dp", "seq"),
            P("tensor", None),
            P(),
            P("tensor", None, None),
            P(None, "tensor", None),
            P(),
            P(None, "tensor"),
            P(None, "tensor"),
            P(None, "tensor"),
            P("tensor", None),
            P(),
            P(None, "tensor"),
            P(None, "tensor"),
            P("tensor", None),
            P(None, "dp", "seq", None),
        ),
        out_specs=(
            P(None, "dp", "seq", None),
            P(None, "dp", "seq", None),
            P("seq"),
            P("tensor", "seq", None),
            P(None, "tensor", "seq"),
            P("seq"),
            P("seq", "tensor"),
            P("seq", "tensor"),
            P("seq", "tensor"),
            P("tensor", "seq"),
            P("seq"),
            P("seq", "tensor"),
            P("seq", "tensor"),
            P("tensor", "seq"),
        ),
        check_vma=False,
    )
```

```python
import functools

import jax
import jax.numpy as jnp
from jax import lax
from jax.experimental import pallas as pl
from jax.experimental.pallas import tpu as pltpu
from jax.sharding import PartitionSpec as P

HD = 64
WINDOW = 1024
EPSILON = 1e-05
LANES = 128
NEGATIVE = -1e30
MESH = pl.DeviceIdType.MESH
BF = jnp.bfloat16
F32 = jnp.float32
VMEM_LIMIT = 63 * 1024 * 1024


def place():
    s = lax.axis_index("seq")
    t = lax.axis_index("tensor")
    y = t // 2
    c = t - 2 * y
    return s, t, y, c, t + 1 - 2 * c, t + 2 - 4 * y


def when(condition, action):
    if condition is True:
        action()
    else:
        pl.when(condition)(action)


def remote(src, dst, send_sem, recv_sem, device):
    return pltpu.make_async_remote_copy(
        src_ref=src, dst_ref=dst, send_sem=send_sem, recv_sem=recv_sem, device_id=device, device_id_type=MESH
    )


def greet(seq_count, hops, wide=False, gains=False):
    s, t, y, c, core, far = place()
    barrier = pltpu.get_barrier_semaphore()

    def signal(device):
        pl.semaphore_signal(barrier, inc=1, device_id=device, device_id_type=MESH)

    signal({"tensor": core})
    signal({"tensor": far})
    if gains:
        signal({"tensor": 3 - t})
    if wide:
        p = lax.axis_index("dp")
        signal({"dp": 1 - p})
        for j in range(seq_count):

            @pl.when(s != j)
            def _():
                signal({"seq": j})
                if gains:
                    signal({"dp": 1 - p, "seq": j})

        peers = 2 + gains + 1 + (seq_count - 1) * (1 + gains)
    else:
        for h in range(1, hops + 1):
            for there, peer in ((s - h >= 0, s - h), (s + h < seq_count, s + h)):

                @pl.when(there)
                def _():
                    signal({"seq": peer})

        peers = 2 + jnp.minimum(s, hops) + jnp.minimum(seq_count - 1 - s, hops)
    pl.semaphore_wait(barrier, peers)


class ReduceScatter:
    def __init__(self, seq_count, hops, streams, part, scratch):
        self.seq_count, self.hops, self.streams, self.part = seq_count, hops, streams, part
        self.near, self.half, self.over, self.hop_out, self.hop_in, self.sem = scratch
        self.pieces, self.rows = self.half.shape[2:4]

    @staticmethod
    def scratch(hops, streams, rows, width, pieces=1):
        quarter = (hops + 1, streams, pieces, rows // pieces, width)
        over_seq = quarter if hops else (1, 1, 1, 16, LANES)
        return [
            pltpu.VMEM((hops + 1, streams, pieces, 2, rows // pieces, width), BF),
            pltpu.VMEM(quarter, BF),
            pltpu.VMEM(quarter, BF),
            pltpu.VMEM(over_seq, BF),
            pltpu.VMEM(over_seq, BF),
            pltpu.SemaphoreType.DMA((6, hops + 1, streams, pieces)),
        ]

    def span(self, n):
        return slice(n * self.rows, (n + 1) * self.rows)

    def move(self, kind, source, target, h, m, n, device, at=None):
        at = h if at is None else at
        return remote(source, target, self.sem.at[2 * kind, h, m, n], self.sem.at[2 * kind + 1, at, m, n], device)

    def to_core(self, h, m, n):
        s, t, y, c, core, far = place()
        source = self.part(h, m).at[:, 1 - c, pl.ds(n * self.rows, self.rows)]
        return self.move(0, source, self.near.at[h, m, n], h, m, n, {"tensor": core})

    def to_far(self, h, m, n):
        far = place()[5]
        return self.move(1, self.half.at[h, m, n], self.over.at[h, m, n], h, m, n, {"tensor": far})

    def to_hop(self, h, m, n):
        peer = {"seq": lax.axis_index("seq") - 1}
        return self.move(2, self.hop_out.at[h, m, n], self.hop_in.at[h - 1, m, n], h, m, n, peer, at=h - 1)

    def add_hop(self, h, m, acc):
        s = lax.axis_index("seq")

        @pl.when(s + 1 < self.seq_count)
        def _():
            for n in range(self.pieces):
                ref = self.hop_in.at[h, m, n]
                self.move(2, self.hop_out.at[h, m, n], ref, h, m, n, {"seq": s + 1}).wait_recv()
                acc[self.span(n)] += self.hop_in[h, m, n].astype(F32)

    def there(self, h):
        return True if isinstance(h, int) and h == 0 else lax.axis_index("seq") - h >= 0

    def order(self):
        return [(h, m) for h in range(self.hops, -1, -1) for m in range(self.streams)]

    def start(self, h, m):
        def act():
            for n in range(self.pieces):
                self.to_core(h, m, n).start()

        when(self.there(h), act)

    def middle(self, h, m):
        s, t, y, c, core, far = place()

        def act():
            for n in range(self.pieces):
                self.to_core(h, m, n).wait_recv()
                mine = self.part(h, m)[1 - y, c, self.span(n)].astype(F32) + self.near[h, m, n, 1 - y].astype(F32)
                self.half[h, m, n] = mine.astype(BF)
                self.to_far(h, m, n).start()

        when(self.there(h), act)

    def own(self, h, m, acc):
        s, t, y, c, core, far = place()
        for n in range(self.pieces):
            self.to_far(h, m, n).wait_recv()
            mine = self.part(h, m)[y, c, self.span(n)].astype(F32) + self.near[h, m, n, y].astype(F32)
            acc[self.span(n)] = mine + self.over[h, m, n].astype(F32)

    def hop(self, h, m, acc):
        def act():
            self.own(h, m, acc)
            if isinstance(h, int):
                if h < self.hops:
                    self.add_hop(h, m, acc)
            else:
                pl.when(h < self.hops)(lambda: self.add_hop(h, m, acc))
            for n in range(self.pieces):
                self.hop_out[h, m, n] = acc[self.span(n)].astype(BF)
                self.to_hop(h, m, n).start()

        when(self.there(h), act)

    def total(self, m, acc):
        self.own(0, m, acc)
        if self.hops:
            self.add_hop(0, m, acc)

    def drain(self):
        for h, m in self.order():

            def act():
                for n in range(self.pieces):
                    self.to_core(h, m, n).wait_send()
                    self.to_far(h, m, n).wait_send()
                    if h:
                        self.to_hop(h, m, n).wait_send()

            when(self.there(h), act)


class AllGather:
    def __init__(self, seq_count, hops, streams, at, sem, first=0):
        self.seq_count, self.hops, self.streams, self.sem, self.first = seq_count, hops, streams, sem, first
        self.at = at if callable(at) else lambda h, m, quarter: at.at[h, m, quarter]
        self.pieces = sem.shape[3]

    @staticmethod
    def scratch(hops, streams, pieces=1):
        return [pltpu.SemaphoreType.DMA((8, hops + 1, streams, pieces))]

    def there(self, h):
        return True if h == 0 else lax.axis_index("seq") - h >= 0

    def piece(self, h, m, quarter, n):
        ref = self.at(h, m, quarter)
        rows = ref.shape[0] // self.pieces
        return ref.at[pl.ds(n * rows, rows)]

    def copy(self, kind, h, m, quarter, n, device):
        ref = self.piece(h, m, quarter, n)
        return remote(ref, ref, self.sem.at[2 * kind, h, m, n], self.sem.at[2 * kind + 1, h, m, n], device)

    def relay(self, h, m, n):
        s, t = lax.axis_index("seq"), place()[1]
        return remote(
            self.piece(h, m, t, n),
            self.piece(h + 1, m, t, n),
            self.sem.at[0, h, m, n],
            self.sem.at[1, h + 1, m, n],
            {"seq": s + 1},
        )

    def relays(self, h):
        s = lax.axis_index("seq")
        return (s - h >= 0) & (s + 1 < self.seq_count)

    def forward(self, h, m, n):
        if h < self.hops:
            pl.when(self.relays(h))(lambda: self.relay(h, m, n).start())

    def spread(self, h, m, n):
        s, t, y, c, core, far = place()
        self.copy(1, h, m, t, n, {"tensor": far}).start()
        self.copy(2, h, m, t, n, {"tensor": core}).start()

    def start(self, m):
        for n in range(self.pieces):
            self.forward(0, m, n)
            if self.first == 0:
                self.spread(0, m, n)

    def arrive(self, h, m):
        @pl.when(self.there(h))
        def _():
            for n in range(self.pieces):
                self.copy(0, h, m, place()[1], n, {"seq": lax.axis_index("seq") - 1}).wait_recv()
                self.forward(h, m, n)
                self.spread(h, m, n)

    def pass_on(self, h, m):
        s, t, y, c, core, far = place()

        def act():
            for n in range(self.pieces):
                self.copy(1, h, m, far, n, {"tensor": far}).wait_recv()
                self.copy(3, h, m, far, n, {"tensor": core}).start()

        when(self.there(h), act)

    def finish(self, h, m):
        s, t, y, c, core, far = place()

        def act():
            for n in range(self.pieces):
                self.copy(2, h, m, core, n, {"tensor": core}).wait_recv()
                self.copy(3, h, m, 3 - t, n, {"tensor": core}).wait_recv()

        when(self.there(h), act)

    def clear(self, h, m):
        @pl.when(lax.axis_index("seq") - h < 0)
        def _():
            for quarter in range(4):
                ref = self.at(h, m, quarter)
                ref[...] = jnp.zeros(ref.shape, ref.dtype)

    def drain(self):
        s, t, y, c, core, far = place()
        for m in range(self.streams):
            for n in range(self.pieces):
                for h in range(self.hops):
                    pl.when(self.relays(h))(functools.partial(lambda h, m, n: self.relay(h, m, n).wait_send(), h, m, n))
                for h in range(self.first, self.hops + 1):

                    def act():
                        self.copy(1, h, m, t, n, {"tensor": far}).wait_send()
                        self.copy(2, h, m, t, n, {"tensor": core}).wait_send()
                        self.copy(3, h, m, far, n, {"tensor": core}).wait_send()

                    when(self.there(h), act)


class GradReduce:
    def __init__(self, seq_count, source, result, scratch):
        self.seq_count, self.source, self.result = seq_count, source, result
        self.x_in, self.z_out, self.z_in, self.back_out, self.back_in, self.x_sem, self.z_sem, self.back_sem = scratch
        self.half = self.x_in.shape[2]
        self.rows = self.back_out.shape[1]

    @staticmethod
    def scratch(seq_count, chunks, depth, width):
        rows, half = depth // seq_count, width // 2
        return [
            pltpu.VMEM((chunks, depth, half), BF),
            pltpu.VMEM((chunks, depth, half), BF),
            pltpu.VMEM((chunks, seq_count + 1, rows, half), BF),
            pltpu.VMEM((chunks, rows, half), BF),
            pltpu.VMEM((chunks, rows, half), BF),
            pltpu.SemaphoreType.DMA((2, chunks)),
            pltpu.SemaphoreType.DMA((2, chunks, seq_count + 1)),
            pltpu.SemaphoreType.DMA((2, chunks)),
        ]

    def columns(self, p):
        return pl.ds(pl.multiple_of(p * self.half, LANES), self.half)

    def block(self, j):
        return pl.ds(pl.multiple_of(j * self.rows, 16), self.rows)

    def over(self, c):
        p = lax.axis_index("dp")
        return remote(
            self.source(c).at[:, self.columns(1 - p)], self.x_in.at[c], self.x_sem.at[0, c], self.x_sem.at[1, c], {"dp": 1 - p}
        )

    def row_copy(self, c, s, j):
        peer = s + 1 if j > s else s - 1
        slot = self.seq_count if j == peer and j < s else j
        rows = self.z_out.at[c, j * self.rows : (j + 1) * self.rows]
        return remote(rows, self.z_in.at[c, slot], self.z_sem.at[0, c, j], self.z_sem.at[1, c, slot], {"seq": peer})

    def arrival(self, c, slot, peer):
        ref = self.z_in.at[c, slot]
        return remote(ref, ref, self.z_sem.at[0, c, slot], self.z_sem.at[1, c, slot], {"seq": peer})

    def back(self, c):
        p = lax.axis_index("dp")
        return remote(
            self.back_out.at[c], self.back_in.at[c], self.back_sem.at[0, c], self.back_sem.at[1, c], {"dp": 1 - p}
        )

    def start(self, c):
        self.over(c).start()

    def spread(self, c):
        p = lax.axis_index("dp")
        self.over(c).wait_recv()
        mine = self.source(c)[:, self.columns(p)].astype(F32) + self.x_in[c].astype(F32)
        self.z_out[c] = mine.astype(BF)
        last = self.seq_count - 1
        for s in {0, last}:

            @pl.when(lax.axis_index("seq") == s)
            def _():
                for j in range(self.seq_count):
                    if j != s:
                        self.row_copy(c, s, j).start()

    def relay(self, c, d):
        for right in (True, False):
            s = d if right else self.seq_count - 1 - d
            targets = range(s + 1, self.seq_count) if right else range(s)

            @pl.when(lax.axis_index("seq") == s)
            def _():
                for j in targets:
                    self.arrival(c, j, s - 1 if right else s + 1).wait_recv()
                    rows = slice(j * self.rows, (j + 1) * self.rows)
                    added = self.z_out[c, rows].astype(F32) + self.z_in[c, j].astype(F32)
                    self.z_out[c, rows] = added.astype(BF)
                    self.row_copy(c, s, j).start()

    def collect(self, c, acc):
        s, p = lax.axis_index("seq"), lax.axis_index("dp")
        here = self.block(s)
        acc[...] = self.source(c)[here, self.columns(p)].astype(F32) + self.x_in[c, here].astype(F32)
        for n in range(self.seq_count):

            @pl.when(s == n)
            def _():
                for there, slot, peer in ((n > 0, n, n - 1), (n + 1 < self.seq_count, self.seq_count, n + 1)):
                    if there:
                        self.arrival(c, slot, peer).wait_recv()
                        acc[...] += self.z_in[c, slot].astype(F32)

        self.back_out[c] = acc[...].astype(BF)
        self.back(c).start()

    def finish(self, c):
        p = lax.axis_index("dp")
        self.back(c).wait_recv()
        self.result(c)[:, self.columns(p)] = self.back_out[c]
        self.result(c)[:, self.columns(1 - p)] = self.back_in[c]

    def drain(self, c):
        self.over(c).wait_send()
        for s in range(self.seq_count):

            @pl.when(lax.axis_index("seq") == s)
            def _():
                for j in range(self.seq_count):
                    if j != s:
                        self.row_copy(c, s, j).wait_send()

        self.back(c).wait_send()


def params(cid=None):
    if cid is None:
        return pltpu.CompilerParams(vmem_limit_bytes=VMEM_LIMIT)
    return pltpu.CompilerParams(vmem_limit_bytes=VMEM_LIMIT, collective_id=cid, has_side_effects=True)


def in_vmem(count):
    return [pl.BlockSpec(memory_space=pltpu.VMEM)] * count


def gather_rows(inputs, ids, seq_count):
    streams, quarters, rows, width = inputs.shape
    hops = seq_count - 1

    def kernel(x_ref, id_ref, out, out_ids, sem, id_sem):
        s, t, y, c, core, far = place()
        greet(seq_count, hops)
        out[0] = x_ref[...]
        out_ids[0] = id_ref[...]
        ag = AllGather(seq_count, hops, streams, out, sem, first=1)

        def id_copy(h, peer):
            return remote(id_ref, out_ids.at[h], id_sem.at[0, h], id_sem.at[1, h], {"seq": peer})

        for h in range(1, hops + 1):

            @pl.when(s + h < seq_count)
            def _():
                id_copy(h, s + h).start()

        for m in range(streams):
            ag.start(m)
        for h in range(1, hops + 1):
            for m in range(streams):
                ag.clear(h, m)

            @pl.when(s - h < 0)
            def _():
                out_ids[h] = jnp.full(out_ids.shape[1:], -1, jnp.int32)

        for m in range(streams):
            for h in range(1, hops + 1):
                ag.arrive(h, m)
        for m in range(streams):
            for h in range(1, hops + 1):
                ag.pass_on(h, m)
        for h in range(1, hops + 1):
            for m in range(streams):
                ag.finish(h, m)

            @pl.when(s - h >= 0)
            def _():
                id_copy(h, s - h).wait_recv()

            @pl.when(s + h < seq_count)
            def _():
                id_copy(h, s + h).wait_send()

        ag.drain()

    return pl.pallas_call(
        kernel,
        name="gather_rows",
        out_shape=(
            jax.ShapeDtypeStruct((seq_count,) + inputs.shape, inputs.dtype),
            jax.ShapeDtypeStruct((seq_count,) + ids.shape, jnp.int32),
        ),
        in_specs=in_vmem(2),
        out_specs=tuple(in_vmem(2)),
        scratch_shapes=AllGather.scratch(hops, streams) + [pltpu.SemaphoreType.DMA((2, seq_count))],
        compiler_params=params(1),
    )(inputs, ids)


def exchange(name, cid, seq_count, parts, others, reduce_hops, gather_hops, finish, extra):
    per_part = parts[0].shape[1]
    rows, width = parts[0].shape[4:]
    streams = per_part * len(parts)
    hops = max(reduce_hops, gather_hops)

    def kernel(*refs):
        refs = list(refs)
        part_refs = [refs.pop(0) for _ in parts]
        other_refs = [refs.pop(0) for _ in others]
        out = refs.pop(0)
        extra_refs = [refs.pop(0) for _ in extra]
        acc = refs.pop(0)
        gather_sem = refs.pop(0)
        s, t, y, c, core, far = place()
        greet(seq_count, hops)
        rs = ReduceScatter(
            seq_count, reduce_hops, streams, lambda h, m: part_refs[m // per_part].at[h, m % per_part], refs
        )
        ag = AllGather(seq_count, gather_hops, streams, out, gather_sem)
        for h, m in rs.order():
            rs.start(h, m)
        for h in range(1, gather_hops + 1):
            for m in range(streams):
                ag.clear(h, m)
        for h, m in rs.order():
            rs.middle(h, m)
        for h, m in rs.order():
            if h:
                rs.hop(h, m, acc)
        for m in range(streams):
            rs.total(m, acc)
            out[0, m, t] = finish(m, acc[...], other_refs, extra_refs)
            ag.start(m)
        for m in range(streams):
            ag.pass_on(0, m)
            for h in range(1, gather_hops + 1):
                ag.arrive(h, m)
        for m in range(streams):
            for h in range(1, gather_hops + 1):
                ag.pass_on(h, m)
        for h in range(gather_hops + 1):
            for m in range(streams):
                ag.finish(h, m)
        rs.drain()
        ag.drain()

    return pl.pallas_call(
        kernel,
        name=name,
        out_shape=(jax.ShapeDtypeStruct((gather_hops + 1, streams, 4, rows, width), BF),) + tuple(extra),
        in_specs=in_vmem(len(parts) + len(others)),
        out_specs=tuple(in_vmem(1 + len(extra))),
        scratch_shapes=[pltpu.VMEM((rows, width), F32)]
        + AllGather.scratch(gather_hops, streams)
        + ReduceScatter.scratch(reduce_hops, streams, rows, width),
        compiler_params=params(cid),
    )(*parts, *others)


def norm_of(values, gain_row):
    inverse = lax.rsqrt(jnp.mean(values * values, axis=-1, keepdims=True) + EPSILON)
    return values * inverse * gain_row


def norm_back(values, gain_row, grad_out):
    inverse = lax.rsqrt(jnp.mean(values * values, axis=-1, keepdims=True) + EPSILON)
    scaled = grad_out * gain_row
    dot = jnp.mean(scaled * values, axis=-1, keepdims=True)
    grad_in = inverse * scaled - values * (inverse * inverse * inverse) * dot
    return grad_in, jnp.sum(grad_out * values * inverse, axis=0, keepdims=True)


def strips(base_ref, strip):
    @pl.loop(0, base_ref.shape[0])
    def _(k):
        taps = base_ref[k] if len(base_ref.shape) == 3 else base_ref[pl.ds(k, 1)]
        row = jnp.broadcast_to(taps, strip.shape[1:])
        strip[k] = pltpu.roll(row, 0, 1, stride=1, stride_axis=0).astype(BF)


def lay_taps(taps_ref, base_ref, back):
    count, length = taps_ref.shape
    blocks = length // LANES
    base_ref[...] = jnp.zeros_like(base_ref)
    if back:
        base_ref[:, 3 * LANES : 3 * LANES + length] = taps_ref[...].astype(F32)
        return
    row = lax.broadcasted_iota(jnp.int32, (LANES, LANES), 0)
    lane = lax.broadcasted_iota(jnp.int32, (LANES, LANES), 1)
    turn = jnp.where(row + lane == LANES, 1.0, 0.0).astype(BF)
    first = lax.broadcasted_iota(jnp.int32, (count, LANES), 1) == 0
    turned = [dot_nn(taps_ref[:, j * LANES : (j + 1) * LANES], turn) for j in range(blocks)]
    for b in range(blocks):
        j = blocks - 1 - b
        below = turned[j - 1] if j else jnp.zeros((count, LANES), F32)
        taps = taps_ref[:, j * LANES : (j + 1) * LANES].astype(F32)
        base_ref[:, b * LANES : (b + 1) * LANES] = jnp.where(first, taps, below)
    base_ref[:, (blocks + 3) * LANES :] = turned[blocks - 1]


def convolve(rows, row_ids, col_ids, base, seq_count):
    _, streams, length, width = rows.shape
    count, _, wide = base.shape
    blocks = length // LANES
    at_once = seq_count <= 4

    def whole_kernel(x_ref, row_ref, col_ref, base_ref, out_ref, strip, mask, left):
        strips(base_ref, strip)

        @pl.loop(0, streams)
        def _(m):
            for h in range(seq_count):
                mask[:, h * length : (h + 1) * length] = jnp.where(col_ref[m] == row_ref[h, m], 1.0, 0.0).astype(BF)
            right = jnp.concatenate([x_ref[h, m] for h in range(seq_count)], axis=0)

            @pl.loop(0, count)
            def _(k):
                for a in range(blocks):
                    for h in range(seq_count):
                        start = LANES * (blocks * (seq_count - h) - 1 - a)
                        down, across = slice(a * LANES, (a + 1) * LANES), slice(h * length, (h + 1) * length)
                        left[down, across] = strip[k, :, start : start + length] * mask[down, across]
                out_ref[k, m] = jnp.dot(left[...], right, preferred_element_type=F32).astype(BF)

    def kernel(x_ref, row_ref, col_ref, base_ref, out_ref, strip, mask, acc):
        strips(base_ref, strip)
        s = lax.axis_index("seq")

        @pl.loop(0, streams)
        def _(m):
            acc[...] = jnp.zeros_like(acc)

            @pl.loop(0, s + 1)
            def _(h):
                mask[...] = jnp.where(col_ref[m] == row_ref[h, m], 1.0, 0.0).astype(BF)

                @pl.loop(0, count)
                def _(k):
                    pieces = []
                    for a in range(blocks):
                        start = pl.multiple_of(LANES * (blocks * (seq_count - h) - 1 - a), LANES)
                        pieces.append(strip[k, :, pl.ds(start, length)] * mask[a * LANES : (a + 1) * LANES])
                    acc[k] += jnp.dot(jnp.concatenate(pieces, axis=0), x_ref[h, m], preferred_element_type=F32)

            @pl.loop(0, count)
            def _(k):
                out_ref[k, m] = acc[k].astype(BF)

    span = seq_count * length if at_once else length
    return pl.pallas_call(
        whole_kernel if at_once else kernel,
        name="convolve",
        out_shape=jax.ShapeDtypeStruct((count, streams, length, width), BF),
        in_specs=in_vmem(4),
        out_specs=in_vmem(1)[0],
        scratch_shapes=[
            pltpu.VMEM((count, LANES, wide), BF),
            pltpu.VMEM((length, span), BF),
            pltpu.VMEM((length, span), BF) if at_once else pltpu.VMEM((count, length, width), F32),
        ],
        compiler_params=params(),
    )(rows, row_ids, col_ids, base)


def convolve_back(grads, row_ids, col_ids, base, own_lag, tail_lag, seq_count):
    count, streams, length, width = grads.shape
    wide = base.shape[2]
    blocks = length // LANES
    channels = own_lag.shape[2]
    tail_rows = tail_lag.shape[1]

    def kernel(g_ref, row_ref, col_ref, base_ref, own_ref, tail_ref, out_ref, strip, mask, acc):
        strips(base_ref, strip)
        s = lax.axis_index("seq")
        mine = pl.ds(pl.multiple_of(lax.axis_index("tensor") * channels, LANES), channels)

        @pl.loop(0, s + 1)
        def _(h):
            @pl.loop(0, streams)
            def _(m):
                mask[...] = jnp.where(col_ref[h, m] == row_ref[m], 1.0, 0.0).astype(BF)
                acc[...] = jnp.zeros_like(acc)

                @pl.when(h == 0)
                def _():
                    acc[:, mine] = own_ref[m]

                @pl.when(h == 1)
                def _():
                    acc[length - tail_rows :, mine] = tail_ref[m]

                @pl.loop(0, count)
                def _(k):
                    pieces = []
                    for a in range(blocks):
                        start = pl.multiple_of(LANES * (blocks * h + blocks - 1 - a), LANES)
                        pieces.append(strip[k, :, pl.ds(start, length)] * mask[a * LANES : (a + 1) * LANES])
                    acc[...] += jnp.dot(jnp.concatenate(pieces, axis=0), g_ref[k, m], preferred_element_type=F32)

                out_ref[h, m] = acc[...].astype(BF)

    return pl.pallas_call(
        kernel,
        name="convolve_back",
        out_shape=jax.ShapeDtypeStruct((seq_count, streams, length, width), BF),
        in_specs=in_vmem(6),
        out_specs=in_vmem(1)[0],
        scratch_shapes=[
            pltpu.VMEM((count, LANES, wide), BF),
            pltpu.VMEM((length, length), BF),
            pltpu.VMEM((length, width), F32),
        ],
        compiler_params=params(),
    )(grads, row_ids, col_ids, base, own_lag, tail_lag)


def dot_nn(a, b):
    return jnp.dot(a, b, preferred_element_type=F32)


def dot_nt(a, b):
    return lax.dot_general(a, b, (((1,), (1,)), ((), ())), preferred_element_type=F32)


def dot_tn(a, b):
    return lax.dot_general(a, b, (((0,), (0,)), ((), ())), preferred_element_type=F32)


def allowed_keys(query_ids, key_ids, first_row, distance):
    shape = (query_ids.shape[0], key_ids.shape[1])
    offset = lax.broadcasted_iota(jnp.int32, shape, 0) - lax.broadcasted_iota(jnp.int32, shape, 1) + (first_row + distance)
    return (query_ids == key_ids) & (offset >= 0) & (offset < WINDOW)


def one_head(block, head):
    lane = lax.broadcasted_iota(jnp.int32, block.shape, 1)
    return jnp.where((lane >= head * HD) & (lane < (head + 1) * HD), block, jnp.zeros_like(block))


def attend(rows, row_ids, col_ids, wq, wk, wv, wo):
    spans, streams, length, width = rows.shape
    cols = wq.shape[1]
    heads = cols // HD
    tile = min(256, length)
    scale = HD ** (-0.5)

    def kernel(x_ref, row_ref, col_ref, wq_ref, wk_ref, wv_ref, wo_ref, q_ref, k_ref, v_ref, a_ref, lse_ref, p_ref):
        @pl.loop(0, streams)
        def _(m):
            q_ref[m] = dot_nn(x_ref[0, m], wq_ref[...]).astype(BF)
            for h in range(spans):
                k_ref[h, m] = dot_nn(x_ref[h, m], wk_ref[...]).astype(BF)
                v_ref[h, m] = dot_nn(x_ref[h, m], wv_ref[...]).astype(BF)

            @pl.loop(0, length // tile)
            def _(i):
                first = pl.multiple_of(i * tile, tile)
                here = pl.ds(first, tile)
                masks = [allowed_keys(col_ref[m, here], row_ref[h, m], first, h * length) for h in range(spans)]
                block = q_ref[m, here]
                result = jnp.zeros((tile, cols), F32)
                for head in range(heads):
                    query = one_head(block, head)
                    scores = [
                        jnp.where(masks[h], dot_nt(query, k_ref[h, m]) * scale, NEGATIVE) for h in range(spans)
                    ]
                    peak = functools.reduce(jnp.maximum, [jnp.max(v, axis=-1, keepdims=True) for v in scores])
                    raised = [jnp.exp(v - peak) for v in scores]
                    total = sum([jnp.sum(v, axis=-1, keepdims=True) for v in raised])
                    inverse = 1.0 / total
                    mixed = sum([dot_nn((raised[h] * inverse).astype(BF), v_ref[h, m]) for h in range(spans)])
                    result = result + one_head(mixed, head)
                    lse_ref[m, head, here] = jnp.broadcast_to(peak + jnp.log(total), (tile, LANES))
                a_ref[m, here] = result.astype(BF)

            p_ref[m] = dot_nn(a_ref[m], wo_ref[...]).astype(BF)

    part = jax.ShapeDtypeStruct((streams, length, cols), BF)
    span = jax.ShapeDtypeStruct((spans, streams, length, cols), BF)
    return pl.pallas_call(
        kernel,
        name="attend",
        out_shape=(
            part,
            span,
            span,
            part,
            jax.ShapeDtypeStruct((streams, heads, length, LANES), F32),
            jax.ShapeDtypeStruct((streams, length, width), BF),
        ),
        in_specs=in_vmem(7),
        out_specs=tuple(in_vmem(6)),
        compiler_params=params(),
    )(rows, row_ids, col_ids, wq, wk, wv, wo)


def attend_back(q, k, v, lse, grad_out, row_ids, col_ids, wq, wk, wv, wo):
    spans, streams, length, cols = k.shape
    width = grad_out.shape[2]
    heads = cols // HD
    tile = min(256, length)
    scale = HD ** (-0.5)

    def kernel(
        q_ref, k_ref, v_ref, lse_ref, go_ref, row_ref, col_ref, wq_ref, wk_ref, wv_ref, wo_ref,
        dq_ref, dk_ref, dv_ref, p_ref, ga_ref, dk_acc, dv_acc,
    ):
        @pl.loop(0, streams)
        def _(m):
            ga_ref[...] = dot_nt(go_ref[m], wo_ref[...]).astype(BF)
            dk_acc[...] = jnp.zeros_like(dk_acc)
            dv_acc[...] = jnp.zeros_like(dv_acc)

            @pl.loop(0, length // tile)
            def _(i):
                first = pl.multiple_of(i * tile, tile)
                here = pl.ds(first, tile)
                masks = [allowed_keys(col_ref[m, here], row_ref[h, m], first, h * length) for h in range(spans)]
                block = q_ref[m, here]
                grad_block = ga_ref[here]
                result = jnp.zeros((tile, cols), F32)
                for head in range(heads):
                    query = one_head(block, head)
                    grad = one_head(grad_block, head)
                    level = lse_ref[m, head, here][:, :1]
                    prob = [
                        jnp.where(masks[h], jnp.exp(dot_nt(query, k_ref[h, m]) * scale - level), 0.0)
                        for h in range(spans)
                    ]
                    grad_prob = [dot_nt(grad, v_ref[h, m]) for h in range(spans)]
                    mean = sum([jnp.sum(p * g, axis=-1, keepdims=True) for p, g in zip(prob, grad_prob)])
                    grad_scores = [(p * (g - mean)).astype(BF) for p, g in zip(prob, grad_prob)]
                    for h in range(spans):
                        dv_acc[h] += dot_tn(prob[h].astype(BF), grad)
                        dk_acc[h] += dot_tn(grad_scores[h], query)
                    mixed = sum([dot_nn(grad_scores[h], k_ref[h, m]) for h in range(spans)])
                    result = result + one_head(mixed, head)
                dq_ref[m, here] = (result * scale).astype(BF)

            for h in range(spans):
                dk_ref[h, m] = (dk_acc[h] * scale).astype(BF)
                dv_ref[h, m] = dv_acc[h].astype(BF)
                back = dot_nt(dk_ref[h, m], wk_ref[...]) + dot_nt(dv_ref[h, m], wv_ref[...])
                if h == 0:
                    back = back + dot_nt(dq_ref[m], wq_ref[...])
                p_ref[h, m] = back.astype(BF)

    span = jax.ShapeDtypeStruct((spans, streams, length, cols), BF)
    return pl.pallas_call(
        kernel,
        name="attend_back",
        out_shape=(
            jax.ShapeDtypeStruct((streams, length, cols), BF),
            span,
            span,
            jax.ShapeDtypeStruct((spans, streams, length, width), BF),
        ),
        in_specs=in_vmem(11),
        out_specs=tuple(in_vmem(4)),
        scratch_shapes=[
            pltpu.VMEM((length, cols), BF),
            pltpu.VMEM((spans, length, cols), F32),
            pltpu.VMEM((spans, length, cols), F32),
        ],
        compiler_params=params(),
    )(q, k, v, lse, grad_out, row_ids, col_ids, wq, wk, wv, wo)


def unit_terms(gate_pre, up_pre, grad_inner):
    root = 0.7978845608028654
    square = gate_pre * gate_pre
    bend = jnp.tanh(root * (gate_pre + 0.044715 * (gate_pre * square)))
    half = 0.5 * (1.0 + bend)
    gelu = gate_pre * half
    slope = half + 0.5 * gate_pre * (1.0 - bend * bend) * (root * (1.0 + 3.0 * 0.044715 * square))
    return gelu * up_pre, grad_inner * up_pre * slope, grad_inner * gelu


def head(
    x, ids, stu_gain, filter_proj, lag_proj, filters, attn_gain, feed_gain, wq, wk, wv, wo, wg, wu, wd, cot, seq_count
):
    streams, _, quarter, width = x.shape
    length = 4 * quarter
    hops = WINDOW // length
    spans = hops + 1
    count, taps = filters.shape
    wide = taps + 4 * LANES
    lag_order, channels = lag_proj.shape[:2]
    blocks = length // LANES
    reach = taps * 5 // 8
    window = reach + 2 * quarter
    own = 4 * (seq_count - 1)
    assert reach % (2 * quarter) == 0 and window <= taps
    cols, units = wq.shape[1], wg.shape[1]
    heads = cols // HD
    tile = 2 * quarter
    steps = 2 * streams
    scale = HD ** (-0.5)
    rows = width // seq_count
    chunks = 4
    assert streams == 2 and units == 4 * cols

    rows_of = pltpu.VMEM((streams, length, cols), BF)
    unit_rows = pltpu.VMEM((streams, length, units), BF)
    state = pltpu.VMEM((streams, quarter, width), F32)
    gathered = (1, streams, 4, quarter, width)
    split_part = pltpu.VMEM((1, streams, 2, 2, quarter, width), BF)
    pieces = 2
    zero_hops = ReduceScatter.scratch(0, streams, quarter, width, pieces)

    def kernel(
        x_ref, id_ref, sg_ref, fp_hbm, lp_ref, taps_ref, ag_ref, fg_ref,
        wq_ref, wk_ref, wv_ref, wo_ref, wg_hbm, wu_hbm, wd_hbm, cot_hbm,
        stu_out, layer_out, one_out, gain_out, sum_out, lag_out, ids_out, conv_out, strip_out,
        fp_ref, wg_ref, wu_ref, wd_ref, cot_ref, load_sem, base_ref, ids_row,
        rows_in, ids_in, cols_in, id_ext, lag_ext, part_ref, id_sem, strip_sem, conv_sem,
        attn_in, feed_in, grad_att, hid_one, hid_two, grad_two, grads, total, grad_acc,
        o_part, feed_part, layer_part, attn_part,
        sem_rows, sem_one, sem_two, sem_three, sem_layer, sem_five, *scratch,
    ):
        s, t, y, c, core, far = place()
        scratch = list(scratch)

        def take(count):
            taken = scratch[:count]
            del scratch[:count]
            return taken

        def reducer(ref, distance):
            return ReduceScatter(seq_count, distance, streams, lambda h, m: ref.at[h, m], take(6))

        rs_one, rs_two, rs_three, rs_layer = [reducer(r, 0) for r in (part_ref, o_part, feed_part, layer_part)]
        rs_four = reducer(attn_part, hops)
        gr = GradReduce(seq_count, lambda k: grads.at[k], lambda k: sum_out.at[k], take(8))
        ag_rows = AllGather(
            seq_count,
            seq_count - 1,
            streams,
            lambda h, m, q: rows_in.at[m, 4 * (seq_count - 1 - h) + q],
            sem_rows,
            first=1,
        )
        ag_one = AllGather(seq_count, hops, streams, attn_in, sem_one)
        ag_two = AllGather(seq_count, 0, streams, feed_in, sem_two)
        ag_three = AllGather(seq_count, 0, streams, grad_att, sem_three)
        ag_layer = AllGather(seq_count, 0, streams, layer_out, sem_layer)
        ag_five = AllGather(seq_count, 0, streams, stu_out, sem_five)

        def flat(value):
            return value.reshape(-1, value.shape[-1])

        def all_rows(ref, m):
            return flat(ref[0, m])

        def masks_of(m, here, first):
            return [
                allowed_keys(cols_in[m, here], ids_out[pl.ds(h * streams + m, 1)], first, h * length) for h in range(spans)
            ]

        def first_norm(m):
            rs_one.total(m, total)
            hidden = x_ref[m, t].astype(F32) + total[...]
            hid_one[m] = hidden
            attn_in[0, m, t] = norm_of(hidden, ag_ref[...]).astype(BF)
            ag_one.start(m)

        def after(i, step, *actions):
            @pl.when(i == step)
            def _():
                for action in actions:
                    action()

        def id_copy(h, peer):
            return remote(id_ref, ids_in.at[h], id_sem.at[0, h], id_sem.at[1, h], {"seq": peer})

        far_back = range(1, seq_count)

        pairs = ((fp_hbm, fp_ref), (wg_hbm, wg_ref), (wu_hbm, wu_ref), (wd_hbm, wd_ref), (cot_hbm, cot_ref))
        loads = [pltpu.make_async_copy(a, b, load_sem.at[i]) for i, (a, b) in enumerate(pairs)]
        for load in loads:
            load.start()

        def front(strip, left, mask, conv):
            for m in range(streams):
                rows_in[m, own + t] = norm_of(x_ref[m, t].astype(F32), sg_ref[...]).astype(BF)
            greet(seq_count, 0, wide=True)
            for m in range(streams):
                ag_rows.start(m)
            for h in far_back:
                pl.when(s + h < seq_count)(functools.partial(lambda h: id_copy(h, s + h).start(), h))
            for m in range(streams):
                for q in range(4):

                    @pl.when(t != q)
                    def _():
                        rows_in[m, own + q] = norm_of(x_ref[m, q].astype(F32), sg_ref[...]).astype(BF)

            for m in range(streams):
                for h in far_back:
                    ag_rows.clear(h, m)
                for h in range(1, spans):
                    ag_one.clear(h, m)
            ids_in[0] = id_ref[...]
            for h in far_back:

                @pl.when(s - h < 0)
                def _():
                    ids_in[h] = jnp.full(ids_in.shape[1:], -1, jnp.int32)

            lay_taps(taps_ref, base_ref, True)
            strips(base_ref, strip)
            strip_copy = pltpu.make_async_copy(strip, strip_out, strip_sem)
            strip_copy.start()
            ag_rows.arrive(1, 0)
            ag_rows.arrive(2, 0)
            for h in far_back:
                pl.when(s - h >= 0)(functools.partial(lambda h: id_copy(h, s - h).wait_recv(), h))
            for h in range(seq_count):
                for m in range(streams):
                    ids_out[h * streams + m : h * streams + m + 1] = ids_in[h, m].astype(F32)
                    start = (seq_count - 1 - h) * length
                    ids_row[m : m + 1, start : start + length] = ids_in[h, m].astype(F32)
            turned = jnp.transpose(ids_out[...])
            for m in range(streams):
                cols_in[m] = turned[:, m : m + 1]
                id_ext[m, :8] = turned[length - 8 :, streams + m : streams + m + 1]
                id_ext[m, 8:] = turned[:, m : m + 1]
            lay_taps(taps_ref, base_ref, False)
            strip_copy.wait()
            strips(base_ref, strip)
            for load in loads:
                load.wait()
            ag_rows.pass_on(1, 0)
            ag_rows.arrive(3, 0)
            ag_rows.pass_on(2, 0)
            ag_rows.finish(1, 0)
            ag_rows.finish(2, 0)
            mine = pl.ds(pl.multiple_of(t * channels, LANES), channels)

            def lags(m):
                lag_ext[:8] = rows_in[m, own - 1, quarter - 8 :, mine].astype(F32)
                lag_ext[8:] = rows_in[m, own : own + 4, :, mine].reshape(length, channels).astype(F32)
                for i in range(lag_order):
                    same = id_ext[m, 7 - i : 7 - i + length] == cols_in[m]
                    lag_out[i, m] = jnp.where(same, lag_ext[7 - i : 7 - i + length], 0.0).astype(BF)

            def conv_copy(k, m, half):
                first = pl.multiple_of(half * tile, tile)
                return pltpu.make_async_copy(
                    conv.at[k, pl.ds(first, tile)],
                    conv_out.at[k, pl.ds(pl.multiple_of(m * length + first, tile), tile)],
                    conv_sem.at[k, half],
                )

            lags(0)
            per = 2 * count

            @pl.loop(0, streams * per)
            def _(j):
                m = j // per
                half = 1 - (j - m * per) // count
                k = j - m * per - (1 - half) * count
                first = pl.multiple_of(half * tile, tile)
                here = pl.ds(first, tile)
                offset = taps - length - reach

                @pl.when(k == 0)
                def _():
                    ids_there = ids_row[pl.ds(m, 1), pl.ds(pl.multiple_of(offset + first, tile), window)]
                    mask[...] = jnp.where(cols_in[m, here] == ids_there, 1.0, 0.0).astype(BF)

                for a in range(2 * quarter // LANES):
                    start = taps - LANES - reach - a * LANES
                    down = slice(a * LANES, (a + 1) * LANES)
                    left[down] = strip[k, :, start : start + window] * mask[down]
                right = rows_in[m, pl.ds(offset // quarter + 2 * half, window // quarter)].reshape(window, width)
                result = dot_nn(left[...], right).astype(BF)
                pl.when(m > 0)(lambda: conv_copy(k, m - 1, half).wait())
                conv[k, here] = result
                conv_copy(k, m, half).start()

                @pl.when(k == count - 1)
                def _():
                    mixed = sum([dot_nn(conv[q, here], fp_ref[q]) for q in range(count)])
                    mixed = mixed + sum([dot_nn(lag_out[i, m, here], lp_ref[i]) for i in range(lag_order)])
                    part_ref[0, m, half] = mixed.astype(BF).reshape(2, quarter, width)

                after(j, 0, lambda: ag_rows.arrive(1, 1))
                after(j, 1, lambda: ag_rows.pass_on(3, 0), lambda: ag_rows.arrive(2, 1))
                after(j, 3, lambda: ag_rows.arrive(3, 1), lambda: ag_rows.pass_on(1, 1))
                after(j, count - 1, lambda: ag_rows.finish(3, 0), lambda: ag_rows.pass_on(2, 1))
                after(j, count + 1, lambda: ag_rows.pass_on(3, 1))
                after(
                    j,
                    per - 1,
                    lambda: rs_one.start(0, 0),
                    *[functools.partial(ag_rows.finish, h, 1) for h in far_back],
                    lambda: lags(1),
                )
                after(j, per + 1, lambda: rs_one.middle(0, 0))
                after(j, per + 6, lambda: first_norm(0))

            rs_one.start(0, 1)
            for k in range(count):
                for half in range(2):
                    conv_copy(k, streams - 1, half).wait()

        pl.run_scoped(
            front,
            pltpu.VMEM((count, LANES, wide), BF),
            pltpu.VMEM((tile, window), BF),
            pltpu.VMEM((tile, window), BF),
            pltpu.VMEM((count, length, width), BF),
        )

        def attention_on(
            q_ref, k_ref, v_ref, a_ref, lse_ref, inner_ref, gg_ref, gu_ref, ga_ref, dk_acc, dv_acc, dq_ref, dkv_ref
        ):
            ag_one.pass_on(0, 0)
            rs_one.middle(0, 1)
            for h in range(1, spans):
                ag_one.arrive(h, 0)
            first_norm(1)
            for h in range(1, spans):
                ag_one.pass_on(h, 0)
            for h in range(spans):
                ag_one.finish(h, 0)

            def split_step(i):
                m = i // 2
                return m, i - 2 * m

            @pl.loop(0, steps)
            def _(i):
                m, half = split_step(i)
                first = pl.multiple_of(half * tile, tile)
                here = pl.ds(first, tile)

                @pl.when(half == 0)
                def _():
                    own = flat(attn_in[0, m])
                    q_ref[m] = dot_nn(own, wq_ref[...]).astype(BF)
                    for h in range(spans):
                        block = flat(attn_in[h, m])
                        k_ref[h, m] = dot_nn(block, wk_ref[...]).astype(BF)
                        v_ref[h, m] = dot_nn(block, wv_ref[...]).astype(BF)

                masks = masks_of(m, here, first)
                block = q_ref[m, here]
                result = jnp.zeros((tile, cols), F32)
                for head in range(heads):
                    query = one_head(block, head)
                    scores = [jnp.where(masks[h], dot_nt(query, k_ref[h, m]) * scale, NEGATIVE) for h in range(spans)]
                    peak = functools.reduce(jnp.maximum, [jnp.max(v, axis=-1, keepdims=True) for v in scores])
                    raised = [jnp.exp(v - peak) for v in scores]
                    norm = sum([jnp.sum(v, axis=-1, keepdims=True) for v in raised])
                    inverse = 1.0 / norm
                    mixed = sum([dot_nn((raised[h] * inverse).astype(BF), v_ref[h, m]) for h in range(spans)])
                    result = result + one_head(mixed, head)
                    lse_ref[m, head, here] = jnp.broadcast_to(peak + jnp.log(norm), (tile, LANES))
                low = result.astype(BF)
                a_ref[m, here] = low
                o_part[0, m, half] = dot_nn(low, wo_ref[...]).astype(BF).reshape(2, quarter, width)
                after(i, 0, lambda: ag_one.pass_on(0, 1), *[functools.partial(ag_one.arrive, h, 1) for h in range(1, spans)])
                after(
                    i,
                    1,
                    lambda: rs_two.start(0, 0),
                    *[functools.partial(ag_one.pass_on, h, 1) for h in range(1, spans)],
                    *[functools.partial(ag_one.finish, h, 1) for h in range(spans)],
                )
                after(i, 2, lambda: rs_two.middle(0, 0))
                after(i, 3, lambda: rs_two.start(0, 1))

            def second_norm(m):
                rs_two.total(m, total)
                hidden = hid_one[m] + total[...]
                hid_two[m] = hidden
                feed_in[0, m, t] = norm_of(hidden, fg_ref[...]).astype(BF)
                ag_two.start(m)

            second_norm(0)
            rs_two.middle(0, 1)
            rs_one.drain()
            ag_rows.drain()
            for h in far_back:
                pl.when(s + h < seq_count)(functools.partial(lambda h: id_copy(h, s + h).wait_send(), h))
            ag_two.pass_on(0, 0)
            ag_two.finish(0, 0)

            @pl.loop(0, steps)
            def _(i):
                m, half = split_step(i)
                here = pl.ds(pl.multiple_of(half * tile, tile), tile)
                block = flat(feed_in[0, m, pl.ds(2 * half, 2)])
                inner, grad_gate, grad_up = unit_terms(
                    dot_nn(block, wg_ref[...]), dot_nn(block, wu_ref[...]), dot_nt(cot_ref[m, here], wd_ref[...])
                )
                inner, grad_gate, grad_up = inner.astype(BF), grad_gate.astype(BF), grad_up.astype(BF)
                inner_ref[m, here] = inner
                gg_ref[m, here] = grad_gate
                gu_ref[m, here] = grad_up
                back = dot_nt(grad_gate, wg_ref[...]) + dot_nt(grad_up, wu_ref[...])
                feed_part[0, m, half] = back.astype(BF).reshape(2, quarter, width)
                layer_part[0, m, half] = dot_nn(inner, wd_ref[...]).astype(BF).reshape(2, quarter, width)
                after(i, 0, lambda: second_norm(1))
                after(
                    i,
                    1,
                    lambda: rs_three.start(0, 0),
                    lambda: ag_two.pass_on(0, 1),
                    lambda: rs_three.middle(0, 0),
                    lambda: ag_two.finish(0, 1),
                )
                after(i, 3, lambda: rs_three.start(0, 1))

            def third_norm(m):
                rs_three.total(m, total)
                grad_in, gain_grad = norm_back(hid_two[m], fg_ref[...], total[...])
                value = cot_ref[m, pl.ds(pl.multiple_of(t * quarter, quarter), quarter)].astype(F32) + grad_in
                grad_two[m] = value
                gain_out[1:2] = gain_grad if m == 0 else gain_out[1:2] + gain_grad
                grad_att[0, m, t] = value.astype(BF)
                ag_three.start(m)

            third_norm(0)
            feed_all = flat(feed_in[0])
            grads[0] = dot_tn(feed_all, flat(gg_ref[...])).astype(BF)
            gr.start(0)
            rs_three.middle(0, 1)
            grads[1] = dot_tn(feed_all, flat(gu_ref[...])).astype(BF)
            gr.start(1)
            grads[2] = dot_tn(flat(cot_ref[...]), flat(inner_ref[...])).astype(BF)
            gr.start(2)
            rs_two.drain()
            ag_one.drain()
            ag_three.pass_on(0, 0)
            ag_three.finish(0, 0)
            for m in range(streams):
                rs_layer.start(0, m)

            def layer_sum(m):
                rs_layer.total(m, total)
                layer_out[0, m, t] = (hid_two[m] + total[...]).astype(BF)
                ag_layer.start(m)

            @pl.loop(0, steps)
            def _(i):
                m, half = split_step(i)
                first = pl.multiple_of(half * tile, tile)
                here = pl.ds(first, tile)

                @pl.when(half == 0)
                def _():
                    ga_ref[...] = dot_nt(all_rows(grad_att, m), wo_ref[...]).astype(BF)
                    dk_acc[...] = jnp.zeros_like(dk_acc)
                    dv_acc[...] = jnp.zeros_like(dv_acc)

                masks = masks_of(m, here, first)
                block = q_ref[m, here]
                grad_block = ga_ref[here]
                result = jnp.zeros((tile, cols), F32)
                for head in range(heads):
                    query = one_head(block, head)
                    grad = one_head(grad_block, head)
                    level = lse_ref[m, head, here][:, :1]
                    prob = [
                        jnp.where(masks[h], jnp.exp(dot_nt(query, k_ref[h, m]) * scale - level), 0.0) for h in range(spans)
                    ]
                    grad_prob = [dot_nt(grad, v_ref[h, m]) for h in range(spans)]
                    mean = sum([jnp.sum(p * g, axis=-1, keepdims=True) for p, g in zip(prob, grad_prob)])
                    grad_scores = [(p * (g - mean)).astype(BF) for p, g in zip(prob, grad_prob)]
                    for h in range(spans):
                        dv_acc[h] += dot_tn(prob[h].astype(BF), grad)
                        dk_acc[h] += dot_tn(grad_scores[h], query)
                    mixed = sum([dot_nn(grad_scores[h], k_ref[h, m]) for h in range(spans)])
                    result = result + one_head(mixed, head)
                dq_ref[m, here] = (result * scale).astype(BF)

                @pl.when(half == 1)
                def _():
                    for h in range(hops, -1, -1):
                        grad_k = (dk_acc[h] * scale).astype(BF)
                        grad_v = dv_acc[h].astype(BF)
                        dkv_ref[h, m, :, :cols] = grad_k
                        dkv_ref[h, m, :, cols:] = grad_v
                        back = dot_nt(grad_k, wk_ref[...]) + dot_nt(grad_v, wv_ref[...])
                        if h == 0:
                            back = back + dot_nt(dq_ref[m], wq_ref[...])
                        attn_part[h, m] = back.astype(BF).reshape(2, 2, quarter, width)
                        rs_four.start(h, m)

                after(i, 0, lambda: third_norm(1), lambda: rs_layer.middle(0, 0), lambda: rs_layer.middle(0, 1))
                after(i, 1, lambda: gr.spread(0), lambda: ag_three.pass_on(0, 1), lambda: ag_three.finish(0, 1))
                after(
                    i,
                    2,
                    *[functools.partial(rs_four.middle, h, 0) for h in range(hops, -1, -1)],
                    lambda: gr.spread(1),
                    lambda: gr.relay(0, 1),
                )
                after(
                    i,
                    3,
                    *[functools.partial(rs_four.hop, h, 0, total) for h in range(hops, 0, -1)],
                    lambda: gr.spread(2),
                    lambda: gr.relay(0, 2),
                    lambda: gr.relay(1, 1),
                )

            for h in range(hops, -1, -1):
                rs_four.middle(h, 1)
            attn_all = attn_in[...].reshape(spans * streams * length, width)
            grads[3, :, cols : 3 * cols] = dot_tn(attn_all, flat(dkv_ref[...].reshape(-1, 2 * cols))).astype(BF)
            grads[3, :, :cols] = dot_tn(flat(attn_in[0]), flat(dq_ref[...])).astype(BF)
            grads[3, :, 3 * cols :] = dot_tn(flat(grad_att[0]), flat(a_ref[...])).astype(BF)
            gr.start(3)

            def fourth_norm(m):
                rs_four.total(m, total)
                grad_in, gain_grad = norm_back(hid_one[m], ag_ref[...], total[...])
                value = grad_two[m] + grad_in
                one_out[m] = value
                gain_out[0:1] = gain_grad if m == 0 else gain_out[0:1] + gain_grad
                stu_out[0, m, t] = value.astype(BF)
                ag_five.start(m)

            gr.relay(1, 2)
            gr.relay(2, 1)
            rs_three.drain()
            ag_two.drain()
            ag_three.drain()
            fourth_norm(0)
            for h in range(hops, 0, -1):
                rs_four.hop(h, 1, total)
            gr.spread(3)
            gr.relay(2, 2)
            gr.collect(0, grad_acc)
            fourth_norm(1)
            for m in range(streams):
                layer_sum(m)
            gr.relay(3, 1)
            gr.collect(1, grad_acc)
            for m in range(streams):
                ag_five.pass_on(0, m)
            gr.relay(3, 2)
            gr.collect(2, grad_acc)
            for m in range(streams):
                ag_five.finish(0, m)
            for m in range(streams):
                ag_layer.pass_on(0, m)
            gr.collect(3, grad_acc)
            rs_layer.drain()
            rs_four.drain()
            for m in range(streams):
                ag_layer.finish(0, m)
            for k in range(chunks):
                gr.finish(k)
                gr.drain(k)
            ag_five.drain()
            ag_layer.drain()

        pl.run_scoped(
            attention_on,
            rows_of,
            pltpu.VMEM((spans, streams, length, cols), BF),
            pltpu.VMEM((spans, streams, length, cols), BF),
            rows_of,
            pltpu.VMEM((streams, heads, length, LANES), F32),
            unit_rows,
            unit_rows,
            unit_rows,
            pltpu.VMEM((length, cols), BF),
            pltpu.VMEM((spans, length, cols), F32),
            pltpu.VMEM((spans, length, cols), F32),
            rows_of,
            pltpu.VMEM((spans, streams, length, 2 * cols), BF),
        )

    anywhere = pl.BlockSpec(memory_space=pl.ANY)
    return pl.pallas_call(
        kernel,
        name="head",
        out_shape=(
            jax.ShapeDtypeStruct(gathered, BF),
            jax.ShapeDtypeStruct(gathered, BF),
            jax.ShapeDtypeStruct((streams, quarter, width), F32),
            jax.ShapeDtypeStruct((2, width), F32),
            jax.ShapeDtypeStruct((chunks, rows, units), BF),
            jax.ShapeDtypeStruct((lag_order, streams, length, channels), BF),
            jax.ShapeDtypeStruct((seq_count * streams, length), F32),
            jax.ShapeDtypeStruct((count, streams * length, width), BF),
            jax.ShapeDtypeStruct((count, LANES, wide), BF),
        ),
        in_specs=[anywhere if i in (3, 12, 13, 14, 15) else spec for i, spec in enumerate(in_vmem(16))],
        out_specs=tuple(in_vmem(7)) + (anywhere, anywhere),
        scratch_shapes=[
            pltpu.VMEM(filter_proj.shape, BF),
            pltpu.VMEM(wg.shape, BF),
            pltpu.VMEM(wu.shape, BF),
            pltpu.VMEM(wd.shape, BF),
            pltpu.VMEM(cot.shape, BF),
            pltpu.SemaphoreType.DMA((5,)),
            pltpu.VMEM((count, wide), F32),
            pltpu.VMEM((streams, taps), F32),
            pltpu.VMEM((streams, 4 * seq_count, quarter, width), BF),
            pltpu.VMEM((seq_count,) + ids.shape, jnp.int32),
            pltpu.VMEM((streams, length, 1), F32),
            pltpu.VMEM((streams, length + 8, 1), F32),
            pltpu.VMEM((length + 8, channels), F32),
            split_part,
            pltpu.SemaphoreType.DMA((2, seq_count)),
            pltpu.SemaphoreType.DMA,
            pltpu.SemaphoreType.DMA((count, 2)),
            pltpu.VMEM((spans, streams, 4, quarter, width), BF),
            pltpu.VMEM(gathered, BF),
            pltpu.VMEM(gathered, BF),
            state,
            state,
            state,
            pltpu.VMEM((chunks, width, units), BF),
            pltpu.VMEM((quarter, width), F32),
            pltpu.VMEM((rows, units // 2), F32),
            split_part,
            split_part,
            split_part,
            pltpu.VMEM((spans, streams, 2, 2, quarter, width), BF),
            AllGather.scratch(seq_count - 1, streams, pieces)[0],
            AllGather.scratch(hops, streams, pieces)[0],
        ]
        + [AllGather.scratch(0, streams, pieces)[0]] * 4
        + zero_hops * 4
        + ReduceScatter.scratch(hops, streams, quarter, width, pieces)
        + GradReduce.scratch(seq_count, chunks, width, units),
        compiler_params=params(8),
    )(
        x, ids, stu_gain, filter_proj, lag_proj, filters, attn_gain, feed_gain, wq, wk, wv, wo, wg, wu, wd, cot
    )


def tail(
    grad_stu, filter_proj, lag_proj, conv, lag_stack, ext_ids, strip_back, x, gain, grad_one, gains, seq_count
):
    count, length_all, width = conv.shape
    streams, _, quarter, _ = x.shape
    length = length_all // streams
    lag_order, channels = lag_proj.shape[:2]
    blocks = length // LANES
    hops = seq_count - 1
    chunks = count + 1
    steps = seq_count * streams
    rows = width // seq_count
    gain_rows = 8

    def kernel(
        gs_ref, fp_hbm, lp_ref, conv_hbm, lag_ref, ext_ref, strip_hbm, x_hbm, gain_ref, one_ref, gains_ref,
        out, filter_out, lag_out, gain_out,
        conv_ref, fp_ref, strip, x_own, conv_sem, fp_sem, strip_sem, x_sem, id_ext,
        mask, cols, left, acc, terms, grad_conv, grads, lag_ext, total, grad_acc, gather_sem,
        gain_own, gain_near, gain_sum, gain_far, near_sem, far_sem, *scratch,
    ):
        s, t, y, c, core, far = place()
        p = lax.axis_index("dp")
        rs_scratch, gr_scratch = scratch[:6], scratch[6:]

        def conv_copy(k):
            return pltpu.make_async_copy(conv_hbm.at[k], conv_ref.at[k], conv_sem.at[k])

        def fp_copy(k):
            return pltpu.make_async_copy(fp_hbm.at[k], fp_ref.at[k], fp_sem.at[k])

        strip_copy = pltpu.make_async_copy(strip_hbm, strip, strip_sem)
        for k in range(count):
            conv_copy(k).start()
            fp_copy(k).start()
        strip_copy.start()
        x_copy = pltpu.make_async_copy(x_hbm.at[:, t], x_own, x_sem)
        x_copy.start()
        greet(seq_count, hops, wide=True, gains=True)

        def source(k):
            return grads.at[k]

        def result(k):
            return filter_out.at[k] if k < count else lag_out

        gr = GradReduce(seq_count, source, result, gr_scratch)
        rs = ReduceScatter(seq_count, hops, streams, lambda h, m: terms.at[h, m], rs_scratch)
        ag = AllGather(seq_count, 0, streams, out, gather_sem)

        @pl.loop(0, count)
        def _(k):
            conv_copy(k).wait()
            grads[k] = dot_tn(conv_ref[k], gs_ref[...]).astype(BF)
            gr.start(k)
            fp_copy(k).wait()
            product = dot_nt(gs_ref[...], fp_ref[k]).astype(BF)
            for m in range(streams):
                here = pl.ds(pl.multiple_of(k * length, LANES), length)
                grad_conv[m, here] = product[m * length : (m + 1) * length]

        grads[count] = jnp.zeros_like(grads.at[count])
        for i in range(lag_order):
            grads[count, :, i * channels : (i + 1) * channels] = dot_tn(gs_ref[...], lag_ref[i]).astype(BF)
        gr.start(count)
        turned = jnp.transpose(ext_ref[...])
        for j in range(steps):
            cols[j] = turned[:, j : j + 1]
        for m in range(streams):
            lag_ext[m] = jnp.zeros_like(lag_ext.at[m])
            id_ext[:8] = turned[length - 8 :, streams + m : streams + m + 1]
            id_ext[8:] = turned[:, m : m + 1]
            for i in range(lag_order):
                term = dot_nt(gs_ref[m * length : (m + 1) * length], lp_ref[i])
                same = id_ext[7 - i : 7 - i + length] == cols[m]
                lag_ext[m, 7 - i : 7 - i + length] += jnp.where(same, term, 0.0)
        strip_copy.wait()
        x_copy.wait()
        mine = pl.ds(pl.multiple_of(t * channels, LANES), channels)
        assert seq_count == 4 and steps == 8 and chunks == 7
        spread_at = {0: 0, 1: 1, 4: 2, 6: 3}
        relay_at = {2: (0, 1), 3: (1, 1), 4: (0, 2), 5: (1, 2), 6: (2, 1), 7: (2, 2)}
        collect_at = {6: 0, 7: 1}

        def step_of(i):
            return seq_count - 1 - i // streams, i - i // streams * streams

        @pl.loop(0, steps)
        def _(i):
            h, m = step_of(i)

            @pl.when(h <= s)
            def _():
                mask[...] = jnp.where(cols[h * streams + m] == ext_ref[pl.ds(m, 1)], 1.0, 0.0).astype(BF)
                for k in range(count):
                    for a in range(blocks):
                        start = pl.multiple_of(LANES * (blocks * h + blocks - 1 - a), LANES)
                        down = slice(a * LANES, (a + 1) * LANES)
                        left[down, k * length : (k + 1) * length] = strip[k, :, pl.ds(start, length)] * mask[down]
                acc[...] = jnp.dot(left[...], grad_conv[m], preferred_element_type=F32)

                @pl.when(h == 0)
                def _():
                    acc[:, mine] += lag_ext[m, 8:]

                @pl.when(h == 1)
                def _():
                    acc[length - 8 :, mine] += lag_ext[m, :8]

                for quarter_y in range(2):
                    for quarter_c in range(2):
                        first = (2 * quarter_y + quarter_c) * quarter
                        terms[h, m, quarter_y, quarter_c] = acc[first : first + quarter].astype(BF)
                rs.start(h, m)

            @pl.when(i >= 1)
            def _():
                rs.middle(*step_of(i - 1))

            @pl.when((i >= 2) & (i < steps - streams + 2))
            def _():
                rs.hop(*step_of(i - 2), total)

            for step, k in spread_at.items():
                pl.when(i == step)(functools.partial(gr.spread, k))
            for step, (k, d) in relay_at.items():
                pl.when(i == step)(functools.partial(gr.relay, k, d))
            for step, k in collect_at.items():
                pl.when(i == step)(functools.partial(gr.collect, k, grad_acc))

        rs.middle(0, streams - 1)
        gr.spread(4)
        gr.relay(3, 1)
        gr.spread(5)
        gr.relay(3, 2)
        gr.relay(4, 1)
        gain_own[...] = jnp.zeros_like(gain_own)

        def last_norm(m):
            rs.total(m, total)
            grad_in, gain_grad = norm_back(x_own[m].astype(F32), gain_ref[...], total[...])
            out[0, m, t] = (one_ref[m] + grad_in).astype(BF)
            ag.start(m)
            gain_own[0:1] += gain_grad

        last_norm(0)
        gr.relay(4, 2)
        gr.relay(5, 1)
        gr.spread(6)
        last_norm(1)
        gr.relay(5, 2)
        gain_own[1:3] = gains_ref[...]
        gain_near[t] = gain_own[...]

        def near_copy(j, slot):
            return remote(gain_own, gain_near.at[slot], near_sem.at[0, j], near_sem.at[1, slot], {"tensor": j})

        for j in range(4):
            pl.when(t != j)(functools.partial(lambda j: near_copy(j, t).start(), j))
        gr.collect(2, grad_acc)
        gr.relay(6, 1)
        gr.collect(3, grad_acc)
        for m in range(streams):
            ag.pass_on(0, m)
        gr.relay(6, 2)
        gr.collect(4, grad_acc)
        for j in range(4):
            pl.when(t != j)(functools.partial(lambda j: near_copy(j, j).wait_recv(), j))
        gain_sum[...] = gain_near[0] + gain_near[1] + gain_near[2] + gain_near[3]
        me = p * seq_count + s

        def far_copy(j, slot):
            d, q = j // seq_count, j % seq_count
            return remote(
                gain_sum.at[:, q * rows : (q + 1) * rows], gain_far.at[slot], far_sem.at[0, j], far_sem.at[1, slot],
                {"dp": d, "seq": q},
            )

        gain_far[me] = gain_sum[:, pl.ds(pl.multiple_of(s * rows, LANES), rows)]
        for j in range(2 * seq_count):
            pl.when(me != j)(lambda: far_copy(j, me).start())
        gr.collect(5, grad_acc)
        rs.drain()
        for m in range(streams):
            ag.finish(0, m)
        gr.collect(6, grad_acc)
        for k in range(4):
            gr.finish(k)
            gr.drain(k)
        for j in range(2 * seq_count):
            pl.when(me != j)(lambda: far_copy(j, j).wait_recv())
        gain_out[...] = functools.reduce(jnp.add, [gain_far[j] for j in range(2 * seq_count)])
        for k in range(4, chunks):
            gr.finish(k)
            gr.drain(k)
        for j in range(4):
            pl.when(t != j)(lambda: near_copy(j, t).wait_send())
        for j in range(2 * seq_count):
            pl.when(me != j)(lambda: far_copy(j, me).wait_send())
        ag.drain()

    anywhere = pl.BlockSpec(memory_space=pl.ANY)
    return pl.pallas_call(
        kernel,
        name="tail",
        out_shape=(
            jax.ShapeDtypeStruct((1, streams, 4, quarter, width), BF),
            jax.ShapeDtypeStruct((count, rows, width), BF),
            jax.ShapeDtypeStruct((rows, width), BF),
            jax.ShapeDtypeStruct((gain_rows, rows), F32),
        ),
        in_specs=[anywhere if i in (1, 3, 6, 7) else spec for i, spec in enumerate(in_vmem(11))],
        out_specs=tuple(in_vmem(4)),
        scratch_shapes=[
            pltpu.VMEM(conv.shape, BF),
            pltpu.VMEM(filter_proj.shape, BF),
            pltpu.VMEM(strip_back.shape, BF),
            pltpu.VMEM((streams, quarter, width), BF),
            pltpu.SemaphoreType.DMA((count,)),
            pltpu.SemaphoreType.DMA((count,)),
            pltpu.SemaphoreType.DMA,
            pltpu.SemaphoreType.DMA,
            pltpu.VMEM((length + 8, 1), F32),
            pltpu.VMEM((length, length), BF),
            pltpu.VMEM((steps, length, 1), F32),
            pltpu.VMEM((length, count * length), BF),
            pltpu.VMEM((length, width), F32),
            pltpu.VMEM((seq_count, streams, 2, 2, quarter, width), BF),
            pltpu.VMEM((streams, count * length, width), BF),
            pltpu.VMEM((chunks, width, width), BF),
            pltpu.VMEM((streams, length + 8, channels), F32),
            pltpu.VMEM((quarter, width), F32),
            pltpu.VMEM((rows, width // 2), F32),
            AllGather.scratch(0, streams)[0],
            pltpu.VMEM((gain_rows, width), F32),
            pltpu.VMEM((4, gain_rows, width), F32),
            pltpu.VMEM((gain_rows, width), F32),
            pltpu.VMEM((2 * seq_count, gain_rows, rows), F32),
            pltpu.SemaphoreType.DMA((2, 4)),
            pltpu.SemaphoreType.DMA((2, 2 * seq_count)),
        ]
        + ReduceScatter.scratch(hops, streams, quarter, width)
        + GradReduce.scratch(seq_count, chunks, width, width),
        compiler_params=params(7),
    )(
        grad_stu, filter_proj, lag_proj, conv, lag_stack, ext_ids, strip_back, x, gain, grad_one, gains
    )


def write_out(layer_output, input_gradient, gains, filter_grad, lag_grad, sums, lag_order, channels, cols):
    _, streams, _, quarter, width = layer_output.shape
    rows, units = sums.shape[1:]
    count = filter_grad.shape[0]

    def kernel(
        layer_ref, input_ref, gains_ref, filter_ref, lag_ref, sums_ref,
        layer_out, input_out, stu_out, filter_out, lag_out, attn_out, q_out, k_out, v_out, o_out, feed_out, gate_out, up_out,
        down_out,
    ):
        layer_out[...] = layer_ref[0].reshape(streams, 1, 4 * quarter, width)
        input_out[...] = input_ref[0].reshape(streams, 1, 4 * quarter, width)
        filter_out[...] = filter_ref[...].astype(F32)
        for i, ref in enumerate((stu_out, attn_out, feed_out)):
            ref[...] = gains_ref[i : i + 1]
        for i in range(lag_order):
            lag_out[i] = jnp.transpose(lag_ref[:, i * channels : (i + 1) * channels].astype(F32))
        for i, ref in enumerate((q_out, k_out, v_out)):
            ref[...] = sums_ref[3, :, i * cols : (i + 1) * cols].astype(F32)
        o_out[...] = jnp.transpose(sums_ref[3, :, 3 * cols :].astype(F32))
        gate_out[...] = sums_ref[0].astype(F32)
        up_out[...] = sums_ref[1].astype(F32)
        down_out[...] = jnp.transpose(sums_ref[2].astype(F32))

    def out(*shape, kind=F32):
        return jax.ShapeDtypeStruct(shape, kind)

    shapes = (
        out(streams, 1, 4 * quarter, width, kind=BF),
        out(streams, 1, 4 * quarter, width, kind=BF),
        out(1, rows),
        out(count, rows, width),
        out(lag_order, channels, rows),
        out(1, rows),
        out(rows, cols),
        out(rows, cols),
        out(rows, cols),
        out(cols, rows),
        out(1, rows),
        out(rows, units),
        out(rows, units),
        out(units, rows),
    )
    results = pl.pallas_call(
        kernel,
        name="write_out",
        out_shape=shapes,
        in_specs=in_vmem(6),
        out_specs=tuple(in_vmem(len(shapes))),
        compiler_params=params(),
    )(layer_output, input_gradient, gains, filter_grad, lag_grad, sums)
    return tuple(r.reshape(rows) if r.shape == (1, rows) else r for r in results)


def gated_unit(gate_pre, up_pre):
    return jax.nn.gelu(gate_pre, approximate=True) * up_pre


def local(
    seq_count,
    tokens,
    document_index,
    filters,
    stu_gain,
    filter_proj,
    lag_proj,
    attention_gain,
    query_weight,
    key_weight,
    value_weight,
    output_weight,
    feed_gain,
    gate_weight,
    up_weight,
    down_weight,
    cotangent,
):
    streams, _, length, width = tokens.shape
    row_len = length * seq_count
    quarter = length // 4
    lag_order, channels = lag_proj.shape[:2]
    count = filters.shape[0]
    hops = WINDOW // length
    tensor_place = lax.axis_index("tensor")
    chan_start = tensor_place * channels

    def split(a):
        return a.reshape(a.shape[:-2] + (2, 2, quarter, width))

    def quarters(a):
        return a.reshape(a.shape[:-2] + (4, quarter, width))

    def whole(a):
        return a.reshape(a.shape[:-3] + (length, width))

    def row(gain):
        return gain.reshape(1, width)

    if width // seq_count % LANES == 0:
        rows = tokens.reshape(streams, 4, quarter, width)
        grad_stu, layer_output, grad_one, gain_grads, sums, lag_stack, ext_ids, conv, strip_back = head(
            rows, document_index, row(stu_gain), filter_proj, lag_proj, filters, row(attention_gain), row(feed_gain),
            query_weight, key_weight, value_weight, output_weight, gate_weight, up_weight, down_weight,
            cotangent.reshape(streams, length, width), seq_count,
        )
        input_gradient, filter_grad, lag_grad, gains = tail(
            grad_stu.reshape(streams * length, width), filter_proj, lag_proj, conv,
            lag_stack.reshape(lag_order, streams * length, channels), ext_ids, strip_back, rows, row(stu_gain), grad_one,
            gain_grads, seq_count,
        )
        return write_out(
            layer_output, input_gradient, gains, filter_grad, lag_grad, sums, lag_order, channels, query_weight.shape[1]
        )

    x = tokens[:, 0]
    grad_three = cotangent[:, 0]
    ids = document_index[:, 0]
    id_tile = ids.reshape(streams * length // LANES, LANES)
    pad = jnp.zeros((count, 4 * LANES), filters.dtype)
    ahead = row_len - LANES
    base = jnp.concatenate(
        [
            jnp.flip(filters[:, : ahead + 1], axis=1),
            pad[:, : 4 * LANES],
            jnp.flip(filters[:, ahead + 1 :], axis=1),
        ],
        axis=1,
    ).astype(F32)[:, None]
    base_back = jnp.concatenate(
        [pad[:, : length - LANES], filters, pad[:, :LANES]], axis=1
    ).astype(F32)[:, None]

    tokens_flat = streams * length
    cols = query_weight.shape[1]

    def answer(layer_output, input_gradient, gains, filter_grad, lag_grad, attn_grads, feed_grads):
        query_grad, key_grad, value_grad, output_grad = jnp.split(attn_grads, [cols, 2 * cols, 3 * cols], axis=1)
        gate_grad, up_grad, down_grad = feed_grads
        return (
            layer_output[:, None],
            input_gradient[:, None],
            gains[0],
            filter_grad,
            lag_grad[:, : lag_order * channels].T.reshape(lag_order, channels, -1),
            gains[1],
            query_grad,
            key_grad,
            value_grad,
            output_grad.T,
            gains[2],
            gate_grad,
            up_grad,
            down_grad.T,
        )

    inputs = norm_of(x.astype(F32), stu_gain).astype(BF)
    rows_ext, id_ext = gather_rows(quarters(inputs), id_tile, seq_count)
    rows_ext = whole(rows_ext)
    id_ext = id_ext.reshape(seq_count, streams, length)
    id_rows = id_ext[:, :, None, :]
    id_cols = id_ext[:, :, :, None]

    conv = convolve(rows_ext, id_rows, id_cols[0], base, seq_count)

    chan_rows = lax.dynamic_slice_in_dim(rows_ext[:2], chan_start, channels, 3)
    joined = jnp.concatenate([chan_rows[1][:, length - lag_order :], chan_rows[0]], axis=1)
    joined_ids = jnp.concatenate([id_ext[1][:, length - lag_order :], ids], axis=1)
    masks = []
    lagged = []
    for step in range(1, lag_order + 1):
        low = lag_order - step
        masks.append((joined_ids[:, low : low + length] == ids)[:, :, None])
        lagged.append(jnp.where(masks[-1], joined[:, low : low + length], jnp.zeros((), BF)))
    lag_stack = jnp.stack(lagged)

    mixed = jnp.einsum("kmtd,kde->mte", conv, filter_proj, preferred_element_type=F32)
    mixed = mixed + jnp.einsum("imtc,ice->mte", lag_stack, lag_proj, preferred_element_type=F32)

    state = jax.ShapeDtypeStruct((streams, quarter, width), F32)
    gain_state = jax.ShapeDtypeStruct((1, width), F32)

    def finish_one(m, total, others, extra):
        x_ref, gain_ref = others
        hidden = x_ref[m, place()[1]].astype(F32) + total
        extra[0][m] = hidden
        return norm_of(hidden, gain_ref[...]).astype(BF)

    attn_ext, hidden_one = exchange(
        "exchange_one", 2, seq_count, [split(mixed.astype(BF))[None]], [quarters(x), row(attention_gain)], 0, hops,
        finish_one, [state],
    )
    attn_ext = whole(attn_ext)

    q, k, v, attended, lse, out_part = attend(
        attn_ext, id_rows[: hops + 1], id_cols[0], query_weight, key_weight, value_weight, output_weight
    )

    def finish_two(m, total, others, extra):
        hidden_ref, gain_ref = others
        hidden = hidden_ref[m] + total
        extra[0][m] = hidden
        return norm_of(hidden, gain_ref[...]).astype(BF)

    feed_in, hidden_two = exchange(
        "exchange_two", 3, seq_count, [split(out_part)[None]], [hidden_one, row(feed_gain)], 0, 0, finish_two, [state]
    )
    feed_in = whole(feed_in)[0].reshape(streams * length, width)
    flat_three = grad_three.reshape(streams * length, width)

    gate_pre = dot_nn(feed_in, gate_weight)
    up_pre = dot_nn(feed_in, up_weight)
    grad_inner = dot_nt(flat_three, down_weight)
    unit, pull = jax.vjp(gated_unit, gate_pre, up_pre)
    inner = unit.astype(BF)
    grad_gate, grad_up = pull(grad_inner)
    grad_gate = grad_gate.astype(BF)
    grad_up = grad_up.astype(BF)
    layer_part = dot_nn(inner, down_weight).astype(BF)
    feed_part = (dot_nt(grad_gate, gate_weight) + dot_nt(grad_up, up_weight)).astype(BF)

    def finish_three(m, total, others, extra):
        hidden_ref, gain_ref, cot_ref = others
        if m >= streams:
            return (hidden_ref[m - streams] + total).astype(BF)
        grad_in, gain_grad = norm_back(hidden_ref[m], gain_ref[...], total)
        grad_two = cot_ref[m, place()[1]].astype(F32) + grad_in
        extra[0][m] = grad_two
        extra[1][...] = gain_grad if m == 0 else extra[1][...] + gain_grad
        return grad_two.astype(BF)

    feed_grads = jnp.stack(
        [
            dot_tn(feed_in, grad_gate).astype(BF),
            dot_tn(feed_in, grad_up).astype(BF),
            dot_tn(flat_three, inner).astype(BF),
        ]
    )
    shape = (1, streams, length, width)
    both, grad_two, feed_gain_grad = exchange(
        "exchange_three", 4, seq_count, [split(feed_part.reshape(shape)), split(layer_part.reshape(shape))],
        [hidden_two, row(feed_gain), quarters(grad_three)], 0, 0, finish_three, [state, gain_state],
    )
    both = whole(both)[0]
    grad_att_out = both[:streams]
    layer_output = both[streams:]

    dq, dk, dv, attn_part = attend_back(
        q, k, v, lse, grad_att_out, id_rows[: hops + 1], id_cols[0], query_weight, key_weight, value_weight, output_weight
    )

    go = grad_att_out.reshape(tokens_flat, width)
    attn_grads = jnp.concatenate(
        [
            dot_tn(attn_ext[0].reshape(tokens_flat, width), dq.reshape(tokens_flat, -1)).astype(BF),
            dot_tn(attn_ext.reshape(-1, width), dk.reshape(-1, dk.shape[-1])).astype(BF),
            dot_tn(attn_ext.reshape(-1, width), dv.reshape(-1, dv.shape[-1])).astype(BF),
            dot_tn(go, attended.reshape(tokens_flat, -1)).astype(BF),
        ],
        axis=1,
    )

    def finish_four(m, total, others, extra):
        hidden_ref, gain_ref, grad_ref = others
        grad_in, gain_grad = norm_back(hidden_ref[m], gain_ref[...], total)
        grad_one = grad_ref[m] + grad_in
        extra[0][m] = grad_one
        extra[1][...] = gain_grad if m == 0 else extra[1][...] + gain_grad
        return grad_one.astype(BF)

    grad_stu, grad_one, attn_gain_grad = exchange(
        "exchange_four", 5, seq_count, [split(attn_part)], [hidden_one, row(attention_gain), grad_two], hops, 0,
        finish_four, [state, gain_state],
    )
    grad_stu = whole(grad_stu)[0]
    grad_conv = jnp.einsum("mte,kde->kmtd", grad_stu, filter_proj, preferred_element_type=F32).astype(BF)
    grad_lagged = jnp.einsum("mte,ice->imtc", grad_stu, lag_proj, preferred_element_type=F32)
    ext_grad = jnp.zeros((streams, 8 + length, channels), F32)
    for step in range(1, lag_order + 1):
        term = jnp.where(masks[step - 1], grad_lagged[step - 1], 0.0)
        ext_grad = ext_grad + jnp.pad(term, ((0, 0), (8 - step, step), (0, 0)))
    terms = convolve_back(
        grad_conv, id_rows[0], id_cols, base_back, ext_grad[:, 8:], ext_grad[:, :8], seq_count
    )

    def finish_five(m, total, others, extra):
        x_ref, gain_ref, grad_ref = others
        grad_in, gain_grad = norm_back(x_ref[m, place()[1]].astype(F32), gain_ref[...], total)
        extra[0][...] = gain_grad if m == 0 else extra[0][...] + gain_grad
        return (grad_ref[m] + grad_in).astype(BF)

    input_gradient, stu_gain_grad = exchange(
        "exchange_five", 6, seq_count, [split(terms)], [quarters(x), row(stu_gain), grad_one], seq_count - 1, 0,
        finish_five, [gain_state],
    )
    input_gradient = whole(input_gradient)[0]
    stu = grad_stu.reshape(tokens_flat, width)
    filter_part = jnp.einsum("kmtd,mte->kde", conv, grad_stu, preferred_element_type=F32).astype(BF)
    lag_part = jnp.concatenate(
        [dot_tn(stu, lag_stack[i].reshape(tokens_flat, channels)).astype(BF) for i in range(lag_order)], axis=1
    )
    feed_grads = lax.psum(
        lax.psum_scatter(feed_grads, "seq", scatter_dimension=1, tiled=True), "dp"
    ).astype(F32)
    attn_grads = lax.psum(lax.psum_scatter(attn_grads, "seq", scatter_dimension=0, tiled=True), "dp").astype(F32)
    filter_grad = lax.psum(
        lax.psum_scatter(filter_part, "seq", scatter_dimension=1, tiled=True), "dp"
    ).astype(F32)
    lag_grad = lax.psum(lax.psum_scatter(lag_part, "seq", scatter_dimension=0, tiled=True), "dp").astype(F32)
    gains = jnp.concatenate([stu_gain_grad, attn_gain_grad, feed_gain_grad], axis=0)
    gains = lax.psum(gains, ("dp", "seq", "tensor"))
    gain_width = width // seq_count
    gains = lax.dynamic_slice_in_dim(gains, lax.axis_index("seq") * gain_width, gain_width, 1)
    return answer(layer_output, input_gradient, gains, filter_grad, lag_grad, attn_grads, feed_grads)


def solution(mesh):
    return jax.shard_map(
        functools.partial(local, mesh.shape["seq"]),
        mesh=mesh,
        in_specs=(
            P(None, "dp", "seq", None),
            P(None, "dp", "seq"),
            P("tensor", None),
            P(),
            P("tensor", None, None),
            P(None, "tensor", None),
            P(),
            P(None, "tensor"),
            P(None, "tensor"),
            P(None, "tensor"),
            P("tensor", None),
            P(),
            P(None, "tensor"),
            P(None, "tensor"),
            P("tensor", None),
            P(None, "dp", "seq", None),
        ),
        out_specs=(
            P(None, "dp", "seq", None),
            P(None, "dp", "seq", None),
            P("seq"),
            P("tensor", "seq", None),
            P(None, "tensor", "seq"),
            P("seq"),
            P("seq", "tensor"),
            P("seq", "tensor"),
            P("seq", "tensor"),
            P("tensor", "seq"),
            P("seq"),
            P("seq", "tensor"),
            P("seq", "tensor"),
            P("tensor", "seq"),
        ),
        check_vma=False,
    )
```

```python
import functools

import jax
import jax.numpy as jnp
from jax import lax
from jax.experimental import pallas as pl
from jax.experimental.pallas import tpu as pltpu
from jax.sharding import PartitionSpec as P

HD = 64
WINDOW = 1024
EPSILON = 1e-05
LANES = 128
NEGATIVE = -1e30
MESH = pl.DeviceIdType.MESH
BF = jnp.bfloat16
F32 = jnp.float32
VMEM_LIMIT = 63 * 1024 * 1024


def place():
    s = lax.axis_index("seq")
    t = lax.axis_index("tensor")
    y = t // 2
    c = t - 2 * y
    return s, t, y, c, t + 1 - 2 * c, t + 2 - 4 * y


def when(condition, action):
    if condition is True:
        action()
    else:
        pl.when(condition)(action)


def remote(src, dst, send_sem, recv_sem, device):
    return pltpu.make_async_remote_copy(
        src_ref=src, dst_ref=dst, send_sem=send_sem, recv_sem=recv_sem, device_id=device, device_id_type=MESH
    )


def greet(seq_count, hops, wide=False, gains=False):
    s, t, y, c, core, far = place()
    barrier = pltpu.get_barrier_semaphore()

    def signal(device):
        pl.semaphore_signal(barrier, inc=1, device_id=device, device_id_type=MESH)

    signal({"tensor": core})
    signal({"tensor": far})
    if gains:
        signal({"tensor": 3 - t})
    if wide:
        p = lax.axis_index("dp")
        signal({"dp": 1 - p})
        for j in range(seq_count):

            @pl.when(s != j)
            def _():
                signal({"seq": j})
                if gains:
                    signal({"dp": 1 - p, "seq": j})

        peers = 2 + gains + 1 + (seq_count - 1) * (1 + gains)
    else:
        for h in range(1, hops + 1):
            for there, peer in ((s - h >= 0, s - h), (s + h < seq_count, s + h)):

                @pl.when(there)
                def _():
                    signal({"seq": peer})

        peers = 2 + jnp.minimum(s, hops) + jnp.minimum(seq_count - 1 - s, hops)
    pl.semaphore_wait(barrier, peers)


class ReduceScatter:
    def __init__(self, seq_count, hops, streams, part, scratch):
        self.seq_count, self.hops, self.streams, self.part = seq_count, hops, streams, part
        self.near, self.half, self.over, self.hop_out, self.hop_in, self.sem = scratch
        self.pieces, self.rows = self.half.shape[2:4]

    @staticmethod
    def scratch(hops, streams, rows, width, pieces=1):
        quarter = (hops + 1, streams, pieces, rows // pieces, width)
        over_seq = quarter if hops else (1, 1, 1, 16, LANES)
        return [
            pltpu.VMEM((hops + 1, streams, pieces, 2, rows // pieces, width), BF),
            pltpu.VMEM(quarter, BF),
            pltpu.VMEM(quarter, BF),
            pltpu.VMEM(over_seq, BF),
            pltpu.VMEM(over_seq, BF),
            pltpu.SemaphoreType.DMA((6, hops + 1, streams, pieces)),
        ]

    def span(self, n):
        return slice(n * self.rows, (n + 1) * self.rows)

    def move(self, kind, source, target, h, m, n, device, at=None):
        at = h if at is None else at
        return remote(source, target, self.sem.at[2 * kind, h, m, n], self.sem.at[2 * kind + 1, at, m, n], device)

    def to_core(self, h, m, n):
        s, t, y, c, core, far = place()
        source = self.part(h, m).at[:, 1 - c, pl.ds(n * self.rows, self.rows)]
        return self.move(0, source, self.near.at[h, m, n], h, m, n, {"tensor": core})

    def to_far(self, h, m, n):
        far = place()[5]
        return self.move(1, self.half.at[h, m, n], self.over.at[h, m, n], h, m, n, {"tensor": far})

    def to_hop(self, h, m, n):
        peer = {"seq": lax.axis_index("seq") - 1}
        return self.move(2, self.hop_out.at[h, m, n], self.hop_in.at[h - 1, m, n], h, m, n, peer, at=h - 1)

    def add_hop(self, h, m, acc):
        s = lax.axis_index("seq")

        @pl.when(s + 1 < self.seq_count)
        def _():
            for n in range(self.pieces):
                ref = self.hop_in.at[h, m, n]
                self.move(2, self.hop_out.at[h, m, n], ref, h, m, n, {"seq": s + 1}).wait_recv()
                acc[self.span(n)] += self.hop_in[h, m, n].astype(F32)

    def there(self, h):
        return True if isinstance(h, int) and h == 0 else lax.axis_index("seq") - h >= 0

    def order(self):
        return [(h, m) for h in range(self.hops, -1, -1) for m in range(self.streams)]

    def start(self, h, m):
        def act():
            for n in range(self.pieces):
                self.to_core(h, m, n).start()

        when(self.there(h), act)

    def middle(self, h, m):
        s, t, y, c, core, far = place()

        def act():
            for n in range(self.pieces):
                self.to_core(h, m, n).wait_recv()
                mine = self.part(h, m)[1 - y, c, self.span(n)].astype(F32) + self.near[h, m, n, 1 - y].astype(F32)
                self.half[h, m, n] = mine.astype(BF)
                self.to_far(h, m, n).start()

        when(self.there(h), act)

    def own(self, h, m, acc):
        s, t, y, c, core, far = place()
        for n in range(self.pieces):
            self.to_far(h, m, n).wait_recv()
            mine = self.part(h, m)[y, c, self.span(n)].astype(F32) + self.near[h, m, n, y].astype(F32)
            acc[self.span(n)] = mine + self.over[h, m, n].astype(F32)

    def hop(self, h, m, acc):
        def act():
            self.own(h, m, acc)
            if isinstance(h, int):
                if h < self.hops:
                    self.add_hop(h, m, acc)
            else:
                pl.when(h < self.hops)(lambda: self.add_hop(h, m, acc))
            for n in range(self.pieces):
                self.hop_out[h, m, n] = acc[self.span(n)].astype(BF)
                self.to_hop(h, m, n).start()

        when(self.there(h), act)

    def total(self, m, acc):
        self.own(0, m, acc)
        if self.hops:
            self.add_hop(0, m, acc)

    def drain(self):
        for h, m in self.order():

            def act():
                for n in range(self.pieces):
                    self.to_core(h, m, n).wait_send()
                    self.to_far(h, m, n).wait_send()
                    if h:
                        self.to_hop(h, m, n).wait_send()

            when(self.there(h), act)


class AllGather:
    def __init__(self, seq_count, hops, streams, at, sem, first=0):
        self.seq_count, self.hops, self.streams, self.sem, self.first = seq_count, hops, streams, sem, first
        self.at = at if callable(at) else lambda h, m, quarter: at.at[h, m, quarter]
        self.pieces = sem.shape[3]

    @staticmethod
    def scratch(hops, streams, pieces=1):
        return [pltpu.SemaphoreType.DMA((8, hops + 1, streams, pieces))]

    def there(self, h):
        return True if h == 0 else lax.axis_index("seq") - h >= 0

    def piece(self, h, m, quarter, n):
        ref = self.at(h, m, quarter)
        rows = ref.shape[0] // self.pieces
        return ref.at[pl.ds(n * rows, rows)]

    def copy(self, kind, h, m, quarter, n, device):
        ref = self.piece(h, m, quarter, n)
        return remote(ref, ref, self.sem.at[2 * kind, h, m, n], self.sem.at[2 * kind + 1, h, m, n], device)

    def relay(self, h, m, n):
        s, t = lax.axis_index("seq"), place()[1]
        return remote(
            self.piece(h, m, t, n),
            self.piece(h + 1, m, t, n),
            self.sem.at[0, h, m, n],
            self.sem.at[1, h + 1, m, n],
            {"seq": s + 1},
        )

    def relays(self, h):
        s = lax.axis_index("seq")
        return (s - h >= 0) & (s + 1 < self.seq_count)

    def forward(self, h, m, n):
        if h < self.hops:
            pl.when(self.relays(h))(lambda: self.relay(h, m, n).start())

    def spread(self, h, m, n):
        s, t, y, c, core, far = place()
        self.copy(1, h, m, t, n, {"tensor": far}).start()
        self.copy(2, h, m, t, n, {"tensor": core}).start()

    def start(self, m):
        for n in range(self.pieces):
            self.forward(0, m, n)
            if self.first == 0:
                self.spread(0, m, n)

    def arrive(self, h, m):
        @pl.when(self.there(h))
        def _():
            for n in range(self.pieces):
                self.copy(0, h, m, place()[1], n, {"seq": lax.axis_index("seq") - 1}).wait_recv()
                self.forward(h, m, n)
                self.spread(h, m, n)

    def pass_on(self, h, m):
        s, t, y, c, core, far = place()

        def act():
            for n in range(self.pieces):
                self.copy(1, h, m, far, n, {"tensor": far}).wait_recv()
                self.copy(3, h, m, far, n, {"tensor": core}).start()

        when(self.there(h), act)

    def finish(self, h, m):
        s, t, y, c, core, far = place()

        def act():
            for n in range(self.pieces):
                self.copy(2, h, m, core, n, {"tensor": core}).wait_recv()
                self.copy(3, h, m, 3 - t, n, {"tensor": core}).wait_recv()

        when(self.there(h), act)

    def clear(self, h, m):
        @pl.when(lax.axis_index("seq") - h < 0)
        def _():
            for quarter in range(4):
                ref = self.at(h, m, quarter)
                ref[...] = jnp.zeros(ref.shape, ref.dtype)

    def drain(self):
        s, t, y, c, core, far = place()
        for m in range(self.streams):
            for n in range(self.pieces):
                for h in range(self.hops):
                    pl.when(self.relays(h))(functools.partial(lambda h, m, n: self.relay(h, m, n).wait_send(), h, m, n))
                for h in range(self.first, self.hops + 1):

                    def act():
                        self.copy(1, h, m, t, n, {"tensor": far}).wait_send()
                        self.copy(2, h, m, t, n, {"tensor": core}).wait_send()
                        self.copy(3, h, m, far, n, {"tensor": core}).wait_send()

                    when(self.there(h), act)


class GradReduce:
    def __init__(self, seq_count, source, result, scratch):
        self.seq_count, self.source, self.result = seq_count, source, result
        self.x_in, self.z_out, self.z_in, self.back_out, self.back_in, self.x_sem, self.z_sem, self.back_sem = scratch
        self.half = self.x_in.shape[2]
        self.rows = self.back_out.shape[1]

    @staticmethod
    def scratch(seq_count, chunks, depth, width):
        rows, half = depth // seq_count, width // 2
        return [
            pltpu.VMEM((chunks, depth, half), BF),
            pltpu.VMEM((chunks, depth, half), BF),
            pltpu.VMEM((chunks, seq_count + 1, rows, half), BF),
            pltpu.VMEM((chunks, rows, half), BF),
            pltpu.VMEM((chunks, rows, half), BF),
            pltpu.SemaphoreType.DMA((2, chunks)),
            pltpu.SemaphoreType.DMA((2, chunks, seq_count + 1)),
            pltpu.SemaphoreType.DMA((2, chunks)),
        ]

    def columns(self, p):
        return pl.ds(pl.multiple_of(p * self.half, LANES), self.half)

    def block(self, j):
        return pl.ds(pl.multiple_of(j * self.rows, 16), self.rows)

    def over(self, c):
        p = lax.axis_index("dp")
        return remote(
            self.source(c).at[:, self.columns(1 - p)], self.x_in.at[c], self.x_sem.at[0, c], self.x_sem.at[1, c], {"dp": 1 - p}
        )

    def row_copy(self, c, s, j):
        peer = s + 1 if j > s else s - 1
        slot = self.seq_count if j == peer and j < s else j
        rows = self.z_out.at[c, j * self.rows : (j + 1) * self.rows]
        return remote(rows, self.z_in.at[c, slot], self.z_sem.at[0, c, j], self.z_sem.at[1, c, slot], {"seq": peer})

    def arrival(self, c, slot, peer):
        ref = self.z_in.at[c, slot]
        return remote(ref, ref, self.z_sem.at[0, c, slot], self.z_sem.at[1, c, slot], {"seq": peer})

    def back(self, c):
        p = lax.axis_index("dp")
        return remote(
            self.back_out.at[c], self.back_in.at[c], self.back_sem.at[0, c], self.back_sem.at[1, c], {"dp": 1 - p}
        )

    def start(self, c):
        self.over(c).start()

    def spread(self, c):
        p = lax.axis_index("dp")
        self.over(c).wait_recv()
        mine = self.source(c)[:, self.columns(p)].astype(F32) + self.x_in[c].astype(F32)
        self.z_out[c] = mine.astype(BF)
        last = self.seq_count - 1
        for s in {0, last}:

            @pl.when(lax.axis_index("seq") == s)
            def _():
                for j in range(self.seq_count):
                    if j != s:
                        self.row_copy(c, s, j).start()

    def relay(self, c, d):
        for right in (True, False):
            s = d if right else self.seq_count - 1 - d
            targets = range(s + 1, self.seq_count) if right else range(s)

            @pl.when(lax.axis_index("seq") == s)
            def _():
                for j in targets:
                    self.arrival(c, j, s - 1 if right else s + 1).wait_recv()
                    rows = slice(j * self.rows, (j + 1) * self.rows)
                    added = self.z_out[c, rows].astype(F32) + self.z_in[c, j].astype(F32)
                    self.z_out[c, rows] = added.astype(BF)
                    self.row_copy(c, s, j).start()

    def collect(self, c, acc):
        s, p = lax.axis_index("seq"), lax.axis_index("dp")
        here = self.block(s)
        acc[...] = self.source(c)[here, self.columns(p)].astype(F32) + self.x_in[c, here].astype(F32)
        for n in range(self.seq_count):

            @pl.when(s == n)
            def _():
                for there, slot, peer in ((n > 0, n, n - 1), (n + 1 < self.seq_count, self.seq_count, n + 1)):
                    if there:
                        self.arrival(c, slot, peer).wait_recv()
                        acc[...] += self.z_in[c, slot].astype(F32)

        self.back_out[c] = acc[...].astype(BF)
        self.back(c).start()

    def finish(self, c):
        p = lax.axis_index("dp")
        self.back(c).wait_recv()
        self.result(c)[:, self.columns(p)] = self.back_out[c]
        self.result(c)[:, self.columns(1 - p)] = self.back_in[c]

    def drain(self, c):
        self.over(c).wait_send()
        for s in range(self.seq_count):

            @pl.when(lax.axis_index("seq") == s)
            def _():
                for j in range(self.seq_count):
                    if j != s:
                        self.row_copy(c, s, j).wait_send()

        self.back(c).wait_send()


def params(cid=None):
    if cid is None:
        return pltpu.CompilerParams(vmem_limit_bytes=VMEM_LIMIT)
    return pltpu.CompilerParams(vmem_limit_bytes=VMEM_LIMIT, collective_id=cid, has_side_effects=True)


def in_vmem(count):
    return [pl.BlockSpec(memory_space=pltpu.VMEM)] * count


def gather_rows(inputs, ids, seq_count):
    streams, quarters, rows, width = inputs.shape
    hops = seq_count - 1

    def kernel(x_ref, id_ref, out, out_ids, sem, id_sem):
        s, t, y, c, core, far = place()
        greet(seq_count, hops)
        out[0] = x_ref[...]
        out_ids[0] = id_ref[...]
        ag = AllGather(seq_count, hops, streams, out, sem, first=1)

        def id_copy(h, peer):
            return remote(id_ref, out_ids.at[h], id_sem.at[0, h], id_sem.at[1, h], {"seq": peer})

        for h in range(1, hops + 1):

            @pl.when(s + h < seq_count)
            def _():
                id_copy(h, s + h).start()

        for m in range(streams):
            ag.start(m)
        for h in range(1, hops + 1):
            for m in range(streams):
                ag.clear(h, m)

            @pl.when(s - h < 0)
            def _():
                out_ids[h] = jnp.full(out_ids.shape[1:], -1, jnp.int32)

        for m in range(streams):
            for h in range(1, hops + 1):
                ag.arrive(h, m)
        for m in range(streams):
            for h in range(1, hops + 1):
                ag.pass_on(h, m)
        for h in range(1, hops + 1):
            for m in range(streams):
                ag.finish(h, m)

            @pl.when(s - h >= 0)
            def _():
                id_copy(h, s - h).wait_recv()

            @pl.when(s + h < seq_count)
            def _():
                id_copy(h, s + h).wait_send()

        ag.drain()

    return pl.pallas_call(
        kernel,
        name="gather_rows",
        out_shape=(
            jax.ShapeDtypeStruct((seq_count,) + inputs.shape, inputs.dtype),
            jax.ShapeDtypeStruct((seq_count,) + ids.shape, jnp.int32),
        ),
        in_specs=in_vmem(2),
        out_specs=tuple(in_vmem(2)),
        scratch_shapes=AllGather.scratch(hops, streams) + [pltpu.SemaphoreType.DMA((2, seq_count))],
        compiler_params=params(1),
    )(inputs, ids)


def exchange(name, cid, seq_count, parts, others, reduce_hops, gather_hops, finish, extra):
    per_part = parts[0].shape[1]
    rows, width = parts[0].shape[4:]
    streams = per_part * len(parts)
    hops = max(reduce_hops, gather_hops)

    def kernel(*refs):
        refs = list(refs)
        part_refs = [refs.pop(0) for _ in parts]
        other_refs = [refs.pop(0) for _ in others]
        out = refs.pop(0)
        extra_refs = [refs.pop(0) for _ in extra]
        acc = refs.pop(0)
        gather_sem = refs.pop(0)
        s, t, y, c, core, far = place()
        greet(seq_count, hops)
        rs = ReduceScatter(
            seq_count, reduce_hops, streams, lambda h, m: part_refs[m // per_part].at[h, m % per_part], refs
        )
        ag = AllGather(seq_count, gather_hops, streams, out, gather_sem)
        for h, m in rs.order():
            rs.start(h, m)
        for h in range(1, gather_hops + 1):
            for m in range(streams):
                ag.clear(h, m)
        for h, m in rs.order():
            rs.middle(h, m)
        for h, m in rs.order():
            if h:
                rs.hop(h, m, acc)
        for m in range(streams):
            rs.total(m, acc)
            out[0, m, t] = finish(m, acc[...], other_refs, extra_refs)
            ag.start(m)
        for m in range(streams):
            ag.pass_on(0, m)
            for h in range(1, gather_hops + 1):
                ag.arrive(h, m)
        for m in range(streams):
            for h in range(1, gather_hops + 1):
                ag.pass_on(h, m)
        for h in range(gather_hops + 1):
            for m in range(streams):
                ag.finish(h, m)
        rs.drain()
        ag.drain()

    return pl.pallas_call(
        kernel,
        name=name,
        out_shape=(jax.ShapeDtypeStruct((gather_hops + 1, streams, 4, rows, width), BF),) + tuple(extra),
        in_specs=in_vmem(len(parts) + len(others)),
        out_specs=tuple(in_vmem(1 + len(extra))),
        scratch_shapes=[pltpu.VMEM((rows, width), F32)]
        + AllGather.scratch(gather_hops, streams)
        + ReduceScatter.scratch(reduce_hops, streams, rows, width),
        compiler_params=params(cid),
    )(*parts, *others)


def norm_of(values, gain_row):
    inverse = lax.rsqrt(jnp.mean(values * values, axis=-1, keepdims=True) + EPSILON)
    return values * inverse * gain_row


def norm_back(values, gain_row, grad_out):
    inverse = lax.rsqrt(jnp.mean(values * values, axis=-1, keepdims=True) + EPSILON)
    scaled = grad_out * gain_row
    dot = jnp.mean(scaled * values, axis=-1, keepdims=True)
    grad_in = inverse * scaled - values * (inverse * inverse * inverse) * dot
    return grad_in, jnp.sum(grad_out * values * inverse, axis=0, keepdims=True)


def strips(base_ref, strip):
    @pl.loop(0, base_ref.shape[0])
    def _(k):
        taps = base_ref[k] if len(base_ref.shape) == 3 else base_ref[pl.ds(k, 1)]
        row = jnp.broadcast_to(taps, strip.shape[1:])
        strip[k] = pltpu.roll(row, 0, 1, stride=1, stride_axis=0).astype(BF)


def lay_taps(taps_ref, base_ref, back):
    count, length = taps_ref.shape
    blocks = length // LANES
    base_ref[...] = jnp.zeros_like(base_ref)
    if back:
        base_ref[:, 3 * LANES : 3 * LANES + length] = taps_ref[...].astype(F32)
        return
    row = lax.broadcasted_iota(jnp.int32, (LANES, LANES), 0)
    lane = lax.broadcasted_iota(jnp.int32, (LANES, LANES), 1)
    turn = jnp.where(row + lane == LANES, 1.0, 0.0).astype(BF)
    first = lax.broadcasted_iota(jnp.int32, (count, LANES), 1) == 0
    turned = [dot_nn(taps_ref[:, j * LANES : (j + 1) * LANES], turn) for j in range(blocks)]
    for b in range(blocks):
        j = blocks - 1 - b
        below = turned[j - 1] if j else jnp.zeros((count, LANES), F32)
        taps = taps_ref[:, j * LANES : (j + 1) * LANES].astype(F32)
        base_ref[:, b * LANES : (b + 1) * LANES] = jnp.where(first, taps, below)
    base_ref[:, (blocks + 3) * LANES :] = turned[blocks - 1]


def convolve(rows, row_ids, col_ids, base, seq_count):
    _, streams, length, width = rows.shape
    count, _, wide = base.shape
    blocks = length // LANES
    at_once = seq_count <= 4

    def whole_kernel(x_ref, row_ref, col_ref, base_ref, out_ref, strip, mask, left):
        strips(base_ref, strip)

        @pl.loop(0, streams)
        def _(m):
            for h in range(seq_count):
                mask[:, h * length : (h + 1) * length] = jnp.where(col_ref[m] == row_ref[h, m], 1.0, 0.0).astype(BF)
            right = jnp.concatenate([x_ref[h, m] for h in range(seq_count)], axis=0)

            @pl.loop(0, count)
            def _(k):
                for a in range(blocks):
                    for h in range(seq_count):
                        start = LANES * (blocks * (seq_count - h) - 1 - a)
                        down, across = slice(a * LANES, (a + 1) * LANES), slice(h * length, (h + 1) * length)
                        left[down, across] = strip[k, :, start : start + length] * mask[down, across]
                out_ref[k, m] = jnp.dot(left[...], right, preferred_element_type=F32).astype(BF)

    def kernel(x_ref, row_ref, col_ref, base_ref, out_ref, strip, mask, acc):
        strips(base_ref, strip)
        s = lax.axis_index("seq")

        @pl.loop(0, streams)
        def _(m):
            acc[...] = jnp.zeros_like(acc)

            @pl.loop(0, s + 1)
            def _(h):
                mask[...] = jnp.where(col_ref[m] == row_ref[h, m], 1.0, 0.0).astype(BF)

                @pl.loop(0, count)
                def _(k):
                    pieces = []
                    for a in range(blocks):
                        start = pl.multiple_of(LANES * (blocks * (seq_count - h) - 1 - a), LANES)
                        pieces.append(strip[k, :, pl.ds(start, length)] * mask[a * LANES : (a + 1) * LANES])
                    acc[k] += jnp.dot(jnp.concatenate(pieces, axis=0), x_ref[h, m], preferred_element_type=F32)

            @pl.loop(0, count)
            def _(k):
                out_ref[k, m] = acc[k].astype(BF)

    span = seq_count * length if at_once else length
    return pl.pallas_call(
        whole_kernel if at_once else kernel,
        name="convolve",
        out_shape=jax.ShapeDtypeStruct((count, streams, length, width), BF),
        in_specs=in_vmem(4),
        out_specs=in_vmem(1)[0],
        scratch_shapes=[
            pltpu.VMEM((count, LANES, wide), BF),
            pltpu.VMEM((length, span), BF),
            pltpu.VMEM((length, span), BF) if at_once else pltpu.VMEM((count, length, width), F32),
        ],
        compiler_params=params(),
    )(rows, row_ids, col_ids, base)


def convolve_back(grads, row_ids, col_ids, base, own_lag, tail_lag, seq_count):
    count, streams, length, width = grads.shape
    wide = base.shape[2]
    blocks = length // LANES
    channels = own_lag.shape[2]
    tail_rows = tail_lag.shape[1]

    def kernel(g_ref, row_ref, col_ref, base_ref, own_ref, tail_ref, out_ref, strip, mask, acc):
        strips(base_ref, strip)
        s = lax.axis_index("seq")
        mine = pl.ds(pl.multiple_of(lax.axis_index("tensor") * channels, LANES), channels)

        @pl.loop(0, s + 1)
        def _(h):
            @pl.loop(0, streams)
            def _(m):
                mask[...] = jnp.where(col_ref[h, m] == row_ref[m], 1.0, 0.0).astype(BF)
                acc[...] = jnp.zeros_like(acc)

                @pl.when(h == 0)
                def _():
                    acc[:, mine] = own_ref[m]

                @pl.when(h == 1)
                def _():
                    acc[length - tail_rows :, mine] = tail_ref[m]

                @pl.loop(0, count)
                def _(k):
                    pieces = []
                    for a in range(blocks):
                        start = pl.multiple_of(LANES * (blocks * h + blocks - 1 - a), LANES)
                        pieces.append(strip[k, :, pl.ds(start, length)] * mask[a * LANES : (a + 1) * LANES])
                    acc[...] += jnp.dot(jnp.concatenate(pieces, axis=0), g_ref[k, m], preferred_element_type=F32)

                out_ref[h, m] = acc[...].astype(BF)

    return pl.pallas_call(
        kernel,
        name="convolve_back",
        out_shape=jax.ShapeDtypeStruct((seq_count, streams, length, width), BF),
        in_specs=in_vmem(6),
        out_specs=in_vmem(1)[0],
        scratch_shapes=[
            pltpu.VMEM((count, LANES, wide), BF),
            pltpu.VMEM((length, length), BF),
            pltpu.VMEM((length, width), F32),
        ],
        compiler_params=params(),
    )(grads, row_ids, col_ids, base, own_lag, tail_lag)


def dot_nn(a, b):
    return jnp.dot(a, b, preferred_element_type=F32)


def dot_nt(a, b):
    return lax.dot_general(a, b, (((1,), (1,)), ((), ())), preferred_element_type=F32)


def dot_tn(a, b):
    return lax.dot_general(a, b, (((0,), (0,)), ((), ())), preferred_element_type=F32)


def allowed_keys(query_ids, key_ids, first_row, distance):
    shape = (query_ids.shape[0], key_ids.shape[1])
    offset = lax.broadcasted_iota(jnp.int32, shape, 0) - lax.broadcasted_iota(jnp.int32, shape, 1) + (first_row + distance)
    return (query_ids == key_ids) & (offset >= 0) & (offset < WINDOW)


def one_head(block, head):
    lane = lax.broadcasted_iota(jnp.int32, block.shape, 1)
    return jnp.where((lane >= head * HD) & (lane < (head + 1) * HD), block, jnp.zeros_like(block))


def attend(rows, row_ids, col_ids, wq, wk, wv, wo):
    spans, streams, length, width = rows.shape
    cols = wq.shape[1]
    heads = cols // HD
    tile = min(256, length)
    scale = HD ** (-0.5)

    def kernel(x_ref, row_ref, col_ref, wq_ref, wk_ref, wv_ref, wo_ref, q_ref, k_ref, v_ref, a_ref, lse_ref, p_ref):
        @pl.loop(0, streams)
        def _(m):
            q_ref[m] = dot_nn(x_ref[0, m], wq_ref[...]).astype(BF)
            for h in range(spans):
                k_ref[h, m] = dot_nn(x_ref[h, m], wk_ref[...]).astype(BF)
                v_ref[h, m] = dot_nn(x_ref[h, m], wv_ref[...]).astype(BF)

            @pl.loop(0, length // tile)
            def _(i):
                first = pl.multiple_of(i * tile, tile)
                here = pl.ds(first, tile)
                masks = [allowed_keys(col_ref[m, here], row_ref[h, m], first, h * length) for h in range(spans)]
                block = q_ref[m, here]
                result = jnp.zeros((tile, cols), F32)
                for head in range(heads):
                    query = one_head(block, head)
                    scores = [
                        jnp.where(masks[h], dot_nt(query, k_ref[h, m]) * scale, NEGATIVE) for h in range(spans)
                    ]
                    peak = functools.reduce(jnp.maximum, [jnp.max(v, axis=-1, keepdims=True) for v in scores])
                    raised = [jnp.exp(v - peak) for v in scores]
                    total = sum([jnp.sum(v, axis=-1, keepdims=True) for v in raised])
                    inverse = 1.0 / total
                    mixed = sum([dot_nn((raised[h] * inverse).astype(BF), v_ref[h, m]) for h in range(spans)])
                    result = result + one_head(mixed, head)
                    lse_ref[m, head, here] = jnp.broadcast_to(peak + jnp.log(total), (tile, LANES))
                a_ref[m, here] = result.astype(BF)

            p_ref[m] = dot_nn(a_ref[m], wo_ref[...]).astype(BF)

    part = jax.ShapeDtypeStruct((streams, length, cols), BF)
    span = jax.ShapeDtypeStruct((spans, streams, length, cols), BF)
    return pl.pallas_call(
        kernel,
        name="attend",
        out_shape=(
            part,
            span,
            span,
            part,
            jax.ShapeDtypeStruct((streams, heads, length, LANES), F32),
            jax.ShapeDtypeStruct((streams, length, width), BF),
        ),
        in_specs=in_vmem(7),
        out_specs=tuple(in_vmem(6)),
        compiler_params=params(),
    )(rows, row_ids, col_ids, wq, wk, wv, wo)


def attend_back(q, k, v, lse, grad_out, row_ids, col_ids, wq, wk, wv, wo):
    spans, streams, length, cols = k.shape
    width = grad_out.shape[2]
    heads = cols // HD
    tile = min(256, length)
    scale = HD ** (-0.5)

    def kernel(
        q_ref, k_ref, v_ref, lse_ref, go_ref, row_ref, col_ref, wq_ref, wk_ref, wv_ref, wo_ref,
        dq_ref, dk_ref, dv_ref, p_ref, ga_ref, dk_acc, dv_acc,
    ):
        @pl.loop(0, streams)
        def _(m):
            ga_ref[...] = dot_nt(go_ref[m], wo_ref[...]).astype(BF)
            dk_acc[...] = jnp.zeros_like(dk_acc)
            dv_acc[...] = jnp.zeros_like(dv_acc)

            @pl.loop(0, length // tile)
            def _(i):
                first = pl.multiple_of(i * tile, tile)
                here = pl.ds(first, tile)
                masks = [allowed_keys(col_ref[m, here], row_ref[h, m], first, h * length) for h in range(spans)]
                block = q_ref[m, here]
                grad_block = ga_ref[here]
                result = jnp.zeros((tile, cols), F32)
                for head in range(heads):
                    query = one_head(block, head)
                    grad = one_head(grad_block, head)
                    level = lse_ref[m, head, here][:, :1]
                    prob = [
                        jnp.where(masks[h], jnp.exp(dot_nt(query, k_ref[h, m]) * scale - level), 0.0)
                        for h in range(spans)
                    ]
                    grad_prob = [dot_nt(grad, v_ref[h, m]) for h in range(spans)]
                    mean = sum([jnp.sum(p * g, axis=-1, keepdims=True) for p, g in zip(prob, grad_prob)])
                    grad_scores = [(p * (g - mean)).astype(BF) for p, g in zip(prob, grad_prob)]
                    for h in range(spans):
                        dv_acc[h] += dot_tn(prob[h].astype(BF), grad)
                        dk_acc[h] += dot_tn(grad_scores[h], query)
                    mixed = sum([dot_nn(grad_scores[h], k_ref[h, m]) for h in range(spans)])
                    result = result + one_head(mixed, head)
                dq_ref[m, here] = (result * scale).astype(BF)

            for h in range(spans):
                dk_ref[h, m] = (dk_acc[h] * scale).astype(BF)
                dv_ref[h, m] = dv_acc[h].astype(BF)
                back = dot_nt(dk_ref[h, m], wk_ref[...]) + dot_nt(dv_ref[h, m], wv_ref[...])
                if h == 0:
                    back = back + dot_nt(dq_ref[m], wq_ref[...])
                p_ref[h, m] = back.astype(BF)

    span = jax.ShapeDtypeStruct((spans, streams, length, cols), BF)
    return pl.pallas_call(
        kernel,
        name="attend_back",
        out_shape=(
            jax.ShapeDtypeStruct((streams, length, cols), BF),
            span,
            span,
            jax.ShapeDtypeStruct((spans, streams, length, width), BF),
        ),
        in_specs=in_vmem(11),
        out_specs=tuple(in_vmem(4)),
        scratch_shapes=[
            pltpu.VMEM((length, cols), BF),
            pltpu.VMEM((spans, length, cols), F32),
            pltpu.VMEM((spans, length, cols), F32),
        ],
        compiler_params=params(),
    )(q, k, v, lse, grad_out, row_ids, col_ids, wq, wk, wv, wo)


def unit_terms(gate_pre, up_pre, grad_inner):
    root = 0.7978845608028654
    square = gate_pre * gate_pre
    bend = jnp.tanh(root * (gate_pre + 0.044715 * (gate_pre * square)))
    half = 0.5 * (1.0 + bend)
    gelu = gate_pre * half
    slope = half + 0.5 * gate_pre * (1.0 - bend * bend) * (root * (1.0 + 3.0 * 0.044715 * square))
    return gelu * up_pre, grad_inner * up_pre * slope, grad_inner * gelu


def head(
    x, ids, stu_gain, filter_proj, lag_proj, filters, attn_gain, feed_gain, wq, wk, wv, wo, wg, wu, wd, cot, seq_count
):
    streams, _, quarter, width = x.shape
    length = 4 * quarter
    hops = WINDOW // length
    spans = hops + 1
    count, taps = filters.shape
    wide = taps + 4 * LANES
    lag_order, channels = lag_proj.shape[:2]
    blocks = length // LANES
    reach = taps * 5 // 8
    window = reach + 2 * quarter
    own = 4 * (seq_count - 1)
    assert reach % (2 * quarter) == 0 and window <= taps
    cols, units = wq.shape[1], wg.shape[1]
    heads = cols // HD
    tile = 2 * quarter
    steps = 2 * streams
    scale = HD ** (-0.5)
    rows = width // seq_count
    chunks = 4
    assert streams == 2 and units == 4 * cols

    rows_of = pltpu.VMEM((streams, length, cols), BF)
    unit_rows = pltpu.VMEM((streams, length, units), BF)
    state = pltpu.VMEM((streams, quarter, width), F32)
    gathered = (1, streams, 4, quarter, width)
    split_part = pltpu.VMEM((1, streams, 2, 2, quarter, width), BF)
    pieces = 2
    zero_hops = ReduceScatter.scratch(0, streams, quarter, width, pieces)

    def kernel(
        x_ref, id_ref, sg_ref, fp_hbm, lp_ref, taps_ref, ag_ref, fg_ref,
        wq_ref, wk_ref, wv_ref, wo_ref, wg_hbm, wu_hbm, wd_hbm, cot_hbm,
        stu_hbm, layer_hbm, one_hbm, gain_out, sum_hbm, lag_hbm, ids_out, conv_out, strip_out,
        stu_out, layer_out, one_out, sum_out, lag_out, store_sem,
        fp_ref, wg_ref, wu_ref, wd_ref, cot_ref, load_sem, base_ref, ids_row,
        rows_in, ids_in, cols_in, id_ext, lag_ext, part_ref, id_sem, strip_sem, conv_sem,
        attn_in, feed_in, grad_att, hid_one, hid_two, grad_two, grads, total, grad_acc,
        o_part, feed_part, layer_part, attn_part,
        sem_rows, sem_one, sem_two, sem_three, sem_layer, sem_five, *scratch,
    ):
        s, t, y, c, core, far = place()
        scratch = list(scratch)

        def take(count):
            taken = scratch[:count]
            del scratch[:count]
            return taken

        def reducer(ref, distance):
            return ReduceScatter(seq_count, distance, streams, lambda h, m: ref.at[h, m], take(6))

        rs_one, rs_two, rs_three, rs_layer = [reducer(r, 0) for r in (part_ref, o_part, feed_part, layer_part)]
        rs_four = reducer(attn_part, hops)
        gr = GradReduce(seq_count, lambda k: grads.at[k], lambda k: sum_out.at[k], take(8))
        ag_rows = AllGather(
            seq_count,
            seq_count - 1,
            streams,
            lambda h, m, q: rows_in.at[m, 4 * (seq_count - 1 - h) + q],
            sem_rows,
            first=1,
        )
        ag_one = AllGather(seq_count, hops, streams, attn_in, sem_one)
        ag_two = AllGather(seq_count, 0, streams, feed_in, sem_two)
        ag_three = AllGather(seq_count, 0, streams, grad_att, sem_three)
        ag_layer = AllGather(seq_count, 0, streams, layer_out, sem_layer)
        ag_five = AllGather(seq_count, 0, streams, stu_out, sem_five)

        def flat(value):
            return value.reshape(-1, value.shape[-1])

        def all_rows(ref, m):
            return flat(ref[0, m])

        def masks_of(m, here, first):
            return [
                allowed_keys(cols_in[m, here], ids_out[pl.ds(h * streams + m, 1)], first, h * length) for h in range(spans)
            ]

        def first_norm(m):
            rs_one.total(m, total)
            hidden = x_ref[m, t].astype(F32) + total[...]
            hid_one[m] = hidden
            attn_in[0, m, t] = norm_of(hidden, ag_ref[...]).astype(BF)
            ag_one.start(m)

        def after(i, step, *actions):
            @pl.when(i == step)
            def _():
                for action in actions:
                    action()

        def id_copy(h, peer):
            return remote(id_ref, ids_in.at[h], id_sem.at[0, h], id_sem.at[1, h], {"seq": peer})

        far_back = range(1, seq_count)

        pairs = ((fp_hbm, fp_ref), (wg_hbm, wg_ref), (wu_hbm, wu_ref), (wd_hbm, wd_ref), (cot_hbm, cot_ref))
        loads = [pltpu.make_async_copy(a, b, load_sem.at[i]) for i, (a, b) in enumerate(pairs)]
        pairs = ((stu_out, stu_hbm), (layer_out, layer_hbm), (one_out, one_hbm), (sum_out, sum_hbm), (lag_out, lag_hbm))
        stores = [pltpu.make_async_copy(a, b, store_sem.at[i]) for i, (a, b) in enumerate(pairs)]
        for load in loads:
            load.start()

        def front(strip, left, mask, conv):
            for m in range(streams):
                rows_in[m, own + t] = norm_of(x_ref[m, t].astype(F32), sg_ref[...]).astype(BF)
            greet(seq_count, 0, wide=True)
            for m in range(streams):
                ag_rows.start(m)
            for h in far_back:
                pl.when(s + h < seq_count)(functools.partial(lambda h: id_copy(h, s + h).start(), h))
            for m in range(streams):
                for q in range(4):

                    @pl.when(t != q)
                    def _():
                        rows_in[m, own + q] = norm_of(x_ref[m, q].astype(F32), sg_ref[...]).astype(BF)

            for m in range(streams):
                for h in far_back:
                    ag_rows.clear(h, m)
                for h in range(1, spans):
                    ag_one.clear(h, m)
            ids_in[0] = id_ref[...]
            for h in far_back:

                @pl.when(s - h < 0)
                def _():
                    ids_in[h] = jnp.full(ids_in.shape[1:], -1, jnp.int32)

            lay_taps(taps_ref, base_ref, True)
            strips(base_ref, strip)
            strip_copy = pltpu.make_async_copy(strip, strip_out, strip_sem)
            strip_copy.start()
            ag_rows.arrive(1, 0)
            ag_rows.arrive(2, 0)
            for h in far_back:
                pl.when(s - h >= 0)(functools.partial(lambda h: id_copy(h, s - h).wait_recv(), h))
            for h in range(seq_count):
                for m in range(streams):
                    ids_out[h * streams + m : h * streams + m + 1] = ids_in[h, m].astype(F32)
                    start = (seq_count - 1 - h) * length
                    ids_row[m : m + 1, start : start + length] = ids_in[h, m].astype(F32)
            turned = jnp.transpose(ids_out[...])
            for m in range(streams):
                cols_in[m] = turned[:, m : m + 1]
                id_ext[m, :8] = turned[length - 8 :, streams + m : streams + m + 1]
                id_ext[m, 8:] = turned[:, m : m + 1]
            lay_taps(taps_ref, base_ref, False)
            strip_copy.wait()
            strips(base_ref, strip)
            for load in loads:
                load.wait()
            ag_rows.pass_on(1, 0)
            ag_rows.arrive(3, 0)
            ag_rows.pass_on(2, 0)
            ag_rows.finish(1, 0)
            ag_rows.finish(2, 0)
            mine = pl.ds(pl.multiple_of(t * channels, LANES), channels)

            def lags(m):
                lag_ext[:8] = rows_in[m, own - 1, quarter - 8 :, mine].astype(F32)
                lag_ext[8:] = rows_in[m, own : own + 4, :, mine].reshape(length, channels).astype(F32)
                for i in range(lag_order):
                    same = id_ext[m, 7 - i : 7 - i + length] == cols_in[m]
                    lag_out[i, m] = jnp.where(same, lag_ext[7 - i : 7 - i + length], 0.0).astype(BF)

            def conv_copy(k, m, half):
                first = pl.multiple_of(half * tile, tile)
                return pltpu.make_async_copy(
                    conv.at[k, pl.ds(first, tile)],
                    conv_out.at[k, pl.ds(pl.multiple_of(m * length + first, tile), tile)],
                    conv_sem.at[k, half],
                )

            lags(0)
            per = 2 * count

            @pl.loop(0, streams * per)
            def _(j):
                m = j // per
                half = 1 - (j - m * per) // count
                k = j - m * per - (1 - half) * count
                first = pl.multiple_of(half * tile, tile)
                here = pl.ds(first, tile)
                offset = taps - length - reach

                @pl.when(k == 0)
                def _():
                    ids_there = ids_row[pl.ds(m, 1), pl.ds(pl.multiple_of(offset + first, tile), window)]
                    mask[...] = jnp.where(cols_in[m, here] == ids_there, 1.0, 0.0).astype(BF)

                for a in range(2 * quarter // LANES):
                    start = taps - LANES - reach - a * LANES
                    down = slice(a * LANES, (a + 1) * LANES)
                    left[down] = strip[k, :, start : start + window] * mask[down]
                right = rows_in[m, pl.ds(offset // quarter + 2 * half, window // quarter)].reshape(window, width)
                result = dot_nn(left[...], right).astype(BF)
                pl.when(m > 0)(lambda: conv_copy(k, m - 1, half).wait())
                conv[k, here] = result
                conv_copy(k, m, half).start()

                @pl.when(k == count - 1)
                def _():
                    mixed = sum([dot_nn(conv[q, here], fp_ref[q]) for q in range(count)])
                    mixed = mixed + sum([dot_nn(lag_out[i, m, here], lp_ref[i]) for i in range(lag_order)])
                    part_ref[0, m, half] = mixed.astype(BF).reshape(2, quarter, width)

                after(j, 0, lambda: ag_rows.arrive(1, 1))
                after(j, 1, lambda: ag_rows.pass_on(3, 0), lambda: ag_rows.arrive(2, 1))
                after(j, 3, lambda: ag_rows.arrive(3, 1), lambda: ag_rows.pass_on(1, 1))
                after(j, count - 1, lambda: ag_rows.finish(3, 0), lambda: ag_rows.pass_on(2, 1))
                after(j, count + 1, lambda: ag_rows.pass_on(3, 1))
                after(
                    j,
                    per - 1,
                    lambda: rs_one.start(0, 0),
                    *[functools.partial(ag_rows.finish, h, 1) for h in far_back],
                    lambda: lags(1),
                )
                after(j, per + 1, lambda: rs_one.middle(0, 0))
                after(j, per + 6, lambda: first_norm(0))

            rs_one.start(0, 1)
            stores[4].start()
            for k in range(count):
                for half in range(2):
                    conv_copy(k, streams - 1, half).wait()

        pl.run_scoped(
            front,
            pltpu.VMEM((count, LANES, wide), BF),
            pltpu.VMEM((tile, window), BF),
            pltpu.VMEM((tile, window), BF),
            pltpu.VMEM((count, length, width), BF),
        )

        def attention_on(
            q_ref, k_ref, v_ref, a_ref, lse_ref, inner_ref, gg_ref, gu_ref, ga_ref, dk_acc, dv_acc, dq_ref, dkv_ref
        ):
            ag_one.pass_on(0, 0)
            rs_one.middle(0, 1)
            for h in range(1, spans):
                ag_one.arrive(h, 0)
            first_norm(1)
            for h in range(1, spans):
                ag_one.pass_on(h, 0)
            for h in range(spans):
                ag_one.finish(h, 0)

            def split_step(i):
                m = i // 2
                return m, i - 2 * m

            @pl.loop(0, steps)
            def _(i):
                m, half = split_step(i)
                first = pl.multiple_of(half * tile, tile)
                here = pl.ds(first, tile)

                @pl.when(half == 0)
                def _():
                    own = flat(attn_in[0, m])
                    q_ref[m] = dot_nn(own, wq_ref[...]).astype(BF)
                    for h in range(spans):
                        block = flat(attn_in[h, m])
                        k_ref[h, m] = dot_nn(block, wk_ref[...]).astype(BF)
                        v_ref[h, m] = dot_nn(block, wv_ref[...]).astype(BF)

                masks = masks_of(m, here, first)
                block = q_ref[m, here]
                result = jnp.zeros((tile, cols), F32)
                for head in range(heads):
                    query = one_head(block, head)
                    scores = [jnp.where(masks[h], dot_nt(query, k_ref[h, m]) * scale, NEGATIVE) for h in range(spans)]
                    peak = functools.reduce(jnp.maximum, [jnp.max(v, axis=-1, keepdims=True) for v in scores])
                    raised = [jnp.exp(v - peak) for v in scores]
                    norm = sum([jnp.sum(v, axis=-1, keepdims=True) for v in raised])
                    inverse = 1.0 / norm
                    mixed = sum([dot_nn((raised[h] * inverse).astype(BF), v_ref[h, m]) for h in range(spans)])
                    result = result + one_head(mixed, head)
                    lse_ref[m, head, here] = jnp.broadcast_to(peak + jnp.log(norm), (tile, LANES))
                low = result.astype(BF)
                a_ref[m, here] = low
                o_part[0, m, half] = dot_nn(low, wo_ref[...]).astype(BF).reshape(2, quarter, width)
                after(i, 0, lambda: ag_one.pass_on(0, 1), *[functools.partial(ag_one.arrive, h, 1) for h in range(1, spans)])
                after(
                    i,
                    1,
                    lambda: rs_two.start(0, 0),
                    *[functools.partial(ag_one.pass_on, h, 1) for h in range(1, spans)],
                    *[functools.partial(ag_one.finish, h, 1) for h in range(spans)],
                )
                after(i, 2, lambda: rs_two.middle(0, 0))
                after(i, 3, lambda: rs_two.start(0, 1))

            def second_norm(m):
                rs_two.total(m, total)
                hidden = hid_one[m] + total[...]
                hid_two[m] = hidden
                feed_in[0, m, t] = norm_of(hidden, fg_ref[...]).astype(BF)
                ag_two.start(m)

            second_norm(0)
            rs_two.middle(0, 1)
            rs_one.drain()
            ag_rows.drain()
            for h in far_back:
                pl.when(s + h < seq_count)(functools.partial(lambda h: id_copy(h, s + h).wait_send(), h))
            ag_two.pass_on(0, 0)
            ag_two.finish(0, 0)

            @pl.loop(0, steps)
            def _(i):
                m, half = split_step(i)
                here = pl.ds(pl.multiple_of(half * tile, tile), tile)
                block = flat(feed_in[0, m, pl.ds(2 * half, 2)])
                inner, grad_gate, grad_up = unit_terms(
                    dot_nn(block, wg_ref[...]), dot_nn(block, wu_ref[...]), dot_nt(cot_ref[m, here], wd_ref[...])
                )
                inner, grad_gate, grad_up = inner.astype(BF), grad_gate.astype(BF), grad_up.astype(BF)
                inner_ref[m, here] = inner
                gg_ref[m, here] = grad_gate
                gu_ref[m, here] = grad_up
                back = dot_nt(grad_gate, wg_ref[...]) + dot_nt(grad_up, wu_ref[...])
                feed_part[0, m, half] = back.astype(BF).reshape(2, quarter, width)
                layer_part[0, m, half] = dot_nn(inner, wd_ref[...]).astype(BF).reshape(2, quarter, width)
                after(i, 0, lambda: second_norm(1))
                after(
                    i,
                    1,
                    lambda: rs_three.start(0, 0),
                    lambda: ag_two.pass_on(0, 1),
                    lambda: rs_three.middle(0, 0),
                    lambda: ag_two.finish(0, 1),
                )
                after(i, 3, lambda: rs_three.start(0, 1))

            def third_norm(m):
                rs_three.total(m, total)
                grad_in, gain_grad = norm_back(hid_two[m], fg_ref[...], total[...])
                value = cot_ref[m, pl.ds(pl.multiple_of(t * quarter, quarter), quarter)].astype(F32) + grad_in
                grad_two[m] = value
                gain_out[1:2] = gain_grad if m == 0 else gain_out[1:2] + gain_grad
                grad_att[0, m, t] = value.astype(BF)
                ag_three.start(m)

            third_norm(0)
            feed_all = flat(feed_in[0])
            grads[0] = dot_tn(feed_all, flat(gg_ref[...])).astype(BF)
            gr.start(0)
            rs_three.middle(0, 1)
            grads[1] = dot_tn(feed_all, flat(gu_ref[...])).astype(BF)
            gr.start(1)
            grads[2] = dot_tn(flat(cot_ref[...]), flat(inner_ref[...])).astype(BF)
            gr.start(2)
            rs_two.drain()
            ag_one.drain()
            ag_three.pass_on(0, 0)
            ag_three.finish(0, 0)
            for m in range(streams):
                rs_layer.start(0, m)

            def layer_sum(m):
                rs_layer.total(m, total)
                layer_out[0, m, t] = (hid_two[m] + total[...]).astype(BF)
                ag_layer.start(m)

            @pl.loop(0, steps)
            def _(i):
                m, half = split_step(i)
                first = pl.multiple_of(half * tile, tile)
                here = pl.ds(first, tile)

                @pl.when(half == 0)
                def _():
                    ga_ref[...] = dot_nt(all_rows(grad_att, m), wo_ref[...]).astype(BF)
                    dk_acc[...] = jnp.zeros_like(dk_acc)
                    dv_acc[...] = jnp.zeros_like(dv_acc)

                masks = masks_of(m, here, first)
                block = q_ref[m, here]
                grad_block = ga_ref[here]
                result = jnp.zeros((tile, cols), F32)
                for head in range(heads):
                    query = one_head(block, head)
                    grad = one_head(grad_block, head)
                    level = lse_ref[m, head, here][:, :1]
                    prob = [
                        jnp.where(masks[h], jnp.exp(dot_nt(query, k_ref[h, m]) * scale - level), 0.0) for h in range(spans)
                    ]
                    grad_prob = [dot_nt(grad, v_ref[h, m]) for h in range(spans)]
                    mean = sum([jnp.sum(p * g, axis=-1, keepdims=True) for p, g in zip(prob, grad_prob)])
                    grad_scores = [(p * (g - mean)).astype(BF) for p, g in zip(prob, grad_prob)]
                    for h in range(spans):
                        dv_acc[h] += dot_tn(prob[h].astype(BF), grad)
                        dk_acc[h] += dot_tn(grad_scores[h], query)
                    mixed = sum([dot_nn(grad_scores[h], k_ref[h, m]) for h in range(spans)])
                    result = result + one_head(mixed, head)
                dq_ref[m, here] = (result * scale).astype(BF)

                @pl.when(half == 1)
                def _():
                    for h in range(hops, -1, -1):
                        grad_k = (dk_acc[h] * scale).astype(BF)
                        grad_v = dv_acc[h].astype(BF)
                        dkv_ref[h, m, :, :cols] = grad_k
                        dkv_ref[h, m, :, cols:] = grad_v
                        back = dot_nt(grad_k, wk_ref[...]) + dot_nt(grad_v, wv_ref[...])
                        if h == 0:
                            back = back + dot_nt(dq_ref[m], wq_ref[...])
                        attn_part[h, m] = back.astype(BF).reshape(2, 2, quarter, width)
                        rs_four.start(h, m)

                after(i, 0, lambda: third_norm(1), lambda: rs_layer.middle(0, 0), lambda: rs_layer.middle(0, 1))
                after(i, 1, lambda: gr.spread(0), lambda: ag_three.pass_on(0, 1), lambda: ag_three.finish(0, 1))
                after(
                    i,
                    2,
                    *[functools.partial(rs_four.middle, h, 0) for h in range(hops, -1, -1)],
                    lambda: gr.spread(1),
                    lambda: gr.relay(0, 1),
                )
                after(
                    i,
                    3,
                    *[functools.partial(rs_four.hop, h, 0, total) for h in range(hops, 0, -1)],
                    lambda: gr.spread(2),
                    lambda: gr.relay(0, 2),
                    lambda: gr.relay(1, 1),
                )

            for h in range(hops, -1, -1):
                rs_four.middle(h, 1)
            attn_all = attn_in[...].reshape(spans * streams * length, width)
            grads[3, :, cols : 3 * cols] = dot_tn(attn_all, flat(dkv_ref[...].reshape(-1, 2 * cols))).astype(BF)
            grads[3, :, :cols] = dot_tn(flat(attn_in[0]), flat(dq_ref[...])).astype(BF)
            grads[3, :, 3 * cols :] = dot_tn(flat(grad_att[0]), flat(a_ref[...])).astype(BF)
            gr.start(3)

            def fourth_norm(m):
                rs_four.total(m, total)
                grad_in, gain_grad = norm_back(hid_one[m], ag_ref[...], total[...])
                value = grad_two[m] + grad_in
                one_out[m] = value
                gain_out[0:1] = gain_grad if m == 0 else gain_out[0:1] + gain_grad
                stu_out[0, m, t] = value.astype(BF)
                ag_five.start(m)

            gr.relay(1, 2)
            gr.relay(2, 1)
            rs_three.drain()
            ag_two.drain()
            ag_three.drain()
            fourth_norm(0)
            for h in range(hops, 0, -1):
                rs_four.hop(h, 1, total)
            gr.spread(3)
            gr.relay(2, 2)
            gr.collect(0, grad_acc)
            fourth_norm(1)
            stores[2].start()
            for m in range(streams):
                layer_sum(m)
            gr.relay(3, 1)
            gr.collect(1, grad_acc)
            for m in range(streams):
                ag_five.pass_on(0, m)
            gr.relay(3, 2)
            gr.collect(2, grad_acc)
            for m in range(streams):
                ag_five.finish(0, m)
            stores[0].start()
            for m in range(streams):
                ag_layer.pass_on(0, m)
            gr.collect(3, grad_acc)
            rs_layer.drain()
            rs_four.drain()
            for m in range(streams):
                ag_layer.finish(0, m)
            stores[1].start()
            for k in range(chunks - 1):
                gr.finish(k)
                gr.drain(k)
            ag_five.drain()
            ag_layer.drain()
            gr.finish(chunks - 1)
            stores[3].start()
            gr.drain(chunks - 1)
            for store in stores:
                store.wait()

        pl.run_scoped(
            attention_on,
            rows_of,
            pltpu.VMEM((spans, streams, length, cols), BF),
            pltpu.VMEM((spans, streams, length, cols), BF),
            rows_of,
            pltpu.VMEM((streams, heads, length, LANES), F32),
            unit_rows,
            unit_rows,
            unit_rows,
            pltpu.VMEM((length, cols), BF),
            pltpu.VMEM((spans, length, cols), F32),
            pltpu.VMEM((spans, length, cols), F32),
            rows_of,
            pltpu.VMEM((spans, streams, length, 2 * cols), BF),
        )

    anywhere = pl.BlockSpec(memory_space=pl.ANY)
    return pl.pallas_call(
        kernel,
        name="head",
        out_shape=(
            jax.ShapeDtypeStruct(gathered, BF),
            jax.ShapeDtypeStruct(gathered, BF),
            jax.ShapeDtypeStruct((streams, quarter, width), F32),
            jax.ShapeDtypeStruct((2, width), F32),
            jax.ShapeDtypeStruct((chunks, rows, units), BF),
            jax.ShapeDtypeStruct((lag_order, streams, length, channels), BF),
            jax.ShapeDtypeStruct((seq_count * streams, length), F32),
            jax.ShapeDtypeStruct((count, streams * length, width), BF),
            jax.ShapeDtypeStruct((count, LANES, wide), BF),
        ),
        in_specs=[anywhere if i in (3, 12, 13, 14, 15) else spec for i, spec in enumerate(in_vmem(16))],
        out_specs=tuple(spec if i in (3, 6) else anywhere for i, spec in enumerate(in_vmem(9))),
        scratch_shapes=[
            pltpu.VMEM(gathered, BF),
            pltpu.VMEM(gathered, BF),
            pltpu.VMEM((streams, quarter, width), F32),
            pltpu.VMEM((chunks, rows, units), BF),
            pltpu.VMEM((lag_order, streams, length, channels), BF),
            pltpu.SemaphoreType.DMA((5,)),
            pltpu.VMEM(filter_proj.shape, BF),
            pltpu.VMEM(wg.shape, BF),
            pltpu.VMEM(wu.shape, BF),
            pltpu.VMEM(wd.shape, BF),
            pltpu.VMEM(cot.shape, BF),
            pltpu.SemaphoreType.DMA((5,)),
            pltpu.VMEM((count, wide), F32),
            pltpu.VMEM((streams, taps), F32),
            pltpu.VMEM((streams, 4 * seq_count, quarter, width), BF),
            pltpu.VMEM((seq_count,) + ids.shape, jnp.int32),
            pltpu.VMEM((streams, length, 1), F32),
            pltpu.VMEM((streams, length + 8, 1), F32),
            pltpu.VMEM((length + 8, channels), F32),
            split_part,
            pltpu.SemaphoreType.DMA((2, seq_count)),
            pltpu.SemaphoreType.DMA,
            pltpu.SemaphoreType.DMA((count, 2)),
            pltpu.VMEM((spans, streams, 4, quarter, width), BF),
            pltpu.VMEM(gathered, BF),
            pltpu.VMEM(gathered, BF),
            state,
            state,
            state,
            pltpu.VMEM((chunks, width, units), BF),
            pltpu.VMEM((quarter, width), F32),
            pltpu.VMEM((rows, units // 2), F32),
            split_part,
            split_part,
            split_part,
            pltpu.VMEM((spans, streams, 2, 2, quarter, width), BF),
            AllGather.scratch(seq_count - 1, streams, pieces)[0],
            AllGather.scratch(hops, streams, pieces)[0],
        ]
        + [AllGather.scratch(0, streams, pieces)[0]] * 4
        + zero_hops * 4
        + ReduceScatter.scratch(hops, streams, quarter, width, pieces)
        + GradReduce.scratch(seq_count, chunks, width, units),
        compiler_params=params(8),
    )(
        x, ids, stu_gain, filter_proj, lag_proj, filters, attn_gain, feed_gain, wq, wk, wv, wo, wg, wu, wd, cot
    )


def tail(
    grad_stu, filter_proj, lag_proj, conv, lag_stack, ext_ids, strip_back, x, gain, grad_one, gains, seq_count
):
    count, length_all, width = conv.shape
    streams, _, quarter, _ = x.shape
    length = length_all // streams
    lag_order, channels = lag_proj.shape[:2]
    blocks = length // LANES
    hops = seq_count - 1
    chunks = count + 1
    steps = seq_count * streams
    rows = width // seq_count
    gain_rows = 8

    def kernel(
        gs_ref, fp_hbm, lp_ref, conv_hbm, lag_ref, ext_ref, strip_hbm, x_hbm, gain_ref, one_ref, gains_ref,
        out_hbm, filter_hbm, lag_out, gain_out,
        out, filter_out, out_sem, filter_sem,
        conv_ref, fp_ref, strip, x_own, conv_sem, fp_sem, strip_sem, x_sem, id_ext,
        mask, cols, left, acc, terms, grad_conv, grads, lag_ext, total, grad_acc, gather_sem,
        gain_own, gain_near, gain_sum, gain_far, near_sem, far_sem, *scratch,
    ):
        s, t, y, c, core, far = place()
        p = lax.axis_index("dp")
        rs_scratch, gr_scratch = scratch[:6], scratch[6:]
        out_copy = pltpu.make_async_copy(out, out_hbm, out_sem)

        def filter_copy(k):
            return pltpu.make_async_copy(filter_out.at[k], filter_hbm.at[k], filter_sem.at[k])

        def conv_copy(k):
            return pltpu.make_async_copy(conv_hbm.at[k], conv_ref.at[k], conv_sem.at[k])

        def fp_copy(k):
            return pltpu.make_async_copy(fp_hbm.at[k], fp_ref.at[k], fp_sem.at[k])

        strip_copy = pltpu.make_async_copy(strip_hbm, strip, strip_sem)
        for k in range(count):
            conv_copy(k).start()
            fp_copy(k).start()
        strip_copy.start()
        x_copy = pltpu.make_async_copy(x_hbm.at[:, t], x_own, x_sem)
        x_copy.start()
        greet(seq_count, hops, wide=True, gains=True)

        def source(k):
            return grads.at[k]

        def result(k):
            return filter_out.at[k] if k < count else lag_out

        gr = GradReduce(seq_count, source, result, gr_scratch)
        rs = ReduceScatter(seq_count, hops, streams, lambda h, m: terms.at[h, m], rs_scratch)
        ag = AllGather(seq_count, 0, streams, out, gather_sem)

        @pl.loop(0, count)
        def _(k):
            conv_copy(k).wait()
            grads[k] = dot_tn(conv_ref[k], gs_ref[...]).astype(BF)
            gr.start(k)
            fp_copy(k).wait()
            product = dot_nt(gs_ref[...], fp_ref[k]).astype(BF)
            for m in range(streams):
                here = pl.ds(pl.multiple_of(k * length, LANES), length)
                grad_conv[m, here] = product[m * length : (m + 1) * length]
            pl.when(k == count - 1)(lambda: gr.spread(0))

        grads[count] = jnp.zeros_like(grads.at[count])
        for i in range(lag_order):
            grads[count, :, i * channels : (i + 1) * channels] = dot_tn(gs_ref[...], lag_ref[i]).astype(BF)
        gr.start(count)
        turned = jnp.transpose(ext_ref[...])
        for j in range(steps):
            cols[j] = turned[:, j : j + 1]
        for m in range(streams):
            lag_ext[m] = jnp.zeros_like(lag_ext.at[m])
            id_ext[:8] = turned[length - 8 :, streams + m : streams + m + 1]
            id_ext[8:] = turned[:, m : m + 1]
            for i in range(lag_order):
                term = dot_nt(gs_ref[m * length : (m + 1) * length], lp_ref[i])
                same = id_ext[7 - i : 7 - i + length] == cols[m]
                lag_ext[m, 7 - i : 7 - i + length] += jnp.where(same, term, 0.0)
        strip_copy.wait()
        x_copy.wait()
        mine = pl.ds(pl.multiple_of(t * channels, LANES), channels)
        assert seq_count == 4 and steps == 8 and chunks == 7
        spread_at = {0: 1, 2: 2, 4: 3, 6: 4}
        relay_at = {1: (0, 1), 2: (0, 2), 3: (1, 1), 4: (1, 2), 5: (2, 1), 6: (2, 2), 7: (3, 1)}
        collect_at = {5: 0, 7: 1}

        def step_of(i):
            return seq_count - 1 - i // streams, i - i // streams * streams

        @pl.loop(0, steps)
        def _(i):
            h, m = step_of(i)

            @pl.when(h <= s)
            def _():
                mask[...] = jnp.where(cols[h * streams + m] == ext_ref[pl.ds(m, 1)], 1.0, 0.0).astype(BF)
                for k in range(count):
                    for a in range(blocks):
                        start = pl.multiple_of(LANES * (blocks * h + blocks - 1 - a), LANES)
                        down = slice(a * LANES, (a + 1) * LANES)
                        left[down, k * length : (k + 1) * length] = strip[k, :, pl.ds(start, length)] * mask[down]
                acc[...] = jnp.dot(left[...], grad_conv[m], preferred_element_type=F32)

                @pl.when(h == 0)
                def _():
                    acc[:, mine] += lag_ext[m, 8:]

                @pl.when(h == 1)
                def _():
                    acc[length - 8 :, mine] += lag_ext[m, :8]

                for quarter_y in range(2):
                    for quarter_c in range(2):
                        first = (2 * quarter_y + quarter_c) * quarter
                        terms[h, m, quarter_y, quarter_c] = acc[first : first + quarter].astype(BF)
                rs.start(h, m)

            @pl.when(i >= 1)
            def _():
                rs.middle(*step_of(i - 1))

            @pl.when((i >= 2) & (i < steps - streams + 2))
            def _():
                rs.hop(*step_of(i - 2), total)

            for step, k in spread_at.items():
                pl.when(i == step)(functools.partial(gr.spread, k))
            for step, (k, d) in relay_at.items():
                pl.when(i == step)(functools.partial(gr.relay, k, d))
            for step, k in collect_at.items():
                pl.when(i == step)(functools.partial(gr.collect, k, grad_acc))

        rs.middle(0, streams - 1)
        gr.spread(5)
        gr.relay(3, 2)
        gr.relay(4, 1)
        gain_own[...] = jnp.zeros_like(gain_own)

        def last_norm(m):
            rs.total(m, total)
            grad_in, gain_grad = norm_back(x_own[m].astype(F32), gain_ref[...], total[...])
            out[0, m, t] = (one_ref[m] + grad_in).astype(BF)
            ag.start(m)
            gain_own[0:1] += gain_grad

        last_norm(0)
        gr.relay(4, 2)
        gr.relay(5, 1)
        gr.spread(6)
        last_norm(1)
        gr.relay(5, 2)
        gain_own[1:3] = gains_ref[...]
        gain_near[t] = gain_own[...]

        def near_copy(j, slot):
            return remote(gain_own, gain_near.at[slot], near_sem.at[0, j], near_sem.at[1, slot], {"tensor": j})

        for j in range(4):
            pl.when(t != j)(functools.partial(lambda j: near_copy(j, t).start(), j))
        gr.collect(2, grad_acc)
        gr.relay(6, 1)
        gr.collect(3, grad_acc)
        for m in range(streams):
            ag.pass_on(0, m)
        gr.relay(6, 2)
        gr.collect(4, grad_acc)
        for j in range(4):
            pl.when(t != j)(functools.partial(lambda j: near_copy(j, j).wait_recv(), j))
        gain_sum[...] = gain_near[0] + gain_near[1] + gain_near[2] + gain_near[3]
        me = p * seq_count + s

        def far_copy(j, slot):
            d, q = j // seq_count, j % seq_count
            return remote(
                gain_sum.at[:, q * rows : (q + 1) * rows], gain_far.at[slot], far_sem.at[0, j], far_sem.at[1, slot],
                {"dp": d, "seq": q},
            )

        gain_far[me] = gain_sum[:, pl.ds(pl.multiple_of(s * rows, LANES), rows)]
        for j in range(2 * seq_count):
            pl.when(me != j)(lambda: far_copy(j, me).start())
        gr.collect(5, grad_acc)
        rs.drain()
        for m in range(streams):
            ag.finish(0, m)
        out_copy.start()
        gr.collect(6, grad_acc)
        for k in range(4):
            gr.finish(k)
            filter_copy(k).start()
            gr.drain(k)
        for j in range(2 * seq_count):
            pl.when(me != j)(lambda: far_copy(j, j).wait_recv())
        gain_out[...] = functools.reduce(jnp.add, [gain_far[j] for j in range(2 * seq_count)])
        for k in range(4, chunks):
            gr.finish(k)
            if k < count:
                filter_copy(k).start()
            gr.drain(k)
        for j in range(4):
            pl.when(t != j)(lambda: near_copy(j, t).wait_send())
        for j in range(2 * seq_count):
            pl.when(me != j)(lambda: far_copy(j, me).wait_send())
        ag.drain()
        out_copy.wait()
        for k in range(count):
            filter_copy(k).wait()

    anywhere = pl.BlockSpec(memory_space=pl.ANY)
    return pl.pallas_call(
        kernel,
        name="tail",
        out_shape=(
            jax.ShapeDtypeStruct((1, streams, 4, quarter, width), BF),
            jax.ShapeDtypeStruct((count, rows, width), BF),
            jax.ShapeDtypeStruct((rows, width), BF),
            jax.ShapeDtypeStruct((gain_rows, rows), F32),
        ),
        in_specs=[anywhere if i in (1, 3, 6, 7) else spec for i, spec in enumerate(in_vmem(11))],
        out_specs=(anywhere, anywhere) + tuple(in_vmem(2)),
        scratch_shapes=[
            pltpu.VMEM((1, streams, 4, quarter, width), BF),
            pltpu.VMEM((count, rows, width), BF),
            pltpu.SemaphoreType.DMA,
            pltpu.SemaphoreType.DMA((count,)),
            pltpu.VMEM(conv.shape, BF),
            pltpu.VMEM(filter_proj.shape, BF),
            pltpu.VMEM(strip_back.shape, BF),
            pltpu.VMEM((streams, quarter, width), BF),
            pltpu.SemaphoreType.DMA((count,)),
            pltpu.SemaphoreType.DMA((count,)),
            pltpu.SemaphoreType.DMA,
            pltpu.SemaphoreType.DMA,
            pltpu.VMEM((length + 8, 1), F32),
            pltpu.VMEM((length, length), BF),
            pltpu.VMEM((steps, length, 1), F32),
            pltpu.VMEM((length, count * length), BF),
            pltpu.VMEM((length, width), F32),
            pltpu.VMEM((seq_count, streams, 2, 2, quarter, width), BF),
            pltpu.VMEM((streams, count * length, width), BF),
            pltpu.VMEM((chunks, width, width), BF),
            pltpu.VMEM((streams, length + 8, channels), F32),
            pltpu.VMEM((quarter, width), F32),
            pltpu.VMEM((rows, width // 2), F32),
            AllGather.scratch(0, streams)[0],
            pltpu.VMEM((gain_rows, width), F32),
            pltpu.VMEM((4, gain_rows, width), F32),
            pltpu.VMEM((gain_rows, width), F32),
            pltpu.VMEM((2 * seq_count, gain_rows, rows), F32),
            pltpu.SemaphoreType.DMA((2, 4)),
            pltpu.SemaphoreType.DMA((2, 2 * seq_count)),
        ]
        + ReduceScatter.scratch(hops, streams, quarter, width)
        + GradReduce.scratch(seq_count, chunks, width, width),
        compiler_params=params(7),
    )(
        grad_stu, filter_proj, lag_proj, conv, lag_stack, ext_ids, strip_back, x, gain, grad_one, gains
    )


def write_out(layer_output, input_gradient, gains, filter_grad, lag_grad, sums, lag_order, channels, cols):
    _, streams, _, quarter, width = layer_output.shape
    rows, units = sums.shape[1:]
    count = filter_grad.shape[0]

    def kernel(
        layer_ref, input_ref, gains_ref, filter_ref, lag_ref, sums_ref,
        layer_out, input_out, stu_out, filter_out, lag_out, attn_out, q_out, k_out, v_out, o_out, feed_out, gate_out, up_out,
        down_out,
    ):
        layer_out[...] = layer_ref[0].reshape(streams, 1, 4 * quarter, width)
        input_out[...] = input_ref[0].reshape(streams, 1, 4 * quarter, width)
        filter_out[...] = filter_ref[...].astype(F32)
        for i, ref in enumerate((stu_out, attn_out, feed_out)):
            ref[...] = gains_ref[i : i + 1]
        for i in range(lag_order):
            lag_out[i] = jnp.transpose(lag_ref[:, i * channels : (i + 1) * channels].astype(F32))
        for i, ref in enumerate((q_out, k_out, v_out)):
            ref[...] = sums_ref[3, :, i * cols : (i + 1) * cols].astype(F32)
        o_out[...] = jnp.transpose(sums_ref[3, :, 3 * cols :].astype(F32))
        gate_out[...] = sums_ref[0].astype(F32)
        up_out[...] = sums_ref[1].astype(F32)
        down_out[...] = jnp.transpose(sums_ref[2].astype(F32))

    def out(*shape, kind=F32):
        return jax.ShapeDtypeStruct(shape, kind)

    shapes = (
        out(streams, 1, 4 * quarter, width, kind=BF),
        out(streams, 1, 4 * quarter, width, kind=BF),
        out(1, rows),
        out(count, rows, width),
        out(lag_order, channels, rows),
        out(1, rows),
        out(rows, cols),
        out(rows, cols),
        out(rows, cols),
        out(cols, rows),
        out(1, rows),
        out(rows, units),
        out(rows, units),
        out(units, rows),
    )
    results = pl.pallas_call(
        kernel,
        name="write_out",
        out_shape=shapes,
        in_specs=in_vmem(6),
        out_specs=tuple(in_vmem(len(shapes))),
        compiler_params=params(),
    )(layer_output, input_gradient, gains, filter_grad, lag_grad, sums)
    return tuple(r.reshape(rows) if r.shape == (1, rows) else r for r in results)


def gated_unit(gate_pre, up_pre):
    return jax.nn.gelu(gate_pre, approximate=True) * up_pre


def local(
    seq_count,
    tokens,
    document_index,
    filters,
    stu_gain,
    filter_proj,
    lag_proj,
    attention_gain,
    query_weight,
    key_weight,
    value_weight,
    output_weight,
    feed_gain,
    gate_weight,
    up_weight,
    down_weight,
    cotangent,
):
    streams, _, length, width = tokens.shape
    row_len = length * seq_count
    quarter = length // 4
    lag_order, channels = lag_proj.shape[:2]
    count = filters.shape[0]
    hops = WINDOW // length
    tensor_place = lax.axis_index("tensor")
    chan_start = tensor_place * channels

    def split(a):
        return a.reshape(a.shape[:-2] + (2, 2, quarter, width))

    def quarters(a):
        return a.reshape(a.shape[:-2] + (4, quarter, width))

    def whole(a):
        return a.reshape(a.shape[:-3] + (length, width))

    def row(gain):
        return gain.reshape(1, width)

    if width // seq_count % LANES == 0:
        rows = tokens.reshape(streams, 4, quarter, width)
        grad_stu, layer_output, grad_one, gain_grads, sums, lag_stack, ext_ids, conv, strip_back = head(
            rows, document_index, row(stu_gain), filter_proj, lag_proj, filters, row(attention_gain), row(feed_gain),
            query_weight, key_weight, value_weight, output_weight, gate_weight, up_weight, down_weight,
            cotangent.reshape(streams, length, width), seq_count,
        )
        input_gradient, filter_grad, lag_grad, gains = tail(
            grad_stu.reshape(streams * length, width), filter_proj, lag_proj, conv,
            lag_stack.reshape(lag_order, streams * length, channels), ext_ids, strip_back, rows, row(stu_gain), grad_one,
            gain_grads, seq_count,
        )
        return write_out(
            layer_output, input_gradient, gains, filter_grad, lag_grad, sums, lag_order, channels, query_weight.shape[1]
        )

    x = tokens[:, 0]
    grad_three = cotangent[:, 0]
    ids = document_index[:, 0]
    id_tile = ids.reshape(streams * length // LANES, LANES)
    pad = jnp.zeros((count, 4 * LANES), filters.dtype)
    ahead = row_len - LANES
    base = jnp.concatenate(
        [
            jnp.flip(filters[:, : ahead + 1], axis=1),
            pad[:, : 4 * LANES],
            jnp.flip(filters[:, ahead + 1 :], axis=1),
        ],
        axis=1,
    ).astype(F32)[:, None]
    base_back = jnp.concatenate(
        [pad[:, : length - LANES], filters, pad[:, :LANES]], axis=1
    ).astype(F32)[:, None]

    tokens_flat = streams * length
    cols = query_weight.shape[1]

    def answer(layer_output, input_gradient, gains, filter_grad, lag_grad, attn_grads, feed_grads):
        query_grad, key_grad, value_grad, output_grad = jnp.split(attn_grads, [cols, 2 * cols, 3 * cols], axis=1)
        gate_grad, up_grad, down_grad = feed_grads
        return (
            layer_output[:, None],
            input_gradient[:, None],
            gains[0],
            filter_grad,
            lag_grad[:, : lag_order * channels].T.reshape(lag_order, channels, -1),
            gains[1],
            query_grad,
            key_grad,
            value_grad,
            output_grad.T,
            gains[2],
            gate_grad,
            up_grad,
            down_grad.T,
        )

    inputs = norm_of(x.astype(F32), stu_gain).astype(BF)
    rows_ext, id_ext = gather_rows(quarters(inputs), id_tile, seq_count)
    rows_ext = whole(rows_ext)
    id_ext = id_ext.reshape(seq_count, streams, length)
    id_rows = id_ext[:, :, None, :]
    id_cols = id_ext[:, :, :, None]

    conv = convolve(rows_ext, id_rows, id_cols[0], base, seq_count)

    chan_rows = lax.dynamic_slice_in_dim(rows_ext[:2], chan_start, channels, 3)
    joined = jnp.concatenate([chan_rows[1][:, length - lag_order :], chan_rows[0]], axis=1)
    joined_ids = jnp.concatenate([id_ext[1][:, length - lag_order :], ids], axis=1)
    masks = []
    lagged = []
    for step in range(1, lag_order + 1):
        low = lag_order - step
        masks.append((joined_ids[:, low : low + length] == ids)[:, :, None])
        lagged.append(jnp.where(masks[-1], joined[:, low : low + length], jnp.zeros((), BF)))
    lag_stack = jnp.stack(lagged)

    mixed = jnp.einsum("kmtd,kde->mte", conv, filter_proj, preferred_element_type=F32)
    mixed = mixed + jnp.einsum("imtc,ice->mte", lag_stack, lag_proj, preferred_element_type=F32)

    state = jax.ShapeDtypeStruct((streams, quarter, width), F32)
    gain_state = jax.ShapeDtypeStruct((1, width), F32)

    def finish_one(m, total, others, extra):
        x_ref, gain_ref = others
        hidden = x_ref[m, place()[1]].astype(F32) + total
        extra[0][m] = hidden
        return norm_of(hidden, gain_ref[...]).astype(BF)

    attn_ext, hidden_one = exchange(
        "exchange_one", 2, seq_count, [split(mixed.astype(BF))[None]], [quarters(x), row(attention_gain)], 0, hops,
        finish_one, [state],
    )
    attn_ext = whole(attn_ext)

    q, k, v, attended, lse, out_part = attend(
        attn_ext, id_rows[: hops + 1], id_cols[0], query_weight, key_weight, value_weight, output_weight
    )

    def finish_two(m, total, others, extra):
        hidden_ref, gain_ref = others
        hidden = hidden_ref[m] + total
        extra[0][m] = hidden
        return norm_of(hidden, gain_ref[...]).astype(BF)

    feed_in, hidden_two = exchange(
        "exchange_two", 3, seq_count, [split(out_part)[None]], [hidden_one, row(feed_gain)], 0, 0, finish_two, [state]
    )
    feed_in = whole(feed_in)[0].reshape(streams * length, width)
    flat_three = grad_three.reshape(streams * length, width)

    gate_pre = dot_nn(feed_in, gate_weight)
    up_pre = dot_nn(feed_in, up_weight)
    grad_inner = dot_nt(flat_three, down_weight)
    unit, pull = jax.vjp(gated_unit, gate_pre, up_pre)
    inner = unit.astype(BF)
    grad_gate, grad_up = pull(grad_inner)
    grad_gate = grad_gate.astype(BF)
    grad_up = grad_up.astype(BF)
    layer_part = dot_nn(inner, down_weight).astype(BF)
    feed_part = (dot_nt(grad_gate, gate_weight) + dot_nt(grad_up, up_weight)).astype(BF)

    def finish_three(m, total, others, extra):
        hidden_ref, gain_ref, cot_ref = others
        if m >= streams:
            return (hidden_ref[m - streams] + total).astype(BF)
        grad_in, gain_grad = norm_back(hidden_ref[m], gain_ref[...], total)
        grad_two = cot_ref[m, place()[1]].astype(F32) + grad_in
        extra[0][m] = grad_two
        extra[1][...] = gain_grad if m == 0 else extra[1][...] + gain_grad
        return grad_two.astype(BF)

    feed_grads = jnp.stack(
        [
            dot_tn(feed_in, grad_gate).astype(BF),
            dot_tn(feed_in, grad_up).astype(BF),
            dot_tn(flat_three, inner).astype(BF),
        ]
    )
    shape = (1, streams, length, width)
    both, grad_two, feed_gain_grad = exchange(
        "exchange_three", 4, seq_count, [split(feed_part.reshape(shape)), split(layer_part.reshape(shape))],
        [hidden_two, row(feed_gain), quarters(grad_three)], 0, 0, finish_three, [state, gain_state],
    )
    both = whole(both)[0]
    grad_att_out = both[:streams]
    layer_output = both[streams:]

    dq, dk, dv, attn_part = attend_back(
        q, k, v, lse, grad_att_out, id_rows[: hops + 1], id_cols[0], query_weight, key_weight, value_weight, output_weight
    )

    go = grad_att_out.reshape(tokens_flat, width)
    attn_grads = jnp.concatenate(
        [
            dot_tn(attn_ext[0].reshape(tokens_flat, width), dq.reshape(tokens_flat, -1)).astype(BF),
            dot_tn(attn_ext.reshape(-1, width), dk.reshape(-1, dk.shape[-1])).astype(BF),
            dot_tn(attn_ext.reshape(-1, width), dv.reshape(-1, dv.shape[-1])).astype(BF),
            dot_tn(go, attended.reshape(tokens_flat, -1)).astype(BF),
        ],
        axis=1,
    )

    def finish_four(m, total, others, extra):
        hidden_ref, gain_ref, grad_ref = others
        grad_in, gain_grad = norm_back(hidden_ref[m], gain_ref[...], total)
        grad_one = grad_ref[m] + grad_in
        extra[0][m] = grad_one
        extra[1][...] = gain_grad if m == 0 else extra[1][...] + gain_grad
        return grad_one.astype(BF)

    grad_stu, grad_one, attn_gain_grad = exchange(
        "exchange_four", 5, seq_count, [split(attn_part)], [hidden_one, row(attention_gain), grad_two], hops, 0,
        finish_four, [state, gain_state],
    )
    grad_stu = whole(grad_stu)[0]
    grad_conv = jnp.einsum("mte,kde->kmtd", grad_stu, filter_proj, preferred_element_type=F32).astype(BF)
    grad_lagged = jnp.einsum("mte,ice->imtc", grad_stu, lag_proj, preferred_element_type=F32)
    ext_grad = jnp.zeros((streams, 8 + length, channels), F32)
    for step in range(1, lag_order + 1):
        term = jnp.where(masks[step - 1], grad_lagged[step - 1], 0.0)
        ext_grad = ext_grad + jnp.pad(term, ((0, 0), (8 - step, step), (0, 0)))
    terms = convolve_back(
        grad_conv, id_rows[0], id_cols, base_back, ext_grad[:, 8:], ext_grad[:, :8], seq_count
    )

    def finish_five(m, total, others, extra):
        x_ref, gain_ref, grad_ref = others
        grad_in, gain_grad = norm_back(x_ref[m, place()[1]].astype(F32), gain_ref[...], total)
        extra[0][...] = gain_grad if m == 0 else extra[0][...] + gain_grad
        return (grad_ref[m] + grad_in).astype(BF)

    input_gradient, stu_gain_grad = exchange(
        "exchange_five", 6, seq_count, [split(terms)], [quarters(x), row(stu_gain), grad_one], seq_count - 1, 0,
        finish_five, [gain_state],
    )
    input_gradient = whole(input_gradient)[0]
    stu = grad_stu.reshape(tokens_flat, width)
    filter_part = jnp.einsum("kmtd,mte->kde", conv, grad_stu, preferred_element_type=F32).astype(BF)
    lag_part = jnp.concatenate(
        [dot_tn(stu, lag_stack[i].reshape(tokens_flat, channels)).astype(BF) for i in range(lag_order)], axis=1
    )
    feed_grads = lax.psum(
        lax.psum_scatter(feed_grads, "seq", scatter_dimension=1, tiled=True), "dp"
    ).astype(F32)
    attn_grads = lax.psum(lax.psum_scatter(attn_grads, "seq", scatter_dimension=0, tiled=True), "dp").astype(F32)
    filter_grad = lax.psum(
        lax.psum_scatter(filter_part, "seq", scatter_dimension=1, tiled=True), "dp"
    ).astype(F32)
    lag_grad = lax.psum(lax.psum_scatter(lag_part, "seq", scatter_dimension=0, tiled=True), "dp").astype(F32)
    gains = jnp.concatenate([stu_gain_grad, attn_gain_grad, feed_gain_grad], axis=0)
    gains = lax.psum(gains, ("dp", "seq", "tensor"))
    gain_width = width // seq_count
    gains = lax.dynamic_slice_in_dim(gains, lax.axis_index("seq") * gain_width, gain_width, 1)
    return answer(layer_output, input_gradient, gains, filter_grad, lag_grad, attn_grads, feed_grads)


def solution(mesh):
    return jax.shard_map(
        functools.partial(local, mesh.shape["seq"]),
        mesh=mesh,
        in_specs=(
            P(None, "dp", "seq", None),
            P(None, "dp", "seq"),
            P("tensor", None),
            P(),
            P("tensor", None, None),
            P(None, "tensor", None),
            P(),
            P(None, "tensor"),
            P(None, "tensor"),
            P(None, "tensor"),
            P("tensor", None),
            P(),
            P(None, "tensor"),
            P(None, "tensor"),
            P("tensor", None),
            P(None, "dp", "seq", None),
        ),
        out_specs=(
            P(None, "dp", "seq", None),
            P(None, "dp", "seq", None),
            P("seq"),
            P("tensor", "seq", None),
            P(None, "tensor", "seq"),
            P("seq"),
            P("seq", "tensor"),
            P("seq", "tensor"),
            P("seq", "tensor"),
            P("tensor", "seq"),
            P("seq"),
            P("seq", "tensor"),
            P("seq", "tensor"),
            P("tensor", "seq"),
        ),
        check_vma=False,
    )
```
